128 devices in a mesh: data: 1, cols: 16 (over z, y), model: 8 (over x, core).
Axes of the slice: x: 4, y: 4, z: 4, core: 2. Of those that a mesh axis runs over, the one named last changes fastest.
Arguments:
- x_in: bfloat16 [4, 128, 128, 512], P('data', None, None, ('model', 'cols'))
- w_conv1: bfloat16 [3, 3, 512, 512], P(None, None, ('model', 'cols'))
- b_conv1: float32 [512], replicated
- w_conv2: bfloat16 [3, 3, 512, 512], replicated
- b_conv2: float32 [512], replicated
Outputs:
- output: float32 [4, 128, 128, 512], P('data', 'model', 'cols')
All inputs are finite; a program needn't handle non-finite values.
Results may differ from the reference program's by a relative error of at most 0.001.
Values are sent between devices in bfloat16 or wider.
A program may use at most 1 GiB of HBM per device.

```python
import jax
import jax.numpy as jnp
from jax import lax

IMAGES = 4
HEIGHT = 128
WIDTH = 128
IN_CHANS = 512
MID_CHANS = 512
OUT_CHANS = 512

CONV_DIMS = ("NHWC", "HWIO", "NHWC")


def setup_inputs(seed: int = 0, part: int = 0) -> dict:
    base_key = jax.random.key(seed)
    part_key = jax.random.fold_in(base_key, part)
    key_w1, key_b1, key_w2, key_b2 = jax.random.split(jax.random.fold_in(base_key, 1000), 4)
    x_in = jax.random.normal(part_key, (IMAGES, HEIGHT, WIDTH, IN_CHANS), jnp.float32)
    w_conv1 = jax.random.normal(key_w1, (3, 3, IN_CHANS, MID_CHANS), jnp.float32) * (9 * IN_CHANS) ** -0.5
    b_conv1 = 0.5 * jax.random.normal(key_b1, (MID_CHANS,), jnp.float32)
    w_conv2 = jax.random.normal(key_w2, (3, 3, MID_CHANS, OUT_CHANS), jnp.float32) * (4.5 * MID_CHANS) ** -0.5
    b_conv2 = 0.5 * jax.random.normal(key_b2, (OUT_CHANS,), jnp.float32)
    return {"x_in": x_in.astype(jnp.bfloat16), "w_conv1": w_conv1.astype(jnp.bfloat16), "b_conv1": b_conv1, "w_conv2": w_conv2.astype(jnp.bfloat16), "b_conv2": b_conv2}


def reference(x_in, w_conv1, b_conv1, w_conv2, b_conv2):
    kernel_one = w_conv1.astype(jnp.float32)
    kernel_two = w_conv2.astype(jnp.float32)

    def one_image(image):
        z_sum = lax.conv_general_dilated(image[None].astype(jnp.float32), kernel_one, (1, 1), "SAME", dimension_numbers=CONV_DIMS)
        act_map = jnp.maximum(z_sum + b_conv1, 0.0).astype(jnp.bfloat16)
        out_map = lax.conv_general_dilated(act_map.astype(jnp.float32), kernel_two, (1, 1), "SAME", dimension_numbers=CONV_DIMS)
        return out_map[0] + b_conv2

    return lax.map(one_image, x_in)
```

```python
import jax
import jax.numpy as jnp
from jax import lax
from jax.experimental import pallas as pl
from jax.experimental.pallas import tpu as pltpu
from jax.sharding import PartitionSpec as P

GROUP_AXES = ("model", "cols")
MESH = pl.DeviceIdType.MESH
BF16 = jnp.bfloat16
F32 = jnp.float32
CHANS = 512
LANES = 128
CUT = 96
CHUNKS = ((0,), (1,), (2,))
VMEM_LIMIT = 36 * 2**20
ORDERS = (("y", "z", "x"), ("z", "x", "y"), ("x", "y", "z"))


def one_hot(shape, col_of_row):
    rows = lax.broadcasted_iota(jnp.int32, shape, 0)
    cols = lax.broadcasted_iota(jnp.int32, shape, 1)
    return jnp.where(cols == col_of_row(rows), 1.0, 0.0).astype(BF16)


def column_of(r):
    w = (r % 272) // 4 * 2 - 1 + r // 272
    return jnp.where((w >= 0) & (w < LANES), (r % 4) * LANES + w, -1)


def pack_windows(xv, a_scr, pack):
    to_lanes = one_hot((CHANS, CHANS), lambda r: (r % 4) * LANES + ((r % LANES) // 4) * 4 + r // LANES)
    to_rows = one_hot((544, CHANS), column_of)
    for blk in range(4):
        part = jnp.concatenate([xv[n, 32 * blk : 32 * blk + 32].reshape(LANES, LANES) for n in range(4)], axis=0)
        turned = lax.dot_general(part, to_lanes, (((0,), (0,)), ((), ())), preferred_element_type=F32).astype(BF16)
        for c in range(4):
            a_scr[c * LANES : (c + 1) * LANES, blk * LANES : (blk + 1) * LANES] = turned[:, c * LANES : (c + 1) * LANES]
    mixed = jnp.dot(to_rows, a_scr[...], preferred_element_type=F32)
    for blk in range(4):
        two = [mixed[272 * p : 272 * p + 272, blk * LANES : (blk + 1) * LANES] for p in range(2)]
        for half in range(2):
            tile = jnp.concatenate([t[:, 64 * half : 64 * half + 64] for t in two], axis=1).astype(BF16)
            pack[2 * blk + half] = tile.reshape(68, 4, LANES)


def kernel(
    x_hbm, w1_hbm, w2_hbm, b1_hbm, b2_hbm, o_ref,
    xv, w1v, w2v, b1v, b2v, a_scr, pack, got, x0, x1, x2, edge, side, w1g, z_acc, y0, y1, y2,
    load_sem, xs_send, xs_recv, halo_send, halo_recv, step_send, step_recv,
):
    m = lax.axis_index("model")
    q = lax.axis_index("cols")
    me = {"x": m // 2, "z": q // 4, "y": q % 4}
    core = m % 2
    parts = range(3)
    barrier = pltpu.get_barrier_semaphore()

    at_model = [[(me["x"] + dx) % 4 * 2 + (core + dk) % 2 for dk in range(2)] for dx in range(4)]
    at_cols = [[(me["z"] + dz) % 4 * 4 + (me["y"] + dy) % 4 for dy in range(4)] for dz in range(4)]
    others = [(dx, dz, dy, dk) for dx in range(4) for dz in range(4) for dy in range(4) for dk in range(2)]
    others = sorted(others[1:], key=lambda d: (sum(d[:3]) % 4, d))

    def away(d):
        return {"model": at_model[d[0]][d[3]], "cols": at_cols[d[1]][d[2]]}

    loads = [
        pltpu.make_async_copy(src, dst, load_sem.at[k])
        for k, (src, dst) in enumerate(
            ((x_hbm, xv), (w1_hbm, w1v), (w2_hbm, w2v.at[pl.ds(0, 4608)]), (b1_hbm, b1v), (b2_hbm, b2v))
        )
    ]
    for load in loads:
        load.start()
    with jax.named_scope("announce"):
        for d in sorted(others, key=lambda d: -sum(min(o, 4 - o) for o in d[:3])):
            pl.semaphore_signal(barrier, inc=1, device_id=away(d), device_id_type=MESH)

    def piece(p, t, v, dws, c, half=None):
        done = ORDERS[p][:t]
        rest = [a for a in "xzy" if a != ORDERS[p][2]]
        at = [v if t < 2 and a == ORDERS[p][t] else (pl.ds(0, 4) if a in done else me[a]) for a in rest]
        if half is not None:
            at[0] = pl.ds(2 * half, 2)
        return w1g.at[p, me[ORDERS[p][2]] if t < 2 else v, c, at[0], at[1], pl.ds(dws[0], len(dws))]

    with jax.named_scope("place_w1"):
        loads[1].wait()
        for p in parts:
            spot = [me[a] for a in "xzy" if a != ORDERS[p][2]]
            for dw in range(3):
                for lt in range(4):
                    tile = w1v[3 * p + dw, :, lt * LANES : (lt + 1) * LANES]
                    w1g[p, me[ORDERS[p][2]], core, spot[0], spot[1], dw, lt] = tile
    with jax.named_scope("wait_x"):
        loads[0].wait()
    with jax.named_scope("pack"):
        pack_windows(xv, a_scr, pack)
    with jax.named_scope("wait_barrier"):
        pl.semaphore_wait(barrier, 127)

    n_steps = [0]
    steps = []

    class Step:
        def __init__(self, size, copies):
            k = n_steps[0]
            n_steps[0] += 1
            sems = dict(send_sem=step_send.at[k], recv_sem=step_recv.at[k], device_id_type=MESH)
            for ref, to in copies:
                pltpu.make_async_remote_copy(src_ref=ref, dst_ref=ref, device_id=to, **sems).start()
            span = got.at[pl.ds(0, size)]
            self.all = pltpu.make_async_remote_copy(
                src_ref=span, dst_ref=span, device_id={"model": at_model[0][1], "cols": q}, **sems
            )
            steps.append(self)

        def land(self):
            self.all.wait_recv()

    def chip(p, t, d, c=0):
        axis = ORDERS[p][t]
        pos = me | {axis: (me[axis] + d) % 4}
        return {"model": pos["x"] * 2 + (core + c) % 2, "cols": pos["z"] * 4 + pos["y"]}

    def spread(t, size):
        return Step(size, [(piece(p, t, me[ORDERS[p][t]], parts, core), chip(p, t, d)) for p in parts for d in (1, 3, 2)])

    def plane(p, d):
        return (me[ORDERS[p][2]] + d) % 4

    def hand_over(pieces, size):
        return Step(size, [(ref, {"model": at_model[0][1], "cols": q}) for ref in pieces])

    def send_windows(first, last):
        for d in others[first:last]:
            to = away(d)
            pltpu.make_async_remote_copy(
                src_ref=pack.at[to["model"], pl.ds(4 * to["cols"], 5)],
                dst_ref=got.at[pl.ds(5 * mine, 5)],
                send_sem=xs_send,
                recv_sem=xs_recv,
                device_id=to,
                device_id_type=MESH,
            ).start()

    mine = ((core * 4 + me["x"]) * 4 + me["z"]) * 4 + me["y"]
    with jax.named_scope("send_first"):
        first = spread(0, 108)
        for pair in range(5):
            got[5 * mine + pair] = pack[m, 4 * q + pair]
        send_windows(0, CUT)
    with jax.named_scope("wait_first"):
        first.land()
    with jax.named_scope("send_second"):
        second = spread(1, 432)
        send_windows(CUT, 127)
    with jax.named_scope("wait_second"):
        second.land()
    last, passed, lent, lent_on = {}, {}, {}, {}

    def send_plane(dws):
        size = 384 * len(dws)
        last[dws] = Step(size, [(piece(p, 2, plane(p, 0), dws, core), chip(p, 2, d)) for p in parts for d in (1, 3)])

    def pass_on(dws):
        size = 384 * len(dws)
        with jax.named_scope(f"wait_last{dws[0]}"):
            last[dws].land()
        on = [(piece(p, 2, plane(p, 4 - d), dws, core, d // 2), chip(p, 2, d)) for p in parts for d in (1, 3)]
        passed[dws] = Step(size // 2, on)
        lent[dws] = hand_over([piece(p, 2, plane(p, d), dws, core) for p in parts for d in (1, 3)], size)

    def finish(dws):
        with jax.named_scope(f"wait_passed{dws[0]}"):
            passed[dws].land()
        lent_on[dws] = hand_over([piece(p, 2, plane(p, 2), dws, core) for p in parts], 192 * len(dws))

    with jax.named_scope("send_third"):
        for dws in CHUNKS:
            send_plane(dws)
        own = hand_over([piece(p, 2, plane(p, 0), parts, core) for p in parts], 576)

    span = got.at[pl.ds(0, 635)]
    everything = pltpu.make_async_remote_copy(
        src_ref=span, dst_ref=span, send_sem=xs_send, recv_sem=xs_recv, device_id=chip(0, 0, 0, 1), device_id_type=MESH
    )
    with jax.named_scope("wait_windows"):
        everything.wait_recv()
    xs, ys = (x0, x1, x2), (y0, y1, y2)
    with jax.named_scope("turn"):
        for pair in range(5):
            for p in parts:
                rows = []
                for v in range(4):
                    for at in (pair, 320 + pair):
                        if p == 0:
                            rows.append(got[at + 80 * v : at + 80 * v + 80 : 5])
                        elif p == 1:
                            rows.append(got[at + 5 * v : at + 316 : 20])
                        else:
                            rows += [got[at + 80 * a + 20 * v : at + 80 * a + 20 * v + 20 : 5] for a in range(4)]
                rows = jnp.concatenate([r.reshape(-1, LANES) for r in rows], axis=0).T
                for odd in range(2):
                    main = rows[64 * odd : 64 * odd + 64]
                    xs[p][2 * pair + odd, 8 - 4 * p : 72 - 4 * p] = main
                    if p == 1:
                        edge[0, 2 * pair + odd] = main[60:64]
                        edge[1, 2 * pair + odd] = main[0:4]
    halo = []
    for src, dst, d in (
        (x0.at[:, pl.ds(64, 8)], x0.at[:, pl.ds(0, 8)], 1),
        (x2.at[:, pl.ds(0, 8)], x2.at[:, pl.ds(64, 8)], 7),
        (edge.at[0], edge.at[2], 1),
        (edge.at[1], edge.at[3], 7),
    ):
        halo.append(
            pltpu.make_async_remote_copy(
                src_ref=src,
                dst_ref=dst,
                send_sem=halo_send.at[len(halo)],
                recv_sem=halo_recv.at[len(halo)],
                device_id={"model": (m + d) % 8, "cols": q},
                device_id_type=MESH,
            )
        )
        halo[-1].start()

    def conv1(dws, places, spans):
        total = None
        for p in parts:
            at = [plane(p, d) for d in places]
            lanes = [pl.ds(pl.multiple_of(LANES * v, LANES), LANES) for v in at]
            for dw in dws:
                right = [[w1g[p, v, :, :, :, dw, lt].reshape(LANES, LANES) for lt in range(4)] for v in at]
                right = jnp.concatenate([jnp.concatenate(r, axis=1) for r in right], axis=0)
                left = [jnp.concatenate([xs[p][dw : dw + 8, rows, s] for s in lanes], axis=-1) for rows in spans]
                left = jnp.concatenate(left, axis=1).reshape(-1, 256)
                term = jnp.dot(left, right, preferred_element_type=F32)
                total = term if total is None else total + term
        return total.reshape(8, -1, CHANS)

    every, top_rows, inner, low_rows = pl.ds(0, 72), pl.ds(0, 8), pl.ds(8, 56), pl.ds(64, 8)

    def near(dws):
        with jax.named_scope(f"wait_lent{dws[0]}"):
            lent[dws].land()
        with jax.named_scope(f"near{dws[0]}"):
            top = conv1(dws, (3, 1), (inner,))
            z_acc[:, inner] = top if dws == CHUNKS[0] else z_acc[:, inner] + top

    def rim():
        with jax.named_scope("rim"):
            top = conv1(parts, (3, 1), (top_rows, low_rows))
            z_acc[:, top_rows] = top[:, :8]
            z_acc[:, low_rows] = top[:, 8:]

    def far(dws):
        with jax.named_scope(f"wait_lent_on{dws[0]}"):
            lent_on[dws].land()
        with jax.named_scope(f"far{dws[0]}"):
            total = z_acc[...] + conv1(dws, (0, 2), (every,))
            if dws != CHUNKS[-1]:
                z_acc[...] = total
                return
            act = jnp.maximum(total + b1v[...], 0.0).astype(BF16)
            side[0], side[1] = act[0], act[7]
            for dh in range(3):
                ys[dh][1:9] = act[:, 4 * dh : 4 * dh + 64]
            clear(m == 0, (y0,), pl.ds(1, 8), pl.ds(0, 4))
            clear(m == 7, (y2,), pl.ds(1, 8), pl.ds(60, 4))

    def clear(at_edge, refs, cols, rows):
        @pl.when(at_edge)
        def _():
            for ref in refs:
                ref[cols, rows] = jnp.zeros((cols.size, rows.size, CHANS), BF16)

    def trade_sides():
        for k, d in enumerate((15, 1)):
            halo.append(
                pltpu.make_async_remote_copy(
                    src_ref=side.at[k],
                    dst_ref=side.at[2 + k],
                    send_sem=halo_send.at[4 + k],
                    recv_sem=halo_recv.at[4 + k],
                    device_id={"model": m, "cols": (q + d) % 16},
                    device_id_type=MESH,
                )
            )
            halo[-1].start()

    def take_sides():
        with jax.named_scope("wait_sides"):
            for copy in halo[4:]:
                copy.wait_recv()
        for k, col in enumerate((9, 0)):
            for dh in range(3):
                ys[dh][col] = side[2 + k, 4 * dh : 4 * dh + 64]
            outer = pl.ds(col, 1)
            clear(m == 0, (y0,), outer, pl.ds(0, 4))
            clear(m == 7, (y2,), outer, pl.ds(60, 4))
            clear(q == (15, 0)[k], ys, outer, pl.ds(0, 64))

    def conv2(spans):
        total = None
        for dh in range(3):
            for dw in range(3):
                tap = 3 * dh + dw
                left = [ys[dh][dw + first : dw + last].reshape(-1, CHANS) for first, last in spans]
                left = jnp.concatenate(left, axis=0)
                term = jnp.dot(left, w2v[CHANS * tap : CHANS * tap + CHANS, :], preferred_element_type=F32)
                total = term if total is None else total + term
        return total + b2v[...]

    pass_on(CHUNKS[0])
    pass_on(CHUNKS[1])
    pass_on(CHUNKS[2])
    near(CHUNKS[0])
    near(CHUNKS[1])
    near(CHUNKS[2])
    finish(CHUNKS[0])
    with jax.named_scope("wait_halo"):
        for copy in halo[:4]:
            copy.wait_recv()

    @pl.when(m == 0)
    def _():
        x0[:, 0:8] = jnp.zeros((10, 8, CHANS), BF16)
        x1[:, 0:4] = jnp.zeros((10, 4, CHANS), BF16)

    @pl.when(m > 0)
    def _():
        x1[:, 0:4] = edge[2]

    @pl.when(m == 7)
    def _():
        x2[:, 64:72] = jnp.zeros((10, 8, CHANS), BF16)
        x1[:, 68:72] = jnp.zeros((10, 4, CHANS), BF16)

    @pl.when(m < 7)
    def _():
        x1[:, 68:72] = edge[3]

    rim()
    finish(CHUNKS[1])
    finish(CHUNKS[2])
    with jax.named_scope("wait_own_w2"):
        own.land()
        for load in loads[2:]:
            load.wait()
    far(CHUNKS[0])
    far(CHUNKS[1])
    far(CHUNKS[2])
    trade_sides()
    with jax.named_scope("conv2_in"):
        o_ref[64:448] = conv2(((1, 7),))
    take_sides()
    with jax.named_scope("conv2_out"):
        outer = conv2(((0, 1), (7, 8)))
        o_ref[0:64], o_ref[448:CHANS] = outer[:64], outer[64:]

    with jax.named_scope("wait_sends"):
        everything.wait_send()
        for step in steps:
            step.all.wait_send()
        for copy in halo:
            copy.wait_send()


def arrange(sum_ref, o_hbm, turned, sems):
    copies = []
    for g in range(4):
        rows = jnp.transpose(sum_ref[:, 16 * g : 16 * g + 16], (1, 0, 2))
        for h in range(4):
            for image in range(4):
                turned[g, image, h] = rows[4 * h + image]
        copies.append(pltpu.make_async_copy(turned.at[g], o_hbm.at[:, pl.ds(4 * g, 4)], sems.at[g]))
        copies[-1].start()
    for copy in copies:
        copy.wait()


def solution(mesh):
    scratch = [
        pltpu.VMEM((4, LANES, 4, LANES), BF16),
        pltpu.VMEM((9, 4, CHANS), BF16),
        pltpu.VMEM((4616, CHANS), BF16),
        pltpu.VMEM((1, CHANS), F32),
        pltpu.VMEM((1, CHANS), F32),
        pltpu.VMEM((CHANS, CHANS), BF16),
        pltpu.VMEM((8, 68, 4, LANES), BF16),
        pltpu.VMEM((640, 4, LANES), BF16),
        *[pltpu.VMEM((10, 72, CHANS), BF16) for _ in range(3)],
        pltpu.VMEM((4, 10, 4, CHANS), BF16),
        pltpu.VMEM((4, 72, CHANS), BF16),
        pltpu.VMEM((3, 4, 2, 4, 4, 3, 4, 4, LANES), BF16),
        pltpu.VMEM((8, 72, CHANS), F32),
        *[pltpu.VMEM((10, 64, CHANS), BF16) for _ in range(3)],
        pltpu.SemaphoreType.DMA((5,)),
        pltpu.SemaphoreType.DMA,
        pltpu.SemaphoreType.DMA,
        pltpu.SemaphoreType.DMA((6,)),
        pltpu.SemaphoreType.DMA((6,)),
        pltpu.SemaphoreType.DMA((15,)),
        pltpu.SemaphoreType.DMA((15,)),
    ]
    vmem = pl.BlockSpec(memory_space=pltpu.VMEM)
    anywhere = pl.BlockSpec(memory_space=pl.ANY)

    def run_local(x_in, w_conv1, b_conv1, w_conv2, b_conv2):
        sums = pl.pallas_call(
            kernel,
            out_shape=jax.ShapeDtypeStruct((CHANS, CHANS), F32),
            in_specs=[anywhere] * 5,
            out_specs=vmem,
            scratch_shapes=scratch,
            compiler_params=pltpu.CompilerParams(collective_id=0, has_side_effects=True, vmem_limit_bytes=VMEM_LIMIT),
            name="two_convs",
        )(
            *(
                pltpu.with_memory_space_constraint(a, pltpu.HBM)
                for a in (
                    x_in.transpose(0, 1, 3, 2),
                    w_conv1.reshape(9, 4, CHANS),
                    w_conv2.reshape(4608, CHANS),
                    b_conv1.reshape(1, CHANS),
                    b_conv2.reshape(1, CHANS),
                )
            )
        )
        return pl.pallas_call(
            arrange,
            out_shape=jax.ShapeDtypeStruct((4, 16, 8, CHANS), F32),
            in_specs=[vmem],
            out_specs=anywhere,
            scratch_shapes=[pltpu.VMEM((4, 4, 4, 8, CHANS), F32), pltpu.SemaphoreType.DMA((4,))],
            compiler_params=pltpu.CompilerParams(vmem_limit_bytes=8 * 2**20),
            name="arrange",
        )(sums.reshape(8, 64, CHANS))

    return jax.shard_map(
        run_local,
        mesh=mesh,
        in_specs=(P("data", None, None, GROUP_AXES), P(None, None, GROUP_AXES, None), P(), P(), P()),
        out_specs=P("data", "model", "cols", None),
        check_vma=False,
    )
```

```python
import jax
import jax.numpy as jnp
from jax import lax
from jax.experimental import pallas as pl
from jax.experimental.pallas import tpu as pltpu
from jax.sharding import PartitionSpec as P

GROUP_AXES = ("model", "cols")
MESH = pl.DeviceIdType.MESH
BF16 = jnp.bfloat16
F32 = jnp.float32
CHANS = 512
LANES = 128
CUTS = (96, 127)
VMEM_LIMIT = 36 * 2**20
ORDERS = (("y", "z", "x"), ("z", "x", "y"), ("x", "y", "z"))


def one_hot(shape, col_of_row):
    rows = lax.broadcasted_iota(jnp.int32, shape, 0)
    cols = lax.broadcasted_iota(jnp.int32, shape, 1)
    return jnp.where(cols == col_of_row(rows), 1.0, 0.0).astype(BF16)


def pack_windows(xv, a_scr, pack):
    to_lanes = one_hot((CHANS, CHANS), lambda r: (r % 4) * LANES + ((r % LANES) // 4) * 4 + r // LANES)
    to_rows = one_hot((CHANS, CHANS), lambda r: (r % 4) * LANES + ((r % 256) // 4) * 2 + r // 256)
    for blk in range(4):
        part = jnp.concatenate([xv[n, 32 * blk : 32 * blk + 32].reshape(LANES, LANES) for n in range(4)], axis=0)
        turned = lax.dot_general(part, to_lanes, (((0,), (0,)), ((), ())), preferred_element_type=F32).astype(BF16)
        for c in range(4):
            a_scr[c * LANES : (c + 1) * LANES, blk * LANES : (blk + 1) * LANES] = turned[:, c * LANES : (c + 1) * LANES]
    mixed = jnp.dot(to_rows, a_scr[...], preferred_element_type=F32)
    for blk in range(4):
        even = mixed[0:256, blk * LANES : (blk + 1) * LANES]
        odd = mixed[256:CHANS, blk * LANES : (blk + 1) * LANES]
        for half in range(2):
            s = slice(64 * half, 64 * half + 64)
            tile = jnp.concatenate([even[:, s], odd[:, s]], axis=1).astype(BF16)
            pack[2 * blk + half, 1:65] = tile.reshape(64, 4, LANES)
    edge = jnp.zeros((8, 1, 4, LANES), BF16)
    pack[:, 0:1] = edge
    pack[:, 65:66] = edge


def kernel(
    x_hbm, w1_hbm, w2_hbm, b1_hbm, b2_hbm, o_ref,
    xv, w1v, w2v, b1v, b2v, a_scr, pack, got, x0, x1, x2, edge, w1g, z_acc, y0, y1, y2, acc2,
    load_sem, xs_send, xs_recv, halo_send, halo_recv, step_send, step_recv,
):
    m = lax.axis_index("model")
    q = lax.axis_index("cols")
    me = {"x": m // 2, "z": q // 4, "y": q % 4}
    core = m % 2
    parts = range(3)
    barrier = pltpu.get_barrier_semaphore()

    at_model = [[(me["x"] + dx) % 4 * 2 + (core + dk) % 2 for dk in range(2)] for dx in range(4)]
    at_cols = [[(me["z"] + dz) % 4 * 4 + (me["y"] + dy) % 4 for dy in range(4)] for dz in range(4)]
    others = [(dx, dz, dy, dk) for dx in range(4) for dz in range(4) for dy in range(4) for dk in range(2)]
    others = sorted(others[1:], key=lambda d: (sum(d[:3]) % 4, d))

    def away(d):
        return {"model": at_model[d[0]][d[3]], "cols": at_cols[d[1]][d[2]]}

    loads = [
        pltpu.make_async_copy(src, dst, load_sem.at[k])
        for k, (src, dst) in enumerate(
            ((x_hbm, xv), (w1_hbm, w1v), (w2_hbm, w2v.at[pl.ds(0, 4608)]), (b1_hbm, b1v), (b2_hbm, b2v))
        )
    ]
    for load in loads:
        load.start()
    with jax.named_scope("announce"):
        for d in sorted(others, key=lambda d: -sum(min(o, 4 - o) for o in d[:3])):
            pl.semaphore_signal(barrier, inc=1, device_id=away(d), device_id_type=MESH)

    def piece(p, t, v, n, c, place=None, half=None):
        done = ORDERS[p][:t]
        rest = [a for a in "xzy" if a != ORDERS[p][2]]
        at = [v if t < 2 and a == ORDERS[p][t] else (pl.ds(0, 4) if a in done else me[a]) for a in rest]
        if half is not None:
            at[0] = pl.ds(2 * half, 2)
        return w1g.at[p, pl.ds(0, 2) if n is None else n, me[ORDERS[p][2]] if t < 2 else v, c, at[0], at[1]]

    with jax.named_scope("place_w1"):
        loads[1].wait()
        for p in parts:
            spot = [me[a] for a in "xzy" if a != ORDERS[p][2]]
            for dw in range(3):
                for lt in range(4):
                    tile = w1v[3 * p + dw, :, lt * LANES : (lt + 1) * LANES]
                    w1g[p, lt // 2, me[ORDERS[p][2]], core, spot[0], spot[1], dw, lt % 2] = tile
    with jax.named_scope("wait_x"):
        loads[0].wait()
    with jax.named_scope("pack"):
        pack_windows(xv, a_scr, pack)
    with jax.named_scope("wait_barrier"):
        pl.semaphore_wait(barrier, 127)

    n_steps = [0]
    steps = []

    class Step:
        def __init__(self, slabs, copies):
            k = n_steps[0]
            n_steps[0] += 1
            sems = dict(send_sem=step_send.at[k], recv_sem=step_recv.at[k], device_id_type=MESH)
            for ref, to in copies:
                pltpu.make_async_remote_copy(src_ref=ref, dst_ref=ref, device_id=to, **sems).start()
            span = got.at[pl.ds(0, slabs)]
            self.all = pltpu.make_async_remote_copy(
                src_ref=span, dst_ref=span, device_id={"model": at_model[0][1], "cols": q}, **sems
            )
            steps.append(self)

        def land(self):
            self.all.wait_recv()

    def chip(p, t, d, c=0):
        axis = ORDERS[p][t]
        pos = me | {axis: (me[axis] + d) % 4}
        return {"model": pos["x"] * 2 + (core + c) % 2, "cols": pos["z"] * 4 + pos["y"]}

    def spread(t, slabs):
        return Step(slabs, [(piece(p, t, me[ORDERS[p][t]], None, core), chip(p, t, d)) for p in parts for d in (1, 3, 2)])

    def plane(p, d):
        return (me[ORDERS[p][2]] + d) % 4

    def hand_over(pieces, slabs):
        return Step(slabs, [(ref, {"model": at_model[0][1], "cols": q}) for ref in pieces])

    def send_windows(first, last):
        for d in others[first:last]:
            to = away(d)
            pltpu.make_async_remote_copy(
                src_ref=pack.at[to["model"], pl.ds(4 * to["cols"], 6)],
                dst_ref=got.at[mine],
                send_sem=xs_send,
                recv_sem=xs_recv,
                device_id=to,
                device_id_type=MESH,
            ).start()

    mine = ((core * 4 + me["x"]) * 4 + me["z"]) * 4 + me["y"]
    with jax.named_scope("send_first"):
        first = spread(0, 18)
        for pair in range(6):
            got[mine, pair] = pack[m, 4 * q + pair]
        send_windows(0, CUTS[0])
    with jax.named_scope("wait_first"):
        first.land()
    with jax.named_scope("send_second"):
        second = spread(1, 72)
        send_windows(CUTS[0], CUTS[1])
    with jax.named_scope("wait_second"):
        second.land()
    last, passed, lent, lent_on = {}, {}, {}, {}

    def send_plane(n):
        last[n] = Step(96, [(piece(p, 2, plane(p, 0), n, core), chip(p, 2, d)) for p in parts for d in (1, 3)])

    def pass_on(n):
        with jax.named_scope(f"wait_last{n}"):
            last[n].land()
        passed[n] = Step(48, [(piece(p, 2, plane(p, 4 - d), n, core, half=d // 2), chip(p, 2, d)) for p in parts for d in (1, 3)])
        lent[n] = hand_over([piece(p, 2, plane(p, d), n, core) for p in parts for d in (1, 3)], 96)

    def finish(n):
        with jax.named_scope(f"wait_passed{n}"):
            passed[n].land()
        lent_on[n] = hand_over([piece(p, 2, plane(p, 2), n, core) for p in parts], 48)

    with jax.named_scope("send_third"):
        send_plane(0)
        own = hand_over([piece(p, 2, plane(p, 0), None, core) for p in parts], 96)
        send_windows(CUTS[1], 127)
    send_plane(1)
    span = got.at[pl.ds(0, 127)]
    everything = pltpu.make_async_remote_copy(
        src_ref=span, dst_ref=span, send_sem=xs_send, recv_sem=xs_recv, device_id=chip(0, 0, 0, 1), device_id_type=MESH
    )
    with jax.named_scope("wait_windows"):
        everything.wait_recv()
    pass_on(0)
    xs, ys = (x0, x1, x2), (y0, y1, y2)
    with jax.named_scope("turn"):
        for pair in range(6):
            for p in parts:
                rows = []
                for v in range(4):
                    for c in range(2):
                        at = 64 * c
                        if p == 0:
                            rows.append(got[at + 16 * v : at + 16 * v + 16, pair])
                        elif p == 1:
                            rows.append(got[at + v : at + 64 : 4, pair])
                        else:
                            rows += [got[at + 16 * a + 4 * v : at + 16 * a + 4 * v + 4, pair] for a in range(4)]
                rows = jnp.concatenate([r.reshape(-1, LANES) for r in rows], axis=0).T
                for odd in range(2):
                    main = rows[64 * odd : 64 * odd + 64]
                    xs[p][2 * pair + odd, 8 - 4 * p : 72 - 4 * p] = main
                    if p == 1:
                        edge[0, 2 * pair + odd] = main[60:64]
                        edge[1, 2 * pair + odd] = main[0:4]
    halo = []
    for src, dst, d in (
        (x0.at[:, pl.ds(64, 8)], x0.at[:, pl.ds(0, 8)], 1),
        (x2.at[:, pl.ds(0, 8)], x2.at[:, pl.ds(64, 8)], 7),
        (edge.at[0], edge.at[2], 1),
        (edge.at[1], edge.at[3], 7),
    ):
        halo.append(
            pltpu.make_async_remote_copy(
                src_ref=src,
                dst_ref=dst,
                send_sem=halo_send.at[len(halo)],
                recv_sem=halo_recv.at[len(halo)],
                device_id={"model": (m + d) % 8, "cols": q},
                device_id_type=MESH,
            )
        )
        halo[-1].start()

    def conv1(halves, places, spans, groups):
        width = 10 // groups
        tops = [None] * groups
        for p in parts:
            at = [plane(p, d) for d in places]
            lanes = [pl.ds(pl.multiple_of(LANES * v, LANES), LANES) for v in at]
            for dw in range(3):
                right = [[w1g[p, n, v, :, :, :, dw, i].reshape(LANES, LANES) for n in halves for i in range(2)] for v in at]
                right = jnp.concatenate([jnp.concatenate(r, axis=1) for r in right], axis=0)
                for group in range(groups):
                    cols = pl.ds(dw + width * group, width)
                    left = [jnp.concatenate([xs[p][cols, rows, s] for s in lanes], axis=-1) for rows in spans]
                    left = jnp.concatenate(left, axis=1).reshape(-1, 256)
                    term = jnp.dot(left, right, preferred_element_type=F32)
                    tops[group] = term if tops[group] is None else tops[group] + term
        return [top.reshape(width, -1, 256 * len(halves)) for top in tops]

    top_rows, inner, low_rows = pl.ds(0, 8), pl.ds(8, 56), pl.ds(64, 8)

    def near(n):
        with jax.named_scope(f"wait_lent{n}"):
            lent[n].land()
        with jax.named_scope(f"near{n}"):
            for group, top in enumerate(conv1((n,), (3, 1), (inner,), 2)):
                z_acc[n, pl.ds(5 * group, 5), inner] = top

    def rim():
        with jax.named_scope("rim"):
            (top,) = conv1((0, 1), (3, 1), (top_rows, low_rows), 1)
            for n in range(2):
                part = top[:, :, 256 * n : 256 * n + 256]
                z_acc[n, :, top_rows] = part[:, :8]
                z_acc[n, :, low_rows] = part[:, 8:]

    def far(n):
        with jax.named_scope(f"wait_lent_on{n}"):
            lent_on[n].land()
        lanes = slice(256 * n, 256 * n + 256)
        with jax.named_scope(f"far{n}"):
            for group, top in enumerate(conv1((n,), (0, 2), (pl.ds(0, 72),), 2)):
                cols = pl.ds(5 * group, 5)
                act = jnp.maximum(z_acc[n, cols] + top + b1v[:, lanes], 0.0)
                for dh in range(3):
                    ys[dh][cols, :, lanes] = act[:, 4 * dh : 4 * dh + 64].astype(BF16)

        def clear(at_edge, refs, cols, rows):
            @pl.when(at_edge)
            def _():
                for ref in refs:
                    ref[cols, rows, lanes] = jnp.zeros((cols.size, rows.size, 256), BF16)

        clear(q == 0, ys, pl.ds(0, 1), pl.ds(0, 64))
        clear(q == 15, ys, pl.ds(9, 1), pl.ds(0, 64))
        clear(m == 0, (y0,), pl.ds(0, 10), pl.ds(0, 4))
        clear(m == 7, (y2,), pl.ds(0, 10), pl.ds(60, 4))

    def conv2(n):
        lanes = slice(256 * n, 256 * n + 256)
        total = None
        for dh in range(3):
            for dw in range(3):
                tap = 3 * dh + dw
                left = ys[dh][dw : dw + 8, :, lanes].reshape(CHANS, 256)
                right = w2v[CHANS * tap + 256 * n : CHANS * tap + 256 * n + 256, :]
                term = jnp.dot(left, right, preferred_element_type=F32)
                total = term if total is None else total + term
        return total

    pass_on(1)
    near(0)
    near(1)
    finish(0)
    with jax.named_scope("wait_halo"):
        for copy in halo:
            copy.wait_recv()

    @pl.when(m == 0)
    def _():
        x0[:, 0:8] = jnp.zeros((12, 8, CHANS), BF16)
        x1[:, 0:4] = jnp.zeros((12, 4, CHANS), BF16)

    @pl.when(m > 0)
    def _():
        x1[:, 0:4] = edge[2]

    @pl.when(m == 7)
    def _():
        x2[:, 64:72] = jnp.zeros((12, 8, CHANS), BF16)
        x1[:, 68:72] = jnp.zeros((12, 4, CHANS), BF16)

    @pl.when(m < 7)
    def _():
        x1[:, 68:72] = edge[3]

    rim()
    finish(1)
    with jax.named_scope("wait_own_w2"):
        own.land()
        for load in loads[2:]:
            load.wait()
    far(0)
    with jax.named_scope("conv2_0"):
        acc2[...] = conv2(0)
    far(1)
    with jax.named_scope("conv2_1"):
        o_ref[...] = acc2[...] + conv2(1) + b2v[...]

    with jax.named_scope("wait_sends"):
        everything.wait_send()
        for step in steps:
            step.all.wait_send()
        for copy in halo:
            copy.wait_send()


def arrange(sum_ref, o_hbm, turned, sems):
    copies = []
    for g in range(4):
        rows = jnp.transpose(sum_ref[:, 16 * g : 16 * g + 16], (1, 0, 2))
        for h in range(4):
            for image in range(4):
                turned[g, image, h] = rows[4 * h + image]
        copies.append(pltpu.make_async_copy(turned.at[g], o_hbm.at[:, pl.ds(4 * g, 4)], sems.at[g]))
        copies[-1].start()
    for copy in copies:
        copy.wait()


def solution(mesh):
    scratch = [
        pltpu.VMEM((4, LANES, 4, LANES), BF16),
        pltpu.VMEM((9, 4, CHANS), BF16),
        pltpu.VMEM((4616, CHANS), BF16),
        pltpu.VMEM((1, CHANS), F32),
        pltpu.VMEM((1, CHANS), F32),
        pltpu.VMEM((CHANS, CHANS), BF16),
        pltpu.VMEM((8, 66, 4, LANES), BF16),
        pltpu.VMEM((LANES, 6, 4, LANES), BF16),
        *[pltpu.VMEM((12, 72, CHANS), BF16) for _ in range(3)],
        pltpu.VMEM((4, 12, 4, CHANS), BF16),
        pltpu.VMEM((3, 2, 4, 2, 4, 4, 3, 2, 4, LANES), BF16),
        pltpu.VMEM((2, 10, 72, 256), F32),
        *[pltpu.VMEM((10, 64, CHANS), BF16) for _ in range(3)],
        pltpu.VMEM((CHANS, CHANS), F32),
        pltpu.SemaphoreType.DMA((5,)),
        pltpu.SemaphoreType.DMA,
        pltpu.SemaphoreType.DMA,
        pltpu.SemaphoreType.DMA((4,)),
        pltpu.SemaphoreType.DMA((4,)),
        pltpu.SemaphoreType.DMA((11,)),
        pltpu.SemaphoreType.DMA((11,)),
    ]
    vmem = pl.BlockSpec(memory_space=pltpu.VMEM)
    anywhere = pl.BlockSpec(memory_space=pl.ANY)

    def run_local(x_in, w_conv1, b_conv1, w_conv2, b_conv2):
        sums = pl.pallas_call(
            kernel,
            out_shape=jax.ShapeDtypeStruct((CHANS, CHANS), F32),
            in_specs=[anywhere] * 5,
            out_specs=vmem,
            scratch_shapes=scratch,
            compiler_params=pltpu.CompilerParams(collective_id=0, has_side_effects=True, vmem_limit_bytes=VMEM_LIMIT),
            name="two_convs",
        )(
            *(
                pltpu.with_memory_space_constraint(a, pltpu.HBM)
                for a in (
                    x_in.transpose(0, 1, 3, 2),
                    w_conv1.reshape(9, 4, CHANS),
                    w_conv2.reshape(4608, CHANS),
                    b_conv1.reshape(1, CHANS),
                    b_conv2.reshape(1, CHANS),
                )
            )
        )
        return pl.pallas_call(
            arrange,
            out_shape=jax.ShapeDtypeStruct((4, 16, 8, CHANS), F32),
            in_specs=[vmem],
            out_specs=anywhere,
            scratch_shapes=[pltpu.VMEM((4, 4, 4, 8, CHANS), F32), pltpu.SemaphoreType.DMA((4,))],
            compiler_params=pltpu.CompilerParams(vmem_limit_bytes=8 * 2**20),
            name="arrange",
        )(sums.reshape(8, 64, CHANS))

    return jax.shard_map(
        run_local,
        mesh=mesh,
        in_specs=(P("data", None, None, GROUP_AXES), P(None, None, GROUP_AXES, None), P(), P(), P()),
        out_specs=P("data", "model", "cols", None),
        check_vma=False,
    )
```

```python
import jax
import jax.numpy as jnp
from jax import lax
from jax.experimental import pallas as pl
from jax.experimental.pallas import tpu as pltpu
from jax.sharding import PartitionSpec as P

GROUP_AXES = ("model", "cols")
MESH = pl.DeviceIdType.MESH
BF16 = jnp.bfloat16
F32 = jnp.float32
CHANS = 512
LANES = 128
CUTS = (96, 127)
VMEM_LIMIT = 36 * 2**20
ORDERS = (("y", "z", "x"), ("z", "x", "y"), ("x", "y", "z"))


def one_hot(shape, col_of_row):
    rows = lax.broadcasted_iota(jnp.int32, shape, 0)
    cols = lax.broadcasted_iota(jnp.int32, shape, 1)
    return jnp.where(cols == col_of_row(rows), 1.0, 0.0).astype(BF16)


def pack_windows(xv, a_scr, pack):
    to_lanes = one_hot((CHANS, CHANS), lambda r: (r % 4) * LANES + ((r % LANES) // 4) * 4 + r // LANES)
    to_rows = one_hot((CHANS, CHANS), lambda r: (r % 4) * LANES + ((r % 256) // 4) * 2 + r // 256)
    for blk in range(4):
        part = jnp.concatenate([xv[n, 32 * blk : 32 * blk + 32].reshape(LANES, LANES) for n in range(4)], axis=0)
        turned = lax.dot_general(part, to_lanes, (((0,), (0,)), ((), ())), preferred_element_type=F32).astype(BF16)
        for c in range(4):
            a_scr[c * LANES : (c + 1) * LANES, blk * LANES : (blk + 1) * LANES] = turned[:, c * LANES : (c + 1) * LANES]
    mixed = jnp.dot(to_rows, a_scr[...], preferred_element_type=F32)
    for blk in range(4):
        even = mixed[0:256, blk * LANES : (blk + 1) * LANES]
        odd = mixed[256:CHANS, blk * LANES : (blk + 1) * LANES]
        for half in range(2):
            s = slice(64 * half, 64 * half + 64)
            tile = jnp.concatenate([even[:, s], odd[:, s]], axis=1).astype(BF16)
            pack[2 * blk + half, 1:65] = tile.reshape(64, 4, LANES)
    edge = jnp.zeros((8, 1, 4, LANES), BF16)
    pack[:, 0:1] = edge
    pack[:, 65:66] = edge


def kernel(
    x_hbm, w1_hbm, w2_hbm, b1_hbm, b2_hbm, o_ref,
    xv, w1v, w2v, b1v, b2v, a_scr, pack, got, x0, x1, x2, edge, w1g, z_acc, y0, y1, y2, acc2,
    load_sem, xs_send, xs_recv, halo_send, halo_recv, step_send, step_recv,
):
    m = lax.axis_index("model")
    q = lax.axis_index("cols")
    me = {"x": m // 2, "z": q // 4, "y": q % 4}
    core = m % 2
    parts = range(3)
    barrier = pltpu.get_barrier_semaphore()

    at_model = [[(me["x"] + dx) % 4 * 2 + (core + dk) % 2 for dk in range(2)] for dx in range(4)]
    at_cols = [[(me["z"] + dz) % 4 * 4 + (me["y"] + dy) % 4 for dy in range(4)] for dz in range(4)]
    others = [(dx, dz, dy, dk) for dx in range(4) for dz in range(4) for dy in range(4) for dk in range(2)]
    others = sorted(others[1:], key=lambda d: (sum(d[:3]) % 4, d))

    def away(d):
        return {"model": at_model[d[0]][d[3]], "cols": at_cols[d[1]][d[2]]}

    loads = [
        pltpu.make_async_copy(src, dst, load_sem.at[k])
        for k, (src, dst) in enumerate(
            ((x_hbm, xv), (w1_hbm, w1v), (w2_hbm, w2v.at[pl.ds(0, 4608)]), (b1_hbm, b1v), (b2_hbm, b2v))
        )
    ]
    for load in loads:
        load.start()
    with jax.named_scope("announce"):
        for d in sorted(others, key=lambda d: -sum(min(o, 4 - o) for o in d[:3])):
            pl.semaphore_signal(barrier, inc=1, device_id=away(d), device_id_type=MESH)

    def piece(p, t, v, n, c, place=None, half=None):
        done = ORDERS[p][:t]
        rest = [a for a in "xzy" if a != ORDERS[p][2]]
        at = [v if t < 2 and a == ORDERS[p][t] else (pl.ds(0, 4) if a in done else me[a]) for a in rest]
        if half is not None:
            at[0] = pl.ds(2 * half, 2)
        return w1g.at[p, pl.ds(0, 2) if n is None else n, me[ORDERS[p][2]] if t < 2 else v, c, at[0], at[1]]

    with jax.named_scope("place_w1"):
        loads[1].wait()
        for p in parts:
            spot = [me[a] for a in "xzy" if a != ORDERS[p][2]]
            for dw in range(3):
                for lt in range(4):
                    tile = w1v[3 * p + dw, :, lt * LANES : (lt + 1) * LANES]
                    w1g[p, lt // 2, me[ORDERS[p][2]], core, spot[0], spot[1], dw, lt % 2] = tile
    with jax.named_scope("wait_x"):
        loads[0].wait()
    with jax.named_scope("pack"):
        pack_windows(xv, a_scr, pack)
    with jax.named_scope("wait_barrier"):
        pl.semaphore_wait(barrier, 127)

    n_steps = [0]
    steps = []

    class Step:
        def __init__(self, slabs, copies):
            k = n_steps[0]
            n_steps[0] += 1
            sems = dict(send_sem=step_send.at[k], recv_sem=step_recv.at[k], device_id_type=MESH)
            for ref, to in copies:
                pltpu.make_async_remote_copy(src_ref=ref, dst_ref=ref, device_id=to, **sems).start()
            span = got.at[pl.ds(0, slabs)]
            self.all = pltpu.make_async_remote_copy(
                src_ref=span, dst_ref=span, device_id={"model": at_model[0][1], "cols": q}, **sems
            )
            steps.append(self)

        def land(self):
            self.all.wait_recv()

    def chip(p, t, d, c=0):
        axis = ORDERS[p][t]
        pos = me | {axis: (me[axis] + d) % 4}
        return {"model": pos["x"] * 2 + (core + c) % 2, "cols": pos["z"] * 4 + pos["y"]}

    def spread(t, slabs):
        return Step(slabs, [(piece(p, t, me[ORDERS[p][t]], None, core), chip(p, t, d)) for p in parts for d in (1, 3, 2)])

    def plane(p, d):
        return (me[ORDERS[p][2]] + d) % 4

    def hand_over(pieces, slabs):
        return Step(slabs, [(ref, {"model": at_model[0][1], "cols": q}) for ref in pieces])

    def send_windows(first, last):
        for d in others[first:last]:
            to = away(d)
            pltpu.make_async_remote_copy(
                src_ref=pack.at[to["model"], pl.ds(4 * to["cols"], 6)],
                dst_ref=got.at[mine],
                send_sem=xs_send,
                recv_sem=xs_recv,
                device_id=to,
                device_id_type=MESH,
            ).start()

    mine = ((core * 4 + me["x"]) * 4 + me["z"]) * 4 + me["y"]
    with jax.named_scope("send_first"):
        first = spread(0, 18)
        for pair in range(6):
            got[mine, pair] = pack[m, 4 * q + pair]
        send_windows(0, CUTS[0])
    with jax.named_scope("wait_first"):
        first.land()
    with jax.named_scope("send_second"):
        second = spread(1, 72)
        send_windows(CUTS[0], CUTS[1])
    with jax.named_scope("wait_second"):
        second.land()
    last, passed, lent, lent_on = {}, {}, {}, {}

    def send_plane(n):
        last[n] = Step(96, [(piece(p, 2, plane(p, 0), n, core), chip(p, 2, d)) for p in parts for d in (1, 3)])

    def pass_on(n):
        with jax.named_scope(f"wait_last{n}"):
            last[n].land()
        passed[n] = Step(48, [(piece(p, 2, plane(p, 4 - d), n, core, half=d // 2), chip(p, 2, d)) for p in parts for d in (1, 3)])
        lent[n] = hand_over([piece(p, 2, plane(p, d), n, core) for p in parts for d in (1, 3)], 96)

    def finish(n):
        with jax.named_scope(f"wait_passed{n}"):
            passed[n].land()
        lent_on[n] = hand_over([piece(p, 2, plane(p, 2), n, core) for p in parts], 48)

    with jax.named_scope("send_third"):
        send_plane(0)
        own = hand_over([piece(p, 2, plane(p, 0), None, core) for p in parts], 96)
        send_windows(CUTS[1], 127)
    send_plane(1)
    span = got.at[pl.ds(0, 127)]
    everything = pltpu.make_async_remote_copy(
        src_ref=span, dst_ref=span, send_sem=xs_send, recv_sem=xs_recv, device_id=chip(0, 0, 0, 1), device_id_type=MESH
    )
    with jax.named_scope("wait_windows"):
        everything.wait_recv()
    pass_on(0)
    xs, ys = (x0, x1, x2), (y0, y1, y2)
    with jax.named_scope("turn"):
        for pair in range(6):
            for p in parts:
                rows = []
                for v in range(4):
                    for c in range(2):
                        at = 64 * c
                        if p == 0:
                            rows.append(got[at + 16 * v : at + 16 * v + 16, pair])
                        elif p == 1:
                            rows.append(got[at + v : at + 64 : 4, pair])
                        else:
                            rows += [got[at + 16 * a + 4 * v : at + 16 * a + 4 * v + 4, pair] for a in range(4)]
                rows = jnp.concatenate([r.reshape(-1, LANES) for r in rows], axis=0).T
                for odd in range(2):
                    main = rows[64 * odd : 64 * odd + 64]
                    xs[p][2 * pair + odd, 8 - 4 * p : 72 - 4 * p] = main
                    if p == 1:
                        edge[0, 2 * pair + odd] = main[60:64]
                        edge[1, 2 * pair + odd] = main[0:4]
    halo = []
    for src, dst, d in (
        (x0.at[:, pl.ds(64, 8)], x0.at[:, pl.ds(0, 8)], 1),
        (x2.at[:, pl.ds(0, 8)], x2.at[:, pl.ds(64, 8)], 7),
        (edge.at[0], edge.at[2], 1),
        (edge.at[1], edge.at[3], 7),
    ):
        halo.append(
            pltpu.make_async_remote_copy(
                src_ref=src,
                dst_ref=dst,
                send_sem=halo_send.at[len(halo)],
                recv_sem=halo_recv.at[len(halo)],
                device_id={"model": (m + d) % 8, "cols": q},
                device_id_type=MESH,
            )
        )
        halo[-1].start()

    def conv1(halves, places, spans, groups):
        width = 10 // groups
        tops = [None] * groups
        for p in parts:
            at = [plane(p, d) for d in places]
            lanes = [pl.ds(pl.multiple_of(LANES * v, LANES), LANES) for v in at]
            for dw in range(3):
                right = [[w1g[p, n, v, :, :, :, dw, i].reshape(LANES, LANES) for n in halves for i in range(2)] for v in at]
                right = jnp.concatenate([jnp.concatenate(r, axis=1) for r in right], axis=0)
                for group in range(groups):
                    cols = pl.ds(dw + width * group, width)
                    left = [jnp.concatenate([xs[p][cols, rows, s] for s in lanes], axis=-1) for rows in spans]
                    left = jnp.concatenate(left, axis=1).reshape(-1, 256)
                    term = jnp.dot(left, right, preferred_element_type=F32)
                    tops[group] = term if tops[group] is None else tops[group] + term
        return [top.reshape(width, -1, 256 * len(halves)) for top in tops]

    top_rows, inner, low_rows = pl.ds(0, 8), pl.ds(8, 56), pl.ds(64, 8)

    def near(n):
        with jax.named_scope(f"wait_lent{n}"):
            lent[n].land()
        with jax.named_scope(f"near{n}"):
            for group, top in enumerate(conv1((n,), (3, 1), (inner,), 2)):
                z_acc[n, pl.ds(5 * group, 5), inner] = top

    def rim():
        with jax.named_scope("rim"):
            (top,) = conv1((0, 1), (3, 1), (top_rows, low_rows), 1)
            for n in range(2):
                part = top[:, :, 256 * n : 256 * n + 256]
                z_acc[n, :, top_rows] = part[:, :8]
                z_acc[n, :, low_rows] = part[:, 8:]

    def far(n):
        with jax.named_scope(f"wait_lent_on{n}"):
            lent_on[n].land()
        lanes = slice(256 * n, 256 * n + 256)
        with jax.named_scope(f"far{n}"):
            for group, top in enumerate(conv1((n,), (0, 2), (pl.ds(0, 72),), 2)):
                cols = pl.ds(5 * group, 5)
                act = jnp.maximum(z_acc[n, cols] + top + b1v[:, lanes], 0.0)
                for dh in range(3):
                    ys[dh][cols, :, lanes] = act[:, 4 * dh : 4 * dh + 64].astype(BF16)

        def clear(at_edge, refs, cols, rows):
            @pl.when(at_edge)
            def _():
                for ref in refs:
                    ref[cols, rows, lanes] = jnp.zeros((cols.size, rows.size, 256), BF16)

        clear(q == 0, ys, pl.ds(0, 1), pl.ds(0, 64))
        clear(q == 15, ys, pl.ds(9, 1), pl.ds(0, 64))
        clear(m == 0, (y0,), pl.ds(0, 10), pl.ds(0, 4))
        clear(m == 7, (y2,), pl.ds(0, 10), pl.ds(60, 4))

    def conv2(n):
        lanes = slice(256 * n, 256 * n + 256)
        total = None
        for dh in range(3):
            for dw in range(3):
                tap = 3 * dh + dw
                left = ys[dh][dw : dw + 8, :, lanes].reshape(CHANS, 256)
                right = w2v[CHANS * tap + 256 * n : CHANS * tap + 256 * n + 256, :]
                term = jnp.dot(left, right, preferred_element_type=F32)
                total = term if total is None else total + term
        return total

    pass_on(1)
    near(0)
    finish(0)
    near(1)
    with jax.named_scope("wait_halo"):
        for copy in halo:
            copy.wait_recv()

    @pl.when(m == 0)
    def _():
        x0[:, 0:8] = jnp.zeros((12, 8, CHANS), BF16)
        x1[:, 0:4] = jnp.zeros((12, 4, CHANS), BF16)

    @pl.when(m > 0)
    def _():
        x1[:, 0:4] = edge[2]

    @pl.when(m == 7)
    def _():
        x2[:, 64:72] = jnp.zeros((12, 8, CHANS), BF16)
        x1[:, 68:72] = jnp.zeros((12, 4, CHANS), BF16)

    @pl.when(m < 7)
    def _():
        x1[:, 68:72] = edge[3]

    rim()
    finish(1)
    with jax.named_scope("wait_own_w2"):
        own.land()
        for load in loads[2:]:
            load.wait()
    far(0)
    with jax.named_scope("conv2_0"):
        acc2[...] = conv2(0)
    far(1)
    with jax.named_scope("conv2_1"):
        o_ref[...] = acc2[...] + conv2(1) + b2v[...]

    with jax.named_scope("wait_sends"):
        everything.wait_send()
        for step in steps:
            step.all.wait_send()
        for copy in halo:
            copy.wait_send()


def arrange(sum_ref, o_hbm, turned, sems):
    copies = []
    for g in range(4):
        rows = jnp.transpose(sum_ref[:, 16 * g : 16 * g + 16], (1, 0, 2))
        for h in range(4):
            for image in range(4):
                turned[g, image, h] = rows[4 * h + image]
        copies.append(pltpu.make_async_copy(turned.at[g], o_hbm.at[:, pl.ds(4 * g, 4)], sems.at[g]))
        copies[-1].start()
    for copy in copies:
        copy.wait()


def solution(mesh):
    scratch = [
        pltpu.VMEM((4, LANES, 4, LANES), BF16),
        pltpu.VMEM((9, 4, CHANS), BF16),
        pltpu.VMEM((4616, CHANS), BF16),
        pltpu.VMEM((1, CHANS), F32),
        pltpu.VMEM((1, CHANS), F32),
        pltpu.VMEM((CHANS, CHANS), BF16),
        pltpu.VMEM((8, 66, 4, LANES), BF16),
        pltpu.VMEM((LANES, 6, 4, LANES), BF16),
        *[pltpu.VMEM((12, 72, CHANS), BF16) for _ in range(3)],
        pltpu.VMEM((4, 12, 4, CHANS), BF16),
        pltpu.VMEM((3, 2, 4, 2, 4, 4, 3, 2, 4, LANES), BF16),
        pltpu.VMEM((2, 10, 72, 256), F32),
        *[pltpu.VMEM((10, 64, CHANS), BF16) for _ in range(3)],
        pltpu.VMEM((CHANS, CHANS), F32),
        pltpu.SemaphoreType.DMA((5,)),
        pltpu.SemaphoreType.DMA,
        pltpu.SemaphoreType.DMA,
        pltpu.SemaphoreType.DMA((4,)),
        pltpu.SemaphoreType.DMA((4,)),
        pltpu.SemaphoreType.DMA((11,)),
        pltpu.SemaphoreType.DMA((11,)),
    ]
    vmem = pl.BlockSpec(memory_space=pltpu.VMEM)
    anywhere = pl.BlockSpec(memory_space=pl.ANY)

    def run_local(x_in, w_conv1, b_conv1, w_conv2, b_conv2):
        sums = pl.pallas_call(
            kernel,
            out_shape=jax.ShapeDtypeStruct((CHANS, CHANS), F32),
            in_specs=[anywhere] * 5,
            out_specs=vmem,
            scratch_shapes=scratch,
            compiler_params=pltpu.CompilerParams(collective_id=0, has_side_effects=True, vmem_limit_bytes=VMEM_LIMIT),
            name="two_convs",
        )(
            *(
                pltpu.with_memory_space_constraint(a, pltpu.HBM)
                for a in (
                    x_in.transpose(0, 1, 3, 2),
                    w_conv1.reshape(9, 4, CHANS),
                    w_conv2.reshape(4608, CHANS),
                    b_conv1.reshape(1, CHANS),
                    b_conv2.reshape(1, CHANS),
                )
            )
        )
        return pl.pallas_call(
            arrange,
            out_shape=jax.ShapeDtypeStruct((4, 16, 8, CHANS), F32),
            in_specs=[vmem],
            out_specs=anywhere,
            scratch_shapes=[pltpu.VMEM((4, 4, 4, 8, CHANS), F32), pltpu.SemaphoreType.DMA((4,))],
            compiler_params=pltpu.CompilerParams(vmem_limit_bytes=8 * 2**20),
            name="arrange",
        )(sums.reshape(8, 64, CHANS))

    return jax.shard_map(
        run_local,
        mesh=mesh,
        in_specs=(P("data", None, None, GROUP_AXES), P(None, None, GROUP_AXES, None), P(), P(), P()),
        out_specs=P("data", "model", "cols", None),
        check_vma=False,
    )
```

```python
import jax
import jax.numpy as jnp
from jax import lax
from jax.experimental import pallas as pl
from jax.experimental.pallas import tpu as pltpu
from jax.sharding import PartitionSpec as P

GROUP_AXES = ("model", "cols")
MESH = pl.DeviceIdType.MESH
BF16 = jnp.bfloat16
F32 = jnp.float32
CHANS = 512
LANES = 128
CUT = 96
VMEM_LIMIT = 36 * 2**20
ORDERS = (("y", "z", "x"), ("z", "x", "y"), ("x", "y", "z"))


def one_hot(shape, col_of_row):
    rows = lax.broadcasted_iota(jnp.int32, shape, 0)
    cols = lax.broadcasted_iota(jnp.int32, shape, 1)
    return jnp.where(cols == col_of_row(rows), 1.0, 0.0).astype(BF16)


def pack_windows(xv, a_scr, pack):
    to_lanes = one_hot((CHANS, CHANS), lambda r: (r % 4) * LANES + ((r % LANES) // 4) * 4 + r // LANES)
    to_rows = one_hot((CHANS, CHANS), lambda r: (r % 4) * LANES + ((r % 256) // 4) * 2 + r // 256)
    for blk in range(4):
        part = jnp.concatenate([xv[n, 32 * blk : 32 * blk + 32].reshape(LANES, LANES) for n in range(4)], axis=0)
        turned = lax.dot_general(part, to_lanes, (((0,), (0,)), ((), ())), preferred_element_type=F32).astype(BF16)
        for c in range(4):
            a_scr[c * LANES : (c + 1) * LANES, blk * LANES : (blk + 1) * LANES] = turned[:, c * LANES : (c + 1) * LANES]
    mixed = jnp.dot(to_rows, a_scr[...], preferred_element_type=F32)
    for blk in range(4):
        even = mixed[0:256, blk * LANES : (blk + 1) * LANES]
        odd = mixed[256:CHANS, blk * LANES : (blk + 1) * LANES]
        for half in range(2):
            s = slice(64 * half, 64 * half + 64)
            tile = jnp.concatenate([even[:, s], odd[:, s]], axis=1).astype(BF16)
            pack[2 * blk + half, 1:65] = tile.reshape(64, 4, LANES)
    edge = jnp.zeros((8, 1, 4, LANES), BF16)
    pack[:, 0:1] = edge
    pack[:, 65:66] = edge


def kernel(
    x_hbm, w1_hbm, w2_hbm, b1_hbm, b2_hbm, o_ref,
    xv, w1v, w2v, b1v, b2v, a_scr, pack, got, x0, x1, x2, edge, w1g, z_acc, y0, y1, y2, acc2,
    load_sem, xs_send, xs_recv, halo_send, halo_recv, step_send, step_recv,
):
    m = lax.axis_index("model")
    q = lax.axis_index("cols")
    me = {"x": m // 2, "z": q // 4, "y": q % 4}
    core = m % 2
    parts = range(3)
    barrier = pltpu.get_barrier_semaphore()

    at_model = [[(me["x"] + dx) % 4 * 2 + (core + dk) % 2 for dk in range(2)] for dx in range(4)]
    at_cols = [[(me["z"] + dz) % 4 * 4 + (me["y"] + dy) % 4 for dy in range(4)] for dz in range(4)]
    others = [(dx, dz, dy, dk) for dx in range(4) for dz in range(4) for dy in range(4) for dk in range(2)]
    others = sorted(others[1:], key=lambda d: (sum(d[:3]) % 4, d))

    def away(d):
        return {"model": at_model[d[0]][d[3]], "cols": at_cols[d[1]][d[2]]}

    loads = [
        pltpu.make_async_copy(src, dst, load_sem.at[k])
        for k, (src, dst) in enumerate(
            ((x_hbm, xv), (w1_hbm, w1v), (w2_hbm, w2v.at[pl.ds(0, 4608)]), (b1_hbm, b1v), (b2_hbm, b2v))
        )
    ]
    for load in loads:
        load.start()
    with jax.named_scope("announce"):
        for d in sorted(others, key=lambda d: -sum(min(o, 4 - o) for o in d[:3])):
            pl.semaphore_signal(barrier, inc=1, device_id=away(d), device_id_type=MESH)

    def piece(p, t, v, n, c, place=None, half=None):
        done = ORDERS[p][:t]
        rest = [a for a in "xzy" if a != ORDERS[p][2]]
        at = [v if t < 2 and a == ORDERS[p][t] else (pl.ds(0, 4) if a in done else me[a]) for a in rest]
        if half is not None:
            at[0] = pl.ds(2 * half, 2)
        return w1g.at[p, pl.ds(0, 2) if n is None else n, me[ORDERS[p][2]] if t < 2 else v, c, at[0], at[1]]

    with jax.named_scope("place_w1"):
        loads[1].wait()
        for p in parts:
            spot = [me[a] for a in "xzy" if a != ORDERS[p][2]]
            for dw in range(3):
                for lt in range(4):
                    tile = w1v[3 * p + dw, :, lt * LANES : (lt + 1) * LANES]
                    w1g[p, lt // 2, me[ORDERS[p][2]], core, spot[0], spot[1], dw, lt % 2] = tile
    with jax.named_scope("wait_x"):
        loads[0].wait()
    with jax.named_scope("pack"):
        pack_windows(xv, a_scr, pack)
    with jax.named_scope("wait_barrier"):
        pl.semaphore_wait(barrier, 127)

    n_steps = [0]
    steps = []

    class Step:
        def __init__(self, slabs, copies):
            k = n_steps[0]
            n_steps[0] += 1
            sems = dict(send_sem=step_send.at[k], recv_sem=step_recv.at[k], device_id_type=MESH)
            self.copies, self.sems = copies, sems
            span = got.at[pl.ds(0, slabs)]
            self.all = pltpu.make_async_remote_copy(
                src_ref=span, dst_ref=span, device_id={"model": at_model[0][1], "cols": q}, **sems
            )
            steps.append(self)

        def go(self):
            for ref, to in self.copies:
                pltpu.make_async_remote_copy(src_ref=ref, dst_ref=ref, device_id=to, **self.sems).start()
            return self

        def land(self):
            self.all.wait_recv()

    def chip(p, t, d, c=0):
        axis = ORDERS[p][t]
        pos = me | {axis: (me[axis] + d) % 4}
        return {"model": pos["x"] * 2 + (core + c) % 2, "cols": pos["z"] * 4 + pos["y"]}

    def spread(t, slabs):
        return Step(slabs, [(piece(p, t, me[ORDERS[p][t]], None, core), chip(p, t, d)) for p in parts for d in (1, 3, 2)]).go()

    def plane(p, d):
        return (me[ORDERS[p][2]] + d) % 4

    def hand_over(pieces, slabs):
        return Step(slabs, [(ref, {"model": at_model[0][1], "cols": q}) for ref in pieces]).go()

    def send_windows(first, last):
        for d in others[first:last]:
            to = away(d)
            pltpu.make_async_remote_copy(
                src_ref=pack.at[to["model"], pl.ds(4 * to["cols"], 6)],
                dst_ref=got.at[mine],
                send_sem=xs_send,
                recv_sem=xs_recv,
                device_id=to,
                device_id_type=MESH,
            ).start()

    mine = ((core * 4 + me["x"]) * 4 + me["z"]) * 4 + me["y"]
    with jax.named_scope("send_first"):
        first = spread(0, 18)
        for pair in range(6):
            got[mine, pair] = pack[m, 4 * q + pair]
        send_windows(0, CUT)
    with jax.named_scope("wait_first"):
        first.land()
    with jax.named_scope("send_second"):
        second = spread(1, 72)
        send_windows(CUT, 127)
    with jax.named_scope("wait_second"):
        second.land()
    last, passed, lent, lent_on = {}, {}, {}, {}

    def send_plane(n):
        last[n] = Step(96, [(piece(p, 2, plane(p, 0), n, core), chip(p, 2, d)) for p in parts for d in (1, 3)])

    def pass_on(n):
        with jax.named_scope(f"wait_last{n}"):
            last[n].land()
        passed[n] = Step(48, [(piece(p, 2, plane(p, 4 - d), n, core, half=d // 2), chip(p, 2, d)) for p in parts for d in (1, 3)]).go()
        lent[n] = hand_over([piece(p, 2, plane(p, d), n, core) for p in parts for d in (1, 3)], 96)

    def finish(n):
        with jax.named_scope(f"wait_passed{n}"):
            passed[n].land()
        lent_on[n] = hand_over([piece(p, 2, plane(p, 2), n, core) for p in parts], 48)

    with jax.named_scope("send_third"):
        for n in range(2):
            send_plane(n)
        last[0].go()
        own = hand_over([piece(p, 2, plane(p, 0), None, core) for p in parts], 96)
    @pl.when(core == 0)
    def _():
        last[1].go()

    span = got.at[pl.ds(0, 127)]
    everything = pltpu.make_async_remote_copy(
        src_ref=span, dst_ref=span, send_sem=xs_send, recv_sem=xs_recv, device_id=chip(0, 0, 0, 1), device_id_type=MESH
    )
    with jax.named_scope("wait_windows"):
        everything.wait_recv()

    @pl.when(core == 1)
    def _():
        last[1].go()

    pass_on(0)
    xs, ys = (x0, x1, x2), (y0, y1, y2)
    with jax.named_scope("turn"):
        for pair in range(6):
            for p in parts:
                rows = []
                for v in range(4):
                    for c in range(2):
                        at = 64 * c
                        if p == 0:
                            rows.append(got[at + 16 * v : at + 16 * v + 16, pair])
                        elif p == 1:
                            rows.append(got[at + v : at + 64 : 4, pair])
                        else:
                            rows += [got[at + 16 * a + 4 * v : at + 16 * a + 4 * v + 4, pair] for a in range(4)]
                rows = jnp.concatenate([r.reshape(-1, LANES) for r in rows], axis=0).T
                for odd in range(2):
                    main = rows[64 * odd : 64 * odd + 64]
                    xs[p][2 * pair + odd, 8 - 4 * p : 72 - 4 * p] = main
                    if p == 1:
                        edge[0, 2 * pair + odd] = main[60:64]
                        edge[1, 2 * pair + odd] = main[0:4]
    halo = []
    for src, dst, d in (
        (x0.at[:, pl.ds(64, 8)], x0.at[:, pl.ds(0, 8)], 1),
        (x2.at[:, pl.ds(0, 8)], x2.at[:, pl.ds(64, 8)], 7),
        (edge.at[0], edge.at[2], 1),
        (edge.at[1], edge.at[3], 7),
    ):
        halo.append(
            pltpu.make_async_remote_copy(
                src_ref=src,
                dst_ref=dst,
                send_sem=halo_send.at[len(halo)],
                recv_sem=halo_recv.at[len(halo)],
                device_id={"model": (m + d) % 8, "cols": q},
                device_id_type=MESH,
            )
        )
        halo[-1].start()

    def conv1(halves, places, spans, groups):
        width = 10 // groups
        tops = [None] * groups
        for p in parts:
            at = [plane(p, d) for d in places]
            lanes = [pl.ds(pl.multiple_of(LANES * v, LANES), LANES) for v in at]
            for dw in range(3):
                right = [[w1g[p, n, v, :, :, :, dw, i].reshape(LANES, LANES) for n in halves for i in range(2)] for v in at]
                right = jnp.concatenate([jnp.concatenate(r, axis=1) for r in right], axis=0)
                for group in range(groups):
                    cols = pl.ds(dw + width * group, width)
                    left = [jnp.concatenate([xs[p][cols, rows, s] for s in lanes], axis=-1) for rows in spans]
                    left = jnp.concatenate(left, axis=1).reshape(-1, 256)
                    term = jnp.dot(left, right, preferred_element_type=F32)
                    tops[group] = term if tops[group] is None else tops[group] + term
        return [top.reshape(width, -1, 256 * len(halves)) for top in tops]

    top_rows, inner, low_rows = pl.ds(0, 8), pl.ds(8, 56), pl.ds(64, 8)

    def near(n):
        with jax.named_scope(f"wait_lent{n}"):
            lent[n].land()
        with jax.named_scope(f"near{n}"):
            for group, top in enumerate(conv1((n,), (3, 1), (inner,), 2)):
                z_acc[n, pl.ds(5 * group, 5), inner] = top

    def rim():
        with jax.named_scope("rim"):
            (top,) = conv1((0, 1), (3, 1), (top_rows, low_rows), 1)
            for n in range(2):
                part = top[:, :, 256 * n : 256 * n + 256]
                z_acc[n, :, top_rows] = part[:, :8]
                z_acc[n, :, low_rows] = part[:, 8:]

    def far(n):
        with jax.named_scope(f"wait_lent_on{n}"):
            lent_on[n].land()
        lanes = slice(256 * n, 256 * n + 256)
        with jax.named_scope(f"far{n}"):
            for group, top in enumerate(conv1((n,), (0, 2), (pl.ds(0, 72),), 2)):
                cols = pl.ds(5 * group, 5)
                act = jnp.maximum(z_acc[n, cols] + top + b1v[:, lanes], 0.0)
                for dh in range(3):
                    ys[dh][cols, :, lanes] = act[:, 4 * dh : 4 * dh + 64].astype(BF16)

        def clear(at_edge, refs, cols, rows):
            @pl.when(at_edge)
            def _():
                for ref in refs:
                    ref[cols, rows, lanes] = jnp.zeros((cols.size, rows.size, 256), BF16)

        clear(q == 0, ys, pl.ds(0, 1), pl.ds(0, 64))
        clear(q == 15, ys, pl.ds(9, 1), pl.ds(0, 64))
        clear(m == 0, (y0,), pl.ds(0, 10), pl.ds(0, 4))
        clear(m == 7, (y2,), pl.ds(0, 10), pl.ds(60, 4))

    def conv2(n):
        lanes = slice(256 * n, 256 * n + 256)
        total = None
        for dh in range(3):
            for dw in range(3):
                tap = 3 * dh + dw
                left = ys[dh][dw : dw + 8, :, lanes].reshape(CHANS, 256)
                right = w2v[CHANS * tap + 256 * n : CHANS * tap + 256 * n + 256, :]
                term = jnp.dot(left, right, preferred_element_type=F32)
                total = term if total is None else total + term
        return total

    pass_on(1)
    near(0)
    near(1)
    finish(0)
    with jax.named_scope("wait_halo"):
        for copy in halo:
            copy.wait_recv()

    @pl.when(m == 0)
    def _():
        x0[:, 0:8] = jnp.zeros((12, 8, CHANS), BF16)
        x1[:, 0:4] = jnp.zeros((12, 4, CHANS), BF16)

    @pl.when(m > 0)
    def _():
        x1[:, 0:4] = edge[2]

    @pl.when(m == 7)
    def _():
        x2[:, 64:72] = jnp.zeros((12, 8, CHANS), BF16)
        x1[:, 68:72] = jnp.zeros((12, 4, CHANS), BF16)

    @pl.when(m < 7)
    def _():
        x1[:, 68:72] = edge[3]

    rim()
    finish(1)
    with jax.named_scope("wait_own_w2"):
        own.land()
        for load in loads[2:]:
            load.wait()
    far(0)
    with jax.named_scope("conv2_0"):
        acc2[...] = conv2(0)
    far(1)
    with jax.named_scope("conv2_1"):
        o_ref[...] = acc2[...] + conv2(1) + b2v[...]

    with jax.named_scope("wait_sends"):
        everything.wait_send()
        for step in steps:
            step.all.wait_send()
        for copy in halo:
            copy.wait_send()


def arrange(sum_ref, o_hbm, turned, sems):
    copies = []
    for g in range(4):
        rows = jnp.transpose(sum_ref[:, 16 * g : 16 * g + 16], (1, 0, 2))
        for h in range(4):
            for image in range(4):
                turned[g, image, h] = rows[4 * h + image]
        copies.append(pltpu.make_async_copy(turned.at[g], o_hbm.at[:, pl.ds(4 * g, 4)], sems.at[g]))
        copies[-1].start()
    for copy in copies:
        copy.wait()


def solution(mesh):
    scratch = [
        pltpu.VMEM((4, LANES, 4, LANES), BF16),
        pltpu.VMEM((9, 4, CHANS), BF16),
        pltpu.VMEM((4616, CHANS), BF16),
        pltpu.VMEM((1, CHANS), F32),
        pltpu.VMEM((1, CHANS), F32),
        pltpu.VMEM((CHANS, CHANS), BF16),
        pltpu.VMEM((8, 66, 4, LANES), BF16),
        pltpu.VMEM((LANES, 6, 4, LANES), BF16),
        *[pltpu.VMEM((12, 72, CHANS), BF16) for _ in range(3)],
        pltpu.VMEM((4, 12, 4, CHANS), BF16),
        pltpu.VMEM((3, 2, 4, 2, 4, 4, 3, 2, 4, LANES), BF16),
        pltpu.VMEM((2, 10, 72, 256), F32),
        *[pltpu.VMEM((10, 64, CHANS), BF16) for _ in range(3)],
        pltpu.VMEM((CHANS, CHANS), F32),
        pltpu.SemaphoreType.DMA((5,)),
        pltpu.SemaphoreType.DMA,
        pltpu.SemaphoreType.DMA,
        pltpu.SemaphoreType.DMA((4,)),
        pltpu.SemaphoreType.DMA((4,)),
        pltpu.SemaphoreType.DMA((11,)),
        pltpu.SemaphoreType.DMA((11,)),
    ]
    vmem = pl.BlockSpec(memory_space=pltpu.VMEM)
    anywhere = pl.BlockSpec(memory_space=pl.ANY)

    def run_local(x_in, w_conv1, b_conv1, w_conv2, b_conv2):
        sums = pl.pallas_call(
            kernel,
            out_shape=jax.ShapeDtypeStruct((CHANS, CHANS), F32),
            in_specs=[anywhere] * 5,
            out_specs=vmem,
            scratch_shapes=scratch,
            compiler_params=pltpu.CompilerParams(collective_id=0, has_side_effects=True, vmem_limit_bytes=VMEM_LIMIT),
            name="two_convs",
        )(
            *(
                pltpu.with_memory_space_constraint(a, pltpu.HBM)
                for a in (
                    x_in.transpose(0, 1, 3, 2),
                    w_conv1.reshape(9, 4, CHANS),
                    w_conv2.reshape(4608, CHANS),
                    b_conv1.reshape(1, CHANS),
                    b_conv2.reshape(1, CHANS),
                )
            )
        )
        return pl.pallas_call(
            arrange,
            out_shape=jax.ShapeDtypeStruct((4, 16, 8, CHANS), F32),
            in_specs=[vmem],
            out_specs=anywhere,
            scratch_shapes=[pltpu.VMEM((4, 4, 4, 8, CHANS), F32), pltpu.SemaphoreType.DMA((4,))],
            compiler_params=pltpu.CompilerParams(vmem_limit_bytes=8 * 2**20),
            name="arrange",
        )(sums.reshape(8, 64, CHANS))

    return jax.shard_map(
        run_local,
        mesh=mesh,
        in_specs=(P("data", None, None, GROUP_AXES), P(None, None, GROUP_AXES, None), P(), P(), P()),
        out_specs=P("data", "model", "cols", None),
        check_vma=False,
    )
```

```python
import jax
import jax.numpy as jnp
from jax import lax
from jax.experimental import pallas as pl
from jax.experimental.pallas import tpu as pltpu
from jax.sharding import PartitionSpec as P

GROUP_AXES = ("model", "cols")
MESH = pl.DeviceIdType.MESH
BF16 = jnp.bfloat16
F32 = jnp.float32
CHANS = 512
LANES = 128
CUT = 96
VMEM_LIMIT = 36 * 2**20
ORDERS = (("y", "z", "x"), ("z", "x", "y"), ("x", "y", "z"))


def one_hot(shape, col_of_row):
    rows = lax.broadcasted_iota(jnp.int32, shape, 0)
    cols = lax.broadcasted_iota(jnp.int32, shape, 1)
    return jnp.where(cols == col_of_row(rows), 1.0, 0.0).astype(BF16)


def pack_windows(xv, a_scr, pack):
    to_lanes = one_hot((CHANS, CHANS), lambda r: (r % 4) * LANES + ((r % LANES) // 4) * 4 + r // LANES)
    to_rows = one_hot((CHANS, CHANS), lambda r: (r % 4) * LANES + ((r % 256) // 4) * 2 + r // 256)
    for blk in range(4):
        part = jnp.concatenate([xv[n, 32 * blk : 32 * blk + 32].reshape(LANES, LANES) for n in range(4)], axis=0)
        turned = lax.dot_general(part, to_lanes, (((0,), (0,)), ((), ())), preferred_element_type=F32).astype(BF16)
        for c in range(4):
            a_scr[c * LANES : (c + 1) * LANES, blk * LANES : (blk + 1) * LANES] = turned[:, c * LANES : (c + 1) * LANES]
    mixed = jnp.dot(to_rows, a_scr[...], preferred_element_type=F32)
    for blk in range(4):
        even = mixed[0:256, blk * LANES : (blk + 1) * LANES]
        odd = mixed[256:CHANS, blk * LANES : (blk + 1) * LANES]
        for half in range(2):
            s = slice(64 * half, 64 * half + 64)
            tile = jnp.concatenate([even[:, s], odd[:, s]], axis=1).astype(BF16)
            pack[2 * blk + half, 1:65] = tile.reshape(64, 4, LANES)
    edge = jnp.zeros((8, 1, 4, LANES), BF16)
    pack[:, 0:1] = edge
    pack[:, 65:66] = edge


def kernel(
    x_hbm, w1_hbm, w2_hbm, b1_hbm, b2_hbm, o_ref,
    xv, w1v, w2v, b1v, b2v, a_scr, pack, got, x0, x1, x2, edge, w1g, z_acc, y0, y1, y2, acc2,
    load_sem, xs_send, xs_recv, halo_send, halo_recv, step_send, step_recv,
):
    m = lax.axis_index("model")
    q = lax.axis_index("cols")
    me = {"x": m // 2, "z": q // 4, "y": q % 4}
    core = m % 2
    parts = range(3)
    barrier = pltpu.get_barrier_semaphore()

    at_model = [[(me["x"] + dx) % 4 * 2 + (core + dk) % 2 for dk in range(2)] for dx in range(4)]
    at_cols = [[(me["z"] + dz) % 4 * 4 + (me["y"] + dy) % 4 for dy in range(4)] for dz in range(4)]
    others = [(dx, dz, dy, dk) for dx in range(4) for dz in range(4) for dy in range(4) for dk in range(2)]
    others = sorted(others[1:], key=lambda d: (sum(d[:3]) % 4, d))

    def away(d):
        return {"model": at_model[d[0]][d[3]], "cols": at_cols[d[1]][d[2]]}

    loads = [
        pltpu.make_async_copy(src, dst, load_sem.at[k])
        for k, (src, dst) in enumerate(
            ((x_hbm, xv), (w1_hbm, w1v), (w2_hbm, w2v.at[pl.ds(0, 4608)]), (b1_hbm, b1v), (b2_hbm, b2v))
        )
    ]
    for load in loads:
        load.start()
    with jax.named_scope("announce"):
        for d in sorted(others, key=lambda d: -sum(min(o, 4 - o) for o in d[:3])):
            pl.semaphore_signal(barrier, inc=1, device_id=away(d), device_id_type=MESH)

    def piece(p, t, v, n, c, place=None, half=None):
        done = ORDERS[p][:t]
        rest = [a for a in "xzy" if a != ORDERS[p][2]]
        at = [v if t < 2 and a == ORDERS[p][t] else (pl.ds(0, 4) if a in done else me[a]) for a in rest]
        if half is not None:
            at[0] = pl.ds(2 * half, 2)
        return w1g.at[p, pl.ds(0, 2) if n is None else n, me[ORDERS[p][2]] if t < 2 else v, c, at[0], at[1]]

    with jax.named_scope("place_w1"):
        loads[1].wait()
        for p in parts:
            spot = [me[a] for a in "xzy" if a != ORDERS[p][2]]
            for dw in range(3):
                for lt in range(4):
                    tile = w1v[3 * p + dw, :, lt * LANES : (lt + 1) * LANES]
                    w1g[p, lt // 2, me[ORDERS[p][2]], core, spot[0], spot[1], dw, lt % 2] = tile
    with jax.named_scope("wait_x"):
        loads[0].wait()
    with jax.named_scope("pack"):
        pack_windows(xv, a_scr, pack)
    with jax.named_scope("wait_barrier"):
        pl.semaphore_wait(barrier, 127)

    n_steps = [0]
    steps = []

    class Step:
        def __init__(self, slabs, copies):
            k = n_steps[0]
            n_steps[0] += 1
            sems = dict(send_sem=step_send.at[k], recv_sem=step_recv.at[k], device_id_type=MESH)
            self.copies, self.sems = copies, sems
            span = got.at[pl.ds(0, slabs)]
            self.all = pltpu.make_async_remote_copy(
                src_ref=span, dst_ref=span, device_id={"model": at_model[0][1], "cols": q}, **sems
            )
            steps.append(self)

        def go(self):
            for ref, to in self.copies:
                pltpu.make_async_remote_copy(src_ref=ref, dst_ref=ref, device_id=to, **self.sems).start()
            return self

        def land(self):
            self.all.wait_recv()

    def chip(p, t, d, c=0):
        axis = ORDERS[p][t]
        pos = me | {axis: (me[axis] + d) % 4}
        return {"model": pos["x"] * 2 + (core + c) % 2, "cols": pos["z"] * 4 + pos["y"]}

    def spread(t, slabs):
        return Step(slabs, [(piece(p, t, me[ORDERS[p][t]], None, core), chip(p, t, d)) for p in parts for d in (1, 3, 2)]).go()

    def plane(p, d):
        return (me[ORDERS[p][2]] + d) % 4

    def hand_over(pieces, slabs):
        return Step(slabs, [(ref, {"model": at_model[0][1], "cols": q}) for ref in pieces]).go()

    def send_windows(first, last):
        for d in others[first:last]:
            to = away(d)
            pltpu.make_async_remote_copy(
                src_ref=pack.at[to["model"], pl.ds(4 * to["cols"], 6)],
                dst_ref=got.at[mine],
                send_sem=xs_send,
                recv_sem=xs_recv,
                device_id=to,
                device_id_type=MESH,
            ).start()

    mine = ((core * 4 + me["x"]) * 4 + me["z"]) * 4 + me["y"]
    with jax.named_scope("send_first"):
        first = spread(0, 18)
        for pair in range(6):
            got[mine, pair] = pack[m, 4 * q + pair]
        send_windows(0, CUT)
    with jax.named_scope("wait_first"):
        first.land()
    with jax.named_scope("send_second"):
        second = spread(1, 72)
        send_windows(CUT, 127)
    with jax.named_scope("wait_second"):
        second.land()
    last, passed, lent, lent_on = {}, {}, {}, {}

    def send_plane(n):
        last[n] = Step(96, [(piece(p, 2, plane(p, 0), n, core), chip(p, 2, d)) for p in parts for d in (1, 3)])

    def pass_on(n):
        with jax.named_scope(f"wait_last{n}"):
            last[n].land()
        passed[n] = Step(48, [(piece(p, 2, plane(p, 4 - d), n, core, half=d // 2), chip(p, 2, d)) for p in parts for d in (1, 3)]).go()
        lent[n] = hand_over([piece(p, 2, plane(p, d), n, core) for p in parts for d in (1, 3)], 96)

    def finish(n):
        with jax.named_scope(f"wait_passed{n}"):
            passed[n].land()
        lent_on[n] = hand_over([piece(p, 2, plane(p, 2), n, core) for p in parts], 48)

    with jax.named_scope("send_third"):
        for n in range(2):
            send_plane(n)
        last[0].go()
        own = hand_over([piece(p, 2, plane(p, 0), None, core) for p in parts], 96)
    @pl.when(core == 0)
    def _():
        last[1].go()

    span = got.at[pl.ds(0, 127)]
    everything = pltpu.make_async_remote_copy(
        src_ref=span, dst_ref=span, send_sem=xs_send, recv_sem=xs_recv, device_id=chip(0, 0, 0, 1), device_id_type=MESH
    )
    with jax.named_scope("wait_windows"):
        everything.wait_recv()
    pass_on(0)

    @pl.when(core == 1)
    def _():
        last[1].go()

    xs, ys = (x0, x1, x2), (y0, y1, y2)
    with jax.named_scope("turn"):
        for pair in range(6):
            for p in parts:
                rows = []
                for v in range(4):
                    for c in range(2):
                        at = 64 * c
                        if p == 0:
                            rows.append(got[at + 16 * v : at + 16 * v + 16, pair])
                        elif p == 1:
                            rows.append(got[at + v : at + 64 : 4, pair])
                        else:
                            rows += [got[at + 16 * a + 4 * v : at + 16 * a + 4 * v + 4, pair] for a in range(4)]
                rows = jnp.concatenate([r.reshape(-1, LANES) for r in rows], axis=0).T
                for odd in range(2):
                    main = rows[64 * odd : 64 * odd + 64]
                    xs[p][2 * pair + odd, 8 - 4 * p : 72 - 4 * p] = main
                    if p == 1:
                        edge[0, 2 * pair + odd] = main[60:64]
                        edge[1, 2 * pair + odd] = main[0:4]
    halo = []
    for src, dst, d in (
        (x0.at[:, pl.ds(64, 8)], x0.at[:, pl.ds(0, 8)], 1),
        (x2.at[:, pl.ds(0, 8)], x2.at[:, pl.ds(64, 8)], 7),
        (edge.at[0], edge.at[2], 1),
        (edge.at[1], edge.at[3], 7),
    ):
        halo.append(
            pltpu.make_async_remote_copy(
                src_ref=src,
                dst_ref=dst,
                send_sem=halo_send.at[len(halo)],
                recv_sem=halo_recv.at[len(halo)],
                device_id={"model": (m + d) % 8, "cols": q},
                device_id_type=MESH,
            )
        )
        halo[-1].start()

    def conv1(halves, places, spans, groups):
        width = 10 // groups
        tops = [None] * groups
        for p in parts:
            at = [plane(p, d) for d in places]
            lanes = [pl.ds(pl.multiple_of(LANES * v, LANES), LANES) for v in at]
            for dw in range(3):
                right = [[w1g[p, n, v, :, :, :, dw, i].reshape(LANES, LANES) for n in halves for i in range(2)] for v in at]
                right = jnp.concatenate([jnp.concatenate(r, axis=1) for r in right], axis=0)
                for group in range(groups):
                    cols = pl.ds(dw + width * group, width)
                    left = [jnp.concatenate([xs[p][cols, rows, s] for s in lanes], axis=-1) for rows in spans]
                    left = jnp.concatenate(left, axis=1).reshape(-1, 256)
                    term = jnp.dot(left, right, preferred_element_type=F32)
                    tops[group] = term if tops[group] is None else tops[group] + term
        return [top.reshape(width, -1, 256 * len(halves)) for top in tops]

    top_rows, inner, low_rows = pl.ds(0, 8), pl.ds(8, 56), pl.ds(64, 8)

    def near(n):
        with jax.named_scope(f"wait_lent{n}"):
            lent[n].land()
        with jax.named_scope(f"near{n}"):
            for group, top in enumerate(conv1((n,), (3, 1), (inner,), 2)):
                z_acc[n, pl.ds(5 * group, 5), inner] = top

    def rim():
        with jax.named_scope("rim"):
            (top,) = conv1((0, 1), (3, 1), (top_rows, low_rows), 1)
            for n in range(2):
                part = top[:, :, 256 * n : 256 * n + 256]
                z_acc[n, :, top_rows] = part[:, :8]
                z_acc[n, :, low_rows] = part[:, 8:]

    def far(n):
        with jax.named_scope(f"wait_lent_on{n}"):
            lent_on[n].land()
        lanes = slice(256 * n, 256 * n + 256)
        with jax.named_scope(f"far{n}"):
            for group, top in enumerate(conv1((n,), (0, 2), (pl.ds(0, 72),), 2)):
                cols = pl.ds(5 * group, 5)
                act = jnp.maximum(z_acc[n, cols] + top + b1v[:, lanes], 0.0)
                for dh in range(3):
                    ys[dh][cols, :, lanes] = act[:, 4 * dh : 4 * dh + 64].astype(BF16)

        def clear(at_edge, refs, cols, rows):
            @pl.when(at_edge)
            def _():
                for ref in refs:
                    ref[cols, rows, lanes] = jnp.zeros((cols.size, rows.size, 256), BF16)

        clear(q == 0, ys, pl.ds(0, 1), pl.ds(0, 64))
        clear(q == 15, ys, pl.ds(9, 1), pl.ds(0, 64))
        clear(m == 0, (y0,), pl.ds(0, 10), pl.ds(0, 4))
        clear(m == 7, (y2,), pl.ds(0, 10), pl.ds(60, 4))

    def conv2(n):
        lanes = slice(256 * n, 256 * n + 256)
        total = None
        for dh in range(3):
            for dw in range(3):
                tap = 3 * dh + dw
                left = ys[dh][dw : dw + 8, :, lanes].reshape(CHANS, 256)
                right = w2v[CHANS * tap + 256 * n : CHANS * tap + 256 * n + 256, :]
                term = jnp.dot(left, right, preferred_element_type=F32)
                total = term if total is None else total + term
        return total

    pass_on(1)
    near(0)
    near(1)
    finish(0)
    with jax.named_scope("wait_halo"):
        for copy in halo:
            copy.wait_recv()

    @pl.when(m == 0)
    def _():
        x0[:, 0:8] = jnp.zeros((12, 8, CHANS), BF16)
        x1[:, 0:4] = jnp.zeros((12, 4, CHANS), BF16)

    @pl.when(m > 0)
    def _():
        x1[:, 0:4] = edge[2]

    @pl.when(m == 7)
    def _():
        x2[:, 64:72] = jnp.zeros((12, 8, CHANS), BF16)
        x1[:, 68:72] = jnp.zeros((12, 4, CHANS), BF16)

    @pl.when(m < 7)
    def _():
        x1[:, 68:72] = edge[3]

    rim()
    finish(1)
    with jax.named_scope("wait_own_w2"):
        own.land()
        for load in loads[2:]:
            load.wait()
    far(0)
    with jax.named_scope("conv2_0"):
        acc2[...] = conv2(0)
    far(1)
    with jax.named_scope("conv2_1"):
        o_ref[...] = acc2[...] + conv2(1) + b2v[...]

    with jax.named_scope("wait_sends"):
        everything.wait_send()
        for step in steps:
            step.all.wait_send()
        for copy in halo:
            copy.wait_send()


def arrange(sum_ref, o_hbm, turned, sems):
    copies = []
    for g in range(4):
        rows = jnp.transpose(sum_ref[:, 16 * g : 16 * g + 16], (1, 0, 2))
        for h in range(4):
            for image in range(4):
                turned[g, image, h] = rows[4 * h + image]
        copies.append(pltpu.make_async_copy(turned.at[g], o_hbm.at[:, pl.ds(4 * g, 4)], sems.at[g]))
        copies[-1].start()
    for copy in copies:
        copy.wait()


def solution(mesh):
    scratch = [
        pltpu.VMEM((4, LANES, 4, LANES), BF16),
        pltpu.VMEM((9, 4, CHANS), BF16),
        pltpu.VMEM((4616, CHANS), BF16),
        pltpu.VMEM((1, CHANS), F32),
        pltpu.VMEM((1, CHANS), F32),
        pltpu.VMEM((CHANS, CHANS), BF16),
        pltpu.VMEM((8, 66, 4, LANES), BF16),
        pltpu.VMEM((LANES, 6, 4, LANES), BF16),
        *[pltpu.VMEM((12, 72, CHANS), BF16) for _ in range(3)],
        pltpu.VMEM((4, 12, 4, CHANS), BF16),
        pltpu.VMEM((3, 2, 4, 2, 4, 4, 3, 2, 4, LANES), BF16),
        pltpu.VMEM((2, 10, 72, 256), F32),
        *[pltpu.VMEM((10, 64, CHANS), BF16) for _ in range(3)],
        pltpu.VMEM((CHANS, CHANS), F32),
        pltpu.SemaphoreType.DMA((5,)),
        pltpu.SemaphoreType.DMA,
        pltpu.SemaphoreType.DMA,
        pltpu.SemaphoreType.DMA((4,)),
        pltpu.SemaphoreType.DMA((4,)),
        pltpu.SemaphoreType.DMA((11,)),
        pltpu.SemaphoreType.DMA((11,)),
    ]
    vmem = pl.BlockSpec(memory_space=pltpu.VMEM)
    anywhere = pl.BlockSpec(memory_space=pl.ANY)

    def run_local(x_in, w_conv1, b_conv1, w_conv2, b_conv2):
        sums = pl.pallas_call(
            kernel,
            out_shape=jax.ShapeDtypeStruct((CHANS, CHANS), F32),
            in_specs=[anywhere] * 5,
            out_specs=vmem,
            scratch_shapes=scratch,
            compiler_params=pltpu.CompilerParams(collective_id=0, has_side_effects=True, vmem_limit_bytes=VMEM_LIMIT),
            name="two_convs",
        )(
            *(
                pltpu.with_memory_space_constraint(a, pltpu.HBM)
                for a in (
                    x_in.transpose(0, 1, 3, 2),
                    w_conv1.reshape(9, 4, CHANS),
                    w_conv2.reshape(4608, CHANS),
                    b_conv1.reshape(1, CHANS),
                    b_conv2.reshape(1, CHANS),
                )
            )
        )
        return pl.pallas_call(
            arrange,
            out_shape=jax.ShapeDtypeStruct((4, 16, 8, CHANS), F32),
            in_specs=[vmem],
            out_specs=anywhere,
            scratch_shapes=[pltpu.VMEM((4, 4, 4, 8, CHANS), F32), pltpu.SemaphoreType.DMA((4,))],
            compiler_params=pltpu.CompilerParams(vmem_limit_bytes=8 * 2**20),
            name="arrange",
        )(sums.reshape(8, 64, CHANS))

    return jax.shard_map(
        run_local,
        mesh=mesh,
        in_specs=(P("data", None, None, GROUP_AXES), P(None, None, GROUP_AXES, None), P(), P(), P()),
        out_specs=P("data", "model", "cols", None),
        check_vma=False,
    )
```

```python
import jax
import jax.numpy as jnp
from jax import lax
from jax.experimental import pallas as pl
from jax.experimental.pallas import tpu as pltpu
from jax.sharding import PartitionSpec as P

GROUP_AXES = ("model", "cols")
MESH = pl.DeviceIdType.MESH
BF16 = jnp.bfloat16
F32 = jnp.float32
CHANS = 512
LANES = 128
CUT = 96
VMEM_LIMIT = 36 * 2**20
ORDERS = (("y", "z", "x"), ("z", "x", "y"), ("x", "y", "z"))


def one_hot(shape, col_of_row):
    rows = lax.broadcasted_iota(jnp.int32, shape, 0)
    cols = lax.broadcasted_iota(jnp.int32, shape, 1)
    return jnp.where(cols == col_of_row(rows), 1.0, 0.0).astype(BF16)


def pack_windows(xv, a_scr, pack):
    to_lanes = one_hot((CHANS, CHANS), lambda r: (r % 4) * LANES + ((r % LANES) // 4) * 4 + r // LANES)
    to_rows = one_hot((CHANS, CHANS), lambda r: (r % 4) * LANES + ((r % 256) // 4) * 2 + r // 256)
    for blk in range(4):
        part = jnp.concatenate([xv[n, 32 * blk : 32 * blk + 32].reshape(LANES, LANES) for n in range(4)], axis=0)
        turned = lax.dot_general(part, to_lanes, (((0,), (0,)), ((), ())), preferred_element_type=F32).astype(BF16)
        for c in range(4):
            a_scr[c * LANES : (c + 1) * LANES, blk * LANES : (blk + 1) * LANES] = turned[:, c * LANES : (c + 1) * LANES]
    mixed = jnp.dot(to_rows, a_scr[...], preferred_element_type=F32)
    for blk in range(4):
        even = mixed[0:256, blk * LANES : (blk + 1) * LANES]
        odd = mixed[256:CHANS, blk * LANES : (blk + 1) * LANES]
        for half in range(2):
            s = slice(64 * half, 64 * half + 64)
            tile = jnp.concatenate([even[:, s], odd[:, s]], axis=1).astype(BF16)
            pack[2 * blk + half, 1:65] = tile.reshape(64, 4, LANES)
    edge = jnp.zeros((8, 1, 4, LANES), BF16)
    pack[:, 0:1] = edge
    pack[:, 65:66] = edge


def kernel(
    x_hbm, w1_hbm, w2_hbm, b1_hbm, b2_hbm, o_ref,
    xv, w1v, w2v, b1v, b2v, a_scr, pack, got, x0, x1, x2, edge, w1g, z_acc, y0, y1, y2, acc2,
    load_sem, xs_send, xs_recv, halo_send, halo_recv, step_send, step_recv,
):
    m = lax.axis_index("model")
    q = lax.axis_index("cols")
    me = {"x": m // 2, "z": q // 4, "y": q % 4}
    core = m % 2
    parts = range(3)
    barrier = pltpu.get_barrier_semaphore()

    at_model = [[(me["x"] + dx) % 4 * 2 + (core + dk) % 2 for dk in range(2)] for dx in range(4)]
    at_cols = [[(me["z"] + dz) % 4 * 4 + (me["y"] + dy) % 4 for dy in range(4)] for dz in range(4)]
    others = [(dx, dz, dy, dk) for dx in range(4) for dz in range(4) for dy in range(4) for dk in range(2)]
    others = sorted(others[1:], key=lambda d: (sum(d[:3]) % 4, d))

    def away(d):
        return {"model": at_model[d[0]][d[3]], "cols": at_cols[d[1]][d[2]]}

    loads = [
        pltpu.make_async_copy(src, dst, load_sem.at[k])
        for k, (src, dst) in enumerate(
            ((x_hbm, xv), (w1_hbm, w1v), (w2_hbm, w2v.at[pl.ds(0, 4608)]), (b1_hbm, b1v), (b2_hbm, b2v))
        )
    ]
    for load in loads:
        load.start()
    with jax.named_scope("announce"):
        for d in sorted(others, key=lambda d: -sum(min(o, 4 - o) for o in d[:3])):
            pl.semaphore_signal(barrier, inc=1, device_id=away(d), device_id_type=MESH)

    def piece(p, t, v, n, c, place=None, half=None):
        done = ORDERS[p][:t]
        rest = [a for a in "xzy" if a != ORDERS[p][2]]
        at = [v if t < 2 and a == ORDERS[p][t] else (pl.ds(0, 4) if a in done else me[a]) for a in rest]
        if half is not None:
            at[0] = pl.ds(2 * half, 2)
        return w1g.at[p, pl.ds(0, 2) if n is None else n, me[ORDERS[p][2]] if t < 2 else v, c, at[0], at[1]]

    with jax.named_scope("place_w1"):
        loads[1].wait()
        for p in parts:
            spot = [me[a] for a in "xzy" if a != ORDERS[p][2]]
            for dw in range(3):
                for lt in range(4):
                    tile = w1v[3 * p + dw, :, lt * LANES : (lt + 1) * LANES]
                    w1g[p, lt // 2, me[ORDERS[p][2]], core, spot[0], spot[1], dw, lt % 2] = tile
    with jax.named_scope("wait_x"):
        loads[0].wait()
    with jax.named_scope("pack"):
        pack_windows(xv, a_scr, pack)
    with jax.named_scope("wait_barrier"):
        pl.semaphore_wait(barrier, 127)

    n_steps = [0]
    steps = []

    class Step:
        def __init__(self, slabs, copies):
            k = n_steps[0]
            n_steps[0] += 1
            sems = dict(send_sem=step_send.at[k], recv_sem=step_recv.at[k], device_id_type=MESH)
            self.copies, self.sems = copies, sems
            span = got.at[pl.ds(0, slabs)]
            self.all = pltpu.make_async_remote_copy(
                src_ref=span, dst_ref=span, device_id={"model": at_model[0][1], "cols": q}, **sems
            )
            steps.append(self)

        def go(self):
            for ref, to in self.copies:
                pltpu.make_async_remote_copy(src_ref=ref, dst_ref=ref, device_id=to, **self.sems).start()
            return self

        def land(self):
            self.all.wait_recv()

    def chip(p, t, d, c=0):
        axis = ORDERS[p][t]
        pos = me | {axis: (me[axis] + d) % 4}
        return {"model": pos["x"] * 2 + (core + c) % 2, "cols": pos["z"] * 4 + pos["y"]}

    def spread(t, slabs):
        return Step(slabs, [(piece(p, t, me[ORDERS[p][t]], None, core), chip(p, t, d)) for p in parts for d in (1, 3, 2)]).go()

    def plane(p, d):
        return (me[ORDERS[p][2]] + d) % 4

    def hand_over(pieces, slabs):
        return Step(slabs, [(ref, {"model": at_model[0][1], "cols": q}) for ref in pieces]).go()

    def send_windows(first, last):
        for d in others[first:last]:
            to = away(d)
            pltpu.make_async_remote_copy(
                src_ref=pack.at[to["model"], pl.ds(4 * to["cols"], 6)],
                dst_ref=got.at[mine],
                send_sem=xs_send,
                recv_sem=xs_recv,
                device_id=to,
                device_id_type=MESH,
            ).start()

    mine = ((core * 4 + me["x"]) * 4 + me["z"]) * 4 + me["y"]
    with jax.named_scope("send_first"):
        first = spread(0, 18)
        for pair in range(6):
            got[mine, pair] = pack[m, 4 * q + pair]
        send_windows(0, CUT)
    with jax.named_scope("wait_first"):
        first.land()
    with jax.named_scope("send_second"):
        second = spread(1, 72)
        send_windows(CUT, 127)
    with jax.named_scope("wait_second"):
        second.land()
    last, passed, lent, lent_on = {}, {}, {}, {}

    def send_plane(n):
        last[n] = Step(96, [(piece(p, 2, plane(p, 0), n, core), chip(p, 2, d)) for p in parts for d in (1, 3)])

    def pass_on(n):
        with jax.named_scope(f"wait_last{n}"):
            last[n].land()
        passed[n] = Step(48, [(piece(p, 2, plane(p, 4 - d), n, core, half=d // 2), chip(p, 2, d)) for p in parts for d in (1, 3)]).go()
        lent[n] = hand_over([piece(p, 2, plane(p, d), n, core) for p in parts for d in (1, 3)], 96)

    def finish(n):
        with jax.named_scope(f"wait_passed{n}"):
            passed[n].land()
        lent_on[n] = hand_over([piece(p, 2, plane(p, 2), n, core) for p in parts], 48)

    with jax.named_scope("send_third"):
        for n in range(2):
            send_plane(n)
        last[0].go()
        own = hand_over([piece(p, 2, plane(p, 0), None, core) for p in parts], 96)
    @pl.when(core == 0)
    def _():
        last[1].go()

    span = got.at[pl.ds(0, 127)]
    everything = pltpu.make_async_remote_copy(
        src_ref=span, dst_ref=span, send_sem=xs_send, recv_sem=xs_recv, device_id=chip(0, 0, 0, 1), device_id_type=MESH
    )
    with jax.named_scope("wait_windows"):
        everything.wait_recv()

    @pl.when(core == 1)
    def _():
        last[1].go()

    xs, ys = (x0, x1, x2), (y0, y1, y2)
    with jax.named_scope("turn"):
        for pair in range(6):
            for p in parts:
                rows = []
                for v in range(4):
                    for c in range(2):
                        at = 64 * c
                        if p == 0:
                            rows.append(got[at + 16 * v : at + 16 * v + 16, pair])
                        elif p == 1:
                            rows.append(got[at + v : at + 64 : 4, pair])
                        else:
                            rows += [got[at + 16 * a + 4 * v : at + 16 * a + 4 * v + 4, pair] for a in range(4)]
                rows = jnp.concatenate([r.reshape(-1, LANES) for r in rows], axis=0).T
                for odd in range(2):
                    main = rows[64 * odd : 64 * odd + 64]
                    xs[p][2 * pair + odd, 8 - 4 * p : 72 - 4 * p] = main
                    if p == 1:
                        edge[0, 2 * pair + odd] = main[60:64]
                        edge[1, 2 * pair + odd] = main[0:4]
    halo = []
    for src, dst, d in (
        (x0.at[:, pl.ds(64, 8)], x0.at[:, pl.ds(0, 8)], 1),
        (x2.at[:, pl.ds(0, 8)], x2.at[:, pl.ds(64, 8)], 7),
        (edge.at[0], edge.at[2], 1),
        (edge.at[1], edge.at[3], 7),
    ):
        halo.append(
            pltpu.make_async_remote_copy(
                src_ref=src,
                dst_ref=dst,
                send_sem=halo_send.at[len(halo)],
                recv_sem=halo_recv.at[len(halo)],
                device_id={"model": (m + d) % 8, "cols": q},
                device_id_type=MESH,
            )
        )
        halo[-1].start()

    def conv1(halves, places, spans, groups):
        width = 10 // groups
        tops = [None] * groups
        for p in parts:
            at = [plane(p, d) for d in places]
            lanes = [pl.ds(pl.multiple_of(LANES * v, LANES), LANES) for v in at]
            for dw in range(3):
                right = [[w1g[p, n, v, :, :, :, dw, i].reshape(LANES, LANES) for n in halves for i in range(2)] for v in at]
                right = jnp.concatenate([jnp.concatenate(r, axis=1) for r in right], axis=0)
                for group in range(groups):
                    cols = pl.ds(dw + width * group, width)
                    left = [jnp.concatenate([xs[p][cols, rows, s] for s in lanes], axis=-1) for rows in spans]
                    left = jnp.concatenate(left, axis=1).reshape(-1, 256)
                    term = jnp.dot(left, right, preferred_element_type=F32)
                    tops[group] = term if tops[group] is None else tops[group] + term
        return [top.reshape(width, -1, 256 * len(halves)) for top in tops]

    top_rows, inner, low_rows = pl.ds(0, 8), pl.ds(8, 56), pl.ds(64, 8)

    def near(n):
        with jax.named_scope(f"wait_lent{n}"):
            lent[n].land()
        with jax.named_scope(f"near{n}"):
            for group, top in enumerate(conv1((n,), (3, 1), (inner,), 2)):
                z_acc[n, pl.ds(5 * group, 5), inner] = top

    def rim():
        with jax.named_scope("rim"):
            (top,) = conv1((0, 1), (3, 1), (top_rows, low_rows), 1)
            for n in range(2):
                part = top[:, :, 256 * n : 256 * n + 256]
                z_acc[n, :, top_rows] = part[:, :8]
                z_acc[n, :, low_rows] = part[:, 8:]

    def far(n):
        with jax.named_scope(f"wait_lent_on{n}"):
            lent_on[n].land()
        lanes = slice(256 * n, 256 * n + 256)
        with jax.named_scope(f"far{n}"):
            for group, top in enumerate(conv1((n,), (0, 2), (pl.ds(0, 72),), 2)):
                cols = pl.ds(5 * group, 5)
                act = jnp.maximum(z_acc[n, cols] + top + b1v[:, lanes], 0.0)
                for dh in range(3):
                    ys[dh][cols, :, lanes] = act[:, 4 * dh : 4 * dh + 64].astype(BF16)

        def clear(at_edge, refs, cols, rows):
            @pl.when(at_edge)
            def _():
                for ref in refs:
                    ref[cols, rows, lanes] = jnp.zeros((cols.size, rows.size, 256), BF16)

        clear(q == 0, ys, pl.ds(0, 1), pl.ds(0, 64))
        clear(q == 15, ys, pl.ds(9, 1), pl.ds(0, 64))
        clear(m == 0, (y0,), pl.ds(0, 10), pl.ds(0, 4))
        clear(m == 7, (y2,), pl.ds(0, 10), pl.ds(60, 4))

    def conv2(n):
        lanes = slice(256 * n, 256 * n + 256)
        total = None
        for dh in range(3):
            for dw in range(3):
                tap = 3 * dh + dw
                left = ys[dh][dw : dw + 8, :, lanes].reshape(CHANS, 256)
                right = w2v[CHANS * tap + 256 * n : CHANS * tap + 256 * n + 256, :]
                term = jnp.dot(left, right, preferred_element_type=F32)
                total = term if total is None else total + term
        return total

    pass_on(0)
    pass_on(1)
    near(0)
    near(1)
    finish(0)
    with jax.named_scope("wait_halo"):
        for copy in halo:
            copy.wait_recv()

    @pl.when(m == 0)
    def _():
        x0[:, 0:8] = jnp.zeros((12, 8, CHANS), BF16)
        x1[:, 0:4] = jnp.zeros((12, 4, CHANS), BF16)

    @pl.when(m > 0)
    def _():
        x1[:, 0:4] = edge[2]

    @pl.when(m == 7)
    def _():
        x2[:, 64:72] = jnp.zeros((12, 8, CHANS), BF16)
        x1[:, 68:72] = jnp.zeros((12, 4, CHANS), BF16)

    @pl.when(m < 7)
    def _():
        x1[:, 68:72] = edge[3]

    rim()
    finish(1)
    with jax.named_scope("wait_own_w2"):
        own.land()
        for load in loads[2:]:
            load.wait()
    far(0)
    with jax.named_scope("conv2_0"):
        acc2[...] = conv2(0)
    far(1)
    with jax.named_scope("conv2_1"):
        o_ref[...] = acc2[...] + conv2(1) + b2v[...]

    with jax.named_scope("wait_sends"):
        everything.wait_send()
        for step in steps:
            step.all.wait_send()
        for copy in halo:
            copy.wait_send()


def arrange(sum_ref, o_hbm, turned, sems):
    copies = []
    for g in range(4):
        rows = jnp.transpose(sum_ref[:, 16 * g : 16 * g + 16], (1, 0, 2))
        for h in range(4):
            for image in range(4):
                turned[g, image, h] = rows[4 * h + image]
        copies.append(pltpu.make_async_copy(turned.at[g], o_hbm.at[:, pl.ds(4 * g, 4)], sems.at[g]))
        copies[-1].start()
    for copy in copies:
        copy.wait()


def solution(mesh):
    scratch = [
        pltpu.VMEM((4, LANES, 4, LANES), BF16),
        pltpu.VMEM((9, 4, CHANS), BF16),
        pltpu.VMEM((4616, CHANS), BF16),
        pltpu.VMEM((1, CHANS), F32),
        pltpu.VMEM((1, CHANS), F32),
        pltpu.VMEM((CHANS, CHANS), BF16),
        pltpu.VMEM((8, 66, 4, LANES), BF16),
        pltpu.VMEM((LANES, 6, 4, LANES), BF16),
        *[pltpu.VMEM((12, 72, CHANS), BF16) for _ in range(3)],
        pltpu.VMEM((4, 12, 4, CHANS), BF16),
        pltpu.VMEM((3, 2, 4, 2, 4, 4, 3, 2, 4, LANES), BF16),
        pltpu.VMEM((2, 10, 72, 256), F32),
        *[pltpu.VMEM((10, 64, CHANS), BF16) for _ in range(3)],
        pltpu.VMEM((CHANS, CHANS), F32),
        pltpu.SemaphoreType.DMA((5,)),
        pltpu.SemaphoreType.DMA,
        pltpu.SemaphoreType.DMA,
        pltpu.SemaphoreType.DMA((4,)),
        pltpu.SemaphoreType.DMA((4,)),
        pltpu.SemaphoreType.DMA((11,)),
        pltpu.SemaphoreType.DMA((11,)),
    ]
    vmem = pl.BlockSpec(memory_space=pltpu.VMEM)
    anywhere = pl.BlockSpec(memory_space=pl.ANY)

    def run_local(x_in, w_conv1, b_conv1, w_conv2, b_conv2):
        sums = pl.pallas_call(
            kernel,
            out_shape=jax.ShapeDtypeStruct((CHANS, CHANS), F32),
            in_specs=[anywhere] * 5,
            out_specs=vmem,
            scratch_shapes=scratch,
            compiler_params=pltpu.CompilerParams(collective_id=0, has_side_effects=True, vmem_limit_bytes=VMEM_LIMIT),
            name="two_convs",
        )(
            *(
                pltpu.with_memory_space_constraint(a, pltpu.HBM)
                for a in (
                    x_in.transpose(0, 1, 3, 2),
                    w_conv1.reshape(9, 4, CHANS),
                    w_conv2.reshape(4608, CHANS),
                    b_conv1.reshape(1, CHANS),
                    b_conv2.reshape(1, CHANS),
                )
            )
        )
        return pl.pallas_call(
            arrange,
            out_shape=jax.ShapeDtypeStruct((4, 16, 8, CHANS), F32),
            in_specs=[vmem],
            out_specs=anywhere,
            scratch_shapes=[pltpu.VMEM((4, 4, 4, 8, CHANS), F32), pltpu.SemaphoreType.DMA((4,))],
            compiler_params=pltpu.CompilerParams(vmem_limit_bytes=8 * 2**20),
            name="arrange",
        )(sums.reshape(8, 64, CHANS))

    return jax.shard_map(
        run_local,
        mesh=mesh,
        in_specs=(P("data", None, None, GROUP_AXES), P(None, None, GROUP_AXES, None), P(), P(), P()),
        out_specs=P("data", "model", "cols", None),
        check_vma=False,
    )
```

```python
import jax
import jax.numpy as jnp
from jax import lax
from jax.experimental import pallas as pl
from jax.experimental.pallas import tpu as pltpu
from jax.sharding import PartitionSpec as P

GROUP_AXES = ("model", "cols")
MESH = pl.DeviceIdType.MESH
BF16 = jnp.bfloat16
F32 = jnp.float32
CHANS = 512
LANES = 128
CUT = 96
VMEM_LIMIT = 36 * 2**20
ORDERS = (("y", "z", "x"), ("z", "x", "y"), ("x", "y", "z"))


def one_hot(shape, col_of_row):
    rows = lax.broadcasted_iota(jnp.int32, shape, 0)
    cols = lax.broadcasted_iota(jnp.int32, shape, 1)
    return jnp.where(cols == col_of_row(rows), 1.0, 0.0).astype(BF16)


def pack_windows(xv, a_scr, pack):
    to_lanes = one_hot((CHANS, CHANS), lambda r: (r % 4) * LANES + ((r % LANES) // 4) * 4 + r // LANES)
    to_rows = one_hot((CHANS, CHANS), lambda r: (r % 4) * LANES + ((r % 256) // 4) * 2 + r // 256)
    for blk in range(4):
        part = jnp.concatenate([xv[n, 32 * blk : 32 * blk + 32].reshape(LANES, LANES) for n in range(4)], axis=0)
        turned = lax.dot_general(part, to_lanes, (((0,), (0,)), ((), ())), preferred_element_type=F32).astype(BF16)
        for c in range(4):
            a_scr[c * LANES : (c + 1) * LANES, blk * LANES : (blk + 1) * LANES] = turned[:, c * LANES : (c + 1) * LANES]
    mixed = jnp.dot(to_rows, a_scr[...], preferred_element_type=F32)
    for blk in range(4):
        even = mixed[0:256, blk * LANES : (blk + 1) * LANES]
        odd = mixed[256:CHANS, blk * LANES : (blk + 1) * LANES]
        for half in range(2):
            s = slice(64 * half, 64 * half + 64)
            tile = jnp.concatenate([even[:, s], odd[:, s]], axis=1).astype(BF16)
            pack[2 * blk + half, 1:65] = tile.reshape(64, 4, LANES)
    edge = jnp.zeros((8, 1, 4, LANES), BF16)
    pack[:, 0:1] = edge
    pack[:, 65:66] = edge


def kernel(
    x_hbm, w1_hbm, w2_hbm, b1_hbm, b2_hbm, o_ref,
    xv, w1v, w2v, b1v, b2v, a_scr, pack, got, x0, x1, x2, edge, w1g, z_acc, y0, y1, y2, acc2,
    load_sem, xs_send, xs_recv, halo_send, halo_recv, step_send, step_recv,
):
    m = lax.axis_index("model")
    q = lax.axis_index("cols")
    me = {"x": m // 2, "z": q // 4, "y": q % 4}
    core = m % 2
    parts = range(3)
    barrier = pltpu.get_barrier_semaphore()

    at_model = [[(me["x"] + dx) % 4 * 2 + (core + dk) % 2 for dk in range(2)] for dx in range(4)]
    at_cols = [[(me["z"] + dz) % 4 * 4 + (me["y"] + dy) % 4 for dy in range(4)] for dz in range(4)]
    others = [(dx, dz, dy, dk) for dx in range(4) for dz in range(4) for dy in range(4) for dk in range(2)]
    others = sorted(others[1:], key=lambda d: (sum(d[:3]) % 4, d))

    def away(d):
        return {"model": at_model[d[0]][d[3]], "cols": at_cols[d[1]][d[2]]}

    loads = [
        pltpu.make_async_copy(src, dst, load_sem.at[k])
        for k, (src, dst) in enumerate(
            ((x_hbm, xv), (w1_hbm, w1v), (w2_hbm, w2v.at[pl.ds(0, 4608)]), (b1_hbm, b1v), (b2_hbm, b2v))
        )
    ]
    for load in loads:
        load.start()
    with jax.named_scope("announce"):
        for d in sorted(others, key=lambda d: -sum(min(o, 4 - o) for o in d[:3])):
            pl.semaphore_signal(barrier, inc=1, device_id=away(d), device_id_type=MESH)

    def piece(p, t, v, n, c, place=None, half=None):
        done = ORDERS[p][:t]
        rest = [a for a in "xzy" if a != ORDERS[p][2]]
        at = [v if t < 2 and a == ORDERS[p][t] else (pl.ds(0, 4) if a in done else me[a]) for a in rest]
        if half is not None:
            at[0] = pl.ds(2 * half, 2)
        return w1g.at[p, pl.ds(0, 2) if n is None else n, me[ORDERS[p][2]] if t < 2 else v, c, at[0], at[1]]

    with jax.named_scope("place_w1"):
        loads[1].wait()
        for p in parts:
            spot = [me[a] for a in "xzy" if a != ORDERS[p][2]]
            for dw in range(3):
                for lt in range(4):
                    tile = w1v[3 * p + dw, :, lt * LANES : (lt + 1) * LANES]
                    w1g[p, lt // 2, me[ORDERS[p][2]], core, spot[0], spot[1], dw, lt % 2] = tile
    with jax.named_scope("wait_x"):
        loads[0].wait()
    with jax.named_scope("pack"):
        pack_windows(xv, a_scr, pack)
    with jax.named_scope("wait_barrier"):
        pl.semaphore_wait(barrier, 127)

    n_steps = [0]
    steps = []

    class Step:
        def __init__(self, slabs, copies):
            k = n_steps[0]
            n_steps[0] += 1
            sems = dict(send_sem=step_send.at[k], recv_sem=step_recv.at[k], device_id_type=MESH)
            self.copies, self.sems = copies, sems
            span = got.at[pl.ds(0, slabs)]
            self.all = pltpu.make_async_remote_copy(
                src_ref=span, dst_ref=span, device_id={"model": at_model[0][1], "cols": q}, **sems
            )
            steps.append(self)

        def go(self):
            for ref, to in self.copies:
                pltpu.make_async_remote_copy(src_ref=ref, dst_ref=ref, device_id=to, **self.sems).start()
            return self

        def land(self):
            self.all.wait_recv()

    def chip(p, t, d, c=0):
        axis = ORDERS[p][t]
        pos = me | {axis: (me[axis] + d) % 4}
        return {"model": pos["x"] * 2 + (core + c) % 2, "cols": pos["z"] * 4 + pos["y"]}

    def spread(t, slabs):
        return Step(slabs, [(piece(p, t, me[ORDERS[p][t]], None, core), chip(p, t, d)) for p in parts for d in (1, 3, 2)]).go()

    def plane(p, d):
        return (me[ORDERS[p][2]] + d) % 4

    def hand_over(pieces, slabs):
        return Step(slabs, [(ref, {"model": at_model[0][1], "cols": q}) for ref in pieces]).go()

    def send_windows(first, last):
        for d in others[first:last]:
            to = away(d)
            pltpu.make_async_remote_copy(
                src_ref=pack.at[to["model"], pl.ds(4 * to["cols"], 6)],
                dst_ref=got.at[mine],
                send_sem=xs_send,
                recv_sem=xs_recv,
                device_id=to,
                device_id_type=MESH,
            ).start()

    mine = ((core * 4 + me["x"]) * 4 + me["z"]) * 4 + me["y"]
    with jax.named_scope("send_first"):
        first = spread(0, 18)
        for pair in range(6):
            got[mine, pair] = pack[m, 4 * q + pair]
        send_windows(0, CUT)
    with jax.named_scope("wait_first"):
        first.land()
    with jax.named_scope("send_second"):
        second = spread(1, 72)
        send_windows(CUT, 127)
    with jax.named_scope("wait_second"):
        second.land()
    last, passed, lent, lent_on = {}, {}, {}, {}

    def send_plane(n):
        last[n] = Step(96, [(piece(p, 2, plane(p, 0), n, core), chip(p, 2, d)) for p in parts for d in (1, 3)])

    def pass_on(n):
        with jax.named_scope(f"wait_last{n}"):
            last[n].land()
        passed[n] = Step(48, [(piece(p, 2, plane(p, 4 - d), n, core, half=d // 2), chip(p, 2, d)) for p in parts for d in (1, 3)]).go()
        lent[n] = hand_over([piece(p, 2, plane(p, d), n, core) for p in parts for d in (1, 3)], 96)

    def finish(n):
        with jax.named_scope(f"wait_passed{n}"):
            passed[n].land()
        lent_on[n] = hand_over([piece(p, 2, plane(p, 2), n, core) for p in parts], 48)

    with jax.named_scope("send_third"):
        for n in range(2):
            send_plane(n)
        last[0].go()
        own = hand_over([piece(p, 2, plane(p, 0), None, core) for p in parts], 96)
    @pl.when(core == 0)
    def _():
        last[1].go()

    span = got.at[pl.ds(0, 127)]
    everything = pltpu.make_async_remote_copy(
        src_ref=span, dst_ref=span, send_sem=xs_send, recv_sem=xs_recv, device_id=chip(0, 0, 0, 1), device_id_type=MESH
    )
    with jax.named_scope("wait_windows"):
        everything.wait_recv()

    xs, ys = (x0, x1, x2), (y0, y1, y2)
    with jax.named_scope("turn"):
        for pair in range(6):
            for p in parts:
                rows = []
                for v in range(4):
                    for c in range(2):
                        at = 64 * c
                        if p == 0:
                            rows.append(got[at + 16 * v : at + 16 * v + 16, pair])
                        elif p == 1:
                            rows.append(got[at + v : at + 64 : 4, pair])
                        else:
                            rows += [got[at + 16 * a + 4 * v : at + 16 * a + 4 * v + 4, pair] for a in range(4)]
                rows = jnp.concatenate([r.reshape(-1, LANES) for r in rows], axis=0).T
                for odd in range(2):
                    main = rows[64 * odd : 64 * odd + 64]
                    xs[p][2 * pair + odd, 8 - 4 * p : 72 - 4 * p] = main
                    if p == 1:
                        edge[0, 2 * pair + odd] = main[60:64]
                        edge[1, 2 * pair + odd] = main[0:4]
    halo = []
    for src, dst, d in (
        (x0.at[:, pl.ds(64, 8)], x0.at[:, pl.ds(0, 8)], 1),
        (x2.at[:, pl.ds(0, 8)], x2.at[:, pl.ds(64, 8)], 7),
        (edge.at[0], edge.at[2], 1),
        (edge.at[1], edge.at[3], 7),
    ):
        halo.append(
            pltpu.make_async_remote_copy(
                src_ref=src,
                dst_ref=dst,
                send_sem=halo_send.at[len(halo)],
                recv_sem=halo_recv.at[len(halo)],
                device_id={"model": (m + d) % 8, "cols": q},
                device_id_type=MESH,
            )
        )
        halo[-1].start()

    def conv1(halves, places, spans, groups):
        width = 10 // groups
        tops = [None] * groups
        for p in parts:
            at = [plane(p, d) for d in places]
            lanes = [pl.ds(pl.multiple_of(LANES * v, LANES), LANES) for v in at]
            for dw in range(3):
                right = [[w1g[p, n, v, :, :, :, dw, i].reshape(LANES, LANES) for n in halves for i in range(2)] for v in at]
                right = jnp.concatenate([jnp.concatenate(r, axis=1) for r in right], axis=0)
                for group in range(groups):
                    cols = pl.ds(dw + width * group, width)
                    left = [jnp.concatenate([xs[p][cols, rows, s] for s in lanes], axis=-1) for rows in spans]
                    left = jnp.concatenate(left, axis=1).reshape(-1, 256)
                    term = jnp.dot(left, right, preferred_element_type=F32)
                    tops[group] = term if tops[group] is None else tops[group] + term
        return [top.reshape(width, -1, 256 * len(halves)) for top in tops]

    top_rows, inner, low_rows = pl.ds(0, 8), pl.ds(8, 56), pl.ds(64, 8)

    def near(n):
        with jax.named_scope(f"wait_lent{n}"):
            lent[n].land()
        with jax.named_scope(f"near{n}"):
            for group, top in enumerate(conv1((n,), (3, 1), (inner,), 2)):
                z_acc[n, pl.ds(5 * group, 5), inner] = top

    def rim():
        with jax.named_scope("rim"):
            (top,) = conv1((0, 1), (3, 1), (top_rows, low_rows), 1)
            for n in range(2):
                part = top[:, :, 256 * n : 256 * n + 256]
                z_acc[n, :, top_rows] = part[:, :8]
                z_acc[n, :, low_rows] = part[:, 8:]

    def far(n):
        with jax.named_scope(f"wait_lent_on{n}"):
            lent_on[n].land()
        lanes = slice(256 * n, 256 * n + 256)
        with jax.named_scope(f"far{n}"):
            for group, top in enumerate(conv1((n,), (0, 2), (pl.ds(0, 72),), 2)):
                cols = pl.ds(5 * group, 5)
                act = jnp.maximum(z_acc[n, cols] + top + b1v[:, lanes], 0.0)
                for dh in range(3):
                    ys[dh][cols, :, lanes] = act[:, 4 * dh : 4 * dh + 64].astype(BF16)

        def clear(at_edge, refs, cols, rows):
            @pl.when(at_edge)
            def _():
                for ref in refs:
                    ref[cols, rows, lanes] = jnp.zeros((cols.size, rows.size, 256), BF16)

        clear(q == 0, ys, pl.ds(0, 1), pl.ds(0, 64))
        clear(q == 15, ys, pl.ds(9, 1), pl.ds(0, 64))
        clear(m == 0, (y0,), pl.ds(0, 10), pl.ds(0, 4))
        clear(m == 7, (y2,), pl.ds(0, 10), pl.ds(60, 4))

    def conv2(n):
        lanes = slice(256 * n, 256 * n + 256)
        total = None
        for dh in range(3):
            for dw in range(3):
                tap = 3 * dh + dw
                left = ys[dh][dw : dw + 8, :, lanes].reshape(CHANS, 256)
                right = w2v[CHANS * tap + 256 * n : CHANS * tap + 256 * n + 256, :]
                term = jnp.dot(left, right, preferred_element_type=F32)
                total = term if total is None else total + term
        return total

    @pl.when(core == 1)
    def _():
        last[1].go()

    pass_on(0)
    pass_on(1)
    near(0)
    near(1)
    finish(0)
    with jax.named_scope("wait_halo"):
        for copy in halo:
            copy.wait_recv()

    @pl.when(m == 0)
    def _():
        x0[:, 0:8] = jnp.zeros((12, 8, CHANS), BF16)
        x1[:, 0:4] = jnp.zeros((12, 4, CHANS), BF16)

    @pl.when(m > 0)
    def _():
        x1[:, 0:4] = edge[2]

    @pl.when(m == 7)
    def _():
        x2[:, 64:72] = jnp.zeros((12, 8, CHANS), BF16)
        x1[:, 68:72] = jnp.zeros((12, 4, CHANS), BF16)

    @pl.when(m < 7)
    def _():
        x1[:, 68:72] = edge[3]

    rim()
    finish(1)
    with jax.named_scope("wait_own_w2"):
        own.land()
        for load in loads[2:]:
            load.wait()
    far(0)
    with jax.named_scope("conv2_0"):
        acc2[...] = conv2(0)
    far(1)
    with jax.named_scope("conv2_1"):
        o_ref[...] = acc2[...] + conv2(1) + b2v[...]

    with jax.named_scope("wait_sends"):
        everything.wait_send()
        for step in steps:
            step.all.wait_send()
        for copy in halo:
            copy.wait_send()


def arrange(sum_ref, o_hbm, turned, sems):
    copies = []
    for g in range(4):
        rows = jnp.transpose(sum_ref[:, 16 * g : 16 * g + 16], (1, 0, 2))
        for h in range(4):
            for image in range(4):
                turned[g, image, h] = rows[4 * h + image]
        copies.append(pltpu.make_async_copy(turned.at[g], o_hbm.at[:, pl.ds(4 * g, 4)], sems.at[g]))
        copies[-1].start()
    for copy in copies:
        copy.wait()


def solution(mesh):
    scratch = [
        pltpu.VMEM((4, LANES, 4, LANES), BF16),
        pltpu.VMEM((9, 4, CHANS), BF16),
        pltpu.VMEM((4616, CHANS), BF16),
        pltpu.VMEM((1, CHANS), F32),
        pltpu.VMEM((1, CHANS), F32),
        pltpu.VMEM((CHANS, CHANS), BF16),
        pltpu.VMEM((8, 66, 4, LANES), BF16),
        pltpu.VMEM((LANES, 6, 4, LANES), BF16),
        *[pltpu.VMEM((12, 72, CHANS), BF16) for _ in range(3)],
        pltpu.VMEM((4, 12, 4, CHANS), BF16),
        pltpu.VMEM((3, 2, 4, 2, 4, 4, 3, 2, 4, LANES), BF16),
        pltpu.VMEM((2, 10, 72, 256), F32),
        *[pltpu.VMEM((10, 64, CHANS), BF16) for _ in range(3)],
        pltpu.VMEM((CHANS, CHANS), F32),
        pltpu.SemaphoreType.DMA((5,)),
        pltpu.SemaphoreType.DMA,
        pltpu.SemaphoreType.DMA,
        pltpu.SemaphoreType.DMA((4,)),
        pltpu.SemaphoreType.DMA((4,)),
        pltpu.SemaphoreType.DMA((11,)),
        pltpu.SemaphoreType.DMA((11,)),
    ]
    vmem = pl.BlockSpec(memory_space=pltpu.VMEM)
    anywhere = pl.BlockSpec(memory_space=pl.ANY)

    def run_local(x_in, w_conv1, b_conv1, w_conv2, b_conv2):
        sums = pl.pallas_call(
            kernel,
            out_shape=jax.ShapeDtypeStruct((CHANS, CHANS), F32),
            in_specs=[anywhere] * 5,
            out_specs=vmem,
            scratch_shapes=scratch,
            compiler_params=pltpu.CompilerParams(collective_id=0, has_side_effects=True, vmem_limit_bytes=VMEM_LIMIT),
            name="two_convs",
        )(
            *(
                pltpu.with_memory_space_constraint(a, pltpu.HBM)
                for a in (
                    x_in.transpose(0, 1, 3, 2),
                    w_conv1.reshape(9, 4, CHANS),
                    w_conv2.reshape(4608, CHANS),
                    b_conv1.reshape(1, CHANS),
                    b_conv2.reshape(1, CHANS),
                )
            )
        )
        return pl.pallas_call(
            arrange,
            out_shape=jax.ShapeDtypeStruct((4, 16, 8, CHANS), F32),
            in_specs=[vmem],
            out_specs=anywhere,
            scratch_shapes=[pltpu.VMEM((4, 4, 4, 8, CHANS), F32), pltpu.SemaphoreType.DMA((4,))],
            compiler_params=pltpu.CompilerParams(vmem_limit_bytes=8 * 2**20),
            name="arrange",
        )(sums.reshape(8, 64, CHANS))

    return jax.shard_map(
        run_local,
        mesh=mesh,
        in_specs=(P("data", None, None, GROUP_AXES), P(None, None, GROUP_AXES, None), P(), P(), P()),
        out_specs=P("data", "model", "cols", None),
        check_vma=False,
    )
```

```python
import jax
import jax.numpy as jnp
from jax import lax
from jax.experimental import pallas as pl
from jax.experimental.pallas import tpu as pltpu
from jax.sharding import PartitionSpec as P

GROUP_AXES = ("model", "cols")
MESH = pl.DeviceIdType.MESH
BF16 = jnp.bfloat16
F32 = jnp.float32
CHANS = 512
LANES = 128
CUT = 96
VMEM_LIMIT = 36 * 2**20
ORDERS = (("y", "z", "x"), ("z", "x", "y"), ("x", "y", "z"))


def one_hot(shape, col_of_row):
    rows = lax.broadcasted_iota(jnp.int32, shape, 0)
    cols = lax.broadcasted_iota(jnp.int32, shape, 1)
    return jnp.where(cols == col_of_row(rows), 1.0, 0.0).astype(BF16)


def pack_windows(xv, a_scr, pack):
    to_lanes = one_hot((CHANS, CHANS), lambda r: (r % 4) * LANES + ((r % LANES) // 4) * 4 + r // LANES)
    to_rows = one_hot((CHANS, CHANS), lambda r: (r % 4) * LANES + ((r % 256) // 4) * 2 + r // 256)
    for blk in range(4):
        part = jnp.concatenate([xv[n, 32 * blk : 32 * blk + 32].reshape(LANES, LANES) for n in range(4)], axis=0)
        turned = lax.dot_general(part, to_lanes, (((0,), (0,)), ((), ())), preferred_element_type=F32).astype(BF16)
        for c in range(4):
            a_scr[c * LANES : (c + 1) * LANES, blk * LANES : (blk + 1) * LANES] = turned[:, c * LANES : (c + 1) * LANES]
    mixed = jnp.dot(to_rows, a_scr[...], preferred_element_type=F32)
    for blk in range(4):
        even = mixed[0:256, blk * LANES : (blk + 1) * LANES]
        odd = mixed[256:CHANS, blk * LANES : (blk + 1) * LANES]
        for half in range(2):
            s = slice(64 * half, 64 * half + 64)
            tile = jnp.concatenate([even[:, s], odd[:, s]], axis=1).astype(BF16)
            pack[2 * blk + half, 1:65] = tile.reshape(64, 4, LANES)
    edge = jnp.zeros((8, 1, 4, LANES), BF16)
    pack[:, 0:1] = edge
    pack[:, 65:66] = edge


def kernel(
    x_hbm, w1_hbm, w2_hbm, b1_hbm, b2_hbm, o_ref,
    xv, w1v, w2v, b1v, b2v, a_scr, pack, got, x0, x1, x2, edge, w1g, z_acc, y0, y1, y2, acc2,
    load_sem, xs_send, xs_recv, halo_send, halo_recv, step_send, step_recv,
):
    m = lax.axis_index("model")
    q = lax.axis_index("cols")
    me = {"x": m // 2, "z": q // 4, "y": q % 4}
    core = m % 2
    parts = range(3)
    barrier = pltpu.get_barrier_semaphore()

    at_model = [[(me["x"] + dx) % 4 * 2 + (core + dk) % 2 for dk in range(2)] for dx in range(4)]
    at_cols = [[(me["z"] + dz) % 4 * 4 + (me["y"] + dy) % 4 for dy in range(4)] for dz in range(4)]
    others = [(dx, dz, dy, dk) for dx in range(4) for dz in range(4) for dy in range(4) for dk in range(2)]
    others = sorted(others[1:], key=lambda d: (sum(d[:3]) % 4, d))

    def away(d):
        return {"model": at_model[d[0]][d[3]], "cols": at_cols[d[1]][d[2]]}

    loads = [
        pltpu.make_async_copy(src, dst, load_sem.at[k])
        for k, (src, dst) in enumerate(
            ((x_hbm, xv), (w1_hbm, w1v), (w2_hbm, w2v.at[pl.ds(0, 4608)]), (b1_hbm, b1v), (b2_hbm, b2v))
        )
    ]
    for load in loads:
        load.start()
    with jax.named_scope("announce"):
        for d in sorted(others, key=lambda d: -sum(min(o, 4 - o) for o in d[:3])):
            pl.semaphore_signal(barrier, inc=1, device_id=away(d), device_id_type=MESH)

    def piece(p, t, v, n, c, place=None, half=None):
        done = ORDERS[p][:t]
        rest = [a for a in "xzy" if a != ORDERS[p][2]]
        at = [v if t < 2 and a == ORDERS[p][t] else (pl.ds(0, 4) if a in done else me[a]) for a in rest]
        if half is not None:
            at[0] = pl.ds(2 * half, 2)
        return w1g.at[p, pl.ds(0, 2) if n is None else n, me[ORDERS[p][2]] if t < 2 else v, c, at[0], at[1]]

    with jax.named_scope("place_w1"):
        loads[1].wait()
        for p in parts:
            spot = [me[a] for a in "xzy" if a != ORDERS[p][2]]
            for dw in range(3):
                for lt in range(4):
                    tile = w1v[3 * p + dw, :, lt * LANES : (lt + 1) * LANES]
                    w1g[p, lt // 2, me[ORDERS[p][2]], core, spot[0], spot[1], dw, lt % 2] = tile
    with jax.named_scope("wait_x"):
        loads[0].wait()
    with jax.named_scope("pack"):
        pack_windows(xv, a_scr, pack)
    with jax.named_scope("wait_barrier"):
        pl.semaphore_wait(barrier, 127)

    n_steps = [0]
    steps = []

    class Step:
        def __init__(self, slabs, copies):
            k = n_steps[0]
            n_steps[0] += 1
            sems = dict(send_sem=step_send.at[k], recv_sem=step_recv.at[k], device_id_type=MESH)
            self.copies, self.sems = copies, sems
            span = got.at[pl.ds(0, slabs)]
            self.all = pltpu.make_async_remote_copy(
                src_ref=span, dst_ref=span, device_id={"model": at_model[0][1], "cols": q}, **sems
            )
            steps.append(self)

        def go(self):
            for ref, to in self.copies:
                pltpu.make_async_remote_copy(src_ref=ref, dst_ref=ref, device_id=to, **self.sems).start()
            return self

        def land(self):
            self.all.wait_recv()

    def chip(p, t, d, c=0):
        axis = ORDERS[p][t]
        pos = me | {axis: (me[axis] + d) % 4}
        return {"model": pos["x"] * 2 + (core + c) % 2, "cols": pos["z"] * 4 + pos["y"]}

    def spread(t, slabs):
        return Step(slabs, [(piece(p, t, me[ORDERS[p][t]], None, core), chip(p, t, d)) for p in parts for d in (1, 3, 2)]).go()

    def plane(p, d):
        return (me[ORDERS[p][2]] + d) % 4

    def hand_over(pieces, slabs):
        return Step(slabs, [(ref, {"model": at_model[0][1], "cols": q}) for ref in pieces]).go()

    def send_windows(first, last):
        for d in others[first:last]:
            to = away(d)
            pltpu.make_async_remote_copy(
                src_ref=pack.at[to["model"], pl.ds(4 * to["cols"], 6)],
                dst_ref=got.at[mine],
                send_sem=xs_send,
                recv_sem=xs_recv,
                device_id=to,
                device_id_type=MESH,
            ).start()

    mine = ((core * 4 + me["x"]) * 4 + me["z"]) * 4 + me["y"]
    with jax.named_scope("send_first"):
        first = spread(0, 18)
        for pair in range(6):
            got[mine, pair] = pack[m, 4 * q + pair]
        send_windows(0, CUT)
    with jax.named_scope("wait_first"):
        first.land()
    with jax.named_scope("send_second"):
        second = spread(1, 72)
        send_windows(CUT, 127)
    with jax.named_scope("wait_second"):
        second.land()
    last, passed, lent, lent_on = {}, {}, {}, {}

    def send_plane(n):
        last[n] = Step(96, [(piece(p, 2, plane(p, 0), n, core), chip(p, 2, d)) for p in parts for d in (1, 3)])

    def pass_on(n):
        with jax.named_scope(f"wait_last{n}"):
            last[n].land()
        passed[n] = Step(48, [(piece(p, 2, plane(p, 4 - d), n, core, half=d // 2), chip(p, 2, d)) for p in parts for d in (1, 3)]).go()
        lent[n] = hand_over([piece(p, 2, plane(p, d), n, core) for p in parts for d in (1, 3)], 96)

    def finish(n):
        with jax.named_scope(f"wait_passed{n}"):
            passed[n].land()
        lent_on[n] = hand_over([piece(p, 2, plane(p, 2), n, core) for p in parts], 48)

    with jax.named_scope("send_third"):
        for n in range(2):
            send_plane(n)
        last[0].go()
        own = hand_over([piece(p, 2, plane(p, 0), None, core) for p in parts], 96)
    @pl.when(core == 0)
    def _():
        last[1].go()

    span = got.at[pl.ds(0, 127)]
    everything = pltpu.make_async_remote_copy(
        src_ref=span, dst_ref=span, send_sem=xs_send, recv_sem=xs_recv, device_id=chip(0, 0, 0, 1), device_id_type=MESH
    )
    with jax.named_scope("wait_windows"):
        everything.wait_recv()

    @pl.when(core == 1)
    def _():
        last[1].go()

    xs, ys = (x0, x1, x2), (y0, y1, y2)
    with jax.named_scope("turn"):
        for pair in range(6):
            for p in parts:
                rows = []
                for v in range(4):
                    for c in range(2):
                        at = 64 * c
                        if p == 0:
                            rows.append(got[at + 16 * v : at + 16 * v + 16, pair])
                        elif p == 1:
                            rows.append(got[at + v : at + 64 : 4, pair])
                        else:
                            rows += [got[at + 16 * a + 4 * v : at + 16 * a + 4 * v + 4, pair] for a in range(4)]
                rows = jnp.concatenate([r.reshape(-1, LANES) for r in rows], axis=0).T
                for odd in range(2):
                    main = rows[64 * odd : 64 * odd + 64]
                    xs[p][2 * pair + odd, 8 - 4 * p : 72 - 4 * p] = main
                    if p == 1:
                        edge[0, 2 * pair + odd] = main[60:64]
                        edge[1, 2 * pair + odd] = main[0:4]
    halo = []
    for src, dst, d in (
        (x0.at[:, pl.ds(64, 8)], x0.at[:, pl.ds(0, 8)], 1),
        (x2.at[:, pl.ds(0, 8)], x2.at[:, pl.ds(64, 8)], 7),
        (edge.at[0], edge.at[2], 1),
        (edge.at[1], edge.at[3], 7),
    ):
        halo.append(
            pltpu.make_async_remote_copy(
                src_ref=src,
                dst_ref=dst,
                send_sem=halo_send.at[len(halo)],
                recv_sem=halo_recv.at[len(halo)],
                device_id={"model": (m + d) % 8, "cols": q},
                device_id_type=MESH,
            )
        )
        halo[-1].start()

    def conv1(halves, places, spans, groups):
        width = 10 // groups
        tops = [None] * groups
        for p in parts:
            at = [plane(p, d) for d in places]
            lanes = [pl.ds(pl.multiple_of(LANES * v, LANES), LANES) for v in at]
            for dw in range(3):
                right = [[w1g[p, n, v, :, :, :, dw, i].reshape(LANES, LANES) for n in halves for i in range(2)] for v in at]
                right = jnp.concatenate([jnp.concatenate(r, axis=1) for r in right], axis=0)
                for group in range(groups):
                    cols = pl.ds(dw + width * group, width)
                    left = [jnp.concatenate([xs[p][cols, rows, s] for s in lanes], axis=-1) for rows in spans]
                    left = jnp.concatenate(left, axis=1).reshape(-1, 256)
                    term = jnp.dot(left, right, preferred_element_type=F32)
                    tops[group] = term if tops[group] is None else tops[group] + term
        return [top.reshape(width, -1, 256 * len(halves)) for top in tops]

    top_rows, inner, low_rows = pl.ds(0, 8), pl.ds(8, 56), pl.ds(64, 8)

    def near(n):
        with jax.named_scope(f"wait_lent{n}"):
            lent[n].land()
        with jax.named_scope(f"near{n}"):
            for group, top in enumerate(conv1((n,), (3, 1), (inner,), 2)):
                z_acc[n, pl.ds(5 * group, 5), inner] = top

    def rim():
        with jax.named_scope("rim"):
            (top,) = conv1((0, 1), (3, 1), (top_rows, low_rows), 1)
            for n in range(2):
                part = top[:, :, 256 * n : 256 * n + 256]
                z_acc[n, :, top_rows] = part[:, :8]
                z_acc[n, :, low_rows] = part[:, 8:]

    def far(n):
        with jax.named_scope(f"wait_lent_on{n}"):
            lent_on[n].land()
        lanes = slice(256 * n, 256 * n + 256)
        with jax.named_scope(f"far{n}"):
            for group, top in enumerate(conv1((n,), (0, 2), (pl.ds(0, 72),), 2)):
                cols = pl.ds(5 * group, 5)
                act = jnp.maximum(z_acc[n, cols] + top + b1v[:, lanes], 0.0)
                for dh in range(3):
                    ys[dh][cols, :, lanes] = act[:, 4 * dh : 4 * dh + 64].astype(BF16)

        def clear(at_edge, refs, cols, rows):
            @pl.when(at_edge)
            def _():
                for ref in refs:
                    ref[cols, rows, lanes] = jnp.zeros((cols.size, rows.size, 256), BF16)

        clear(q == 0, ys, pl.ds(0, 1), pl.ds(0, 64))
        clear(q == 15, ys, pl.ds(9, 1), pl.ds(0, 64))
        clear(m == 0, (y0,), pl.ds(0, 10), pl.ds(0, 4))
        clear(m == 7, (y2,), pl.ds(0, 10), pl.ds(60, 4))

    def conv2(n):
        lanes = slice(256 * n, 256 * n + 256)
        total = None
        for dh in range(3):
            for dw in range(3):
                tap = 3 * dh + dw
                left = ys[dh][dw : dw + 8, :, lanes].reshape(CHANS, 256)
                right = w2v[CHANS * tap + 256 * n : CHANS * tap + 256 * n + 256, :]
                term = jnp.dot(left, right, preferred_element_type=F32)
                total = term if total is None else total + term
        return total

    pass_on(0)
    near(0)
    pass_on(1)
    near(1)
    finish(0)
    with jax.named_scope("wait_halo"):
        for copy in halo:
            copy.wait_recv()

    @pl.when(m == 0)
    def _():
        x0[:, 0:8] = jnp.zeros((12, 8, CHANS), BF16)
        x1[:, 0:4] = jnp.zeros((12, 4, CHANS), BF16)

    @pl.when(m > 0)
    def _():
        x1[:, 0:4] = edge[2]

    @pl.when(m == 7)
    def _():
        x2[:, 64:72] = jnp.zeros((12, 8, CHANS), BF16)
        x1[:, 68:72] = jnp.zeros((12, 4, CHANS), BF16)

    @pl.when(m < 7)
    def _():
        x1[:, 68:72] = edge[3]

    rim()
    finish(1)
    with jax.named_scope("wait_own_w2"):
        own.land()
        for load in loads[2:]:
            load.wait()
    far(0)
    with jax.named_scope("conv2_0"):
        acc2[...] = conv2(0)
    far(1)
    with jax.named_scope("conv2_1"):
        o_ref[...] = acc2[...] + conv2(1) + b2v[...]

    with jax.named_scope("wait_sends"):
        everything.wait_send()
        for step in steps:
            step.all.wait_send()
        for copy in halo:
            copy.wait_send()


def arrange(sum_ref, o_hbm, turned, sems):
    copies = []
    for g in range(4):
        rows = jnp.transpose(sum_ref[:, 16 * g : 16 * g + 16], (1, 0, 2))
        for h in range(4):
            for image in range(4):
                turned[g, image, h] = rows[4 * h + image]
        copies.append(pltpu.make_async_copy(turned.at[g], o_hbm.at[:, pl.ds(4 * g, 4)], sems.at[g]))
        copies[-1].start()
    for copy in copies:
        copy.wait()


def solution(mesh):
    scratch = [
        pltpu.VMEM((4, LANES, 4, LANES), BF16),
        pltpu.VMEM((9, 4, CHANS), BF16),
        pltpu.VMEM((4616, CHANS), BF16),
        pltpu.VMEM((1, CHANS), F32),
        pltpu.VMEM((1, CHANS), F32),
        pltpu.VMEM((CHANS, CHANS), BF16),
        pltpu.VMEM((8, 66, 4, LANES), BF16),
        pltpu.VMEM((LANES, 6, 4, LANES), BF16),
        *[pltpu.VMEM((12, 72, CHANS), BF16) for _ in range(3)],
        pltpu.VMEM((4, 12, 4, CHANS), BF16),
        pltpu.VMEM((3, 2, 4, 2, 4, 4, 3, 2, 4, LANES), BF16),
        pltpu.VMEM((2, 10, 72, 256), F32),
        *[pltpu.VMEM((10, 64, CHANS), BF16) for _ in range(3)],
        pltpu.VMEM((CHANS, CHANS), F32),
        pltpu.SemaphoreType.DMA((5,)),
        pltpu.SemaphoreType.DMA,
        pltpu.SemaphoreType.DMA,
        pltpu.SemaphoreType.DMA((4,)),
        pltpu.SemaphoreType.DMA((4,)),
        pltpu.SemaphoreType.DMA((11,)),
        pltpu.SemaphoreType.DMA((11,)),
    ]
    vmem = pl.BlockSpec(memory_space=pltpu.VMEM)
    anywhere = pl.BlockSpec(memory_space=pl.ANY)

    def run_local(x_in, w_conv1, b_conv1, w_conv2, b_conv2):
        sums = pl.pallas_call(
            kernel,
            out_shape=jax.ShapeDtypeStruct((CHANS, CHANS), F32),
            in_specs=[anywhere] * 5,
            out_specs=vmem,
            scratch_shapes=scratch,
            compiler_params=pltpu.CompilerParams(collective_id=0, has_side_effects=True, vmem_limit_bytes=VMEM_LIMIT),
            name="two_convs",
        )(
            *(
                pltpu.with_memory_space_constraint(a, pltpu.HBM)
                for a in (
                    x_in.transpose(0, 1, 3, 2),
                    w_conv1.reshape(9, 4, CHANS),
                    w_conv2.reshape(4608, CHANS),
                    b_conv1.reshape(1, CHANS),
                    b_conv2.reshape(1, CHANS),
                )
            )
        )
        return pl.pallas_call(
            arrange,
            out_shape=jax.ShapeDtypeStruct((4, 16, 8, CHANS), F32),
            in_specs=[vmem],
            out_specs=anywhere,
            scratch_shapes=[pltpu.VMEM((4, 4, 4, 8, CHANS), F32), pltpu.SemaphoreType.DMA((4,))],
            compiler_params=pltpu.CompilerParams(vmem_limit_bytes=8 * 2**20),
            name="arrange",
        )(sums.reshape(8, 64, CHANS))

    return jax.shard_map(
        run_local,
        mesh=mesh,
        in_specs=(P("data", None, None, GROUP_AXES), P(None, None, GROUP_AXES, None), P(), P(), P()),
        out_specs=P("data", "model", "cols", None),
        check_vma=False,
    )
```

```python
import jax
import jax.numpy as jnp
from jax import lax
from jax.experimental import pallas as pl
from jax.experimental.pallas import tpu as pltpu
from jax.sharding import PartitionSpec as P

GROUP_AXES = ("model", "cols")
MESH = pl.DeviceIdType.MESH
BF16 = jnp.bfloat16
F32 = jnp.float32
CHANS = 512
LANES = 128
CUT = 96
VMEM_LIMIT = 36 * 2**20
ORDERS = (("y", "z", "x"), ("z", "x", "y"), ("x", "y", "z"))


def one_hot(shape, col_of_row):
    rows = lax.broadcasted_iota(jnp.int32, shape, 0)
    cols = lax.broadcasted_iota(jnp.int32, shape, 1)
    return jnp.where(cols == col_of_row(rows), 1.0, 0.0).astype(BF16)


def pack_windows(xv, a_scr, pack):
    to_lanes = one_hot((CHANS, CHANS), lambda r: (r % 4) * LANES + ((r % LANES) // 4) * 4 + r // LANES)
    to_rows = one_hot((CHANS, CHANS), lambda r: (r % 4) * LANES + ((r % 256) // 4) * 2 + r // 256)
    for blk in range(4):
        part = jnp.concatenate([xv[n, 32 * blk : 32 * blk + 32].reshape(LANES, LANES) for n in range(4)], axis=0)
        turned = lax.dot_general(part, to_lanes, (((0,), (0,)), ((), ())), preferred_element_type=F32).astype(BF16)
        for c in range(4):
            a_scr[c * LANES : (c + 1) * LANES, blk * LANES : (blk + 1) * LANES] = turned[:, c * LANES : (c + 1) * LANES]
    mixed = jnp.dot(to_rows, a_scr[...], preferred_element_type=F32)
    for blk in range(4):
        even = mixed[0:256, blk * LANES : (blk + 1) * LANES]
        odd = mixed[256:CHANS, blk * LANES : (blk + 1) * LANES]
        for half in range(2):
            s = slice(64 * half, 64 * half + 64)
            tile = jnp.concatenate([even[:, s], odd[:, s]], axis=1).astype(BF16)
            pack[2 * blk + half, 1:65] = tile.reshape(64, 4, LANES)
    edge = jnp.zeros((8, 1, 4, LANES), BF16)
    pack[:, 0:1] = edge
    pack[:, 65:66] = edge


def kernel(
    x_hbm, w1_hbm, w2_hbm, b1_hbm, b2_hbm, o_ref,
    xv, w1v, w2v, b1v, b2v, a_scr, pack, got, x0, x1, x2, edge, w1g, z_acc, y0, y1, y2, acc2,
    load_sem, xs_send, xs_recv, halo_send, halo_recv, step_send, step_recv,
):
    m = lax.axis_index("model")
    q = lax.axis_index("cols")
    me = {"x": m // 2, "z": q // 4, "y": q % 4}
    core = m % 2
    parts = range(3)
    barrier = pltpu.get_barrier_semaphore()

    at_model = [[(me["x"] + dx) % 4 * 2 + (core + dk) % 2 for dk in range(2)] for dx in range(4)]
    at_cols = [[(me["z"] + dz) % 4 * 4 + (me["y"] + dy) % 4 for dy in range(4)] for dz in range(4)]
    others = [(dx, dz, dy, dk) for dx in range(4) for dz in range(4) for dy in range(4) for dk in range(2)]
    others = sorted(others[1:], key=lambda d: (sum(d[:3]) % 4, d))

    def away(d):
        return {"model": at_model[d[0]][d[3]], "cols": at_cols[d[1]][d[2]]}

    loads = [
        pltpu.make_async_copy(src, dst, load_sem.at[k])
        for k, (src, dst) in enumerate(
            ((x_hbm, xv), (w1_hbm, w1v), (w2_hbm, w2v.at[pl.ds(0, 4608)]), (b1_hbm, b1v), (b2_hbm, b2v))
        )
    ]
    for load in loads:
        load.start()
    with jax.named_scope("announce"):
        for d in sorted(others, key=lambda d: -sum(min(o, 4 - o) for o in d[:3])):
            pl.semaphore_signal(barrier, inc=1, device_id=away(d), device_id_type=MESH)

    def piece(p, t, v, n, c, place=None, half=None):
        done = ORDERS[p][:t]
        rest = [a for a in "xzy" if a != ORDERS[p][2]]
        at = [v if t < 2 and a == ORDERS[p][t] else (pl.ds(0, 4) if a in done else me[a]) for a in rest]
        if half is not None:
            at[0] = pl.ds(2 * half, 2)
        return w1g.at[p, pl.ds(0, 2) if n is None else n, me[ORDERS[p][2]] if t < 2 else v, c, at[0], at[1]]

    with jax.named_scope("place_w1"):
        loads[1].wait()
        for p in parts:
            spot = [me[a] for a in "xzy" if a != ORDERS[p][2]]
            for dw in range(3):
                for lt in range(4):
                    tile = w1v[3 * p + dw, :, lt * LANES : (lt + 1) * LANES]
                    w1g[p, lt // 2, me[ORDERS[p][2]], core, spot[0], spot[1], dw, lt % 2] = tile
    with jax.named_scope("wait_x"):
        loads[0].wait()
    with jax.named_scope("pack"):
        pack_windows(xv, a_scr, pack)
    with jax.named_scope("wait_barrier"):
        pl.semaphore_wait(barrier, 127)

    n_steps = [0]
    steps = []

    class Step:
        def __init__(self, slabs, copies):
            k = n_steps[0]
            n_steps[0] += 1
            sems = dict(send_sem=step_send.at[k], recv_sem=step_recv.at[k], device_id_type=MESH)
            self.copies, self.sems = copies, sems
            span = got.at[pl.ds(0, slabs)]
            self.all = pltpu.make_async_remote_copy(
                src_ref=span, dst_ref=span, device_id={"model": at_model[0][1], "cols": q}, **sems
            )
            steps.append(self)

        def go(self):
            for ref, to in self.copies:
                pltpu.make_async_remote_copy(src_ref=ref, dst_ref=ref, device_id=to, **self.sems).start()
            return self

        def land(self):
            self.all.wait_recv()

    def chip(p, t, d, c=0):
        axis = ORDERS[p][t]
        pos = me | {axis: (me[axis] + d) % 4}
        return {"model": pos["x"] * 2 + (core + c) % 2, "cols": pos["z"] * 4 + pos["y"]}

    def spread(t, slabs):
        return Step(slabs, [(piece(p, t, me[ORDERS[p][t]], None, core), chip(p, t, d)) for p in parts for d in (1, 3, 2)]).go()

    def plane(p, d):
        return (me[ORDERS[p][2]] + d) % 4

    def hand_over(pieces, slabs):
        return Step(slabs, [(ref, {"model": at_model[0][1], "cols": q}) for ref in pieces]).go()

    def send_windows(first, last):
        for d in others[first:last]:
            to = away(d)
            pltpu.make_async_remote_copy(
                src_ref=pack.at[to["model"], pl.ds(4 * to["cols"], 6)],
                dst_ref=got.at[mine],
                send_sem=xs_send,
                recv_sem=xs_recv,
                device_id=to,
                device_id_type=MESH,
            ).start()

    mine = ((core * 4 + me["x"]) * 4 + me["z"]) * 4 + me["y"]
    with jax.named_scope("send_first"):
        first = spread(0, 18)
        for pair in range(6):
            got[mine, pair] = pack[m, 4 * q + pair]
        send_windows(0, CUT)
    with jax.named_scope("wait_first"):
        first.land()
    with jax.named_scope("send_second"):
        second = spread(1, 72)
        send_windows(CUT, 127)
    with jax.named_scope("wait_second"):
        second.land()
    last, passed, lent, lent_on = {}, {}, {}, {}

    def send_plane(n):
        last[n] = Step(96, [(piece(p, 2, plane(p, 0), n, core), chip(p, 2, d)) for p in parts for d in (1, 3)])

    def pass_on(n):
        with jax.named_scope(f"wait_last{n}"):
            last[n].land()
        passed[n] = Step(48, [(piece(p, 2, plane(p, 4 - d), n, core, half=d // 2), chip(p, 2, d)) for p in parts for d in (1, 3)]).go()
        lent[n] = hand_over([piece(p, 2, plane(p, d), n, core) for p in parts for d in (1, 3)], 96)

    def finish(n):
        with jax.named_scope(f"wait_passed{n}"):
            passed[n].land()
        lent_on[n] = hand_over([piece(p, 2, plane(p, 2), n, core) for p in parts], 48)

    with jax.named_scope("send_third"):
        for n in range(2):
            send_plane(n)
        last[0].go()
        own = hand_over([piece(p, 2, plane(p, 0), None, core) for p in parts], 96)
    last[1].go()
    span = got.at[pl.ds(0, 127)]
    everything = pltpu.make_async_remote_copy(
        src_ref=span, dst_ref=span, send_sem=xs_send, recv_sem=xs_recv, device_id=chip(0, 0, 0, 1), device_id_type=MESH
    )
    with jax.named_scope("wait_windows"):
        everything.wait_recv()

    xs, ys = (x0, x1, x2), (y0, y1, y2)
    with jax.named_scope("turn"):
        for pair in range(6):
            for p in parts:
                rows = []
                for v in range(4):
                    for c in range(2):
                        at = 64 * c
                        if p == 0:
                            rows.append(got[at + 16 * v : at + 16 * v + 16, pair])
                        elif p == 1:
                            rows.append(got[at + v : at + 64 : 4, pair])
                        else:
                            rows += [got[at + 16 * a + 4 * v : at + 16 * a + 4 * v + 4, pair] for a in range(4)]
                rows = jnp.concatenate([r.reshape(-1, LANES) for r in rows], axis=0).T
                for odd in range(2):
                    main = rows[64 * odd : 64 * odd + 64]
                    xs[p][2 * pair + odd, 8 - 4 * p : 72 - 4 * p] = main
                    if p == 1:
                        edge[0, 2 * pair + odd] = main[60:64]
                        edge[1, 2 * pair + odd] = main[0:4]
    halo = []
    for src, dst, d in (
        (x0.at[:, pl.ds(64, 8)], x0.at[:, pl.ds(0, 8)], 1),
        (x2.at[:, pl.ds(0, 8)], x2.at[:, pl.ds(64, 8)], 7),
        (edge.at[0], edge.at[2], 1),
        (edge.at[1], edge.at[3], 7),
    ):
        halo.append(
            pltpu.make_async_remote_copy(
                src_ref=src,
                dst_ref=dst,
                send_sem=halo_send.at[len(halo)],
                recv_sem=halo_recv.at[len(halo)],
                device_id={"model": (m + d) % 8, "cols": q},
                device_id_type=MESH,
            )
        )
        halo[-1].start()

    def conv1(halves, places, spans, groups):
        width = 10 // groups
        tops = [None] * groups
        for p in parts:
            at = [plane(p, d) for d in places]
            lanes = [pl.ds(pl.multiple_of(LANES * v, LANES), LANES) for v in at]
            for dw in range(3):
                right = [[w1g[p, n, v, :, :, :, dw, i].reshape(LANES, LANES) for n in halves for i in range(2)] for v in at]
                right = jnp.concatenate([jnp.concatenate(r, axis=1) for r in right], axis=0)
                for group in range(groups):
                    cols = pl.ds(dw + width * group, width)
                    left = [jnp.concatenate([xs[p][cols, rows, s] for s in lanes], axis=-1) for rows in spans]
                    left = jnp.concatenate(left, axis=1).reshape(-1, 256)
                    term = jnp.dot(left, right, preferred_element_type=F32)
                    tops[group] = term if tops[group] is None else tops[group] + term
        return [top.reshape(width, -1, 256 * len(halves)) for top in tops]

    top_rows, inner, low_rows = pl.ds(0, 8), pl.ds(8, 56), pl.ds(64, 8)

    def near(n):
        with jax.named_scope(f"wait_lent{n}"):
            lent[n].land()
        with jax.named_scope(f"near{n}"):
            for group, top in enumerate(conv1((n,), (3, 1), (inner,), 2)):
                z_acc[n, pl.ds(5 * group, 5), inner] = top

    def rim():
        with jax.named_scope("rim"):
            (top,) = conv1((0, 1), (3, 1), (top_rows, low_rows), 1)
            for n in range(2):
                part = top[:, :, 256 * n : 256 * n + 256]
                z_acc[n, :, top_rows] = part[:, :8]
                z_acc[n, :, low_rows] = part[:, 8:]

    def far(n):
        with jax.named_scope(f"wait_lent_on{n}"):
            lent_on[n].land()
        lanes = slice(256 * n, 256 * n + 256)
        with jax.named_scope(f"far{n}"):
            for group, top in enumerate(conv1((n,), (0, 2), (pl.ds(0, 72),), 2)):
                cols = pl.ds(5 * group, 5)
                act = jnp.maximum(z_acc[n, cols] + top + b1v[:, lanes], 0.0)
                for dh in range(3):
                    ys[dh][cols, :, lanes] = act[:, 4 * dh : 4 * dh + 64].astype(BF16)

        def clear(at_edge, refs, cols, rows):
            @pl.when(at_edge)
            def _():
                for ref in refs:
                    ref[cols, rows, lanes] = jnp.zeros((cols.size, rows.size, 256), BF16)

        clear(q == 0, ys, pl.ds(0, 1), pl.ds(0, 64))
        clear(q == 15, ys, pl.ds(9, 1), pl.ds(0, 64))
        clear(m == 0, (y0,), pl.ds(0, 10), pl.ds(0, 4))
        clear(m == 7, (y2,), pl.ds(0, 10), pl.ds(60, 4))

    def conv2(n):
        lanes = slice(256 * n, 256 * n + 256)
        total = None
        for dh in range(3):
            for dw in range(3):
                tap = 3 * dh + dw
                left = ys[dh][dw : dw + 8, :, lanes].reshape(CHANS, 256)
                right = w2v[CHANS * tap + 256 * n : CHANS * tap + 256 * n + 256, :]
                term = jnp.dot(left, right, preferred_element_type=F32)
                total = term if total is None else total + term
        return total

    pass_on(0)
    near(0)
    pass_on(1)
    near(1)
    finish(0)
    with jax.named_scope("wait_halo"):
        for copy in halo:
            copy.wait_recv()

    @pl.when(m == 0)
    def _():
        x0[:, 0:8] = jnp.zeros((12, 8, CHANS), BF16)
        x1[:, 0:4] = jnp.zeros((12, 4, CHANS), BF16)

    @pl.when(m > 0)
    def _():
        x1[:, 0:4] = edge[2]

    @pl.when(m == 7)
    def _():
        x2[:, 64:72] = jnp.zeros((12, 8, CHANS), BF16)
        x1[:, 68:72] = jnp.zeros((12, 4, CHANS), BF16)

    @pl.when(m < 7)
    def _():
        x1[:, 68:72] = edge[3]

    rim()
    finish(1)
    with jax.named_scope("wait_own_w2"):
        own.land()
        for load in loads[2:]:
            load.wait()
    far(0)
    with jax.named_scope("conv2_0"):
        acc2[...] = conv2(0)
    far(1)
    with jax.named_scope("conv2_1"):
        o_ref[...] = acc2[...] + conv2(1) + b2v[...]

    with jax.named_scope("wait_sends"):
        everything.wait_send()
        for step in steps:
            step.all.wait_send()
        for copy in halo:
            copy.wait_send()


def arrange(sum_ref, o_hbm, turned, sems):
    copies = []
    for g in range(4):
        rows = jnp.transpose(sum_ref[:, 16 * g : 16 * g + 16], (1, 0, 2))
        for h in range(4):
            for image in range(4):
                turned[g, image, h] = rows[4 * h + image]
        copies.append(pltpu.make_async_copy(turned.at[g], o_hbm.at[:, pl.ds(4 * g, 4)], sems.at[g]))
        copies[-1].start()
    for copy in copies:
        copy.wait()


def solution(mesh):
    scratch = [
        pltpu.VMEM((4, LANES, 4, LANES), BF16),
        pltpu.VMEM((9, 4, CHANS), BF16),
        pltpu.VMEM((4616, CHANS), BF16),
        pltpu.VMEM((1, CHANS), F32),
        pltpu.VMEM((1, CHANS), F32),
        pltpu.VMEM((CHANS, CHANS), BF16),
        pltpu.VMEM((8, 66, 4, LANES), BF16),
        pltpu.VMEM((LANES, 6, 4, LANES), BF16),
        *[pltpu.VMEM((12, 72, CHANS), BF16) for _ in range(3)],
        pltpu.VMEM((4, 12, 4, CHANS), BF16),
        pltpu.VMEM((3, 2, 4, 2, 4, 4, 3, 2, 4, LANES), BF16),
        pltpu.VMEM((2, 10, 72, 256), F32),
        *[pltpu.VMEM((10, 64, CHANS), BF16) for _ in range(3)],
        pltpu.VMEM((CHANS, CHANS), F32),
        pltpu.SemaphoreType.DMA((5,)),
        pltpu.SemaphoreType.DMA,
        pltpu.SemaphoreType.DMA,
        pltpu.SemaphoreType.DMA((4,)),
        pltpu.SemaphoreType.DMA((4,)),
        pltpu.SemaphoreType.DMA((11,)),
        pltpu.SemaphoreType.DMA((11,)),
    ]
    vmem = pl.BlockSpec(memory_space=pltpu.VMEM)
    anywhere = pl.BlockSpec(memory_space=pl.ANY)

    def run_local(x_in, w_conv1, b_conv1, w_conv2, b_conv2):
        sums = pl.pallas_call(
            kernel,
            out_shape=jax.ShapeDtypeStruct((CHANS, CHANS), F32),
            in_specs=[anywhere] * 5,
            out_specs=vmem,
            scratch_shapes=scratch,
            compiler_params=pltpu.CompilerParams(collective_id=0, has_side_effects=True, vmem_limit_bytes=VMEM_LIMIT),
            name="two_convs",
        )(
            *(
                pltpu.with_memory_space_constraint(a, pltpu.HBM)
                for a in (
                    x_in.transpose(0, 1, 3, 2),
                    w_conv1.reshape(9, 4, CHANS),
                    w_conv2.reshape(4608, CHANS),
                    b_conv1.reshape(1, CHANS),
                    b_conv2.reshape(1, CHANS),
                )
            )
        )
        return pl.pallas_call(
            arrange,
            out_shape=jax.ShapeDtypeStruct((4, 16, 8, CHANS), F32),
            in_specs=[vmem],
            out_specs=anywhere,
            scratch_shapes=[pltpu.VMEM((4, 4, 4, 8, CHANS), F32), pltpu.SemaphoreType.DMA((4,))],
            compiler_params=pltpu.CompilerParams(vmem_limit_bytes=8 * 2**20),
            name="arrange",
        )(sums.reshape(8, 64, CHANS))

    return jax.shard_map(
        run_local,
        mesh=mesh,
        in_specs=(P("data", None, None, GROUP_AXES), P(None, None, GROUP_AXES, None), P(), P(), P()),
        out_specs=P("data", "model", "cols", None),
        check_vma=False,
    )
```

```python
import jax
import jax.numpy as jnp
from jax import lax
from jax.experimental import pallas as pl
from jax.experimental.pallas import tpu as pltpu
from jax.sharding import PartitionSpec as P

GROUP_AXES = ("model", "cols")
MESH = pl.DeviceIdType.MESH
BF16 = jnp.bfloat16
F32 = jnp.float32
CHANS = 512
LANES = 128
CUT = 96
VMEM_LIMIT = 36 * 2**20
ORDERS = (("y", "z", "x"), ("z", "x", "y"), ("x", "y", "z"))


def one_hot(shape, col_of_row):
    rows = lax.broadcasted_iota(jnp.int32, shape, 0)
    cols = lax.broadcasted_iota(jnp.int32, shape, 1)
    return jnp.where(cols == col_of_row(rows), 1.0, 0.0).astype(BF16)


def pack_windows(xv, a_scr, pack):
    to_lanes = one_hot((CHANS, CHANS), lambda r: (r % 4) * LANES + ((r % LANES) // 4) * 4 + r // LANES)
    to_rows = one_hot((CHANS, CHANS), lambda r: (r % 4) * LANES + ((r % 256) // 4) * 2 + r // 256)
    for blk in range(4):
        part = jnp.concatenate([xv[n, 32 * blk : 32 * blk + 32].reshape(LANES, LANES) for n in range(4)], axis=0)
        turned = lax.dot_general(part, to_lanes, (((0,), (0,)), ((), ())), preferred_element_type=F32).astype(BF16)
        for c in range(4):
            a_scr[c * LANES : (c + 1) * LANES, blk * LANES : (blk + 1) * LANES] = turned[:, c * LANES : (c + 1) * LANES]
    mixed = jnp.dot(to_rows, a_scr[...], preferred_element_type=F32)
    for blk in range(4):
        even = mixed[0:256, blk * LANES : (blk + 1) * LANES]
        odd = mixed[256:CHANS, blk * LANES : (blk + 1) * LANES]
        for half in range(2):
            s = slice(64 * half, 64 * half + 64)
            tile = jnp.concatenate([even[:, s], odd[:, s]], axis=1).astype(BF16)
            pack[2 * blk + half, 1:65] = tile.reshape(64, 4, LANES)
    edge = jnp.zeros((8, 1, 4, LANES), BF16)
    pack[:, 0:1] = edge
    pack[:, 65:66] = edge


def kernel(
    x_hbm, w1_hbm, w2_hbm, b1_hbm, b2_hbm, o_ref,
    xv, w1v, w2v, b1v, b2v, a_scr, pack, got, x0, x1, x2, edge, w1g, z_acc, y0, y1, y2, acc2,
    load_sem, xs_send, xs_recv, halo_send, halo_recv, step_send, step_recv,
):
    m = lax.axis_index("model")
    q = lax.axis_index("cols")
    me = {"x": m // 2, "z": q // 4, "y": q % 4}
    core = m % 2
    parts = range(3)
    barrier = pltpu.get_barrier_semaphore()

    at_model = [[(me["x"] + dx) % 4 * 2 + (core + dk) % 2 for dk in range(2)] for dx in range(4)]
    at_cols = [[(me["z"] + dz) % 4 * 4 + (me["y"] + dy) % 4 for dy in range(4)] for dz in range(4)]
    others = [(dx, dz, dy, dk) for dx in range(4) for dz in range(4) for dy in range(4) for dk in range(2)]
    others = sorted(others[1:], key=lambda d: (sum(d[:3]) % 4, d))

    def away(d):
        return {"model": at_model[d[0]][d[3]], "cols": at_cols[d[1]][d[2]]}

    loads = [
        pltpu.make_async_copy(src, dst, load_sem.at[k])
        for k, (src, dst) in enumerate(
            ((x_hbm, xv), (w1_hbm, w1v), (w2_hbm, w2v.at[pl.ds(0, 4608)]), (b1_hbm, b1v), (b2_hbm, b2v))
        )
    ]
    for load in loads:
        load.start()
    with jax.named_scope("announce"):
        for d in sorted(others, key=lambda d: -sum(min(o, 4 - o) for o in d[:3])):
            pl.semaphore_signal(barrier, inc=1, device_id=away(d), device_id_type=MESH)

    def piece(p, t, v, n, c, place=None, half=None):
        done = ORDERS[p][:t]
        rest = [a for a in "xzy" if a != ORDERS[p][2]]
        at = [v if t < 2 and a == ORDERS[p][t] else (pl.ds(0, 4) if a in done else me[a]) for a in rest]
        if half is not None:
            at[0] = pl.ds(2 * half, 2)
        return w1g.at[p, pl.ds(0, 2) if n is None else n, me[ORDERS[p][2]] if t < 2 else v, c, at[0], at[1]]

    with jax.named_scope("place_w1"):
        loads[1].wait()
        for p in parts:
            spot = [me[a] for a in "xzy" if a != ORDERS[p][2]]
            for dw in range(3):
                for lt in range(4):
                    tile = w1v[3 * p + dw, :, lt * LANES : (lt + 1) * LANES]
                    w1g[p, lt // 2, me[ORDERS[p][2]], core, spot[0], spot[1], dw, lt % 2] = tile
    with jax.named_scope("wait_x"):
        loads[0].wait()
    with jax.named_scope("pack"):
        pack_windows(xv, a_scr, pack)
    with jax.named_scope("wait_barrier"):
        pl.semaphore_wait(barrier, 127)

    n_steps = [0]
    steps = []

    class Step:
        def __init__(self, slabs, copies):
            k = n_steps[0]
            n_steps[0] += 1
            sems = dict(send_sem=step_send.at[k], recv_sem=step_recv.at[k], device_id_type=MESH)
            self.copies, self.sems = copies, sems
            span = got.at[pl.ds(0, slabs)]
            self.all = pltpu.make_async_remote_copy(
                src_ref=span, dst_ref=span, device_id={"model": at_model[0][1], "cols": q}, **sems
            )
            steps.append(self)

        def go(self):
            for ref, to in self.copies:
                pltpu.make_async_remote_copy(src_ref=ref, dst_ref=ref, device_id=to, **self.sems).start()
            return self

        def land(self):
            self.all.wait_recv()

    def chip(p, t, d, c=0):
        axis = ORDERS[p][t]
        pos = me | {axis: (me[axis] + d) % 4}
        return {"model": pos["x"] * 2 + (core + c) % 2, "cols": pos["z"] * 4 + pos["y"]}

    def spread(t, slabs):
        return Step(slabs, [(piece(p, t, me[ORDERS[p][t]], None, core), chip(p, t, d)) for p in parts for d in (1, 3, 2)]).go()

    def plane(p, d):
        return (me[ORDERS[p][2]] + d) % 4

    def hand_over(pieces, slabs):
        return Step(slabs, [(ref, {"model": at_model[0][1], "cols": q}) for ref in pieces]).go()

    def send_windows(first, last):
        for d in others[first:last]:
            to = away(d)
            pltpu.make_async_remote_copy(
                src_ref=pack.at[to["model"], pl.ds(4 * to["cols"], 6)],
                dst_ref=got.at[mine],
                send_sem=xs_send,
                recv_sem=xs_recv,
                device_id=to,
                device_id_type=MESH,
            ).start()

    mine = ((core * 4 + me["x"]) * 4 + me["z"]) * 4 + me["y"]
    with jax.named_scope("send_first"):
        first = spread(0, 18)
        for pair in range(6):
            got[mine, pair] = pack[m, 4 * q + pair]
        send_windows(0, CUT)
    with jax.named_scope("wait_first"):
        first.land()
    with jax.named_scope("send_second"):
        second = spread(1, 72)
        send_windows(CUT, 127)
    with jax.named_scope("wait_second"):
        second.land()
    last, passed, lent, lent_on = {}, {}, {}, {}

    def send_plane(n):
        last[n] = Step(96, [(piece(p, 2, plane(p, 0), n, core), chip(p, 2, d)) for p in parts for d in (1, 3)])

    def pass_on(n):
        with jax.named_scope(f"wait_last{n}"):
            last[n].land()
        passed[n] = Step(48, [(piece(p, 2, plane(p, 4 - d), n, core, half=d // 2), chip(p, 2, d)) for p in parts for d in (1, 3)]).go()
        lent[n] = hand_over([piece(p, 2, plane(p, d), n, core) for p in parts for d in (1, 3)], 96)

    def finish(n):
        with jax.named_scope(f"wait_passed{n}"):
            passed[n].land()
        lent_on[n] = hand_over([piece(p, 2, plane(p, 2), n, core) for p in parts], 48)

    with jax.named_scope("send_third"):
        for n in range(2):
            send_plane(n)
        last[0].go()
        own = hand_over([piece(p, 2, plane(p, 0), None, core) for p in parts], 96)
    last[1].go()
    span = got.at[pl.ds(0, 127)]
    everything = pltpu.make_async_remote_copy(
        src_ref=span, dst_ref=span, send_sem=xs_send, recv_sem=xs_recv, device_id=chip(0, 0, 0, 1), device_id_type=MESH
    )
    with jax.named_scope("wait_windows"):
        everything.wait_recv()

    xs, ys = (x0, x1, x2), (y0, y1, y2)
    with jax.named_scope("turn"):
        for pair in range(6):
            for p in parts:
                rows = []
                for v in range(4):
                    for c in range(2):
                        at = 64 * c
                        if p == 0:
                            rows.append(got[at + 16 * v : at + 16 * v + 16, pair])
                        elif p == 1:
                            rows.append(got[at + v : at + 64 : 4, pair])
                        else:
                            rows += [got[at + 16 * a + 4 * v : at + 16 * a + 4 * v + 4, pair] for a in range(4)]
                rows = jnp.concatenate([r.reshape(-1, LANES) for r in rows], axis=0).T
                for odd in range(2):
                    main = rows[64 * odd : 64 * odd + 64]
                    xs[p][2 * pair + odd, 8 - 4 * p : 72 - 4 * p] = main
                    if p == 1:
                        edge[0, 2 * pair + odd] = main[60:64]
                        edge[1, 2 * pair + odd] = main[0:4]
    halo = []
    for src, dst, d in (
        (x0.at[:, pl.ds(64, 8)], x0.at[:, pl.ds(0, 8)], 1),
        (x2.at[:, pl.ds(0, 8)], x2.at[:, pl.ds(64, 8)], 7),
        (edge.at[0], edge.at[2], 1),
        (edge.at[1], edge.at[3], 7),
    ):
        halo.append(
            pltpu.make_async_remote_copy(
                src_ref=src,
                dst_ref=dst,
                send_sem=halo_send.at[len(halo)],
                recv_sem=halo_recv.at[len(halo)],
                device_id={"model": (m + d) % 8, "cols": q},
                device_id_type=MESH,
            )
        )
        halo[-1].start()

    def conv1(halves, places, spans, groups):
        width = 10 // groups
        tops = [None] * groups
        taps = [(p, dw, plane(p, d)) for p in parts for dw in range(3) for d in places]
        for first in range(0, len(taps), 2):
            two = taps[first : first + 2]
            right = [[w1g[p, n, v, :, :, :, dw, i].reshape(LANES, LANES) for n in halves for i in range(2)] for p, dw, v in two]
            right = jnp.concatenate([jnp.concatenate(r, axis=1) for r in right], axis=0)
            for group in range(groups):
                left = []
                for rows in spans:
                    some = []
                    for p, dw, v in two:
                        lanes = pl.ds(pl.multiple_of(LANES * v, LANES), LANES)
                        some.append(xs[p][pl.ds(dw + width * group, width), rows, lanes])
                    left.append(jnp.concatenate(some, axis=-1))
                left = jnp.concatenate(left, axis=1).reshape(-1, LANES * len(two))
                term = jnp.dot(left, right, preferred_element_type=F32)
                tops[group] = term if tops[group] is None else tops[group] + term
        return [top.reshape(width, -1, 256 * len(halves)) for top in tops]

    top_rows, inner, low_rows = pl.ds(0, 8), pl.ds(8, 56), pl.ds(64, 8)

    def here(n):
        with jax.named_scope(f"here{n}"):
            for group, top in enumerate(conv1((n,), (0,), (inner,), 2)):
                z_acc[n, pl.ds(5 * group, 5), inner] = top

    def near(n):
        with jax.named_scope(f"wait_lent{n}"):
            lent[n].land()
        with jax.named_scope(f"near{n}"):
            for group, top in enumerate(conv1((n,), (3, 1), (inner,), 2)):
                z_acc[n, pl.ds(5 * group, 5), inner] += top

    def rim():
        with jax.named_scope("rim"):
            (top,) = conv1((0, 1), (0, 3, 1), (top_rows, low_rows), 1)
            for n in range(2):
                part = top[:, :, 256 * n : 256 * n + 256]
                z_acc[n, :, top_rows] = part[:, :8]
                z_acc[n, :, low_rows] = part[:, 8:]

    def far(n):
        with jax.named_scope(f"wait_lent_on{n}"):
            lent_on[n].land()
        lanes = slice(256 * n, 256 * n + 256)
        with jax.named_scope(f"far{n}"):
            for group, top in enumerate(conv1((n,), (2,), (pl.ds(0, 72),), 2)):
                cols = pl.ds(5 * group, 5)
                act = jnp.maximum(z_acc[n, cols] + top + b1v[:, lanes], 0.0)
                for dh in range(3):
                    ys[dh][cols, :, lanes] = act[:, 4 * dh : 4 * dh + 64].astype(BF16)

        def clear(at_edge, refs, cols, rows):
            @pl.when(at_edge)
            def _():
                for ref in refs:
                    ref[cols, rows, lanes] = jnp.zeros((cols.size, rows.size, 256), BF16)

        clear(q == 0, ys, pl.ds(0, 1), pl.ds(0, 64))
        clear(q == 15, ys, pl.ds(9, 1), pl.ds(0, 64))
        clear(m == 0, (y0,), pl.ds(0, 10), pl.ds(0, 4))
        clear(m == 7, (y2,), pl.ds(0, 10), pl.ds(60, 4))

    def conv2(n):
        lanes = slice(256 * n, 256 * n + 256)
        total = None
        for dh in range(3):
            for dw in range(3):
                tap = 3 * dh + dw
                left = ys[dh][dw : dw + 8, :, lanes].reshape(CHANS, 256)
                right = w2v[CHANS * tap + 256 * n : CHANS * tap + 256 * n + 256, :]
                term = jnp.dot(left, right, preferred_element_type=F32)
                total = term if total is None else total + term
        return total

    pass_on(0)
    with jax.named_scope("wait_own"):
        own.land()
    here(0)
    here(1)
    pass_on(1)
    near(0)
    near(1)
    finish(0)
    with jax.named_scope("wait_halo"):
        for copy in halo:
            copy.wait_recv()

    @pl.when(m == 0)
    def _():
        x0[:, 0:8] = jnp.zeros((12, 8, CHANS), BF16)
        x1[:, 0:4] = jnp.zeros((12, 4, CHANS), BF16)

    @pl.when(m > 0)
    def _():
        x1[:, 0:4] = edge[2]

    @pl.when(m == 7)
    def _():
        x2[:, 64:72] = jnp.zeros((12, 8, CHANS), BF16)
        x1[:, 68:72] = jnp.zeros((12, 4, CHANS), BF16)

    @pl.when(m < 7)
    def _():
        x1[:, 68:72] = edge[3]

    rim()
    finish(1)
    with jax.named_scope("wait_w2"):
        for load in loads[2:]:
            load.wait()
    far(0)
    with jax.named_scope("conv2_0"):
        acc2[...] = conv2(0)
    far(1)
    with jax.named_scope("conv2_1"):
        o_ref[...] = acc2[...] + conv2(1) + b2v[...]

    with jax.named_scope("wait_sends"):
        everything.wait_send()
        for step in steps:
            step.all.wait_send()
        for copy in halo:
            copy.wait_send()


def arrange(sum_ref, o_hbm, turned, sems):
    copies = []
    for g in range(4):
        rows = jnp.transpose(sum_ref[:, 16 * g : 16 * g + 16], (1, 0, 2))
        for h in range(4):
            for image in range(4):
                turned[g, image, h] = rows[4 * h + image]
        copies.append(pltpu.make_async_copy(turned.at[g], o_hbm.at[:, pl.ds(4 * g, 4)], sems.at[g]))
        copies[-1].start()
    for copy in copies:
        copy.wait()


def solution(mesh):
    scratch = [
        pltpu.VMEM((4, LANES, 4, LANES), BF16),
        pltpu.VMEM((9, 4, CHANS), BF16),
        pltpu.VMEM((4616, CHANS), BF16),
        pltpu.VMEM((1, CHANS), F32),
        pltpu.VMEM((1, CHANS), F32),
        pltpu.VMEM((CHANS, CHANS), BF16),
        pltpu.VMEM((8, 66, 4, LANES), BF16),
        pltpu.VMEM((LANES, 6, 4, LANES), BF16),
        *[pltpu.VMEM((12, 72, CHANS), BF16) for _ in range(3)],
        pltpu.VMEM((4, 12, 4, CHANS), BF16),
        pltpu.VMEM((3, 2, 4, 2, 4, 4, 3, 2, 4, LANES), BF16),
        pltpu.VMEM((2, 10, 72, 256), F32),
        *[pltpu.VMEM((10, 64, CHANS), BF16) for _ in range(3)],
        pltpu.VMEM((CHANS, CHANS), F32),
        pltpu.SemaphoreType.DMA((5,)),
        pltpu.SemaphoreType.DMA,
        pltpu.SemaphoreType.DMA,
        pltpu.SemaphoreType.DMA((4,)),
        pltpu.SemaphoreType.DMA((4,)),
        pltpu.SemaphoreType.DMA((11,)),
        pltpu.SemaphoreType.DMA((11,)),
    ]
    vmem = pl.BlockSpec(memory_space=pltpu.VMEM)
    anywhere = pl.BlockSpec(memory_space=pl.ANY)

    def run_local(x_in, w_conv1, b_conv1, w_conv2, b_conv2):
        sums = pl.pallas_call(
            kernel,
            out_shape=jax.ShapeDtypeStruct((CHANS, CHANS), F32),
            in_specs=[anywhere] * 5,
            out_specs=vmem,
            scratch_shapes=scratch,
            compiler_params=pltpu.CompilerParams(collective_id=0, has_side_effects=True, vmem_limit_bytes=VMEM_LIMIT),
            name="two_convs",
        )(
            *(
                pltpu.with_memory_space_constraint(a, pltpu.HBM)
                for a in (
                    x_in.transpose(0, 1, 3, 2),
                    w_conv1.reshape(9, 4, CHANS),
                    w_conv2.reshape(4608, CHANS),
                    b_conv1.reshape(1, CHANS),
                    b_conv2.reshape(1, CHANS),
                )
            )
        )
        return pl.pallas_call(
            arrange,
            out_shape=jax.ShapeDtypeStruct((4, 16, 8, CHANS), F32),
            in_specs=[vmem],
            out_specs=anywhere,
            scratch_shapes=[pltpu.VMEM((4, 4, 4, 8, CHANS), F32), pltpu.SemaphoreType.DMA((4,))],
            compiler_params=pltpu.CompilerParams(vmem_limit_bytes=8 * 2**20),
            name="arrange",
        )(sums.reshape(8, 64, CHANS))

    return jax.shard_map(
        run_local,
        mesh=mesh,
        in_specs=(P("data", None, None, GROUP_AXES), P(None, None, GROUP_AXES, None), P(), P(), P()),
        out_specs=P("data", "model", "cols", None),
        check_vma=False,
    )
```

```python
import jax
import jax.numpy as jnp
from jax import lax
from jax.experimental import pallas as pl
from jax.experimental.pallas import tpu as pltpu
from jax.sharding import PartitionSpec as P

GROUP_AXES = ("model", "cols")
MESH = pl.DeviceIdType.MESH
BF16 = jnp.bfloat16
F32 = jnp.float32
CHANS = 512
LANES = 128
CUT = 96
VMEM_LIMIT = 36 * 2**20
ORDERS = (("y", "z", "x"), ("z", "x", "y"), ("x", "y", "z"))


def one_hot(shape, col_of_row):
    rows = lax.broadcasted_iota(jnp.int32, shape, 0)
    cols = lax.broadcasted_iota(jnp.int32, shape, 1)
    return jnp.where(cols == col_of_row(rows), 1.0, 0.0).astype(BF16)


def pack_windows(xv, a_scr, pack):
    to_lanes = one_hot((CHANS, CHANS), lambda r: (r % 4) * LANES + ((r % LANES) // 4) * 4 + r // LANES)
    to_rows = one_hot((CHANS, CHANS), lambda r: (r % 4) * LANES + ((r % 256) // 4) * 2 + r // 256)
    for blk in range(4):
        part = jnp.concatenate([xv[n, 32 * blk : 32 * blk + 32].reshape(LANES, LANES) for n in range(4)], axis=0)
        turned = lax.dot_general(part, to_lanes, (((0,), (0,)), ((), ())), preferred_element_type=F32).astype(BF16)
        for c in range(4):
            a_scr[c * LANES : (c + 1) * LANES, blk * LANES : (blk + 1) * LANES] = turned[:, c * LANES : (c + 1) * LANES]
    mixed = jnp.dot(to_rows, a_scr[...], preferred_element_type=F32)
    for blk in range(4):
        even = mixed[0:256, blk * LANES : (blk + 1) * LANES]
        odd = mixed[256:CHANS, blk * LANES : (blk + 1) * LANES]
        for half in range(2):
            s = slice(64 * half, 64 * half + 64)
            tile = jnp.concatenate([even[:, s], odd[:, s]], axis=1).astype(BF16)
            pack[2 * blk + half, 1:65] = tile.reshape(64, 4, LANES)
    edge = jnp.zeros((8, 1, 4, LANES), BF16)
    pack[:, 0:1] = edge
    pack[:, 65:66] = edge


def kernel(
    x_hbm, w1_hbm, w2_hbm, b1_hbm, b2_hbm, o_ref,
    xv, w1v, w2v, b1v, b2v, a_scr, pack, got, x0, x1, x2, edge, w1g, z_acc, y0, y1, y2, acc2,
    load_sem, xs_send, xs_recv, halo_send, halo_recv, step_send, step_recv,
):
    m = lax.axis_index("model")
    q = lax.axis_index("cols")
    me = {"x": m // 2, "z": q // 4, "y": q % 4}
    core = m % 2
    parts = range(3)
    barrier = pltpu.get_barrier_semaphore()

    at_model = [[(me["x"] + dx) % 4 * 2 + (core + dk) % 2 for dk in range(2)] for dx in range(4)]
    at_cols = [[(me["z"] + dz) % 4 * 4 + (me["y"] + dy) % 4 for dy in range(4)] for dz in range(4)]
    others = [(dx, dz, dy, dk) for dx in range(4) for dz in range(4) for dy in range(4) for dk in range(2)]
    others = sorted(others[1:], key=lambda d: (sum(d[:3]) % 4, d))

    def away(d):
        return {"model": at_model[d[0]][d[3]], "cols": at_cols[d[1]][d[2]]}

    loads = [
        pltpu.make_async_copy(src, dst, load_sem.at[k])
        for k, (src, dst) in enumerate(
            ((x_hbm, xv), (w1_hbm, w1v), (w2_hbm, w2v.at[pl.ds(0, 4608)]), (b1_hbm, b1v), (b2_hbm, b2v))
        )
    ]
    for load in loads:
        load.start()
    with jax.named_scope("announce"):
        for d in sorted(others, key=lambda d: -sum(min(o, 4 - o) for o in d[:3])):
            pl.semaphore_signal(barrier, inc=1, device_id=away(d), device_id_type=MESH)

    def piece(p, t, v, n, c, place=None, half=None):
        done = ORDERS[p][:t]
        rest = [a for a in "xzy" if a != ORDERS[p][2]]
        at = [v if t < 2 and a == ORDERS[p][t] else (pl.ds(0, 4) if a in done else me[a]) for a in rest]
        if half is not None:
            at[0] = pl.ds(2 * half, 2)
        return w1g.at[p, pl.ds(0, 2) if n is None else n, me[ORDERS[p][2]] if t < 2 else v, c, at[0], at[1]]

    with jax.named_scope("place_w1"):
        loads[1].wait()
        for p in parts:
            spot = [me[a] for a in "xzy" if a != ORDERS[p][2]]
            for dw in range(3):
                for lt in range(4):
                    tile = w1v[3 * p + dw, :, lt * LANES : (lt + 1) * LANES]
                    w1g[p, lt // 2, me[ORDERS[p][2]], core, spot[0], spot[1], dw, lt % 2] = tile
    with jax.named_scope("wait_x"):
        loads[0].wait()
    with jax.named_scope("pack"):
        pack_windows(xv, a_scr, pack)
    with jax.named_scope("wait_barrier"):
        pl.semaphore_wait(barrier, 127)

    n_steps = [0]
    steps = []

    class Step:
        def __init__(self, slabs, copies):
            k = n_steps[0]
            n_steps[0] += 1
            sems = dict(send_sem=step_send.at[k], recv_sem=step_recv.at[k], device_id_type=MESH)
            self.copies, self.sems = copies, sems
            span = got.at[pl.ds(0, slabs)]
            self.all = pltpu.make_async_remote_copy(
                src_ref=span, dst_ref=span, device_id={"model": at_model[0][1], "cols": q}, **sems
            )
            steps.append(self)

        def go(self):
            for ref, to in self.copies:
                pltpu.make_async_remote_copy(src_ref=ref, dst_ref=ref, device_id=to, **self.sems).start()
            return self

        def land(self):
            self.all.wait_recv()

    def chip(p, t, d, c=0):
        axis = ORDERS[p][t]
        pos = me | {axis: (me[axis] + d) % 4}
        return {"model": pos["x"] * 2 + (core + c) % 2, "cols": pos["z"] * 4 + pos["y"]}

    def spread(t, slabs):
        return Step(slabs, [(piece(p, t, me[ORDERS[p][t]], None, core), chip(p, t, d)) for p in parts for d in (1, 3, 2)]).go()

    def plane(p, d):
        return (me[ORDERS[p][2]] + d) % 4

    def hand_over(pieces, slabs):
        return Step(slabs, [(ref, {"model": at_model[0][1], "cols": q}) for ref in pieces]).go()

    def send_windows(first, last):
        for d in others[first:last]:
            to = away(d)
            pltpu.make_async_remote_copy(
                src_ref=pack.at[to["model"], pl.ds(4 * to["cols"], 6)],
                dst_ref=got.at[mine],
                send_sem=xs_send,
                recv_sem=xs_recv,
                device_id=to,
                device_id_type=MESH,
            ).start()

    mine = ((core * 4 + me["x"]) * 4 + me["z"]) * 4 + me["y"]
    with jax.named_scope("send_first"):
        first = spread(0, 18)
        for pair in range(6):
            got[mine, pair] = pack[m, 4 * q + pair]
        send_windows(0, CUT)
    with jax.named_scope("wait_first"):
        first.land()
    with jax.named_scope("send_second"):
        second = spread(1, 72)
        send_windows(CUT, 127)
    with jax.named_scope("wait_second"):
        second.land()
    last, passed, lent, lent_on = {}, {}, {}, {}

    def send_plane(n):
        last[n] = Step(96, [(piece(p, 2, plane(p, 0), n, core), chip(p, 2, d)) for p in parts for d in (1, 3)])

    def pass_on(n):
        with jax.named_scope(f"wait_last{n}"):
            last[n].land()
        passed[n] = Step(48, [(piece(p, 2, plane(p, 4 - d), n, core, half=d // 2), chip(p, 2, d)) for p in parts for d in (1, 3)]).go()
        lent[n] = hand_over([piece(p, 2, plane(p, d), n, core) for p in parts for d in (1, 3)], 96)

    def finish(n):
        with jax.named_scope(f"wait_passed{n}"):
            passed[n].land()
        lent_on[n] = hand_over([piece(p, 2, plane(p, 2), n, core) for p in parts], 48)

    with jax.named_scope("send_third"):
        for n in range(2):
            send_plane(n)
        last[0].go()
        own = hand_over([piece(p, 2, plane(p, 0), None, core) for p in parts], 96)
    last[1].go()
    span = got.at[pl.ds(0, 127)]
    everything = pltpu.make_async_remote_copy(
        src_ref=span, dst_ref=span, send_sem=xs_send, recv_sem=xs_recv, device_id=chip(0, 0, 0, 1), device_id_type=MESH
    )
    with jax.named_scope("wait_windows"):
        everything.wait_recv()

    xs, ys = (x0, x1, x2), (y0, y1, y2)
    with jax.named_scope("turn"):
        for pair in range(6):
            for p in parts:
                rows = []
                for v in range(4):
                    for c in range(2):
                        at = 64 * c
                        if p == 0:
                            rows.append(got[at + 16 * v : at + 16 * v + 16, pair])
                        elif p == 1:
                            rows.append(got[at + v : at + 64 : 4, pair])
                        else:
                            rows += [got[at + 16 * a + 4 * v : at + 16 * a + 4 * v + 4, pair] for a in range(4)]
                rows = jnp.concatenate([r.reshape(-1, LANES) for r in rows], axis=0).T
                for odd in range(2):
                    main = rows[64 * odd : 64 * odd + 64]
                    xs[p][2 * pair + odd, 8 - 4 * p : 72 - 4 * p] = main
                    if p == 1:
                        edge[0, 2 * pair + odd] = main[60:64]
                        edge[1, 2 * pair + odd] = main[0:4]
    halo = []
    for src, dst, d in (
        (x0.at[:, pl.ds(64, 8)], x0.at[:, pl.ds(0, 8)], 1),
        (x2.at[:, pl.ds(0, 8)], x2.at[:, pl.ds(64, 8)], 7),
        (edge.at[0], edge.at[2], 1),
        (edge.at[1], edge.at[3], 7),
    ):
        halo.append(
            pltpu.make_async_remote_copy(
                src_ref=src,
                dst_ref=dst,
                send_sem=halo_send.at[len(halo)],
                recv_sem=halo_recv.at[len(halo)],
                device_id={"model": (m + d) % 8, "cols": q},
                device_id_type=MESH,
            )
        )
        halo[-1].start()

    def conv1(halves, places, spans, groups):
        width = 10 // groups
        tops = [None] * groups
        taps = [(p, dw, plane(p, d)) for p in parts for dw in range(3) for d in places]
        for first in range(0, len(taps), 2):
            two = taps[first : first + 2]
            right = [[w1g[p, n, v, :, :, :, dw, i].reshape(LANES, LANES) for n in halves for i in range(2)] for p, dw, v in two]
            right = jnp.concatenate([jnp.concatenate(r, axis=1) for r in right], axis=0)
            for group in range(groups):
                left = []
                for rows in spans:
                    some = []
                    for p, dw, v in two:
                        lanes = pl.ds(pl.multiple_of(LANES * v, LANES), LANES)
                        some.append(xs[p][pl.ds(dw + width * group, width), rows, lanes])
                    left.append(jnp.concatenate(some, axis=-1))
                left = jnp.concatenate(left, axis=1).reshape(-1, LANES * len(two))
                term = jnp.dot(left, right, preferred_element_type=F32)
                tops[group] = term if tops[group] is None else tops[group] + term
        return [top.reshape(width, -1, 256 * len(halves)) for top in tops]

    top_rows, inner, low_rows = pl.ds(0, 8), pl.ds(8, 56), pl.ds(64, 8)

    def here(n):
        with jax.named_scope(f"here{n}"):
            for group, top in enumerate(conv1((n,), (0,), (inner,), 2)):
                z_acc[n, pl.ds(5 * group, 5), inner] = top

    def near(n):
        with jax.named_scope(f"wait_lent{n}"):
            lent[n].land()
        with jax.named_scope(f"near{n}"):
            for group, top in enumerate(conv1((n,), (3, 1), (inner,), 2)):
                z_acc[n, pl.ds(5 * group, 5), inner] += top

    def rim():
        with jax.named_scope("rim"):
            (top,) = conv1((0, 1), (0, 3, 1), (top_rows, low_rows), 1)
            for n in range(2):
                part = top[:, :, 256 * n : 256 * n + 256]
                z_acc[n, :, top_rows] = part[:, :8]
                z_acc[n, :, low_rows] = part[:, 8:]

    def far(n):
        with jax.named_scope(f"wait_lent_on{n}"):
            lent_on[n].land()
        lanes = slice(256 * n, 256 * n + 256)
        with jax.named_scope(f"far{n}"):
            for group, top in enumerate(conv1((n,), (2,), (pl.ds(0, 72),), 2)):
                cols = pl.ds(5 * group, 5)
                act = jnp.maximum(z_acc[n, cols] + top + b1v[:, lanes], 0.0)
                for dh in range(3):
                    ys[dh][cols, :, lanes] = act[:, 4 * dh : 4 * dh + 64].astype(BF16)

        def clear(at_edge, refs, cols, rows):
            @pl.when(at_edge)
            def _():
                for ref in refs:
                    ref[cols, rows, lanes] = jnp.zeros((cols.size, rows.size, 256), BF16)

        clear(q == 0, ys, pl.ds(0, 1), pl.ds(0, 64))
        clear(q == 15, ys, pl.ds(9, 1), pl.ds(0, 64))
        clear(m == 0, (y0,), pl.ds(0, 10), pl.ds(0, 4))
        clear(m == 7, (y2,), pl.ds(0, 10), pl.ds(60, 4))

    def conv2(n):
        lanes = slice(256 * n, 256 * n + 256)
        total = None
        for dh in range(3):
            for dw in range(3):
                tap = 3 * dh + dw
                left = ys[dh][dw : dw + 8, :, lanes].reshape(CHANS, 256)
                right = w2v[CHANS * tap + 256 * n : CHANS * tap + 256 * n + 256, :]
                term = jnp.dot(left, right, preferred_element_type=F32)
                total = term if total is None else total + term
        return total

    with jax.named_scope("wait_own"):
        own.land()
    here(0)
    pass_on(0)
    here(1)
    pass_on(1)
    near(0)
    near(1)
    finish(0)
    with jax.named_scope("wait_halo"):
        for copy in halo:
            copy.wait_recv()

    @pl.when(m == 0)
    def _():
        x0[:, 0:8] = jnp.zeros((12, 8, CHANS), BF16)
        x1[:, 0:4] = jnp.zeros((12, 4, CHANS), BF16)

    @pl.when(m > 0)
    def _():
        x1[:, 0:4] = edge[2]

    @pl.when(m == 7)
    def _():
        x2[:, 64:72] = jnp.zeros((12, 8, CHANS), BF16)
        x1[:, 68:72] = jnp.zeros((12, 4, CHANS), BF16)

    @pl.when(m < 7)
    def _():
        x1[:, 68:72] = edge[3]

    rim()
    finish(1)
    with jax.named_scope("wait_w2"):
        for load in loads[2:]:
            load.wait()
    far(0)
    with jax.named_scope("conv2_0"):
        acc2[...] = conv2(0)
    far(1)
    with jax.named_scope("conv2_1"):
        o_ref[...] = acc2[...] + conv2(1) + b2v[...]

    with jax.named_scope("wait_sends"):
        everything.wait_send()
        for step in steps:
            step.all.wait_send()
        for copy in halo:
            copy.wait_send()


def arrange(sum_ref, o_hbm, turned, sems):
    copies = []
    for g in range(4):
        rows = jnp.transpose(sum_ref[:, 16 * g : 16 * g + 16], (1, 0, 2))
        for h in range(4):
            for image in range(4):
                turned[g, image, h] = rows[4 * h + image]
        copies.append(pltpu.make_async_copy(turned.at[g], o_hbm.at[:, pl.ds(4 * g, 4)], sems.at[g]))
        copies[-1].start()
    for copy in copies:
        copy.wait()


def solution(mesh):
    scratch = [
        pltpu.VMEM((4, LANES, 4, LANES), BF16),
        pltpu.VMEM((9, 4, CHANS), BF16),
        pltpu.VMEM((4616, CHANS), BF16),
        pltpu.VMEM((1, CHANS), F32),
        pltpu.VMEM((1, CHANS), F32),
        pltpu.VMEM((CHANS, CHANS), BF16),
        pltpu.VMEM((8, 66, 4, LANES), BF16),
        pltpu.VMEM((LANES, 6, 4, LANES), BF16),
        *[pltpu.VMEM((12, 72, CHANS), BF16) for _ in range(3)],
        pltpu.VMEM((4, 12, 4, CHANS), BF16),
        pltpu.VMEM((3, 2, 4, 2, 4, 4, 3, 2, 4, LANES), BF16),
        pltpu.VMEM((2, 10, 72, 256), F32),
        *[pltpu.VMEM((10, 64, CHANS), BF16) for _ in range(3)],
        pltpu.VMEM((CHANS, CHANS), F32),
        pltpu.SemaphoreType.DMA((5,)),
        pltpu.SemaphoreType.DMA,
        pltpu.SemaphoreType.DMA,
        pltpu.SemaphoreType.DMA((4,)),
        pltpu.SemaphoreType.DMA((4,)),
        pltpu.SemaphoreType.DMA((11,)),
        pltpu.SemaphoreType.DMA((11,)),
    ]
    vmem = pl.BlockSpec(memory_space=pltpu.VMEM)
    anywhere = pl.BlockSpec(memory_space=pl.ANY)

    def run_local(x_in, w_conv1, b_conv1, w_conv2, b_conv2):
        sums = pl.pallas_call(
            kernel,
            out_shape=jax.ShapeDtypeStruct((CHANS, CHANS), F32),
            in_specs=[anywhere] * 5,
            out_specs=vmem,
            scratch_shapes=scratch,
            compiler_params=pltpu.CompilerParams(collective_id=0, has_side_effects=True, vmem_limit_bytes=VMEM_LIMIT),
            name="two_convs",
        )(
            *(
                pltpu.with_memory_space_constraint(a, pltpu.HBM)
                for a in (
                    x_in.transpose(0, 1, 3, 2),
                    w_conv1.reshape(9, 4, CHANS),
                    w_conv2.reshape(4608, CHANS),
                    b_conv1.reshape(1, CHANS),
                    b_conv2.reshape(1, CHANS),
                )
            )
        )
        return pl.pallas_call(
            arrange,
            out_shape=jax.ShapeDtypeStruct((4, 16, 8, CHANS), F32),
            in_specs=[vmem],
            out_specs=anywhere,
            scratch_shapes=[pltpu.VMEM((4, 4, 4, 8, CHANS), F32), pltpu.SemaphoreType.DMA((4,))],
            compiler_params=pltpu.CompilerParams(vmem_limit_bytes=8 * 2**20),
            name="arrange",
        )(sums.reshape(8, 64, CHANS))

    return jax.shard_map(
        run_local,
        mesh=mesh,
        in_specs=(P("data", None, None, GROUP_AXES), P(None, None, GROUP_AXES, None), P(), P(), P()),
        out_specs=P("data", "model", "cols", None),
        check_vma=False,
    )
```

```python
import jax
import jax.numpy as jnp
from jax import lax
from jax.experimental import pallas as pl
from jax.experimental.pallas import tpu as pltpu
from jax.sharding import PartitionSpec as P

GROUP_AXES = ("model", "cols")
MESH = pl.DeviceIdType.MESH
BF16 = jnp.bfloat16
F32 = jnp.float32
CHANS = 512
LANES = 128
CUT = 96
VMEM_LIMIT = 36 * 2**20
ORDERS = (("y", "z", "x"), ("z", "x", "y"), ("x", "y", "z"))


def one_hot(shape, col_of_row):
    rows = lax.broadcasted_iota(jnp.int32, shape, 0)
    cols = lax.broadcasted_iota(jnp.int32, shape, 1)
    return jnp.where(cols == col_of_row(rows), 1.0, 0.0).astype(BF16)


def pack_windows(xv, a_scr, pack):
    to_lanes = one_hot((CHANS, CHANS), lambda r: (r % 4) * LANES + ((r % LANES) // 4) * 4 + r // LANES)
    to_rows = one_hot((CHANS, CHANS), lambda r: (r % 4) * LANES + ((r % 256) // 4) * 2 + r // 256)
    for blk in range(4):
        part = jnp.concatenate([xv[n, 32 * blk : 32 * blk + 32].reshape(LANES, LANES) for n in range(4)], axis=0)
        turned = lax.dot_general(part, to_lanes, (((0,), (0,)), ((), ())), preferred_element_type=F32).astype(BF16)
        for c in range(4):
            a_scr[c * LANES : (c + 1) * LANES, blk * LANES : (blk + 1) * LANES] = turned[:, c * LANES : (c + 1) * LANES]
    mixed = jnp.dot(to_rows, a_scr[...], preferred_element_type=F32)
    for blk in range(4):
        even = mixed[0:256, blk * LANES : (blk + 1) * LANES]
        odd = mixed[256:CHANS, blk * LANES : (blk + 1) * LANES]
        for half in range(2):
            s = slice(64 * half, 64 * half + 64)
            tile = jnp.concatenate([even[:, s], odd[:, s]], axis=1).astype(BF16)
            pack[2 * blk + half, 1:65] = tile.reshape(64, 4, LANES)
    edge = jnp.zeros((8, 1, 4, LANES), BF16)
    pack[:, 0:1] = edge
    pack[:, 65:66] = edge


def kernel(
    x_hbm, w1_hbm, w2_hbm, b1_hbm, b2_hbm, o_ref,
    xv, w1v, w2v, b1v, b2v, a_scr, pack, got, x0, x1, x2, edge, w1g, z_acc, y0, y1, y2, acc2,
    load_sem, xs_send, xs_recv, halo_send, halo_recv, step_send, step_recv,
):
    m = lax.axis_index("model")
    q = lax.axis_index("cols")
    me = {"x": m // 2, "z": q // 4, "y": q % 4}
    core = m % 2
    parts = range(3)
    barrier = pltpu.get_barrier_semaphore()

    at_model = [[(me["x"] + dx) % 4 * 2 + (core + dk) % 2 for dk in range(2)] for dx in range(4)]
    at_cols = [[(me["z"] + dz) % 4 * 4 + (me["y"] + dy) % 4 for dy in range(4)] for dz in range(4)]
    others = [(dx, dz, dy, dk) for dx in range(4) for dz in range(4) for dy in range(4) for dk in range(2)]
    others = sorted(others[1:], key=lambda d: (sum(d[:3]) % 4, d))

    def away(d):
        return {"model": at_model[d[0]][d[3]], "cols": at_cols[d[1]][d[2]]}

    loads = [
        pltpu.make_async_copy(src, dst, load_sem.at[k])
        for k, (src, dst) in enumerate(
            ((x_hbm, xv), (w1_hbm, w1v), (w2_hbm, w2v.at[pl.ds(0, 4608)]), (b1_hbm, b1v), (b2_hbm, b2v))
        )
    ]
    for load in loads:
        load.start()
    with jax.named_scope("announce"):
        for d in sorted(others, key=lambda d: -sum(min(o, 4 - o) for o in d[:3])):
            pl.semaphore_signal(barrier, inc=1, device_id=away(d), device_id_type=MESH)

    def piece(p, t, v, n, c, place=None, half=None):
        done = ORDERS[p][:t]
        rest = [a for a in "xzy" if a != ORDERS[p][2]]
        at = [v if t < 2 and a == ORDERS[p][t] else (pl.ds(0, 4) if a in done else me[a]) for a in rest]
        if half is not None:
            at[0] = pl.ds(2 * half, 2)
        return w1g.at[p, pl.ds(0, 2) if n is None else n, me[ORDERS[p][2]] if t < 2 else v, c, at[0], at[1]]

    with jax.named_scope("place_w1"):
        loads[1].wait()
        for p in parts:
            spot = [me[a] for a in "xzy" if a != ORDERS[p][2]]
            for dw in range(3):
                for lt in range(4):
                    tile = w1v[3 * p + dw, :, lt * LANES : (lt + 1) * LANES]
                    w1g[p, lt // 2, me[ORDERS[p][2]], core, spot[0], spot[1], dw, lt % 2] = tile
    with jax.named_scope("wait_x"):
        loads[0].wait()
    with jax.named_scope("pack"):
        pack_windows(xv, a_scr, pack)
    with jax.named_scope("wait_barrier"):
        pl.semaphore_wait(barrier, 127)

    n_steps = [0]
    steps = []

    class Step:
        def __init__(self, slabs, copies):
            k = n_steps[0]
            n_steps[0] += 1
            sems = dict(send_sem=step_send.at[k], recv_sem=step_recv.at[k], device_id_type=MESH)
            self.copies, self.sems = copies, sems
            span = got.at[pl.ds(0, slabs)]
            self.all = pltpu.make_async_remote_copy(
                src_ref=span, dst_ref=span, device_id={"model": at_model[0][1], "cols": q}, **sems
            )
            steps.append(self)

        def go(self):
            for ref, to in self.copies:
                pltpu.make_async_remote_copy(src_ref=ref, dst_ref=ref, device_id=to, **self.sems).start()
            return self

        def land(self):
            self.all.wait_recv()

    def chip(p, t, d, c=0):
        axis = ORDERS[p][t]
        pos = me | {axis: (me[axis] + d) % 4}
        return {"model": pos["x"] * 2 + (core + c) % 2, "cols": pos["z"] * 4 + pos["y"]}

    def spread(t, slabs):
        return Step(slabs, [(piece(p, t, me[ORDERS[p][t]], None, core), chip(p, t, d)) for p in parts for d in (1, 3, 2)]).go()

    def plane(p, d):
        return (me[ORDERS[p][2]] + d) % 4

    def hand_over(pieces, slabs):
        return Step(slabs, [(ref, {"model": at_model[0][1], "cols": q}) for ref in pieces]).go()

    def send_windows(first, last):
        for d in others[first:last]:
            to = away(d)
            pltpu.make_async_remote_copy(
                src_ref=pack.at[to["model"], pl.ds(4 * to["cols"], 6)],
                dst_ref=got.at[mine],
                send_sem=xs_send,
                recv_sem=xs_recv,
                device_id=to,
                device_id_type=MESH,
            ).start()

    mine = ((core * 4 + me["x"]) * 4 + me["z"]) * 4 + me["y"]
    with jax.named_scope("send_first"):
        first = spread(0, 18)
        for pair in range(6):
            got[mine, pair] = pack[m, 4 * q + pair]
        send_windows(0, CUT)
    with jax.named_scope("wait_first"):
        first.land()
    with jax.named_scope("send_second"):
        second = spread(1, 72)
        send_windows(CUT, 127)
    with jax.named_scope("wait_second"):
        second.land()
    last, passed, lent, lent_on = {}, {}, {}, {}

    def send_plane(n):
        last[n] = Step(96, [(piece(p, 2, plane(p, 0), n, core), chip(p, 2, d)) for p in parts for d in (1, 3)])

    def pass_on(n):
        with jax.named_scope(f"wait_last{n}"):
            last[n].land()
        passed[n] = Step(48, [(piece(p, 2, plane(p, 4 - d), n, core, half=d // 2), chip(p, 2, d)) for p in parts for d in (1, 3)]).go()
        lent[n] = hand_over([piece(p, 2, plane(p, d), n, core) for p in parts for d in (1, 3)], 96)

    def finish(n):
        with jax.named_scope(f"wait_passed{n}"):
            passed[n].land()
        lent_on[n] = hand_over([piece(p, 2, plane(p, 2), n, core) for p in parts], 48)

    with jax.named_scope("send_third"):
        for n in range(2):
            send_plane(n)
        own = hand_over([piece(p, 2, plane(p, 0), None, core) for p in parts], 96)

    @pl.when(core == 0)
    def _():
        last[0].go()
        last[1].go()

    span = got.at[pl.ds(0, 127)]
    everything = pltpu.make_async_remote_copy(
        src_ref=span, dst_ref=span, send_sem=xs_send, recv_sem=xs_recv, device_id=chip(0, 0, 0, 1), device_id_type=MESH
    )
    with jax.named_scope("wait_windows"):
        everything.wait_recv()

    @pl.when(core == 1)
    def _():
        last[0].go()
        last[1].go()


    xs, ys = (x0, x1, x2), (y0, y1, y2)
    with jax.named_scope("turn"):
        for pair in range(6):
            for p in parts:
                rows = []
                for v in range(4):
                    for c in range(2):
                        at = 64 * c
                        if p == 0:
                            rows.append(got[at + 16 * v : at + 16 * v + 16, pair])
                        elif p == 1:
                            rows.append(got[at + v : at + 64 : 4, pair])
                        else:
                            rows += [got[at + 16 * a + 4 * v : at + 16 * a + 4 * v + 4, pair] for a in range(4)]
                rows = jnp.concatenate([r.reshape(-1, LANES) for r in rows], axis=0).T
                for odd in range(2):
                    main = rows[64 * odd : 64 * odd + 64]
                    xs[p][2 * pair + odd, 8 - 4 * p : 72 - 4 * p] = main
                    if p == 1:
                        edge[0, 2 * pair + odd] = main[60:64]
                        edge[1, 2 * pair + odd] = main[0:4]
    halo = []
    for src, dst, d in (
        (x0.at[:, pl.ds(64, 8)], x0.at[:, pl.ds(0, 8)], 1),
        (x2.at[:, pl.ds(0, 8)], x2.at[:, pl.ds(64, 8)], 7),
        (edge.at[0], edge.at[2], 1),
        (edge.at[1], edge.at[3], 7),
    ):
        halo.append(
            pltpu.make_async_remote_copy(
                src_ref=src,
                dst_ref=dst,
                send_sem=halo_send.at[len(halo)],
                recv_sem=halo_recv.at[len(halo)],
                device_id={"model": (m + d) % 8, "cols": q},
                device_id_type=MESH,
            )
        )
        halo[-1].start()

    def conv1(halves, places, spans, groups):
        width = 10 // groups
        tops = [None] * groups
        taps = [(p, dw, plane(p, d)) for p in parts for dw in range(3) for d in places]
        for first in range(0, len(taps), 2):
            two = taps[first : first + 2]
            right = [[w1g[p, n, v, :, :, :, dw, i].reshape(LANES, LANES) for n in halves for i in range(2)] for p, dw, v in two]
            right = jnp.concatenate([jnp.concatenate(r, axis=1) for r in right], axis=0)
            for group in range(groups):
                left = []
                for rows in spans:
                    some = []
                    for p, dw, v in two:
                        lanes = pl.ds(pl.multiple_of(LANES * v, LANES), LANES)
                        some.append(xs[p][pl.ds(dw + width * group, width), rows, lanes])
                    left.append(jnp.concatenate(some, axis=-1))
                left = jnp.concatenate(left, axis=1).reshape(-1, LANES * len(two))
                term = jnp.dot(left, right, preferred_element_type=F32)
                tops[group] = term if tops[group] is None else tops[group] + term
        return [top.reshape(width, -1, 256 * len(halves)) for top in tops]

    top_rows, inner, low_rows = pl.ds(0, 8), pl.ds(8, 56), pl.ds(64, 8)

    def here(n):
        with jax.named_scope(f"here{n}"):
            for group, top in enumerate(conv1((n,), (0,), (inner,), 2)):
                z_acc[n, pl.ds(5 * group, 5), inner] = top

    def near(n):
        with jax.named_scope(f"wait_lent{n}"):
            lent[n].land()
        with jax.named_scope(f"near{n}"):
            for group, top in enumerate(conv1((n,), (3, 1), (inner,), 2)):
                z_acc[n, pl.ds(5 * group, 5), inner] += top

    def rim():
        with jax.named_scope("rim"):
            (top,) = conv1((0, 1), (0, 3, 1), (top_rows, low_rows), 1)
            for n in range(2):
                part = top[:, :, 256 * n : 256 * n + 256]
                z_acc[n, :, top_rows] = part[:, :8]
                z_acc[n, :, low_rows] = part[:, 8:]

    def far(n):
        with jax.named_scope(f"wait_lent_on{n}"):
            lent_on[n].land()
        lanes = slice(256 * n, 256 * n + 256)
        with jax.named_scope(f"far{n}"):
            for group, top in enumerate(conv1((n,), (2,), (pl.ds(0, 72),), 2)):
                cols = pl.ds(5 * group, 5)
                act = jnp.maximum(z_acc[n, cols] + top + b1v[:, lanes], 0.0)
                for dh in range(3):
                    ys[dh][cols, :, lanes] = act[:, 4 * dh : 4 * dh + 64].astype(BF16)

        def clear(at_edge, refs, cols, rows):
            @pl.when(at_edge)
            def _():
                for ref in refs:
                    ref[cols, rows, lanes] = jnp.zeros((cols.size, rows.size, 256), BF16)

        clear(q == 0, ys, pl.ds(0, 1), pl.ds(0, 64))
        clear(q == 15, ys, pl.ds(9, 1), pl.ds(0, 64))
        clear(m == 0, (y0,), pl.ds(0, 10), pl.ds(0, 4))
        clear(m == 7, (y2,), pl.ds(0, 10), pl.ds(60, 4))

    def conv2(n):
        lanes = slice(256 * n, 256 * n + 256)
        total = None
        for dh in range(3):
            for dw in range(3):
                tap = 3 * dh + dw
                left = ys[dh][dw : dw + 8, :, lanes].reshape(CHANS, 256)
                right = w2v[CHANS * tap + 256 * n : CHANS * tap + 256 * n + 256, :]
                term = jnp.dot(left, right, preferred_element_type=F32)
                total = term if total is None else total + term
        return total

    pass_on(0)
    with jax.named_scope("wait_own"):
        own.land()
    here(0)
    here(1)
    pass_on(1)
    near(0)
    near(1)
    finish(0)
    with jax.named_scope("wait_halo"):
        for copy in halo:
            copy.wait_recv()

    @pl.when(m == 0)
    def _():
        x0[:, 0:8] = jnp.zeros((12, 8, CHANS), BF16)
        x1[:, 0:4] = jnp.zeros((12, 4, CHANS), BF16)

    @pl.when(m > 0)
    def _():
        x1[:, 0:4] = edge[2]

    @pl.when(m == 7)
    def _():
        x2[:, 64:72] = jnp.zeros((12, 8, CHANS), BF16)
        x1[:, 68:72] = jnp.zeros((12, 4, CHANS), BF16)

    @pl.when(m < 7)
    def _():
        x1[:, 68:72] = edge[3]

    rim()
    finish(1)
    with jax.named_scope("wait_w2"):
        for load in loads[2:]:
            load.wait()
    far(0)
    with jax.named_scope("conv2_0"):
        acc2[...] = conv2(0)
    far(1)
    with jax.named_scope("conv2_1"):
        o_ref[...] = acc2[...] + conv2(1) + b2v[...]

    with jax.named_scope("wait_sends"):
        everything.wait_send()
        for step in steps:
            step.all.wait_send()
        for copy in halo:
            copy.wait_send()


def arrange(sum_ref, o_hbm, turned, sems):
    copies = []
    for g in range(4):
        rows = jnp.transpose(sum_ref[:, 16 * g : 16 * g + 16], (1, 0, 2))
        for h in range(4):
            for image in range(4):
                turned[g, image, h] = rows[4 * h + image]
        copies.append(pltpu.make_async_copy(turned.at[g], o_hbm.at[:, pl.ds(4 * g, 4)], sems.at[g]))
        copies[-1].start()
    for copy in copies:
        copy.wait()


def solution(mesh):
    scratch = [
        pltpu.VMEM((4, LANES, 4, LANES), BF16),
        pltpu.VMEM((9, 4, CHANS), BF16),
        pltpu.VMEM((4616, CHANS), BF16),
        pltpu.VMEM((1, CHANS), F32),
        pltpu.VMEM((1, CHANS), F32),
        pltpu.VMEM((CHANS, CHANS), BF16),
        pltpu.VMEM((8, 66, 4, LANES), BF16),
        pltpu.VMEM((LANES, 6, 4, LANES), BF16),
        *[pltpu.VMEM((12, 72, CHANS), BF16) for _ in range(3)],
        pltpu.VMEM((4, 12, 4, CHANS), BF16),
        pltpu.VMEM((3, 2, 4, 2, 4, 4, 3, 2, 4, LANES), BF16),
        pltpu.VMEM((2, 10, 72, 256), F32),
        *[pltpu.VMEM((10, 64, CHANS), BF16) for _ in range(3)],
        pltpu.VMEM((CHANS, CHANS), F32),
        pltpu.SemaphoreType.DMA((5,)),
        pltpu.SemaphoreType.DMA,
        pltpu.SemaphoreType.DMA,
        pltpu.SemaphoreType.DMA((4,)),
        pltpu.SemaphoreType.DMA((4,)),
        pltpu.SemaphoreType.DMA((11,)),
        pltpu.SemaphoreType.DMA((11,)),
    ]
    vmem = pl.BlockSpec(memory_space=pltpu.VMEM)
    anywhere = pl.BlockSpec(memory_space=pl.ANY)

    def run_local(x_in, w_conv1, b_conv1, w_conv2, b_conv2):
        sums = pl.pallas_call(
            kernel,
            out_shape=jax.ShapeDtypeStruct((CHANS, CHANS), F32),
            in_specs=[anywhere] * 5,
            out_specs=vmem,
            scratch_shapes=scratch,
            compiler_params=pltpu.CompilerParams(collective_id=0, has_side_effects=True, vmem_limit_bytes=VMEM_LIMIT),
            name="two_convs",
        )(
            *(
                pltpu.with_memory_space_constraint(a, pltpu.HBM)
                for a in (
                    x_in.transpose(0, 1, 3, 2),
                    w_conv1.reshape(9, 4, CHANS),
                    w_conv2.reshape(4608, CHANS),
                    b_conv1.reshape(1, CHANS),
                    b_conv2.reshape(1, CHANS),
                )
            )
        )
        return pl.pallas_call(
            arrange,
            out_shape=jax.ShapeDtypeStruct((4, 16, 8, CHANS), F32),
            in_specs=[vmem],
            out_specs=anywhere,
            scratch_shapes=[pltpu.VMEM((4, 4, 4, 8, CHANS), F32), pltpu.SemaphoreType.DMA((4,))],
            compiler_params=pltpu.CompilerParams(vmem_limit_bytes=8 * 2**20),
            name="arrange",
        )(sums.reshape(8, 64, CHANS))

    return jax.shard_map(
        run_local,
        mesh=mesh,
        in_specs=(P("data", None, None, GROUP_AXES), P(None, None, GROUP_AXES, None), P(), P(), P()),
        out_specs=P("data", "model", "cols", None),
        check_vma=False,
    )
```

```python
import jax
import jax.numpy as jnp
from jax import lax
from jax.experimental import pallas as pl
from jax.experimental.pallas import tpu as pltpu
from jax.sharding import PartitionSpec as P

GROUP_AXES = ("model", "cols")
MESH = pl.DeviceIdType.MESH
BF16 = jnp.bfloat16
F32 = jnp.float32
CHANS = 512
LANES = 128
CUT = 96
VMEM_LIMIT = 36 * 2**20
ORDERS = (("y", "z", "x"), ("z", "x", "y"), ("x", "y", "z"))


def one_hot(shape, col_of_row):
    rows = lax.broadcasted_iota(jnp.int32, shape, 0)
    cols = lax.broadcasted_iota(jnp.int32, shape, 1)
    return jnp.where(cols == col_of_row(rows), 1.0, 0.0).astype(BF16)


def pack_windows(xv, a_scr, pack):
    to_lanes = one_hot((CHANS, CHANS), lambda r: (r % 4) * LANES + ((r % LANES) // 4) * 4 + r // LANES)
    to_rows = one_hot((CHANS, CHANS), lambda r: (r % 4) * LANES + ((r % 256) // 4) * 2 + r // 256)
    for blk in range(4):
        part = jnp.concatenate([xv[n, 32 * blk : 32 * blk + 32].reshape(LANES, LANES) for n in range(4)], axis=0)
        turned = lax.dot_general(part, to_lanes, (((0,), (0,)), ((), ())), preferred_element_type=F32).astype(BF16)
        for c in range(4):
            a_scr[c * LANES : (c + 1) * LANES, blk * LANES : (blk + 1) * LANES] = turned[:, c * LANES : (c + 1) * LANES]
    mixed = jnp.dot(to_rows, a_scr[...], preferred_element_type=F32)
    for blk in range(4):
        even = mixed[0:256, blk * LANES : (blk + 1) * LANES]
        odd = mixed[256:CHANS, blk * LANES : (blk + 1) * LANES]
        for half in range(2):
            s = slice(64 * half, 64 * half + 64)
            tile = jnp.concatenate([even[:, s], odd[:, s]], axis=1).astype(BF16)
            pack[2 * blk + half, 1:65] = tile.reshape(64, 4, LANES)
    edge = jnp.zeros((8, 1, 4, LANES), BF16)
    pack[:, 0:1] = edge
    pack[:, 65:66] = edge


def kernel(
    x_hbm, w1_hbm, w2_hbm, b1_hbm, b2_hbm, o_ref,
    xv, w1v, w2v, b1v, b2v, a_scr, pack, got, x0, x1, x2, edge, w1g, z_acc, y0, y1, y2, acc2,
    load_sem, xs_send, xs_recv, halo_send, halo_recv, step_send, step_recv,
):
    m = lax.axis_index("model")
    q = lax.axis_index("cols")
    me = {"x": m // 2, "z": q // 4, "y": q % 4}
    core = m % 2
    parts = range(3)
    barrier = pltpu.get_barrier_semaphore()

    at_model = [[(me["x"] + dx) % 4 * 2 + (core + dk) % 2 for dk in range(2)] for dx in range(4)]
    at_cols = [[(me["z"] + dz) % 4 * 4 + (me["y"] + dy) % 4 for dy in range(4)] for dz in range(4)]
    others = [(dx, dz, dy, dk) for dx in range(4) for dz in range(4) for dy in range(4) for dk in range(2)]
    others = sorted(others[1:], key=lambda d: (sum(d[:3]) % 4, d))

    def away(d):
        return {"model": at_model[d[0]][d[3]], "cols": at_cols[d[1]][d[2]]}

    loads = [
        pltpu.make_async_copy(src, dst, load_sem.at[k])
        for k, (src, dst) in enumerate(
            ((x_hbm, xv), (w1_hbm, w1v), (w2_hbm, w2v.at[pl.ds(0, 4608)]), (b1_hbm, b1v), (b2_hbm, b2v))
        )
    ]
    for load in loads:
        load.start()
    with jax.named_scope("announce"):
        for d in sorted(others, key=lambda d: -sum(min(o, 4 - o) for o in d[:3])):
            pl.semaphore_signal(barrier, inc=1, device_id=away(d), device_id_type=MESH)

    def piece(p, t, v, n, c, place=None, half=None):
        done = ORDERS[p][:t]
        rest = [a for a in "xzy" if a != ORDERS[p][2]]
        at = [v if t < 2 and a == ORDERS[p][t] else (pl.ds(0, 4) if a in done else me[a]) for a in rest]
        if half is not None:
            at[0] = pl.ds(2 * half, 2)
        return w1g.at[p, pl.ds(0, 2) if n is None else n, me[ORDERS[p][2]] if t < 2 else v, c, at[0], at[1]]

    with jax.named_scope("place_w1"):
        loads[1].wait()
        for p in parts:
            spot = [me[a] for a in "xzy" if a != ORDERS[p][2]]
            for dw in range(3):
                for lt in range(4):
                    tile = w1v[3 * p + dw, :, lt * LANES : (lt + 1) * LANES]
                    w1g[p, lt // 2, me[ORDERS[p][2]], core, spot[0], spot[1], dw, lt % 2] = tile
    with jax.named_scope("wait_x"):
        loads[0].wait()
    with jax.named_scope("pack"):
        pack_windows(xv, a_scr, pack)
    with jax.named_scope("wait_barrier"):
        pl.semaphore_wait(barrier, 127)

    n_steps = [0]
    steps = []

    class Step:
        def __init__(self, slabs, copies):
            k = n_steps[0]
            n_steps[0] += 1
            sems = dict(send_sem=step_send.at[k], recv_sem=step_recv.at[k], device_id_type=MESH)
            self.copies, self.sems = copies, sems
            span = got.at[pl.ds(0, slabs)]
            self.all = pltpu.make_async_remote_copy(
                src_ref=span, dst_ref=span, device_id={"model": at_model[0][1], "cols": q}, **sems
            )
            steps.append(self)

        def go(self):
            for ref, to in self.copies:
                pltpu.make_async_remote_copy(src_ref=ref, dst_ref=ref, device_id=to, **self.sems).start()
            return self

        def land(self):
            self.all.wait_recv()

    def chip(p, t, d, c=0):
        axis = ORDERS[p][t]
        pos = me | {axis: (me[axis] + d) % 4}
        return {"model": pos["x"] * 2 + (core + c) % 2, "cols": pos["z"] * 4 + pos["y"]}

    def spread(t, slabs):
        return Step(slabs, [(piece(p, t, me[ORDERS[p][t]], None, core), chip(p, t, d)) for p in parts for d in (1, 3, 2)]).go()

    def plane(p, d):
        return (me[ORDERS[p][2]] + d) % 4

    def hand_over(pieces, slabs):
        return Step(slabs, [(ref, {"model": at_model[0][1], "cols": q}) for ref in pieces]).go()

    def send_windows(first, last):
        for d in others[first:last]:
            to = away(d)
            pltpu.make_async_remote_copy(
                src_ref=pack.at[to["model"], pl.ds(4 * to["cols"], 6)],
                dst_ref=got.at[mine],
                send_sem=xs_send,
                recv_sem=xs_recv,
                device_id=to,
                device_id_type=MESH,
            ).start()

    mine = ((core * 4 + me["x"]) * 4 + me["z"]) * 4 + me["y"]
    with jax.named_scope("send_first"):
        first = spread(0, 18)
        for pair in range(6):
            got[mine, pair] = pack[m, 4 * q + pair]
        send_windows(0, CUT)
    with jax.named_scope("wait_first"):
        first.land()
    with jax.named_scope("send_second"):
        second = spread(1, 72)
        send_windows(CUT, 127)
    with jax.named_scope("wait_second"):
        second.land()
    last, passed, lent, lent_on = {}, {}, {}, {}

    def send_plane(n):
        last[n] = Step(96, [(piece(p, 2, plane(p, 0), n, core), chip(p, 2, d)) for p in parts for d in (1, 3)])

    def pass_on(n):
        with jax.named_scope(f"wait_last{n}"):
            last[n].land()
        passed[n] = Step(48, [(piece(p, 2, plane(p, 4 - d), n, core, half=d // 2), chip(p, 2, d)) for p in parts for d in (1, 3)]).go()
        lent[n] = hand_over([piece(p, 2, plane(p, d), n, core) for p in parts for d in (1, 3)], 96)

    def finish(n):
        with jax.named_scope(f"wait_passed{n}"):
            passed[n].land()
        lent_on[n] = hand_over([piece(p, 2, plane(p, 2), n, core) for p in parts], 48)

    with jax.named_scope("send_third"):
        for n in range(2):
            send_plane(n)
        last[0].go()
        own = hand_over([piece(p, 2, plane(p, 0), None, core) for p in parts], 96)

    @pl.when(core == 0)
    def _():
        last[1].go()

    span = got.at[pl.ds(0, 127)]
    everything = pltpu.make_async_remote_copy(
        src_ref=span, dst_ref=span, send_sem=xs_send, recv_sem=xs_recv, device_id=chip(0, 0, 0, 1), device_id_type=MESH
    )
    with jax.named_scope("wait_windows"):
        everything.wait_recv()

    @pl.when(core == 1)
    def _():
        last[1].go()


    xs, ys = (x0, x1, x2), (y0, y1, y2)
    with jax.named_scope("turn"):
        for pair in range(6):
            for p in parts:
                rows = []
                for v in range(4):
                    for c in range(2):
                        at = 64 * c
                        if p == 0:
                            rows.append(got[at + 16 * v : at + 16 * v + 16, pair])
                        elif p == 1:
                            rows.append(got[at + v : at + 64 : 4, pair])
                        else:
                            rows += [got[at + 16 * a + 4 * v : at + 16 * a + 4 * v + 4, pair] for a in range(4)]
                rows = jnp.concatenate([r.reshape(-1, LANES) for r in rows], axis=0).T
                for odd in range(2):
                    main = rows[64 * odd : 64 * odd + 64]
                    xs[p][2 * pair + odd, 8 - 4 * p : 72 - 4 * p] = main
                    if p == 1:
                        edge[0, 2 * pair + odd] = main[60:64]
                        edge[1, 2 * pair + odd] = main[0:4]
    halo = []
    for src, dst, d in (
        (x0.at[:, pl.ds(64, 8)], x0.at[:, pl.ds(0, 8)], 1),
        (x2.at[:, pl.ds(0, 8)], x2.at[:, pl.ds(64, 8)], 7),
        (edge.at[0], edge.at[2], 1),
        (edge.at[1], edge.at[3], 7),
    ):
        halo.append(
            pltpu.make_async_remote_copy(
                src_ref=src,
                dst_ref=dst,
                send_sem=halo_send.at[len(halo)],
                recv_sem=halo_recv.at[len(halo)],
                device_id={"model": (m + d) % 8, "cols": q},
                device_id_type=MESH,
            )
        )
        halo[-1].start()

    def conv1(halves, places, spans, groups):
        width = 10 // groups
        tops = [None] * groups
        taps = [(p, dw, plane(p, d)) for p in parts for dw in range(3) for d in places]
        for first in range(0, len(taps), 2):
            two = taps[first : first + 2]
            right = [[w1g[p, n, v, :, :, :, dw, i].reshape(LANES, LANES) for n in halves for i in range(2)] for p, dw, v in two]
            right = jnp.concatenate([jnp.concatenate(r, axis=1) for r in right], axis=0)
            for group in range(groups):
                left = []
                for rows in spans:
                    some = []
                    for p, dw, v in two:
                        lanes = pl.ds(pl.multiple_of(LANES * v, LANES), LANES)
                        some.append(xs[p][pl.ds(dw + width * group, width), rows, lanes])
                    left.append(jnp.concatenate(some, axis=-1))
                left = jnp.concatenate(left, axis=1).reshape(-1, LANES * len(two))
                term = jnp.dot(left, right, preferred_element_type=F32)
                tops[group] = term if tops[group] is None else tops[group] + term
        return [top.reshape(width, -1, 256 * len(halves)) for top in tops]

    top_rows, inner, low_rows = pl.ds(0, 8), pl.ds(8, 56), pl.ds(64, 8)

    def here(n):
        with jax.named_scope(f"here{n}"):
            for group, top in enumerate(conv1((n,), (0,), (inner,), 2)):
                z_acc[n, pl.ds(5 * group, 5), inner] = top

    def near(n):
        with jax.named_scope(f"wait_lent{n}"):
            lent[n].land()
        with jax.named_scope(f"near{n}"):
            for group, top in enumerate(conv1((n,), (3, 1), (inner,), 2)):
                z_acc[n, pl.ds(5 * group, 5), inner] += top

    def rim():
        with jax.named_scope("rim"):
            (top,) = conv1((0, 1), (0, 3, 1), (top_rows, low_rows), 1)
            for n in range(2):
                part = top[:, :, 256 * n : 256 * n + 256]
                z_acc[n, :, top_rows] = part[:, :8]
                z_acc[n, :, low_rows] = part[:, 8:]

    def far(n):
        with jax.named_scope(f"wait_lent_on{n}"):
            lent_on[n].land()
        lanes = slice(256 * n, 256 * n + 256)
        with jax.named_scope(f"far{n}"):
            for group, top in enumerate(conv1((n,), (2,), (pl.ds(0, 72),), 2)):
                cols = pl.ds(5 * group, 5)
                act = jnp.maximum(z_acc[n, cols] + top + b1v[:, lanes], 0.0)
                for dh in range(3):
                    ys[dh][cols, :, lanes] = act[:, 4 * dh : 4 * dh + 64].astype(BF16)

        def clear(at_edge, refs, cols, rows):
            @pl.when(at_edge)
            def _():
                for ref in refs:
                    ref[cols, rows, lanes] = jnp.zeros((cols.size, rows.size, 256), BF16)

        clear(q == 0, ys, pl.ds(0, 1), pl.ds(0, 64))
        clear(q == 15, ys, pl.ds(9, 1), pl.ds(0, 64))
        clear(m == 0, (y0,), pl.ds(0, 10), pl.ds(0, 4))
        clear(m == 7, (y2,), pl.ds(0, 10), pl.ds(60, 4))

    def conv2(n):
        lanes = slice(256 * n, 256 * n + 256)
        total = None
        for dh in range(3):
            for dw in range(3):
                tap = 3 * dh + dw
                left = ys[dh][dw : dw + 8, :, lanes].reshape(CHANS, 256)
                right = w2v[CHANS * tap + 256 * n : CHANS * tap + 256 * n + 256, :]
                term = jnp.dot(left, right, preferred_element_type=F32)
                total = term if total is None else total + term
        return total

    pass_on(0)
    with jax.named_scope("wait_own"):
        own.land()
    here(0)
    here(1)
    pass_on(1)
    near(0)
    near(1)
    finish(0)
    with jax.named_scope("wait_halo"):
        for copy in halo:
            copy.wait_recv()

    @pl.when(m == 0)
    def _():
        x0[:, 0:8] = jnp.zeros((12, 8, CHANS), BF16)
        x1[:, 0:4] = jnp.zeros((12, 4, CHANS), BF16)

    @pl.when(m > 0)
    def _():
        x1[:, 0:4] = edge[2]

    @pl.when(m == 7)
    def _():
        x2[:, 64:72] = jnp.zeros((12, 8, CHANS), BF16)
        x1[:, 68:72] = jnp.zeros((12, 4, CHANS), BF16)

    @pl.when(m < 7)
    def _():
        x1[:, 68:72] = edge[3]

    rim()
    finish(1)
    with jax.named_scope("wait_w2"):
        for load in loads[2:]:
            load.wait()
    far(0)
    with jax.named_scope("conv2_0"):
        acc2[...] = conv2(0)
    far(1)
    with jax.named_scope("conv2_1"):
        o_ref[...] = acc2[...] + conv2(1) + b2v[...]

    with jax.named_scope("wait_sends"):
        everything.wait_send()
        for step in steps:
            step.all.wait_send()
        for copy in halo:
            copy.wait_send()


def arrange(sum_ref, o_hbm, turned, sems):
    copies = []
    for g in range(4):
        rows = jnp.transpose(sum_ref[:, 16 * g : 16 * g + 16], (1, 0, 2))
        for h in range(4):
            for image in range(4):
                turned[g, image, h] = rows[4 * h + image]
        copies.append(pltpu.make_async_copy(turned.at[g], o_hbm.at[:, pl.ds(4 * g, 4)], sems.at[g]))
        copies[-1].start()
    for copy in copies:
        copy.wait()


def solution(mesh):
    scratch = [
        pltpu.VMEM((4, LANES, 4, LANES), BF16),
        pltpu.VMEM((9, 4, CHANS), BF16),
        pltpu.VMEM((4616, CHANS), BF16),
        pltpu.VMEM((1, CHANS), F32),
        pltpu.VMEM((1, CHANS), F32),
        pltpu.VMEM((CHANS, CHANS), BF16),
        pltpu.VMEM((8, 66, 4, LANES), BF16),
        pltpu.VMEM((LANES, 6, 4, LANES), BF16),
        *[pltpu.VMEM((12, 72, CHANS), BF16) for _ in range(3)],
        pltpu.VMEM((4, 12, 4, CHANS), BF16),
        pltpu.VMEM((3, 2, 4, 2, 4, 4, 3, 2, 4, LANES), BF16),
        pltpu.VMEM((2, 10, 72, 256), F32),
        *[pltpu.VMEM((10, 64, CHANS), BF16) for _ in range(3)],
        pltpu.VMEM((CHANS, CHANS), F32),
        pltpu.SemaphoreType.DMA((5,)),
        pltpu.SemaphoreType.DMA,
        pltpu.SemaphoreType.DMA,
        pltpu.SemaphoreType.DMA((4,)),
        pltpu.SemaphoreType.DMA((4,)),
        pltpu.SemaphoreType.DMA((11,)),
        pltpu.SemaphoreType.DMA((11,)),
    ]
    vmem = pl.BlockSpec(memory_space=pltpu.VMEM)
    anywhere = pl.BlockSpec(memory_space=pl.ANY)

    def run_local(x_in, w_conv1, b_conv1, w_conv2, b_conv2):
        sums = pl.pallas_call(
            kernel,
            out_shape=jax.ShapeDtypeStruct((CHANS, CHANS), F32),
            in_specs=[anywhere] * 5,
            out_specs=vmem,
            scratch_shapes=scratch,
            compiler_params=pltpu.CompilerParams(collective_id=0, has_side_effects=True, vmem_limit_bytes=VMEM_LIMIT),
            name="two_convs",
        )(
            *(
                pltpu.with_memory_space_constraint(a, pltpu.HBM)
                for a in (
                    x_in.transpose(0, 1, 3, 2),
                    w_conv1.reshape(9, 4, CHANS),
                    w_conv2.reshape(4608, CHANS),
                    b_conv1.reshape(1, CHANS),
                    b_conv2.reshape(1, CHANS),
                )
            )
        )
        return pl.pallas_call(
            arrange,
            out_shape=jax.ShapeDtypeStruct((4, 16, 8, CHANS), F32),
            in_specs=[vmem],
            out_specs=anywhere,
            scratch_shapes=[pltpu.VMEM((4, 4, 4, 8, CHANS), F32), pltpu.SemaphoreType.DMA((4,))],
            compiler_params=pltpu.CompilerParams(vmem_limit_bytes=8 * 2**20),
            name="arrange",
        )(sums.reshape(8, 64, CHANS))

    return jax.shard_map(
        run_local,
        mesh=mesh,
        in_specs=(P("data", None, None, GROUP_AXES), P(None, None, GROUP_AXES, None), P(), P(), P()),
        out_specs=P("data", "model", "cols", None),
        check_vma=False,
    )
```

```python
import jax
import jax.numpy as jnp
from jax import lax
from jax.experimental import pallas as pl
from jax.experimental.pallas import tpu as pltpu
from jax.sharding import PartitionSpec as P

GROUP_AXES = ("model", "cols")
MESH = pl.DeviceIdType.MESH
BF16 = jnp.bfloat16
F32 = jnp.float32
CHANS = 512
LANES = 128
CUT = 96
VMEM_LIMIT = 36 * 2**20
ORDERS = (("y", "z", "x"), ("z", "x", "y"), ("x", "y", "z"))


def one_hot(shape, col_of_row):
    rows = lax.broadcasted_iota(jnp.int32, shape, 0)
    cols = lax.broadcasted_iota(jnp.int32, shape, 1)
    return jnp.where(cols == col_of_row(rows), 1.0, 0.0).astype(BF16)


def pack_windows(xv, a_scr, pack):
    to_lanes = one_hot((CHANS, CHANS), lambda r: (r % 4) * LANES + ((r % LANES) // 4) * 4 + r // LANES)
    to_rows = one_hot((CHANS, CHANS), lambda r: (r % 4) * LANES + ((r % 256) // 4) * 2 + r // 256)
    for blk in range(4):
        part = jnp.concatenate([xv[n, 32 * blk : 32 * blk + 32].reshape(LANES, LANES) for n in range(4)], axis=0)
        turned = lax.dot_general(part, to_lanes, (((0,), (0,)), ((), ())), preferred_element_type=F32).astype(BF16)
        for c in range(4):
            a_scr[c * LANES : (c + 1) * LANES, blk * LANES : (blk + 1) * LANES] = turned[:, c * LANES : (c + 1) * LANES]
    mixed = jnp.dot(to_rows, a_scr[...], preferred_element_type=F32)
    for blk in range(4):
        even = mixed[0:256, blk * LANES : (blk + 1) * LANES]
        odd = mixed[256:CHANS, blk * LANES : (blk + 1) * LANES]
        for half in range(2):
            s = slice(64 * half, 64 * half + 64)
            tile = jnp.concatenate([even[:, s], odd[:, s]], axis=1).astype(BF16)
            pack[2 * blk + half, 1:65] = tile.reshape(64, 4, LANES)
    edge = jnp.zeros((8, 1, 4, LANES), BF16)
    pack[:, 0:1] = edge
    pack[:, 65:66] = edge


def kernel(
    x_hbm, w1_hbm, w2_hbm, b1_hbm, b2_hbm, o_ref,
    xv, w1v, w2v, b1v, b2v, a_scr, pack, got, x0, x1, x2, edge, w1g, z_acc, y0, y1, y2, acc2,
    load_sem, xs_send, xs_recv, halo_send, halo_recv, step_send, step_recv,
):
    m = lax.axis_index("model")
    q = lax.axis_index("cols")
    me = {"x": m // 2, "z": q // 4, "y": q % 4}
    core = m % 2
    parts = range(3)

    at_model = [[(me["x"] + dx) % 4 * 2 + (core + dk) % 2 for dk in range(2)] for dx in range(4)]
    at_cols = [[(me["z"] + dz) % 4 * 4 + (me["y"] + dy) % 4 for dy in range(4)] for dz in range(4)]
    others = [(dx, dz, dy, dk) for dx in range(4) for dz in range(4) for dy in range(4) for dk in range(2)]
    others = sorted(others[1:], key=lambda d: (sum(d[:3]) % 4, d))

    def away(d):
        return {"model": at_model[d[0]][d[3]], "cols": at_cols[d[1]][d[2]]}

    loads = [
        pltpu.make_async_copy(src, dst, load_sem.at[k])
        for k, (src, dst) in enumerate(
            ((x_hbm, xv), (w1_hbm, w1v), (w2_hbm, w2v.at[pl.ds(0, 4608)]), (b1_hbm, b1v), (b2_hbm, b2v))
        )
    ]
    for load in loads:
        load.start()
    def piece(p, t, v, n, c, place=None, half=None):
        done = ORDERS[p][:t]
        rest = [a for a in "xzy" if a != ORDERS[p][2]]
        at = [v if t < 2 and a == ORDERS[p][t] else (pl.ds(0, 4) if a in done else me[a]) for a in rest]
        if half is not None:
            at[0] = pl.ds(2 * half, 2)
        return w1g.at[p, pl.ds(0, 2) if n is None else n, me[ORDERS[p][2]] if t < 2 else v, c, at[0], at[1]]

    with jax.named_scope("place_w1"):
        loads[1].wait()
        for p in parts:
            spot = [me[a] for a in "xzy" if a != ORDERS[p][2]]
            for dw in range(3):
                for lt in range(4):
                    tile = w1v[3 * p + dw, :, lt * LANES : (lt + 1) * LANES]
                    w1g[p, lt // 2, me[ORDERS[p][2]], core, spot[0], spot[1], dw, lt % 2] = tile
    with jax.named_scope("wait_x"):
        loads[0].wait()
    with jax.named_scope("pack"):
        pack_windows(xv, a_scr, pack)

    n_steps = [0]
    steps = []

    class Step:
        def __init__(self, slabs, copies):
            k = n_steps[0]
            n_steps[0] += 1
            sems = dict(send_sem=step_send.at[k], recv_sem=step_recv.at[k], device_id_type=MESH)
            self.copies, self.sems = copies, sems
            span = got.at[pl.ds(0, slabs)]
            self.all = pltpu.make_async_remote_copy(
                src_ref=span, dst_ref=span, device_id={"model": at_model[0][1], "cols": q}, **sems
            )
            steps.append(self)

        def go(self):
            for ref, to in self.copies:
                pltpu.make_async_remote_copy(src_ref=ref, dst_ref=ref, device_id=to, **self.sems).start()
            return self

        def land(self):
            self.all.wait_recv()

    def chip(p, t, d, c=0):
        axis = ORDERS[p][t]
        pos = me | {axis: (me[axis] + d) % 4}
        return {"model": pos["x"] * 2 + (core + c) % 2, "cols": pos["z"] * 4 + pos["y"]}

    def spread(t, slabs):
        return Step(slabs, [(piece(p, t, me[ORDERS[p][t]], None, core), chip(p, t, d)) for p in parts for d in (1, 3, 2)]).go()

    def plane(p, d):
        return (me[ORDERS[p][2]] + d) % 4

    def hand_over(pieces, slabs):
        return Step(slabs, [(ref, {"model": at_model[0][1], "cols": q}) for ref in pieces]).go()

    def send_windows(first, last):
        for d in others[first:last]:
            to = away(d)
            pltpu.make_async_remote_copy(
                src_ref=pack.at[to["model"], pl.ds(4 * to["cols"], 6)],
                dst_ref=got.at[mine],
                send_sem=xs_send,
                recv_sem=xs_recv,
                device_id=to,
                device_id_type=MESH,
            ).start()

    mine = ((core * 4 + me["x"]) * 4 + me["z"]) * 4 + me["y"]
    with jax.named_scope("send_first"):
        first = spread(0, 18)
        for pair in range(6):
            got[mine, pair] = pack[m, 4 * q + pair]
        send_windows(0, CUT)
    with jax.named_scope("wait_first"):
        first.land()
    with jax.named_scope("send_second"):
        second = spread(1, 72)
        send_windows(CUT, 127)
    with jax.named_scope("wait_second"):
        second.land()
    last, passed, lent, lent_on = {}, {}, {}, {}

    def send_plane(n):
        last[n] = Step(96, [(piece(p, 2, plane(p, 0), n, core), chip(p, 2, d)) for p in parts for d in (1, 3)])

    def pass_on(n):
        with jax.named_scope(f"wait_last{n}"):
            last[n].land()
        passed[n] = Step(48, [(piece(p, 2, plane(p, 4 - d), n, core, half=d // 2), chip(p, 2, d)) for p in parts for d in (1, 3)]).go()
        lent[n] = hand_over([piece(p, 2, plane(p, d), n, core) for p in parts for d in (1, 3)], 96)

    def finish(n):
        with jax.named_scope(f"wait_passed{n}"):
            passed[n].land()
        lent_on[n] = hand_over([piece(p, 2, plane(p, 2), n, core) for p in parts], 48)

    with jax.named_scope("send_third"):
        for n in range(2):
            send_plane(n)
        last[0].go()
        own = hand_over([piece(p, 2, plane(p, 0), None, core) for p in parts], 96)
    last[1].go()
    span = got.at[pl.ds(0, 127)]
    everything = pltpu.make_async_remote_copy(
        src_ref=span, dst_ref=span, send_sem=xs_send, recv_sem=xs_recv, device_id=chip(0, 0, 0, 1), device_id_type=MESH
    )
    with jax.named_scope("wait_windows"):
        everything.wait_recv()

    xs, ys = (x0, x1, x2), (y0, y1, y2)
    with jax.named_scope("turn"):
        for pair in range(6):
            for p in parts:
                rows = []
                for v in range(4):
                    for c in range(2):
                        at = 64 * c
                        if p == 0:
                            rows.append(got[at + 16 * v : at + 16 * v + 16, pair])
                        elif p == 1:
                            rows.append(got[at + v : at + 64 : 4, pair])
                        else:
                            rows += [got[at + 16 * a + 4 * v : at + 16 * a + 4 * v + 4, pair] for a in range(4)]
                rows = jnp.concatenate([r.reshape(-1, LANES) for r in rows], axis=0).T
                for odd in range(2):
                    main = rows[64 * odd : 64 * odd + 64]
                    xs[p][2 * pair + odd, 8 - 4 * p : 72 - 4 * p] = main
                    if p == 1:
                        edge[0, 2 * pair + odd] = main[60:64]
                        edge[1, 2 * pair + odd] = main[0:4]
    halo = []
    for src, dst, d in (
        (x0.at[:, pl.ds(64, 8)], x0.at[:, pl.ds(0, 8)], 1),
        (x2.at[:, pl.ds(0, 8)], x2.at[:, pl.ds(64, 8)], 7),
        (edge.at[0], edge.at[2], 1),
        (edge.at[1], edge.at[3], 7),
    ):
        halo.append(
            pltpu.make_async_remote_copy(
                src_ref=src,
                dst_ref=dst,
                send_sem=halo_send.at[len(halo)],
                recv_sem=halo_recv.at[len(halo)],
                device_id={"model": (m + d) % 8, "cols": q},
                device_id_type=MESH,
            )
        )
        halo[-1].start()

    def conv1(halves, places, spans, groups):
        width = 10 // groups
        tops = [None] * groups
        taps = [(p, dw, plane(p, d)) for p in parts for dw in range(3) for d in places]
        for first in range(0, len(taps), 2):
            two = taps[first : first + 2]
            right = [[w1g[p, n, v, :, :, :, dw, i].reshape(LANES, LANES) for n in halves for i in range(2)] for p, dw, v in two]
            right = jnp.concatenate([jnp.concatenate(r, axis=1) for r in right], axis=0)
            for group in range(groups):
                left = []
                for rows in spans:
                    some = []
                    for p, dw, v in two:
                        lanes = pl.ds(pl.multiple_of(LANES * v, LANES), LANES)
                        some.append(xs[p][pl.ds(dw + width * group, width), rows, lanes])
                    left.append(jnp.concatenate(some, axis=-1))
                left = jnp.concatenate(left, axis=1).reshape(-1, LANES * len(two))
                term = jnp.dot(left, right, preferred_element_type=F32)
                tops[group] = term if tops[group] is None else tops[group] + term
        return [top.reshape(width, -1, 256 * len(halves)) for top in tops]

    top_rows, inner, low_rows = pl.ds(0, 8), pl.ds(8, 56), pl.ds(64, 8)

    def here(n):
        with jax.named_scope(f"here{n}"):
            for group, top in enumerate(conv1((n,), (0,), (inner,), 2)):
                z_acc[n, pl.ds(5 * group, 5), inner] = top

    def near(n):
        with jax.named_scope(f"wait_lent{n}"):
            lent[n].land()
        with jax.named_scope(f"near{n}"):
            for group, top in enumerate(conv1((n,), (3, 1), (inner,), 2)):
                z_acc[n, pl.ds(5 * group, 5), inner] += top

    def rim():
        with jax.named_scope("rim"):
            (top,) = conv1((0, 1), (0, 3, 1), (top_rows, low_rows), 1)
            for n in range(2):
                part = top[:, :, 256 * n : 256 * n + 256]
                z_acc[n, :, top_rows] = part[:, :8]
                z_acc[n, :, low_rows] = part[:, 8:]

    def far(n):
        with jax.named_scope(f"wait_lent_on{n}"):
            lent_on[n].land()
        lanes = slice(256 * n, 256 * n + 256)
        with jax.named_scope(f"far{n}"):
            for group, top in enumerate(conv1((n,), (2,), (pl.ds(0, 72),), 2)):
                cols = pl.ds(5 * group, 5)
                act = jnp.maximum(z_acc[n, cols] + top + b1v[:, lanes], 0.0)
                for dh in range(3):
                    ys[dh][cols, :, lanes] = act[:, 4 * dh : 4 * dh + 64].astype(BF16)

        def clear(at_edge, refs, cols, rows):
            @pl.when(at_edge)
            def _():
                for ref in refs:
                    ref[cols, rows, lanes] = jnp.zeros((cols.size, rows.size, 256), BF16)

        clear(q == 0, ys, pl.ds(0, 1), pl.ds(0, 64))
        clear(q == 15, ys, pl.ds(9, 1), pl.ds(0, 64))
        clear(m == 0, (y0,), pl.ds(0, 10), pl.ds(0, 4))
        clear(m == 7, (y2,), pl.ds(0, 10), pl.ds(60, 4))

    def conv2(n):
        lanes = slice(256 * n, 256 * n + 256)
        total = None
        for dh in range(3):
            for dw in range(3):
                tap = 3 * dh + dw
                left = ys[dh][dw : dw + 8, :, lanes].reshape(CHANS, 256)
                right = w2v[CHANS * tap + 256 * n : CHANS * tap + 256 * n + 256, :]
                term = jnp.dot(left, right, preferred_element_type=F32)
                total = term if total is None else total + term
        return total

    pass_on(0)
    with jax.named_scope("wait_own"):
        own.land()
    here(0)
    here(1)
    pass_on(1)
    near(0)
    near(1)
    finish(0)
    with jax.named_scope("wait_halo"):
        for copy in halo:
            copy.wait_recv()

    @pl.when(m == 0)
    def _():
        x0[:, 0:8] = jnp.zeros((12, 8, CHANS), BF16)
        x1[:, 0:4] = jnp.zeros((12, 4, CHANS), BF16)

    @pl.when(m > 0)
    def _():
        x1[:, 0:4] = edge[2]

    @pl.when(m == 7)
    def _():
        x2[:, 64:72] = jnp.zeros((12, 8, CHANS), BF16)
        x1[:, 68:72] = jnp.zeros((12, 4, CHANS), BF16)

    @pl.when(m < 7)
    def _():
        x1[:, 68:72] = edge[3]

    rim()
    finish(1)
    with jax.named_scope("wait_w2"):
        for load in loads[2:]:
            load.wait()
    far(0)
    with jax.named_scope("conv2_0"):
        acc2[...] = conv2(0)
    far(1)
    with jax.named_scope("conv2_1"):
        o_ref[...] = acc2[...] + conv2(1) + b2v[...]

    with jax.named_scope("wait_sends"):
        everything.wait_send()
        for step in steps:
            step.all.wait_send()
        for copy in halo:
            copy.wait_send()


def arrange(sum_ref, o_hbm, turned, sems):
    copies = []
    for g in range(4):
        rows = jnp.transpose(sum_ref[:, 16 * g : 16 * g + 16], (1, 0, 2))
        for h in range(4):
            for image in range(4):
                turned[g, image, h] = rows[4 * h + image]
        copies.append(pltpu.make_async_copy(turned.at[g], o_hbm.at[:, pl.ds(4 * g, 4)], sems.at[g]))
        copies[-1].start()
    for copy in copies:
        copy.wait()


def solution(mesh):
    scratch = [
        pltpu.VMEM((4, LANES, 4, LANES), BF16),
        pltpu.VMEM((9, 4, CHANS), BF16),
        pltpu.VMEM((4616, CHANS), BF16),
        pltpu.VMEM((1, CHANS), F32),
        pltpu.VMEM((1, CHANS), F32),
        pltpu.VMEM((CHANS, CHANS), BF16),
        pltpu.VMEM((8, 66, 4, LANES), BF16),
        pltpu.VMEM((LANES, 6, 4, LANES), BF16),
        *[pltpu.VMEM((12, 72, CHANS), BF16) for _ in range(3)],
        pltpu.VMEM((4, 12, 4, CHANS), BF16),
        pltpu.VMEM((3, 2, 4, 2, 4, 4, 3, 2, 4, LANES), BF16),
        pltpu.VMEM((2, 10, 72, 256), F32),
        *[pltpu.VMEM((10, 64, CHANS), BF16) for _ in range(3)],
        pltpu.VMEM((CHANS, CHANS), F32),
        pltpu.SemaphoreType.DMA((5,)),
        pltpu.SemaphoreType.DMA,
        pltpu.SemaphoreType.DMA,
        pltpu.SemaphoreType.DMA((4,)),
        pltpu.SemaphoreType.DMA((4,)),
        pltpu.SemaphoreType.DMA((11,)),
        pltpu.SemaphoreType.DMA((11,)),
    ]
    vmem = pl.BlockSpec(memory_space=pltpu.VMEM)
    anywhere = pl.BlockSpec(memory_space=pl.ANY)

    def run_local(x_in, w_conv1, b_conv1, w_conv2, b_conv2):
        sums = pl.pallas_call(
            kernel,
            out_shape=jax.ShapeDtypeStruct((CHANS, CHANS), F32),
            in_specs=[anywhere] * 5,
            out_specs=vmem,
            scratch_shapes=scratch,
            compiler_params=pltpu.CompilerParams(has_side_effects=True, vmem_limit_bytes=VMEM_LIMIT),
            name="two_convs",
        )(
            *(
                pltpu.with_memory_space_constraint(a, pltpu.HBM)
                for a in (
                    x_in.transpose(0, 1, 3, 2),
                    w_conv1.reshape(9, 4, CHANS),
                    w_conv2.reshape(4608, CHANS),
                    b_conv1.reshape(1, CHANS),
                    b_conv2.reshape(1, CHANS),
                )
            )
        )
        return pl.pallas_call(
            arrange,
            out_shape=jax.ShapeDtypeStruct((4, 16, 8, CHANS), F32),
            in_specs=[vmem],
            out_specs=anywhere,
            scratch_shapes=[pltpu.VMEM((4, 4, 4, 8, CHANS), F32), pltpu.SemaphoreType.DMA((4,))],
            compiler_params=pltpu.CompilerParams(vmem_limit_bytes=8 * 2**20),
            name="arrange",
        )(sums.reshape(8, 64, CHANS))

    return jax.shard_map(
        run_local,
        mesh=mesh,
        in_specs=(P("data", None, None, GROUP_AXES), P(None, None, GROUP_AXES, None), P(), P(), P()),
        out_specs=P("data", "model", "cols", None),
        check_vma=False,
    )
```

```python
import jax
import jax.numpy as jnp
from jax import lax
from jax.experimental import pallas as pl
from jax.experimental.pallas import tpu as pltpu
from jax.sharding import PartitionSpec as P

GROUP_AXES = ("model", "cols")
MESH = pl.DeviceIdType.MESH
BF16 = jnp.bfloat16
F32 = jnp.float32
CHANS = 512
LANES = 128
CUT = 96
VMEM_LIMIT = 36 * 2**20
ORDERS = (("y", "z", "x"), ("z", "x", "y"), ("x", "y", "z"))


def one_hot(shape, col_of_row):
    rows = lax.broadcasted_iota(jnp.int32, shape, 0)
    cols = lax.broadcasted_iota(jnp.int32, shape, 1)
    return jnp.where(cols == col_of_row(rows), 1.0, 0.0).astype(BF16)


def pack_windows(xv, a_scr, pack):
    to_lanes = one_hot((CHANS, CHANS), lambda r: (r % 4) * LANES + ((r % LANES) // 4) * 4 + r // LANES)
    to_rows = one_hot((CHANS, CHANS), lambda r: (r % 4) * LANES + ((r % 256) // 4) * 2 + r // 256)
    for blk in range(4):
        part = jnp.concatenate([xv[n, 32 * blk : 32 * blk + 32].reshape(LANES, LANES) for n in range(4)], axis=0)
        turned = lax.dot_general(part, to_lanes, (((0,), (0,)), ((), ())), preferred_element_type=F32).astype(BF16)
        for c in range(4):
            a_scr[c * LANES : (c + 1) * LANES, blk * LANES : (blk + 1) * LANES] = turned[:, c * LANES : (c + 1) * LANES]
    mixed = jnp.dot(to_rows, a_scr[...], preferred_element_type=F32)
    for blk in range(4):
        even = mixed[0:256, blk * LANES : (blk + 1) * LANES]
        odd = mixed[256:CHANS, blk * LANES : (blk + 1) * LANES]
        for half in range(2):
            s = slice(64 * half, 64 * half + 64)
            tile = jnp.concatenate([even[:, s], odd[:, s]], axis=1).astype(BF16)
            pack[2 * blk + half, 1:65] = tile.reshape(64, 4, LANES)
    edge = jnp.zeros((8, 1, 4, LANES), BF16)
    pack[:, 0:1] = edge
    pack[:, 65:66] = edge


def kernel(
    x_hbm, w1_hbm, w2_hbm, b1_hbm, b2_hbm, o_ref,
    xv, w1v, w2v, b1v, b2v, a_scr, pack, got, x0, x1, x2, edge, w1g, z_acc, y0, y1, y2, acc2,
    load_sem, xs_send, xs_recv, halo_send, halo_recv, step_send, step_recv,
):
    m = lax.axis_index("model")
    q = lax.axis_index("cols")
    me = {"x": m // 2, "z": q // 4, "y": q % 4}
    core = m % 2
    parts = range(3)
    barrier = pltpu.get_barrier_semaphore()

    at_model = [[(me["x"] + dx) % 4 * 2 + (core + dk) % 2 for dk in range(2)] for dx in range(4)]
    at_cols = [[(me["z"] + dz) % 4 * 4 + (me["y"] + dy) % 4 for dy in range(4)] for dz in range(4)]
    others = [(dx, dz, dy, dk) for dx in range(4) for dz in range(4) for dy in range(4) for dk in range(2)]
    others = sorted(others[1:], key=lambda d: (sum(d[:3]) % 4, d))

    def away(d):
        return {"model": at_model[d[0]][d[3]], "cols": at_cols[d[1]][d[2]]}

    loads = [
        pltpu.make_async_copy(src, dst, load_sem.at[k])
        for k, (src, dst) in enumerate(
            ((x_hbm, xv), (w1_hbm, w1v), (w2_hbm, w2v.at[pl.ds(0, 4608)]), (b1_hbm, b1v), (b2_hbm, b2v))
        )
    ]
    for load in loads:
        load.start()
    with jax.named_scope("announce"):
        for d in sorted(others, key=lambda d: -sum(min(o, 4 - o) for o in d[:3])):
            pl.semaphore_signal(barrier, inc=1, device_id=away(d), device_id_type=MESH)

    def piece(p, t, v, n, c, place=None, half=None):
        done = ORDERS[p][:t]
        rest = [a for a in "xzy" if a != ORDERS[p][2]]
        at = [v if t < 2 and a == ORDERS[p][t] else (pl.ds(0, 4) if a in done else me[a]) for a in rest]
        if half is not None:
            at[0] = pl.ds(2 * half, 2)
        return w1g.at[p, pl.ds(0, 2) if n is None else n, me[ORDERS[p][2]] if t < 2 else v, c, at[0], at[1]]

    with jax.named_scope("place_w1"):
        loads[1].wait()
        for p in parts:
            spot = [me[a] for a in "xzy" if a != ORDERS[p][2]]
            for dw in range(3):
                for lt in range(4):
                    tile = w1v[3 * p + dw, :, lt * LANES : (lt + 1) * LANES]
                    w1g[p, lt // 2, me[ORDERS[p][2]], core, spot[0], spot[1], dw, lt % 2] = tile
    with jax.named_scope("wait_x"):
        loads[0].wait()
    with jax.named_scope("pack"):
        pack_windows(xv, a_scr, pack)
    with jax.named_scope("wait_barrier"):
        pl.semaphore_wait(barrier, 127)

    n_steps = [0]
    steps = []

    class Step:
        def __init__(self, slabs, copies):
            k = n_steps[0]
            n_steps[0] += 1
            sems = dict(send_sem=step_send.at[k], recv_sem=step_recv.at[k], device_id_type=MESH)
            self.copies, self.sems = copies, sems
            span = got.at[pl.ds(0, slabs)]
            self.all = pltpu.make_async_remote_copy(
                src_ref=span, dst_ref=span, device_id={"model": at_model[0][1], "cols": q}, **sems
            )
            steps.append(self)

        def go(self):
            for ref, to in self.copies:
                pltpu.make_async_remote_copy(src_ref=ref, dst_ref=ref, device_id=to, **self.sems).start()
            return self

        def land(self):
            self.all.wait_recv()

    def chip(p, t, d, c=0):
        axis = ORDERS[p][t]
        pos = me | {axis: (me[axis] + d) % 4}
        return {"model": pos["x"] * 2 + (core + c) % 2, "cols": pos["z"] * 4 + pos["y"]}

    def spread(t, slabs):
        return Step(slabs, [(piece(p, t, me[ORDERS[p][t]], None, core), chip(p, t, d)) for p in parts for d in (1, 3, 2)]).go()

    def plane(p, d):
        return (me[ORDERS[p][2]] + d) % 4

    def hand_over(pieces, slabs):
        return Step(slabs, [(ref, {"model": at_model[0][1], "cols": q}) for ref in pieces]).go()

    def send_windows(first, last):
        for d in others[first:last]:
            to = away(d)
            pltpu.make_async_remote_copy(
                src_ref=pack.at[to["model"], pl.ds(4 * to["cols"], 6)],
                dst_ref=got.at[mine],
                send_sem=xs_send,
                recv_sem=xs_recv,
                device_id=to,
                device_id_type=MESH,
            ).start()

    mine = ((core * 4 + me["x"]) * 4 + me["z"]) * 4 + me["y"]
    with jax.named_scope("send_first"):
        first = spread(0, 18)
        for pair in range(6):
            got[mine, pair] = pack[m, 4 * q + pair]
        send_windows(0, CUT)
    with jax.named_scope("wait_first"):
        first.land()
    with jax.named_scope("send_second"):
        second = spread(1, 72)
        send_windows(CUT, 127)
    with jax.named_scope("wait_second"):
        second.land()
    last, passed, lent, lent_on = {}, {}, {}, {}

    def send_plane(n):
        last[n] = Step(96, [(piece(p, 2, plane(p, 0), n, core), chip(p, 2, d)) for p in parts for d in (1, 3)])

    def pass_on(n):
        with jax.named_scope(f"wait_last{n}"):
            last[n].land()
        passed[n] = Step(48, [(piece(p, 2, plane(p, 4 - d), n, core, half=d // 2), chip(p, 2, d)) for p in parts for d in (1, 3)]).go()
        if n == 0:

            @pl.when(core == 1)
            def _():
                last[1].go()

        lent[n] = hand_over([piece(p, 2, plane(p, d), n, core) for p in parts for d in (1, 3)], 96)

    def finish(n):
        with jax.named_scope(f"wait_passed{n}"):
            passed[n].land()
        lent_on[n] = hand_over([piece(p, 2, plane(p, 2), n, core) for p in parts], 48)

    with jax.named_scope("send_third"):
        for n in range(2):
            send_plane(n)
        last[0].go()
        own = hand_over([piece(p, 2, plane(p, 0), None, core) for p in parts], 96)

    @pl.when(core == 0)
    def _():
        last[1].go()

    span = got.at[pl.ds(0, 127)]
    everything = pltpu.make_async_remote_copy(
        src_ref=span, dst_ref=span, send_sem=xs_send, recv_sem=xs_recv, device_id=chip(0, 0, 0, 1), device_id_type=MESH
    )
    with jax.named_scope("wait_windows"):
        everything.wait_recv()

    xs, ys = (x0, x1, x2), (y0, y1, y2)
    with jax.named_scope("turn"):
        for pair in range(6):
            for p in parts:
                rows = []
                for v in range(4):
                    for c in range(2):
                        at = 64 * c
                        if p == 0:
                            rows.append(got[at + 16 * v : at + 16 * v + 16, pair])
                        elif p == 1:
                            rows.append(got[at + v : at + 64 : 4, pair])
                        else:
                            rows += [got[at + 16 * a + 4 * v : at + 16 * a + 4 * v + 4, pair] for a in range(4)]
                rows = jnp.concatenate([r.reshape(-1, LANES) for r in rows], axis=0).T
                for odd in range(2):
                    main = rows[64 * odd : 64 * odd + 64]
                    xs[p][2 * pair + odd, 8 - 4 * p : 72 - 4 * p] = main
                    if p == 1:
                        edge[0, 2 * pair + odd] = main[60:64]
                        edge[1, 2 * pair + odd] = main[0:4]
    halo = []
    for src, dst, d in (
        (x0.at[:, pl.ds(64, 8)], x0.at[:, pl.ds(0, 8)], 1),
        (x2.at[:, pl.ds(0, 8)], x2.at[:, pl.ds(64, 8)], 7),
        (edge.at[0], edge.at[2], 1),
        (edge.at[1], edge.at[3], 7),
    ):
        halo.append(
            pltpu.make_async_remote_copy(
                src_ref=src,
                dst_ref=dst,
                send_sem=halo_send.at[len(halo)],
                recv_sem=halo_recv.at[len(halo)],
                device_id={"model": (m + d) % 8, "cols": q},
                device_id_type=MESH,
            )
        )
        halo[-1].start()

    def conv1(halves, places, spans, groups):
        width = 10 // groups
        tops = [None] * groups
        taps = [(p, dw, plane(p, d)) for p in parts for dw in range(3) for d in places]
        for first in range(0, len(taps), 2):
            two = taps[first : first + 2]
            right = [[w1g[p, n, v, :, :, :, dw, i].reshape(LANES, LANES) for n in halves for i in range(2)] for p, dw, v in two]
            right = jnp.concatenate([jnp.concatenate(r, axis=1) for r in right], axis=0)
            for group in range(groups):
                left = []
                for rows in spans:
                    some = []
                    for p, dw, v in two:
                        lanes = pl.ds(pl.multiple_of(LANES * v, LANES), LANES)
                        some.append(xs[p][pl.ds(dw + width * group, width), rows, lanes])
                    left.append(jnp.concatenate(some, axis=-1))
                left = jnp.concatenate(left, axis=1).reshape(-1, LANES * len(two))
                term = jnp.dot(left, right, preferred_element_type=F32)
                tops[group] = term if tops[group] is None else tops[group] + term
        return [top.reshape(width, -1, 256 * len(halves)) for top in tops]

    top_rows, inner, low_rows = pl.ds(0, 8), pl.ds(8, 56), pl.ds(64, 8)

    def here(n):
        with jax.named_scope(f"here{n}"):
            for group, top in enumerate(conv1((n,), (0,), (inner,), 2)):
                z_acc[n, pl.ds(5 * group, 5), inner] = top

    def near(n):
        with jax.named_scope(f"wait_lent{n}"):
            lent[n].land()
        with jax.named_scope(f"near{n}"):
            for group, top in enumerate(conv1((n,), (3, 1), (inner,), 2)):
                z_acc[n, pl.ds(5 * group, 5), inner] += top

    def rim():
        with jax.named_scope("rim"):
            (top,) = conv1((0, 1), (0, 3, 1), (top_rows, low_rows), 1)
            for n in range(2):
                part = top[:, :, 256 * n : 256 * n + 256]
                z_acc[n, :, top_rows] = part[:, :8]
                z_acc[n, :, low_rows] = part[:, 8:]

    def far(n):
        with jax.named_scope(f"wait_lent_on{n}"):
            lent_on[n].land()
        lanes = slice(256 * n, 256 * n + 256)
        with jax.named_scope(f"far{n}"):
            for group, top in enumerate(conv1((n,), (2,), (pl.ds(0, 72),), 2)):
                cols = pl.ds(5 * group, 5)
                act = jnp.maximum(z_acc[n, cols] + top + b1v[:, lanes], 0.0)
                for dh in range(3):
                    ys[dh][cols, :, lanes] = act[:, 4 * dh : 4 * dh + 64].astype(BF16)

        def clear(at_edge, refs, cols, rows):
            @pl.when(at_edge)
            def _():
                for ref in refs:
                    ref[cols, rows, lanes] = jnp.zeros((cols.size, rows.size, 256), BF16)

        clear(q == 0, ys, pl.ds(0, 1), pl.ds(0, 64))
        clear(q == 15, ys, pl.ds(9, 1), pl.ds(0, 64))
        clear(m == 0, (y0,), pl.ds(0, 10), pl.ds(0, 4))
        clear(m == 7, (y2,), pl.ds(0, 10), pl.ds(60, 4))

    def conv2(n):
        lanes = slice(256 * n, 256 * n + 256)
        total = None
        for dh in range(3):
            for dw in range(3):
                tap = 3 * dh + dw
                left = ys[dh][dw : dw + 8, :, lanes].reshape(CHANS, 256)
                right = w2v[CHANS * tap + 256 * n : CHANS * tap + 256 * n + 256, :]
                term = jnp.dot(left, right, preferred_element_type=F32)
                total = term if total is None else total + term
        return total

    pass_on(0)
    with jax.named_scope("wait_own"):
        own.land()
    here(0)
    here(1)
    near(0)
    pass_on(1)
    near(1)
    finish(0)
    with jax.named_scope("wait_halo"):
        for copy in halo:
            copy.wait_recv()

    @pl.when(m == 0)
    def _():
        x0[:, 0:8] = jnp.zeros((12, 8, CHANS), BF16)
        x1[:, 0:4] = jnp.zeros((12, 4, CHANS), BF16)

    @pl.when(m > 0)
    def _():
        x1[:, 0:4] = edge[2]

    @pl.when(m == 7)
    def _():
        x2[:, 64:72] = jnp.zeros((12, 8, CHANS), BF16)
        x1[:, 68:72] = jnp.zeros((12, 4, CHANS), BF16)

    @pl.when(m < 7)
    def _():
        x1[:, 68:72] = edge[3]

    rim()
    finish(1)
    with jax.named_scope("wait_w2"):
        for load in loads[2:]:
            load.wait()
    far(0)
    with jax.named_scope("conv2_0"):
        acc2[...] = conv2(0)
    far(1)
    with jax.named_scope("conv2_1"):
        o_ref[...] = acc2[...] + conv2(1) + b2v[...]

    with jax.named_scope("wait_sends"):
        everything.wait_send()
        for step in steps:
            step.all.wait_send()
        for copy in halo:
            copy.wait_send()


def arrange(sum_ref, o_hbm, turned, sems):
    copies = []
    for g in range(4):
        rows = jnp.transpose(sum_ref[:, 16 * g : 16 * g + 16], (1, 0, 2))
        for h in range(4):
            for image in range(4):
                turned[g, image, h] = rows[4 * h + image]
        copies.append(pltpu.make_async_copy(turned.at[g], o_hbm.at[:, pl.ds(4 * g, 4)], sems.at[g]))
        copies[-1].start()
    for copy in copies:
        copy.wait()


def solution(mesh):
    scratch = [
        pltpu.VMEM((4, LANES, 4, LANES), BF16),
        pltpu.VMEM((9, 4, CHANS), BF16),
        pltpu.VMEM((4616, CHANS), BF16),
        pltpu.VMEM((1, CHANS), F32),
        pltpu.VMEM((1, CHANS), F32),
        pltpu.VMEM((CHANS, CHANS), BF16),
        pltpu.VMEM((8, 66, 4, LANES), BF16),
        pltpu.VMEM((LANES, 6, 4, LANES), BF16),
        *[pltpu.VMEM((12, 72, CHANS), BF16) for _ in range(3)],
        pltpu.VMEM((4, 12, 4, CHANS), BF16),
        pltpu.VMEM((3, 2, 4, 2, 4, 4, 3, 2, 4, LANES), BF16),
        pltpu.VMEM((2, 10, 72, 256), F32),
        *[pltpu.VMEM((10, 64, CHANS), BF16) for _ in range(3)],
        pltpu.VMEM((CHANS, CHANS), F32),
        pltpu.SemaphoreType.DMA((5,)),
        pltpu.SemaphoreType.DMA,
        pltpu.SemaphoreType.DMA,
        pltpu.SemaphoreType.DMA((4,)),
        pltpu.SemaphoreType.DMA((4,)),
        pltpu.SemaphoreType.DMA((11,)),
        pltpu.SemaphoreType.DMA((11,)),
    ]
    vmem = pl.BlockSpec(memory_space=pltpu.VMEM)
    anywhere = pl.BlockSpec(memory_space=pl.ANY)

    def run_local(x_in, w_conv1, b_conv1, w_conv2, b_conv2):
        sums = pl.pallas_call(
            kernel,
            out_shape=jax.ShapeDtypeStruct((CHANS, CHANS), F32),
            in_specs=[anywhere] * 5,
            out_specs=vmem,
            scratch_shapes=scratch,
            compiler_params=pltpu.CompilerParams(collective_id=0, has_side_effects=True, vmem_limit_bytes=VMEM_LIMIT),
            name="two_convs",
        )(
            *(
                pltpu.with_memory_space_constraint(a, pltpu.HBM)
                for a in (
                    x_in.transpose(0, 1, 3, 2),
                    w_conv1.reshape(9, 4, CHANS),
                    w_conv2.reshape(4608, CHANS),
                    b_conv1.reshape(1, CHANS),
                    b_conv2.reshape(1, CHANS),
                )
            )
        )
        return pl.pallas_call(
            arrange,
            out_shape=jax.ShapeDtypeStruct((4, 16, 8, CHANS), F32),
            in_specs=[vmem],
            out_specs=anywhere,
            scratch_shapes=[pltpu.VMEM((4, 4, 4, 8, CHANS), F32), pltpu.SemaphoreType.DMA((4,))],
            compiler_params=pltpu.CompilerParams(vmem_limit_bytes=8 * 2**20),
            name="arrange",
        )(sums.reshape(8, 64, CHANS))

    return jax.shard_map(
        run_local,
        mesh=mesh,
        in_specs=(P("data", None, None, GROUP_AXES), P(None, None, GROUP_AXES, None), P(), P(), P()),
        out_specs=P("data", "model", "cols", None),
        check_vma=False,
    )
```

```python
import jax
import jax.numpy as jnp
from jax import lax
from jax.experimental import pallas as pl
from jax.experimental.pallas import tpu as pltpu
from jax.sharding import PartitionSpec as P

GROUP_AXES = ("model", "cols")
MESH = pl.DeviceIdType.MESH
BF16 = jnp.bfloat16
F32 = jnp.float32
CHANS = 512
LANES = 128
CUT = 96
VMEM_LIMIT = 36 * 2**20
ORDERS = (("y", "z", "x"), ("z", "x", "y"), ("x", "y", "z"))


def one_hot(shape, col_of_row):
    rows = lax.broadcasted_iota(jnp.int32, shape, 0)
    cols = lax.broadcasted_iota(jnp.int32, shape, 1)
    return jnp.where(cols == col_of_row(rows), 1.0, 0.0).astype(BF16)


def pack_windows(xv, a_scr, pack):
    to_lanes = one_hot((CHANS, CHANS), lambda r: (r % 4) * LANES + ((r % LANES) // 4) * 4 + r // LANES)
    to_rows = one_hot((CHANS, CHANS), lambda r: (r % 4) * LANES + ((r % 256) // 4) * 2 + r // 256)
    for blk in range(4):
        part = jnp.concatenate([xv[n, 32 * blk : 32 * blk + 32].reshape(LANES, LANES) for n in range(4)], axis=0)
        turned = lax.dot_general(part, to_lanes, (((0,), (0,)), ((), ())), preferred_element_type=F32).astype(BF16)
        for c in range(4):
            a_scr[c * LANES : (c + 1) * LANES, blk * LANES : (blk + 1) * LANES] = turned[:, c * LANES : (c + 1) * LANES]
    mixed = jnp.dot(to_rows, a_scr[...], preferred_element_type=F32)
    for blk in range(4):
        even = mixed[0:256, blk * LANES : (blk + 1) * LANES]
        odd = mixed[256:CHANS, blk * LANES : (blk + 1) * LANES]
        for half in range(2):
            s = slice(64 * half, 64 * half + 64)
            tile = jnp.concatenate([even[:, s], odd[:, s]], axis=1).astype(BF16)
            pack[2 * blk + half, 1:65] = tile.reshape(64, 4, LANES)
    edge = jnp.zeros((8, 1, 4, LANES), BF16)
    pack[:, 0:1] = edge
    pack[:, 65:66] = edge


def kernel(
    x_hbm, w1_hbm, w2_hbm, b1_hbm, b2_hbm, o_ref,
    xv, w1v, w2v, b1v, b2v, a_scr, pack, got, x0, x1, x2, edge, w1g, z_acc, y0, y1, y2, acc2,
    load_sem, xs_send, xs_recv, halo_send, halo_recv, step_send, step_recv,
):
    m = lax.axis_index("model")
    q = lax.axis_index("cols")
    me = {"x": m // 2, "z": q // 4, "y": q % 4}
    core = m % 2
    parts = range(3)
    barrier = pltpu.get_barrier_semaphore()

    at_model = [[(me["x"] + dx) % 4 * 2 + (core + dk) % 2 for dk in range(2)] for dx in range(4)]
    at_cols = [[(me["z"] + dz) % 4 * 4 + (me["y"] + dy) % 4 for dy in range(4)] for dz in range(4)]
    others = [(dx, dz, dy, dk) for dx in range(4) for dz in range(4) for dy in range(4) for dk in range(2)]
    others = sorted(others[1:], key=lambda d: (sum(d[:3]) % 4, d))

    def away(d):
        return {"model": at_model[d[0]][d[3]], "cols": at_cols[d[1]][d[2]]}

    loads = [
        pltpu.make_async_copy(src, dst, load_sem.at[k])
        for k, (src, dst) in enumerate(
            ((x_hbm, xv), (w1_hbm, w1v), (w2_hbm, w2v.at[pl.ds(0, 4608)]), (b1_hbm, b1v), (b2_hbm, b2v))
        )
    ]
    for load in loads:
        load.start()
    with jax.named_scope("announce"):
        for d in sorted(others, key=lambda d: -sum(min(o, 4 - o) for o in d[:3])):
            pl.semaphore_signal(barrier, inc=1, device_id=away(d), device_id_type=MESH)

    def piece(p, t, v, n, c, place=None, half=None):
        done = ORDERS[p][:t]
        rest = [a for a in "xzy" if a != ORDERS[p][2]]
        at = [v if t < 2 and a == ORDERS[p][t] else (pl.ds(0, 4) if a in done else me[a]) for a in rest]
        if half is not None:
            at[0] = pl.ds(2 * half, 2)
        return w1g.at[p, pl.ds(0, 2) if n is None else n, me[ORDERS[p][2]] if t < 2 else v, c, at[0], at[1]]

    with jax.named_scope("place_w1"):
        loads[1].wait()
        for p in parts:
            spot = [me[a] for a in "xzy" if a != ORDERS[p][2]]
            for dw in range(3):
                for lt in range(4):
                    tile = w1v[3 * p + dw, :, lt * LANES : (lt + 1) * LANES]
                    w1g[p, lt // 2, me[ORDERS[p][2]], core, spot[0], spot[1], dw, lt % 2] = tile
    with jax.named_scope("wait_x"):
        loads[0].wait()
    with jax.named_scope("pack"):
        pack_windows(xv, a_scr, pack)
    with jax.named_scope("wait_barrier"):
        pl.semaphore_wait(barrier, 127)

    n_steps = [0]
    steps = []

    class Step:
        def __init__(self, slabs, copies):
            k = n_steps[0]
            n_steps[0] += 1
            sems = dict(send_sem=step_send.at[k], recv_sem=step_recv.at[k], device_id_type=MESH)
            self.copies, self.sems = copies, sems
            span = got.at[pl.ds(0, slabs)]
            self.all = pltpu.make_async_remote_copy(
                src_ref=span, dst_ref=span, device_id={"model": at_model[0][1], "cols": q}, **sems
            )
            steps.append(self)

        def go(self):
            for ref, to in self.copies:
                pltpu.make_async_remote_copy(src_ref=ref, dst_ref=ref, device_id=to, **self.sems).start()
            return self

        def land(self):
            self.all.wait_recv()

    def chip(p, t, d, c=0):
        axis = ORDERS[p][t]
        pos = me | {axis: (me[axis] + d) % 4}
        return {"model": pos["x"] * 2 + (core + c) % 2, "cols": pos["z"] * 4 + pos["y"]}

    def spread(t, slabs):
        return Step(slabs, [(piece(p, t, me[ORDERS[p][t]], None, core), chip(p, t, d)) for p in parts for d in (1, 3, 2)]).go()

    def plane(p, d):
        return (me[ORDERS[p][2]] + d) % 4

    def hand_over(pieces, slabs):
        return Step(slabs, [(ref, {"model": at_model[0][1], "cols": q}) for ref in pieces]).go()

    def send_windows(first, last):
        for d in others[first:last]:
            to = away(d)
            pltpu.make_async_remote_copy(
                src_ref=pack.at[to["model"], pl.ds(4 * to["cols"], 6)],
                dst_ref=got.at[mine],
                send_sem=xs_send,
                recv_sem=xs_recv,
                device_id=to,
                device_id_type=MESH,
            ).start()

    mine = ((core * 4 + me["x"]) * 4 + me["z"]) * 4 + me["y"]
    with jax.named_scope("send_first"):
        first = spread(0, 18)
        for pair in range(6):
            got[mine, pair] = pack[m, 4 * q + pair]
        send_windows(0, CUT)
    with jax.named_scope("wait_first"):
        first.land()
    with jax.named_scope("send_second"):
        second = spread(1, 72)
        send_windows(CUT, 127)
    with jax.named_scope("wait_second"):
        second.land()
    last, passed, lent, lent_on = {}, {}, {}, {}

    def send_plane(n):
        last[n] = Step(96, [(piece(p, 2, plane(p, 0), n, core), chip(p, 2, d)) for p in parts for d in (1, 3)])

    def pass_on(n):
        with jax.named_scope(f"wait_last{n}"):
            last[n].land()
        passed[n] = Step(48, [(piece(p, 2, plane(p, 4 - d), n, core, half=d // 2), chip(p, 2, d)) for p in parts for d in (1, 3)]).go()
        if n == 0:

            @pl.when(core == 1)
            def _():
                last[1].go()

        lent[n] = hand_over([piece(p, 2, plane(p, d), n, core) for p in parts for d in (1, 3)], 96)

    def finish(n):
        with jax.named_scope(f"wait_passed{n}"):
            passed[n].land()
        lent_on[n] = hand_over([piece(p, 2, plane(p, 2), n, core) for p in parts], 48)

    with jax.named_scope("send_third"):
        for n in range(2):
            send_plane(n)
        last[0].go()
        own = hand_over([piece(p, 2, plane(p, 0), None, core) for p in parts], 96)

    @pl.when(core == 0)
    def _():
        last[1].go()

    span = got.at[pl.ds(0, 127)]
    everything = pltpu.make_async_remote_copy(
        src_ref=span, dst_ref=span, send_sem=xs_send, recv_sem=xs_recv, device_id=chip(0, 0, 0, 1), device_id_type=MESH
    )
    with jax.named_scope("wait_windows"):
        everything.wait_recv()

    xs, ys = (x0, x1, x2), (y0, y1, y2)
    with jax.named_scope("turn"):
        for pair in range(6):
            for p in parts:
                rows = []
                for v in range(4):
                    for c in range(2):
                        at = 64 * c
                        if p == 0:
                            rows.append(got[at + 16 * v : at + 16 * v + 16, pair])
                        elif p == 1:
                            rows.append(got[at + v : at + 64 : 4, pair])
                        else:
                            rows += [got[at + 16 * a + 4 * v : at + 16 * a + 4 * v + 4, pair] for a in range(4)]
                rows = jnp.concatenate([r.reshape(-1, LANES) for r in rows], axis=0).T
                for odd in range(2):
                    main = rows[64 * odd : 64 * odd + 64]
                    xs[p][2 * pair + odd, 8 - 4 * p : 72 - 4 * p] = main
                    if p == 1:
                        edge[0, 2 * pair + odd] = main[60:64]
                        edge[1, 2 * pair + odd] = main[0:4]
    halo = []
    for src, dst, d in (
        (x0.at[:, pl.ds(64, 8)], x0.at[:, pl.ds(0, 8)], 1),
        (x2.at[:, pl.ds(0, 8)], x2.at[:, pl.ds(64, 8)], 7),
        (edge.at[0], edge.at[2], 1),
        (edge.at[1], edge.at[3], 7),
    ):
        halo.append(
            pltpu.make_async_remote_copy(
                src_ref=src,
                dst_ref=dst,
                send_sem=halo_send.at[len(halo)],
                recv_sem=halo_recv.at[len(halo)],
                device_id={"model": (m + d) % 8, "cols": q},
                device_id_type=MESH,
            )
        )
        halo[-1].start()

    def conv1(halves, places, spans, groups):
        width = 10 // groups
        tops = [None] * groups
        taps = [(p, dw, plane(p, d)) for p in parts for dw in range(3) for d in places]
        for first in range(0, len(taps), 2):
            two = taps[first : first + 2]
            right = [[w1g[p, n, v, :, :, :, dw, i].reshape(LANES, LANES) for n in halves for i in range(2)] for p, dw, v in two]
            right = jnp.concatenate([jnp.concatenate(r, axis=1) for r in right], axis=0)
            for group in range(groups):
                left = []
                for rows in spans:
                    some = []
                    for p, dw, v in two:
                        lanes = pl.ds(pl.multiple_of(LANES * v, LANES), LANES)
                        some.append(xs[p][pl.ds(dw + width * group, width), rows, lanes])
                    left.append(jnp.concatenate(some, axis=-1))
                left = jnp.concatenate(left, axis=1).reshape(-1, LANES * len(two))
                term = jnp.dot(left, right, preferred_element_type=F32)
                tops[group] = term if tops[group] is None else tops[group] + term
        return [top.reshape(width, -1, 256 * len(halves)) for top in tops]

    top_rows, inner, low_rows = pl.ds(0, 8), pl.ds(8, 56), pl.ds(64, 8)

    def here(n):
        with jax.named_scope(f"here{n}"):
            for group, top in enumerate(conv1((n,), (0,), (inner,), 2)):
                z_acc[n, pl.ds(5 * group, 5), inner] = top

    def near(n):
        with jax.named_scope(f"wait_lent{n}"):
            lent[n].land()
        with jax.named_scope(f"near{n}"):
            for group, top in enumerate(conv1((n,), (3, 1), (inner,), 2)):
                z_acc[n, pl.ds(5 * group, 5), inner] += top

    def rim():
        with jax.named_scope("rim"):
            (top,) = conv1((0, 1), (0, 3, 1), (top_rows, low_rows), 1)
            for n in range(2):
                part = top[:, :, 256 * n : 256 * n + 256]
                z_acc[n, :, top_rows] = part[:, :8]
                z_acc[n, :, low_rows] = part[:, 8:]

    def far(n):
        with jax.named_scope(f"wait_lent_on{n}"):
            lent_on[n].land()
        lanes = slice(256 * n, 256 * n + 256)
        with jax.named_scope(f"far{n}"):
            for group, top in enumerate(conv1((n,), (2,), (pl.ds(0, 72),), 2)):
                cols = pl.ds(5 * group, 5)
                act = jnp.maximum(z_acc[n, cols] + top + b1v[:, lanes], 0.0)
                for dh in range(3):
                    ys[dh][cols, :, lanes] = act[:, 4 * dh : 4 * dh + 64].astype(BF16)

        def clear(at_edge, refs, cols, rows):
            @pl.when(at_edge)
            def _():
                for ref in refs:
                    ref[cols, rows, lanes] = jnp.zeros((cols.size, rows.size, 256), BF16)

        clear(q == 0, ys, pl.ds(0, 1), pl.ds(0, 64))
        clear(q == 15, ys, pl.ds(9, 1), pl.ds(0, 64))
        clear(m == 0, (y0,), pl.ds(0, 10), pl.ds(0, 4))
        clear(m == 7, (y2,), pl.ds(0, 10), pl.ds(60, 4))

    def conv2(n):
        lanes = slice(256 * n, 256 * n + 256)
        total = None
        for dh in range(3):
            for dw in range(3):
                tap = 3 * dh + dw
                left = ys[dh][dw : dw + 8, :, lanes].reshape(CHANS, 256)
                right = w2v[CHANS * tap + 256 * n : CHANS * tap + 256 * n + 256, :]
                term = jnp.dot(left, right, preferred_element_type=F32)
                total = term if total is None else total + term
        return total

    pass_on(0)
    with jax.named_scope("wait_own"):
        own.land()
    here(0)
    here(1)
    pass_on(1)
    near(0)
    near(1)
    finish(0)
    with jax.named_scope("wait_halo"):
        for copy in halo:
            copy.wait_recv()

    @pl.when(m == 0)
    def _():
        x0[:, 0:8] = jnp.zeros((12, 8, CHANS), BF16)
        x1[:, 0:4] = jnp.zeros((12, 4, CHANS), BF16)

    @pl.when(m > 0)
    def _():
        x1[:, 0:4] = edge[2]

    @pl.when(m == 7)
    def _():
        x2[:, 64:72] = jnp.zeros((12, 8, CHANS), BF16)
        x1[:, 68:72] = jnp.zeros((12, 4, CHANS), BF16)

    @pl.when(m < 7)
    def _():
        x1[:, 68:72] = edge[3]

    rim()
    finish(1)
    with jax.named_scope("wait_w2"):
        for load in loads[2:]:
            load.wait()
    far(0)
    with jax.named_scope("conv2_0"):
        acc2[...] = conv2(0)
    far(1)
    with jax.named_scope("conv2_1"):
        o_ref[...] = acc2[...] + conv2(1) + b2v[...]

    with jax.named_scope("wait_sends"):
        everything.wait_send()
        for step in steps:
            step.all.wait_send()
        for copy in halo:
            copy.wait_send()


def arrange(sum_ref, o_hbm, turned, sems):
    copies = []
    for g in range(4):
        rows = jnp.transpose(sum_ref[:, 16 * g : 16 * g + 16], (1, 0, 2))
        for h in range(4):
            for image in range(4):
                turned[g, image, h] = rows[4 * h + image]
        copies.append(pltpu.make_async_copy(turned.at[g], o_hbm.at[:, pl.ds(4 * g, 4)], sems.at[g]))
        copies[-1].start()
    for copy in copies:
        copy.wait()


def solution(mesh):
    scratch = [
        pltpu.VMEM((4, LANES, 4, LANES), BF16),
        pltpu.VMEM((9, 4, CHANS), BF16),
        pltpu.VMEM((4616, CHANS), BF16),
        pltpu.VMEM((1, CHANS), F32),
        pltpu.VMEM((1, CHANS), F32),
        pltpu.VMEM((CHANS, CHANS), BF16),
        pltpu.VMEM((8, 66, 4, LANES), BF16),
        pltpu.VMEM((LANES, 6, 4, LANES), BF16),
        *[pltpu.VMEM((12, 72, CHANS), BF16) for _ in range(3)],
        pltpu.VMEM((4, 12, 4, CHANS), BF16),
        pltpu.VMEM((3, 2, 4, 2, 4, 4, 3, 2, 4, LANES), BF16),
        pltpu.VMEM((2, 10, 72, 256), F32),
        *[pltpu.VMEM((10, 64, CHANS), BF16) for _ in range(3)],
        pltpu.VMEM((CHANS, CHANS), F32),
        pltpu.SemaphoreType.DMA((5,)),
        pltpu.SemaphoreType.DMA,
        pltpu.SemaphoreType.DMA,
        pltpu.SemaphoreType.DMA((4,)),
        pltpu.SemaphoreType.DMA((4,)),
        pltpu.SemaphoreType.DMA((11,)),
        pltpu.SemaphoreType.DMA((11,)),
    ]
    vmem = pl.BlockSpec(memory_space=pltpu.VMEM)
    anywhere = pl.BlockSpec(memory_space=pl.ANY)

    def run_local(x_in, w_conv1, b_conv1, w_conv2, b_conv2):
        sums = pl.pallas_call(
            kernel,
            out_shape=jax.ShapeDtypeStruct((CHANS, CHANS), F32),
            in_specs=[anywhere] * 5,
            out_specs=vmem,
            scratch_shapes=scratch,
            compiler_params=pltpu.CompilerParams(collective_id=0, has_side_effects=True, vmem_limit_bytes=VMEM_LIMIT),
            name="two_convs",
        )(
            *(
                pltpu.with_memory_space_constraint(a, pltpu.HBM)
                for a in (
                    x_in.transpose(0, 1, 3, 2),
                    w_conv1.reshape(9, 4, CHANS),
                    w_conv2.reshape(4608, CHANS),
                    b_conv1.reshape(1, CHANS),
                    b_conv2.reshape(1, CHANS),
                )
            )
        )
        return pl.pallas_call(
            arrange,
            out_shape=jax.ShapeDtypeStruct((4, 16, 8, CHANS), F32),
            in_specs=[vmem],
            out_specs=anywhere,
            scratch_shapes=[pltpu.VMEM((4, 4, 4, 8, CHANS), F32), pltpu.SemaphoreType.DMA((4,))],
            compiler_params=pltpu.CompilerParams(vmem_limit_bytes=8 * 2**20),
            name="arrange",
        )(sums.reshape(8, 64, CHANS))

    return jax.shard_map(
        run_local,
        mesh=mesh,
        in_specs=(P("data", None, None, GROUP_AXES), P(None, None, GROUP_AXES, None), P(), P(), P()),
        out_specs=P("data", "model", "cols", None),
        check_vma=False,
    )
```

```python
import jax
import jax.numpy as jnp
from jax import lax
from jax.experimental import pallas as pl
from jax.experimental.pallas import tpu as pltpu
from jax.sharding import PartitionSpec as P

GROUP_AXES = ("model", "cols")
MESH = pl.DeviceIdType.MESH
BF16 = jnp.bfloat16
F32 = jnp.float32
CHANS = 512
LANES = 128
CUT = 96
VMEM_LIMIT = 36 * 2**20
ORDERS = (("y", "z", "x"), ("z", "x", "y"), ("x", "y", "z"))


def one_hot(shape, col_of_row):
    rows = lax.broadcasted_iota(jnp.int32, shape, 0)
    cols = lax.broadcasted_iota(jnp.int32, shape, 1)
    return jnp.where(cols == col_of_row(rows), 1.0, 0.0).astype(BF16)


def pack_windows(xv, a_scr, pack):
    to_lanes = one_hot((CHANS, CHANS), lambda r: (r % 4) * LANES + ((r % LANES) // 4) * 4 + r // LANES)
    to_rows = one_hot((CHANS, CHANS), lambda r: (r % 4) * LANES + ((r % 256) // 4) * 2 + r // 256)
    for blk in range(4):
        part = jnp.concatenate([xv[n, 32 * blk : 32 * blk + 32].reshape(LANES, LANES) for n in range(4)], axis=0)
        turned = lax.dot_general(part, to_lanes, (((0,), (0,)), ((), ())), preferred_element_type=F32).astype(BF16)
        for c in range(4):
            a_scr[c * LANES : (c + 1) * LANES, blk * LANES : (blk + 1) * LANES] = turned[:, c * LANES : (c + 1) * LANES]
    mixed = jnp.dot(to_rows, a_scr[...], preferred_element_type=F32)
    for blk in range(4):
        even = mixed[0:256, blk * LANES : (blk + 1) * LANES]
        odd = mixed[256:CHANS, blk * LANES : (blk + 1) * LANES]
        for half in range(2):
            s = slice(64 * half, 64 * half + 64)
            tile = jnp.concatenate([even[:, s], odd[:, s]], axis=1).astype(BF16)
            pack[2 * blk + half, 1:65] = tile.reshape(64, 4, LANES)
    edge = jnp.zeros((8, 1, 4, LANES), BF16)
    pack[:, 0:1] = edge
    pack[:, 65:66] = edge


def kernel(
    x_hbm, w1_hbm, w2_hbm, b1_hbm, b2_hbm, o_ref,
    xv, w1v, w2v, b1v, b2v, a_scr, pack, got, x0, x1, x2, edge, w1g, z_acc, y0, y1, y2, acc2,
    load_sem, xs_send, xs_recv, halo_send, halo_recv, step_send, step_recv,
):
    m = lax.axis_index("model")
    q = lax.axis_index("cols")
    me = {"x": m // 2, "z": q // 4, "y": q % 4}
    core = m % 2
    parts = range(3)
    barrier = pltpu.get_barrier_semaphore()

    at_model = [[(me["x"] + dx) % 4 * 2 + (core + dk) % 2 for dk in range(2)] for dx in range(4)]
    at_cols = [[(me["z"] + dz) % 4 * 4 + (me["y"] + dy) % 4 for dy in range(4)] for dz in range(4)]
    others = [(dx, dz, dy, dk) for dx in range(4) for dz in range(4) for dy in range(4) for dk in range(2)]
    others = sorted(others[1:], key=lambda d: (sum(d[:3]) % 4, d))

    def away(d):
        return {"model": at_model[d[0]][d[3]], "cols": at_cols[d[1]][d[2]]}

    loads = [
        pltpu.make_async_copy(src, dst, load_sem.at[k])
        for k, (src, dst) in enumerate(
            ((x_hbm, xv), (w1_hbm, w1v), (w2_hbm, w2v.at[pl.ds(0, 4608)]), (b1_hbm, b1v), (b2_hbm, b2v))
        )
    ]
    for load in loads:
        load.start()
    with jax.named_scope("announce"):
        for d in sorted(others, key=lambda d: -sum(min(o, 4 - o) for o in d[:3])):
            pl.semaphore_signal(barrier, inc=1, device_id=away(d), device_id_type=MESH)

    def piece(p, t, v, n, c, place=None, half=None):
        done = ORDERS[p][:t]
        rest = [a for a in "xzy" if a != ORDERS[p][2]]
        at = [v if t < 2 and a == ORDERS[p][t] else (pl.ds(0, 4) if a in done else me[a]) for a in rest]
        if half is not None:
            at[0] = pl.ds(2 * half, 2)
        return w1g.at[p, pl.ds(0, 2) if n is None else n, me[ORDERS[p][2]] if t < 2 else v, c, at[0], at[1]]

    with jax.named_scope("place_w1"):
        loads[1].wait()
        for p in parts:
            spot = [me[a] for a in "xzy" if a != ORDERS[p][2]]
            for dw in range(3):
                for lt in range(4):
                    tile = w1v[3 * p + dw, :, lt * LANES : (lt + 1) * LANES]
                    w1g[p, lt // 2, me[ORDERS[p][2]], core, spot[0], spot[1], dw, lt % 2] = tile
    with jax.named_scope("wait_x"):
        loads[0].wait()
    with jax.named_scope("pack"):
        pack_windows(xv, a_scr, pack)
    with jax.named_scope("wait_barrier"):
        pl.semaphore_wait(barrier, 127)

    n_steps = [0]
    steps = []

    class Step:
        def __init__(self, slabs, copies):
            k = n_steps[0]
            n_steps[0] += 1
            sems = dict(send_sem=step_send.at[k], recv_sem=step_recv.at[k], device_id_type=MESH)
            self.copies, self.sems = copies, sems
            span = got.at[pl.ds(0, slabs)]
            self.all = pltpu.make_async_remote_copy(
                src_ref=span, dst_ref=span, device_id={"model": at_model[0][1], "cols": q}, **sems
            )
            steps.append(self)

        def go(self):
            for ref, to in self.copies:
                pltpu.make_async_remote_copy(src_ref=ref, dst_ref=ref, device_id=to, **self.sems).start()
            return self

        def land(self):
            self.all.wait_recv()

    def chip(p, t, d, c=0):
        axis = ORDERS[p][t]
        pos = me | {axis: (me[axis] + d) % 4}
        return {"model": pos["x"] * 2 + (core + c) % 2, "cols": pos["z"] * 4 + pos["y"]}

    def spread(t, slabs):
        return Step(slabs, [(piece(p, t, me[ORDERS[p][t]], None, core), chip(p, t, d)) for p in parts for d in (1, 3, 2)]).go()

    def plane(p, d):
        return (me[ORDERS[p][2]] + d) % 4

    def hand_over(pieces, slabs):
        return Step(slabs, [(ref, {"model": at_model[0][1], "cols": q}) for ref in pieces]).go()

    def send_windows(first, last):
        for d in others[first:last]:
            to = away(d)
            pltpu.make_async_remote_copy(
                src_ref=pack.at[to["model"], pl.ds(4 * to["cols"], 6)],
                dst_ref=got.at[mine],
                send_sem=xs_send,
                recv_sem=xs_recv,
                device_id=to,
                device_id_type=MESH,
            ).start()

    mine = ((core * 4 + me["x"]) * 4 + me["z"]) * 4 + me["y"]
    with jax.named_scope("send_first"):
        first = spread(0, 18)
        for pair in range(6):
            got[mine, pair] = pack[m, 4 * q + pair]
        send_windows(0, CUT)
    with jax.named_scope("wait_first"):
        first.land()
    with jax.named_scope("send_second"):
        second = spread(1, 72)
        send_windows(CUT, 127)
    with jax.named_scope("wait_second"):
        second.land()
    last, passed, lent, lent_on = {}, {}, {}, {}

    def send_plane(n):
        last[n] = Step(96, [(piece(p, 2, plane(p, 0), n, core), chip(p, 2, d)) for p in parts for d in (1, 3)])

    def pass_on(n):
        with jax.named_scope(f"wait_last{n}"):
            last[n].land()
        passed[n] = Step(48, [(piece(p, 2, plane(p, 4 - d), n, core, half=d // 2), chip(p, 2, d)) for p in parts for d in (1, 3)]).go()
        lent[n] = hand_over([piece(p, 2, plane(p, d), n, core) for p in parts for d in (1, 3)], 96)

    def finish(n):
        with jax.named_scope(f"wait_passed{n}"):
            passed[n].land()
        lent_on[n] = hand_over([piece(p, 2, plane(p, 2), n, core) for p in parts], 48)

    with jax.named_scope("send_third"):
        for n in range(2):
            send_plane(n)
        last[0].go()
        own = hand_over([piece(p, 2, plane(p, 0), None, core) for p in parts], 96)
    last[1].go()
    span = got.at[pl.ds(0, 127)]
    everything = pltpu.make_async_remote_copy(
        src_ref=span, dst_ref=span, send_sem=xs_send, recv_sem=xs_recv, device_id=chip(0, 0, 0, 1), device_id_type=MESH
    )
    with jax.named_scope("wait_windows"):
        everything.wait_recv()

    xs, ys = (x0, x1, x2), (y0, y1, y2)
    with jax.named_scope("turn"):
        for pair in range(6):
            for p in parts:
                rows = []
                for v in range(4):
                    for c in range(2):
                        at = 64 * c
                        if p == 0:
                            rows.append(got[at + 16 * v : at + 16 * v + 16, pair])
                        elif p == 1:
                            rows.append(got[at + v : at + 64 : 4, pair])
                        else:
                            rows += [got[at + 16 * a + 4 * v : at + 16 * a + 4 * v + 4, pair] for a in range(4)]
                rows = jnp.concatenate([r.reshape(-1, LANES) for r in rows], axis=0).T
                for odd in range(2):
                    main = rows[64 * odd : 64 * odd + 64]
                    xs[p][2 * pair + odd, 8 - 4 * p : 72 - 4 * p] = main
                    if p == 1:
                        edge[0, 2 * pair + odd] = main[60:64]
                        edge[1, 2 * pair + odd] = main[0:4]
    def conv1(halves, places, spans, groups):
        width = 10 // groups
        tops = [None] * groups
        taps = [(p, dw, plane(p, d)) for p in parts for dw in range(3) for d in places]
        for first in range(0, len(taps), 2):
            two = taps[first : first + 2]
            right = [[w1g[p, n, v, :, :, :, dw, i].reshape(LANES, LANES) for n in halves for i in range(2)] for p, dw, v in two]
            right = jnp.concatenate([jnp.concatenate(r, axis=1) for r in right], axis=0)
            for group in range(groups):
                left = []
                for rows in spans:
                    some = []
                    for p, dw, v in two:
                        lanes = pl.ds(pl.multiple_of(LANES * v, LANES), LANES)
                        some.append(xs[p][pl.ds(dw + width * group, width), rows, lanes])
                    left.append(jnp.concatenate(some, axis=-1))
                left = jnp.concatenate(left, axis=1).reshape(-1, LANES * len(two))
                term = jnp.dot(left, right, preferred_element_type=F32)
                tops[group] = term if tops[group] is None else tops[group] + term
        return [top.reshape(width, -1, 256 * len(halves)) for top in tops]

    top_rows, inner, low_rows = pl.ds(0, 8), pl.ds(8, 56), pl.ds(64, 8)

    def here(n):
        with jax.named_scope(f"here{n}"):
            for group, top in enumerate(conv1((n,), (0,), (inner,), 2)):
                z_acc[n, pl.ds(5 * group, 5), inner] = top

    def near(n):
        with jax.named_scope(f"wait_lent{n}"):
            lent[n].land()
        with jax.named_scope(f"near{n}"):
            for group, top in enumerate(conv1((n,), (3, 1), (inner,), 2)):
                z_acc[n, pl.ds(5 * group, 5), inner] += top

    def rim():
        with jax.named_scope("rim"):
            (top,) = conv1((0, 1), (0, 3, 1), (top_rows, low_rows), 1)
            for n in range(2):
                part = top[:, :, 256 * n : 256 * n + 256]
                z_acc[n, :, top_rows] = part[:, :8]
                z_acc[n, :, low_rows] = part[:, 8:]

    def far(n):
        with jax.named_scope(f"wait_lent_on{n}"):
            lent_on[n].land()
        lanes = slice(256 * n, 256 * n + 256)
        with jax.named_scope(f"far{n}"):
            for group, top in enumerate(conv1((n,), (2,), (pl.ds(0, 72),), 2)):
                cols = pl.ds(5 * group, 5)
                act = jnp.maximum(z_acc[n, cols] + top + b1v[:, lanes], 0.0)
                for dh in range(3):
                    ys[dh][cols, :, lanes] = act[:, 4 * dh : 4 * dh + 64].astype(BF16)

        def clear(at_edge, refs, cols, rows):
            @pl.when(at_edge)
            def _():
                for ref in refs:
                    ref[cols, rows, lanes] = jnp.zeros((cols.size, rows.size, 256), BF16)

        clear(q == 0, ys, pl.ds(0, 1), pl.ds(0, 64))
        clear(q == 15, ys, pl.ds(9, 1), pl.ds(0, 64))
        clear(m == 0, (y0,), pl.ds(0, 10), pl.ds(0, 4))
        clear(m == 7, (y2,), pl.ds(0, 10), pl.ds(60, 4))

    def conv2(n):
        lanes = slice(256 * n, 256 * n + 256)
        total = None
        for dh in range(3):
            for dw in range(3):
                tap = 3 * dh + dw
                left = ys[dh][dw : dw + 8, :, lanes].reshape(CHANS, 256)
                right = w2v[CHANS * tap + 256 * n : CHANS * tap + 256 * n + 256, :]
                term = jnp.dot(left, right, preferred_element_type=F32)
                total = term if total is None else total + term
        return total

    pass_on(0)
    halo = []
    for src, dst, d in (
        (x0.at[:, pl.ds(64, 8)], x0.at[:, pl.ds(0, 8)], 1),
        (x2.at[:, pl.ds(0, 8)], x2.at[:, pl.ds(64, 8)], 7),
        (edge.at[0], edge.at[2], 1),
        (edge.at[1], edge.at[3], 7),
    ):
        halo.append(
            pltpu.make_async_remote_copy(
                src_ref=src,
                dst_ref=dst,
                send_sem=halo_send.at[len(halo)],
                recv_sem=halo_recv.at[len(halo)],
                device_id={"model": (m + d) % 8, "cols": q},
                device_id_type=MESH,
            )
        )
        halo[-1].start()
    with jax.named_scope("wait_own"):
        own.land()
    here(0)
    here(1)
    pass_on(1)
    near(0)
    near(1)
    finish(0)
    with jax.named_scope("wait_halo"):
        for copy in halo:
            copy.wait_recv()

    @pl.when(m == 0)
    def _():
        x0[:, 0:8] = jnp.zeros((12, 8, CHANS), BF16)
        x1[:, 0:4] = jnp.zeros((12, 4, CHANS), BF16)

    @pl.when(m > 0)
    def _():
        x1[:, 0:4] = edge[2]

    @pl.when(m == 7)
    def _():
        x2[:, 64:72] = jnp.zeros((12, 8, CHANS), BF16)
        x1[:, 68:72] = jnp.zeros((12, 4, CHANS), BF16)

    @pl.when(m < 7)
    def _():
        x1[:, 68:72] = edge[3]

    rim()
    finish(1)
    with jax.named_scope("wait_w2"):
        for load in loads[2:]:
            load.wait()
    far(0)
    with jax.named_scope("conv2_0"):
        acc2[...] = conv2(0)
    far(1)
    with jax.named_scope("conv2_1"):
        o_ref[...] = acc2[...] + conv2(1) + b2v[...]

    with jax.named_scope("wait_sends"):
        everything.wait_send()
        for step in steps:
            step.all.wait_send()
        for copy in halo:
            copy.wait_send()


def arrange(sum_ref, o_hbm, turned, sems):
    copies = []
    for g in range(4):
        rows = jnp.transpose(sum_ref[:, 16 * g : 16 * g + 16], (1, 0, 2))
        for h in range(4):
            for image in range(4):
                turned[g, image, h] = rows[4 * h + image]
        copies.append(pltpu.make_async_copy(turned.at[g], o_hbm.at[:, pl.ds(4 * g, 4)], sems.at[g]))
        copies[-1].start()
    for copy in copies:
        copy.wait()


def solution(mesh):
    scratch = [
        pltpu.VMEM((4, LANES, 4, LANES), BF16),
        pltpu.VMEM((9, 4, CHANS), BF16),
        pltpu.VMEM((4616, CHANS), BF16),
        pltpu.VMEM((1, CHANS), F32),
        pltpu.VMEM((1, CHANS), F32),
        pltpu.VMEM((CHANS, CHANS), BF16),
        pltpu.VMEM((8, 66, 4, LANES), BF16),
        pltpu.VMEM((LANES, 6, 4, LANES), BF16),
        *[pltpu.VMEM((12, 72, CHANS), BF16) for _ in range(3)],
        pltpu.VMEM((4, 12, 4, CHANS), BF16),
        pltpu.VMEM((3, 2, 4, 2, 4, 4, 3, 2, 4, LANES), BF16),
        pltpu.VMEM((2, 10, 72, 256), F32),
        *[pltpu.VMEM((10, 64, CHANS), BF16) for _ in range(3)],
        pltpu.VMEM((CHANS, CHANS), F32),
        pltpu.SemaphoreType.DMA((5,)),
        pltpu.SemaphoreType.DMA,
        pltpu.SemaphoreType.DMA,
        pltpu.SemaphoreType.DMA((4,)),
        pltpu.SemaphoreType.DMA((4,)),
        pltpu.SemaphoreType.DMA((11,)),
        pltpu.SemaphoreType.DMA((11,)),
    ]
    vmem = pl.BlockSpec(memory_space=pltpu.VMEM)
    anywhere = pl.BlockSpec(memory_space=pl.ANY)

    def run_local(x_in, w_conv1, b_conv1, w_conv2, b_conv2):
        sums = pl.pallas_call(
            kernel,
            out_shape=jax.ShapeDtypeStruct((CHANS, CHANS), F32),
            in_specs=[anywhere] * 5,
            out_specs=vmem,
            scratch_shapes=scratch,
            compiler_params=pltpu.CompilerParams(collective_id=0, has_side_effects=True, vmem_limit_bytes=VMEM_LIMIT),
            name="two_convs",
        )(
            *(
                pltpu.with_memory_space_constraint(a, pltpu.HBM)
                for a in (
                    x_in.transpose(0, 1, 3, 2),
                    w_conv1.reshape(9, 4, CHANS),
                    w_conv2.reshape(4608, CHANS),
                    b_conv1.reshape(1, CHANS),
                    b_conv2.reshape(1, CHANS),
                )
            )
        )
        return pl.pallas_call(
            arrange,
            out_shape=jax.ShapeDtypeStruct((4, 16, 8, CHANS), F32),
            in_specs=[vmem],
            out_specs=anywhere,
            scratch_shapes=[pltpu.VMEM((4, 4, 4, 8, CHANS), F32), pltpu.SemaphoreType.DMA((4,))],
            compiler_params=pltpu.CompilerParams(vmem_limit_bytes=8 * 2**20),
            name="arrange",
        )(sums.reshape(8, 64, CHANS))

    return jax.shard_map(
        run_local,
        mesh=mesh,
        in_specs=(P("data", None, None, GROUP_AXES), P(None, None, GROUP_AXES, None), P(), P(), P()),
        out_specs=P("data", "model", "cols", None),
        check_vma=False,
    )
```

```python
import jax
import jax.numpy as jnp
from jax import lax
from jax.experimental import pallas as pl
from jax.experimental.pallas import tpu as pltpu
from jax.sharding import PartitionSpec as P

GROUP_AXES = ("model", "cols")
MESH = pl.DeviceIdType.MESH
BF16 = jnp.bfloat16
F32 = jnp.float32
CHANS = 512
LANES = 128
CUT = 96
VMEM_LIMIT = 36 * 2**20
ORDERS = (("y", "z", "x"), ("z", "x", "y"), ("x", "y", "z"))


def one_hot(shape, col_of_row):
    rows = lax.broadcasted_iota(jnp.int32, shape, 0)
    cols = lax.broadcasted_iota(jnp.int32, shape, 1)
    return jnp.where(cols == col_of_row(rows), 1.0, 0.0).astype(BF16)


def pack_windows(xv, a_scr, pack):
    to_lanes = one_hot((CHANS, CHANS), lambda r: (r % 4) * LANES + ((r % LANES) // 4) * 4 + r // LANES)
    to_rows = one_hot((CHANS, CHANS), lambda r: (r % 4) * LANES + ((r % 256) // 4) * 2 + r // 256)
    for blk in range(4):
        part = jnp.concatenate([xv[n, 32 * blk : 32 * blk + 32].reshape(LANES, LANES) for n in range(4)], axis=0)
        turned = lax.dot_general(part, to_lanes, (((0,), (0,)), ((), ())), preferred_element_type=F32).astype(BF16)
        for c in range(4):
            a_scr[c * LANES : (c + 1) * LANES, blk * LANES : (blk + 1) * LANES] = turned[:, c * LANES : (c + 1) * LANES]
    mixed = jnp.dot(to_rows, a_scr[...], preferred_element_type=F32)
    for blk in range(4):
        even = mixed[0:256, blk * LANES : (blk + 1) * LANES]
        odd = mixed[256:CHANS, blk * LANES : (blk + 1) * LANES]
        for half in range(2):
            s = slice(64 * half, 64 * half + 64)
            tile = jnp.concatenate([even[:, s], odd[:, s]], axis=1).astype(BF16)
            pack[2 * blk + half, 1:65] = tile.reshape(64, 4, LANES)
    edge = jnp.zeros((8, 1, 4, LANES), BF16)
    pack[:, 0:1] = edge
    pack[:, 65:66] = edge


def kernel(
    x_hbm, w1_hbm, w2_hbm, b1_hbm, b2_hbm, o_ref,
    xv, w1v, w2v, b1v, b2v, a_scr, pack, got, x0, x1, x2, edge, w1g, z_acc, y0, y1, y2, acc2,
    load_sem, xs_send, xs_recv, halo_send, halo_recv, step_send, step_recv,
):
    m = lax.axis_index("model")
    q = lax.axis_index("cols")
    me = {"x": m // 2, "z": q // 4, "y": q % 4}
    core = m % 2
    parts = range(3)
    barrier = pltpu.get_barrier_semaphore()

    at_model = [[(me["x"] + dx) % 4 * 2 + (core + dk) % 2 for dk in range(2)] for dx in range(4)]
    at_cols = [[(me["z"] + dz) % 4 * 4 + (me["y"] + dy) % 4 for dy in range(4)] for dz in range(4)]
    others = [(dx, dz, dy, dk) for dx in range(4) for dz in range(4) for dy in range(4) for dk in range(2)]
    others = sorted(others[1:], key=lambda d: (sum(d[:3]) % 4, d))

    def away(d):
        return {"model": at_model[d[0]][d[3]], "cols": at_cols[d[1]][d[2]]}

    loads = [
        pltpu.make_async_copy(src, dst, load_sem.at[k])
        for k, (src, dst) in enumerate(
            ((x_hbm, xv), (w1_hbm, w1v), (w2_hbm, w2v.at[pl.ds(0, 4608)]), (b1_hbm, b1v), (b2_hbm, b2v))
        )
    ]
    for load in loads:
        load.start()
    with jax.named_scope("announce"):
        for d in sorted(others, key=lambda d: -sum(min(o, 4 - o) for o in d[:3])):
            pl.semaphore_signal(barrier, inc=1, device_id=away(d), device_id_type=MESH)

    def piece(p, t, v, n, c, place=None, half=None):
        done = ORDERS[p][:t]
        rest = [a for a in "xzy" if a != ORDERS[p][2]]
        at = [v if t < 2 and a == ORDERS[p][t] else (pl.ds(0, 4) if a in done else me[a]) for a in rest]
        if half is not None:
            at[0] = pl.ds(2 * half, 2)
        return w1g.at[p, pl.ds(0, 2) if n is None else n, me[ORDERS[p][2]] if t < 2 else v, c, at[0], at[1]]

    with jax.named_scope("place_w1"):
        loads[1].wait()
        for p in parts:
            spot = [me[a] for a in "xzy" if a != ORDERS[p][2]]
            for dw in range(3):
                for lt in range(4):
                    tile = w1v[3 * p + dw, :, lt * LANES : (lt + 1) * LANES]
                    w1g[p, lt // 2, me[ORDERS[p][2]], core, spot[0], spot[1], dw, lt % 2] = tile
    with jax.named_scope("wait_x"):
        loads[0].wait()
    with jax.named_scope("pack"):
        pack_windows(xv, a_scr, pack)
    with jax.named_scope("wait_barrier"):
        pl.semaphore_wait(barrier, 127)

    n_steps = [0]
    steps = []

    class Step:
        def __init__(self, slabs, copies):
            k = n_steps[0]
            n_steps[0] += 1
            sems = dict(send_sem=step_send.at[k], recv_sem=step_recv.at[k], device_id_type=MESH)
            self.copies, self.sems = copies, sems
            span = got.at[pl.ds(0, slabs)]
            self.all = pltpu.make_async_remote_copy(
                src_ref=span, dst_ref=span, device_id={"model": at_model[0][1], "cols": q}, **sems
            )
            steps.append(self)

        def go(self):
            for ref, to in self.copies:
                pltpu.make_async_remote_copy(src_ref=ref, dst_ref=ref, device_id=to, **self.sems).start()
            return self

        def land(self):
            self.all.wait_recv()

    def chip(p, t, d, c=0):
        axis = ORDERS[p][t]
        pos = me | {axis: (me[axis] + d) % 4}
        return {"model": pos["x"] * 2 + (core + c) % 2, "cols": pos["z"] * 4 + pos["y"]}

    def spread(t, slabs):
        return Step(slabs, [(piece(p, t, me[ORDERS[p][t]], None, core), chip(p, t, d)) for p in parts for d in (1, 3, 2)]).go()

    def plane(p, d):
        return (me[ORDERS[p][2]] + d) % 4

    def hand_over(pieces, slabs):
        return Step(slabs, [(ref, {"model": at_model[0][1], "cols": q}) for ref in pieces]).go()

    def send_windows(first, last):
        for d in others[first:last]:
            to = away(d)
            pltpu.make_async_remote_copy(
                src_ref=pack.at[to["model"], pl.ds(4 * to["cols"], 6)],
                dst_ref=got.at[mine],
                send_sem=xs_send,
                recv_sem=xs_recv,
                device_id=to,
                device_id_type=MESH,
            ).start()

    mine = ((core * 4 + me["x"]) * 4 + me["z"]) * 4 + me["y"]
    with jax.named_scope("send_first"):
        first = spread(0, 18)
        for pair in range(6):
            got[mine, pair] = pack[m, 4 * q + pair]
        send_windows(0, CUT)
    with jax.named_scope("wait_first"):
        first.land()
    with jax.named_scope("send_second"):
        second = spread(1, 72)
        send_windows(CUT, 127)
    with jax.named_scope("wait_second"):
        second.land()
    last, passed, lent, lent_on = {}, {}, {}, {}

    def send_plane(n):
        last[n] = Step(96, [(piece(p, 2, plane(p, 0), n, core), chip(p, 2, d)) for p in parts for d in (1, 3)])

    def pass_on(n):
        with jax.named_scope(f"wait_last{n}"):
            last[n].land()
        passed[n] = Step(48, [(piece(p, 2, plane(p, 4 - d), n, core, half=d // 2), chip(p, 2, d)) for p in parts for d in (1, 3)]).go()
        lent[n] = hand_over([piece(p, 2, plane(p, d), n, core) for p in parts for d in (1, 3)], 96)

    def finish(n):
        with jax.named_scope(f"wait_passed{n}"):
            passed[n].land()
        lent_on[n] = hand_over([piece(p, 2, plane(p, 2), n, core) for p in parts], 48)

    with jax.named_scope("send_third"):
        for n in range(2):
            send_plane(n)
        last[0].go()
        own = hand_over([piece(p, 2, plane(p, 0), None, core) for p in parts], 96)
    last[1].go()
    span = got.at[pl.ds(0, 127)]
    everything = pltpu.make_async_remote_copy(
        src_ref=span, dst_ref=span, send_sem=xs_send, recv_sem=xs_recv, device_id=chip(0, 0, 0, 1), device_id_type=MESH
    )
    with jax.named_scope("wait_windows"):
        everything.wait_recv()

    xs, ys = (x0, x1, x2), (y0, y1, y2)
    with jax.named_scope("turn"):
        for pair in range(6):
            for p in parts:
                rows = []
                for v in range(4):
                    for c in range(2):
                        at = 64 * c
                        if p == 0:
                            rows.append(got[at + 16 * v : at + 16 * v + 16, pair])
                        elif p == 1:
                            rows.append(got[at + v : at + 64 : 4, pair])
                        else:
                            rows += [got[at + 16 * a + 4 * v : at + 16 * a + 4 * v + 4, pair] for a in range(4)]
                rows = jnp.concatenate([r.reshape(-1, LANES) for r in rows], axis=0).T
                for odd in range(2):
                    main = rows[64 * odd : 64 * odd + 64]
                    xs[p][2 * pair + odd, 8 - 4 * p : 72 - 4 * p] = main
                    if p == 1:
                        edge[0, 2 * pair + odd] = main[60:64]
                        edge[1, 2 * pair + odd] = main[0:4]
    def conv1(halves, places, spans, groups):
        width = 10 // groups
        tops = [None] * groups
        taps = [(p, dw, plane(p, d)) for p in parts for dw in range(3) for d in places]
        for first in range(0, len(taps), 2):
            two = taps[first : first + 2]
            right = [[w1g[p, n, v, :, :, :, dw, i].reshape(LANES, LANES) for n in halves for i in range(2)] for p, dw, v in two]
            right = jnp.concatenate([jnp.concatenate(r, axis=1) for r in right], axis=0)
            for group in range(groups):
                left = []
                for rows in spans:
                    some = []
                    for p, dw, v in two:
                        lanes = pl.ds(pl.multiple_of(LANES * v, LANES), LANES)
                        some.append(xs[p][pl.ds(dw + width * group, width), rows, lanes])
                    left.append(jnp.concatenate(some, axis=-1))
                left = jnp.concatenate(left, axis=1).reshape(-1, LANES * len(two))
                term = jnp.dot(left, right, preferred_element_type=F32)
                tops[group] = term if tops[group] is None else tops[group] + term
        return [top.reshape(width, -1, 256 * len(halves)) for top in tops]

    top_rows, inner, low_rows = pl.ds(0, 8), pl.ds(8, 56), pl.ds(64, 8)

    def here(n):
        with jax.named_scope(f"here{n}"):
            for group, top in enumerate(conv1((n,), (0,), (inner,), 2)):
                z_acc[n, pl.ds(5 * group, 5), inner] = top

    def near(n):
        with jax.named_scope(f"wait_lent{n}"):
            lent[n].land()
        with jax.named_scope(f"near{n}"):
            for group, top in enumerate(conv1((n,), (3, 1), (inner,), 2)):
                z_acc[n, pl.ds(5 * group, 5), inner] += top

    def rim():
        with jax.named_scope("rim"):
            (top,) = conv1((0, 1), (0, 3, 1), (top_rows, low_rows), 1)
            for n in range(2):
                part = top[:, :, 256 * n : 256 * n + 256]
                z_acc[n, :, top_rows] = part[:, :8]
                z_acc[n, :, low_rows] = part[:, 8:]

    def far(n):
        with jax.named_scope(f"wait_lent_on{n}"):
            lent_on[n].land()
        lanes = slice(256 * n, 256 * n + 256)
        with jax.named_scope(f"far{n}"):
            for group, top in enumerate(conv1((n,), (2,), (pl.ds(0, 72),), 2)):
                cols = pl.ds(5 * group, 5)
                act = jnp.maximum(z_acc[n, cols] + top + b1v[:, lanes], 0.0)
                for dh in range(3):
                    ys[dh][cols, :, lanes] = act[:, 4 * dh : 4 * dh + 64].astype(BF16)

        def clear(at_edge, refs, cols, rows):
            @pl.when(at_edge)
            def _():
                for ref in refs:
                    ref[cols, rows, lanes] = jnp.zeros((cols.size, rows.size, 256), BF16)

        clear(q == 0, ys, pl.ds(0, 1), pl.ds(0, 64))
        clear(q == 15, ys, pl.ds(9, 1), pl.ds(0, 64))
        clear(m == 0, (y0,), pl.ds(0, 10), pl.ds(0, 4))
        clear(m == 7, (y2,), pl.ds(0, 10), pl.ds(60, 4))

    def conv2(n):
        lanes = slice(256 * n, 256 * n + 256)
        total = None
        for dh in range(3):
            for dw in range(3):
                tap = 3 * dh + dw
                left = ys[dh][dw : dw + 8, :, lanes].reshape(CHANS, 256)
                right = w2v[CHANS * tap + 256 * n : CHANS * tap + 256 * n + 256, :]
                term = jnp.dot(left, right, preferred_element_type=F32)
                total = term if total is None else total + term
        return total

    pass_on(0)
    with jax.named_scope("wait_own"):
        own.land()
    here(0)
    here(1)
    pass_on(1)
    halo = []
    for src, dst, d in (
        (x0.at[:, pl.ds(64, 8)], x0.at[:, pl.ds(0, 8)], 1),
        (x2.at[:, pl.ds(0, 8)], x2.at[:, pl.ds(64, 8)], 7),
        (edge.at[0], edge.at[2], 1),
        (edge.at[1], edge.at[3], 7),
    ):
        halo.append(
            pltpu.make_async_remote_copy(
                src_ref=src,
                dst_ref=dst,
                send_sem=halo_send.at[len(halo)],
                recv_sem=halo_recv.at[len(halo)],
                device_id={"model": (m + d) % 8, "cols": q},
                device_id_type=MESH,
            )
        )
        halo[-1].start()
    near(0)
    near(1)
    finish(0)
    with jax.named_scope("wait_halo"):
        for copy in halo:
            copy.wait_recv()

    @pl.when(m == 0)
    def _():
        x0[:, 0:8] = jnp.zeros((12, 8, CHANS), BF16)
        x1[:, 0:4] = jnp.zeros((12, 4, CHANS), BF16)

    @pl.when(m > 0)
    def _():
        x1[:, 0:4] = edge[2]

    @pl.when(m == 7)
    def _():
        x2[:, 64:72] = jnp.zeros((12, 8, CHANS), BF16)
        x1[:, 68:72] = jnp.zeros((12, 4, CHANS), BF16)

    @pl.when(m < 7)
    def _():
        x1[:, 68:72] = edge[3]

    rim()
    finish(1)
    with jax.named_scope("wait_w2"):
        for load in loads[2:]:
            load.wait()
    far(0)
    with jax.named_scope("conv2_0"):
        acc2[...] = conv2(0)
    far(1)
    with jax.named_scope("conv2_1"):
        o_ref[...] = acc2[...] + conv2(1) + b2v[...]

    with jax.named_scope("wait_sends"):
        everything.wait_send()
        for step in steps:
            step.all.wait_send()
        for copy in halo:
            copy.wait_send()


def arrange(sum_ref, o_hbm, turned, sems):
    copies = []
    for g in range(4):
        rows = jnp.transpose(sum_ref[:, 16 * g : 16 * g + 16], (1, 0, 2))
        for h in range(4):
            for image in range(4):
                turned[g, image, h] = rows[4 * h + image]
        copies.append(pltpu.make_async_copy(turned.at[g], o_hbm.at[:, pl.ds(4 * g, 4)], sems.at[g]))
        copies[-1].start()
    for copy in copies:
        copy.wait()


def solution(mesh):
    scratch = [
        pltpu.VMEM((4, LANES, 4, LANES), BF16),
        pltpu.VMEM((9, 4, CHANS), BF16),
        pltpu.VMEM((4616, CHANS), BF16),
        pltpu.VMEM((1, CHANS), F32),
        pltpu.VMEM((1, CHANS), F32),
        pltpu.VMEM((CHANS, CHANS), BF16),
        pltpu.VMEM((8, 66, 4, LANES), BF16),
        pltpu.VMEM((LANES, 6, 4, LANES), BF16),
        *[pltpu.VMEM((12, 72, CHANS), BF16) for _ in range(3)],
        pltpu.VMEM((4, 12, 4, CHANS), BF16),
        pltpu.VMEM((3, 2, 4, 2, 4, 4, 3, 2, 4, LANES), BF16),
        pltpu.VMEM((2, 10, 72, 256), F32),
        *[pltpu.VMEM((10, 64, CHANS), BF16) for _ in range(3)],
        pltpu.VMEM((CHANS, CHANS), F32),
        pltpu.SemaphoreType.DMA((5,)),
        pltpu.SemaphoreType.DMA,
        pltpu.SemaphoreType.DMA,
        pltpu.SemaphoreType.DMA((4,)),
        pltpu.SemaphoreType.DMA((4,)),
        pltpu.SemaphoreType.DMA((11,)),
        pltpu.SemaphoreType.DMA((11,)),
    ]
    vmem = pl.BlockSpec(memory_space=pltpu.VMEM)
    anywhere = pl.BlockSpec(memory_space=pl.ANY)

    def run_local(x_in, w_conv1, b_conv1, w_conv2, b_conv2):
        sums = pl.pallas_call(
            kernel,
            out_shape=jax.ShapeDtypeStruct((CHANS, CHANS), F32),
            in_specs=[anywhere] * 5,
            out_specs=vmem,
            scratch_shapes=scratch,
            compiler_params=pltpu.CompilerParams(collective_id=0, has_side_effects=True, vmem_limit_bytes=VMEM_LIMIT),
            name="two_convs",
        )(
            *(
                pltpu.with_memory_space_constraint(a, pltpu.HBM)
                for a in (
                    x_in.transpose(0, 1, 3, 2),
                    w_conv1.reshape(9, 4, CHANS),
                    w_conv2.reshape(4608, CHANS),
                    b_conv1.reshape(1, CHANS),
                    b_conv2.reshape(1, CHANS),
                )
            )
        )
        return pl.pallas_call(
            arrange,
            out_shape=jax.ShapeDtypeStruct((4, 16, 8, CHANS), F32),
            in_specs=[vmem],
            out_specs=anywhere,
            scratch_shapes=[pltpu.VMEM((4, 4, 4, 8, CHANS), F32), pltpu.SemaphoreType.DMA((4,))],
            compiler_params=pltpu.CompilerParams(vmem_limit_bytes=8 * 2**20),
            name="arrange",
        )(sums.reshape(8, 64, CHANS))

    return jax.shard_map(
        run_local,
        mesh=mesh,
        in_specs=(P("data", None, None, GROUP_AXES), P(None, None, GROUP_AXES, None), P(), P(), P()),
        out_specs=P("data", "model", "cols", None),
        check_vma=False,
    )
```

```python
import jax
import jax.numpy as jnp
from jax import lax
from jax.experimental import pallas as pl
from jax.experimental.pallas import tpu as pltpu
from jax.sharding import PartitionSpec as P

GROUP_AXES = ("model", "cols")
MESH = pl.DeviceIdType.MESH
BF16 = jnp.bfloat16
F32 = jnp.float32
CHANS = 512
LANES = 128
CUT = 104
VMEM_LIMIT = 36 * 2**20
ORDERS = (("y", "z", "x"), ("z", "x", "y"), ("x", "y", "z"))


def one_hot(shape, col_of_row):
    rows = lax.broadcasted_iota(jnp.int32, shape, 0)
    cols = lax.broadcasted_iota(jnp.int32, shape, 1)
    return jnp.where(cols == col_of_row(rows), 1.0, 0.0).astype(BF16)


def pack_windows(xv, a_scr, pack):
    to_lanes = one_hot((CHANS, CHANS), lambda r: (r % 4) * LANES + ((r % LANES) // 4) * 4 + r // LANES)
    to_rows = one_hot((CHANS, CHANS), lambda r: (r % 4) * LANES + ((r % 256) // 4) * 2 + r // 256)
    for blk in range(4):
        part = jnp.concatenate([xv[n, 32 * blk : 32 * blk + 32].reshape(LANES, LANES) for n in range(4)], axis=0)
        turned = lax.dot_general(part, to_lanes, (((0,), (0,)), ((), ())), preferred_element_type=F32).astype(BF16)
        for c in range(4):
            a_scr[c * LANES : (c + 1) * LANES, blk * LANES : (blk + 1) * LANES] = turned[:, c * LANES : (c + 1) * LANES]
    mixed = jnp.dot(to_rows, a_scr[...], preferred_element_type=F32)
    for blk in range(4):
        even = mixed[0:256, blk * LANES : (blk + 1) * LANES]
        odd = mixed[256:CHANS, blk * LANES : (blk + 1) * LANES]
        for half in range(2):
            s = slice(64 * half, 64 * half + 64)
            tile = jnp.concatenate([even[:, s], odd[:, s]], axis=1).astype(BF16)
            pack[2 * blk + half, 1:65] = tile.reshape(64, 4, LANES)
    edge = jnp.zeros((8, 1, 4, LANES), BF16)
    pack[:, 0:1] = edge
    pack[:, 65:66] = edge


def kernel(
    x_hbm, w1_hbm, w2_hbm, b1_hbm, b2_hbm, o_ref,
    xv, w1v, w2v, b1v, b2v, a_scr, pack, got, x0, x1, x2, edge, w1g, z_acc, y0, y1, y2, acc2,
    load_sem, xs_send, xs_recv, halo_send, halo_recv, step_send, step_recv,
):
    m = lax.axis_index("model")
    q = lax.axis_index("cols")
    me = {"x": m // 2, "z": q // 4, "y": q % 4}
    core = m % 2
    parts = range(3)
    barrier = pltpu.get_barrier_semaphore()

    at_model = [[(me["x"] + dx) % 4 * 2 + (core + dk) % 2 for dk in range(2)] for dx in range(4)]
    at_cols = [[(me["z"] + dz) % 4 * 4 + (me["y"] + dy) % 4 for dy in range(4)] for dz in range(4)]
    others = [(dx, dz, dy, dk) for dx in range(4) for dz in range(4) for dy in range(4) for dk in range(2)]
    others = sorted(others[1:], key=lambda d: (sum(d[:3]) % 4, d))

    def away(d):
        return {"model": at_model[d[0]][d[3]], "cols": at_cols[d[1]][d[2]]}

    loads = [
        pltpu.make_async_copy(src, dst, load_sem.at[k])
        for k, (src, dst) in enumerate(
            ((x_hbm, xv), (w1_hbm, w1v), (w2_hbm, w2v.at[pl.ds(0, 4608)]), (b1_hbm, b1v), (b2_hbm, b2v))
        )
    ]
    for load in loads:
        load.start()
    with jax.named_scope("announce"):
        for d in sorted(others, key=lambda d: -sum(min(o, 4 - o) for o in d[:3])):
            pl.semaphore_signal(barrier, inc=1, device_id=away(d), device_id_type=MESH)

    def piece(p, t, v, n, c, place=None, half=None):
        done = ORDERS[p][:t]
        rest = [a for a in "xzy" if a != ORDERS[p][2]]
        at = [v if t < 2 and a == ORDERS[p][t] else (pl.ds(0, 4) if a in done else me[a]) for a in rest]
        if half is not None:
            at[0] = pl.ds(2 * half, 2)
        return w1g.at[p, pl.ds(0, 2) if n is None else n, me[ORDERS[p][2]] if t < 2 else v, c, at[0], at[1]]

    with jax.named_scope("place_w1"):
        loads[1].wait()
        for p in parts:
            spot = [me[a] for a in "xzy" if a != ORDERS[p][2]]
            for dw in range(3):
                for lt in range(4):
                    tile = w1v[3 * p + dw, :, lt * LANES : (lt + 1) * LANES]
                    w1g[p, lt // 2, me[ORDERS[p][2]], core, spot[0], spot[1], dw, lt % 2] = tile
    with jax.named_scope("wait_x"):
        loads[0].wait()
    with jax.named_scope("pack"):
        pack_windows(xv, a_scr, pack)
    with jax.named_scope("wait_barrier"):
        pl.semaphore_wait(barrier, 127)

    n_steps = [0]
    steps = []

    class Step:
        def __init__(self, slabs, copies):
            k = n_steps[0]
            n_steps[0] += 1
            sems = dict(send_sem=step_send.at[k], recv_sem=step_recv.at[k], device_id_type=MESH)
            self.copies, self.sems = copies, sems
            span = got.at[pl.ds(0, slabs)]
            self.all = pltpu.make_async_remote_copy(
                src_ref=span, dst_ref=span, device_id={"model": at_model[0][1], "cols": q}, **sems
            )
            steps.append(self)

        def go(self):
            for ref, to in self.copies:
                pltpu.make_async_remote_copy(src_ref=ref, dst_ref=ref, device_id=to, **self.sems).start()
            return self

        def land(self):
            self.all.wait_recv()

    def chip(p, t, d, c=0):
        axis = ORDERS[p][t]
        pos = me | {axis: (me[axis] + d) % 4}
        return {"model": pos["x"] * 2 + (core + c) % 2, "cols": pos["z"] * 4 + pos["y"]}

    def spread(t, slabs):
        return Step(slabs, [(piece(p, t, me[ORDERS[p][t]], None, core), chip(p, t, d)) for p in parts for d in (1, 3, 2)]).go()

    def plane(p, d):
        return (me[ORDERS[p][2]] + d) % 4

    def hand_over(pieces, slabs):
        return Step(slabs, [(ref, {"model": at_model[0][1], "cols": q}) for ref in pieces]).go()

    def send_windows(first, last):
        for d in others[first:last]:
            to = away(d)
            pltpu.make_async_remote_copy(
                src_ref=pack.at[to["model"], pl.ds(4 * to["cols"], 6)],
                dst_ref=got.at[mine],
                send_sem=xs_send,
                recv_sem=xs_recv,
                device_id=to,
                device_id_type=MESH,
            ).start()

    mine = ((core * 4 + me["x"]) * 4 + me["z"]) * 4 + me["y"]
    with jax.named_scope("send_first"):
        first = spread(0, 18)
        for pair in range(6):
            got[mine, pair] = pack[m, 4 * q + pair]
        send_windows(0, CUT)
    with jax.named_scope("wait_first"):
        first.land()
    with jax.named_scope("send_second"):
        second = spread(1, 72)
        send_windows(CUT, 127)
    with jax.named_scope("wait_second"):
        second.land()
    last, passed, lent, lent_on = {}, {}, {}, {}

    def send_plane(n):
        last[n] = Step(96, [(piece(p, 2, plane(p, 0), n, core), chip(p, 2, d)) for p in parts for d in (1, 3)])

    def pass_on(n):
        with jax.named_scope(f"wait_last{n}"):
            last[n].land()
        passed[n] = Step(48, [(piece(p, 2, plane(p, 4 - d), n, core, half=d // 2), chip(p, 2, d)) for p in parts for d in (1, 3)]).go()
        lent[n] = hand_over([piece(p, 2, plane(p, d), n, core) for p in parts for d in (1, 3)], 96)

    def finish(n):
        with jax.named_scope(f"wait_passed{n}"):
            passed[n].land()
        lent_on[n] = hand_over([piece(p, 2, plane(p, 2), n, core) for p in parts], 48)

    with jax.named_scope("send_third"):
        for n in range(2):
            send_plane(n)
        last[0].go()
        own = hand_over([piece(p, 2, plane(p, 0), None, core) for p in parts], 96)
    last[1].go()
    span = got.at[pl.ds(0, 127)]
    everything = pltpu.make_async_remote_copy(
        src_ref=span, dst_ref=span, send_sem=xs_send, recv_sem=xs_recv, device_id=chip(0, 0, 0, 1), device_id_type=MESH
    )
    with jax.named_scope("wait_windows"):
        everything.wait_recv()

    xs, ys = (x0, x1, x2), (y0, y1, y2)
    with jax.named_scope("turn"):
        for pair in range(6):
            for p in parts:
                rows = []
                for v in range(4):
                    for c in range(2):
                        at = 64 * c
                        if p == 0:
                            rows.append(got[at + 16 * v : at + 16 * v + 16, pair])
                        elif p == 1:
                            rows.append(got[at + v : at + 64 : 4, pair])
                        else:
                            rows += [got[at + 16 * a + 4 * v : at + 16 * a + 4 * v + 4, pair] for a in range(4)]
                rows = jnp.concatenate([r.reshape(-1, LANES) for r in rows], axis=0).T
                for odd in range(2):
                    main = rows[64 * odd : 64 * odd + 64]
                    xs[p][2 * pair + odd, 8 - 4 * p : 72 - 4 * p] = main
                    if p == 1:
                        edge[0, 2 * pair + odd] = main[60:64]
                        edge[1, 2 * pair + odd] = main[0:4]
    halo = []
    for src, dst, d in (
        (x0.at[:, pl.ds(64, 8)], x0.at[:, pl.ds(0, 8)], 1),
        (x2.at[:, pl.ds(0, 8)], x2.at[:, pl.ds(64, 8)], 7),
        (edge.at[0], edge.at[2], 1),
        (edge.at[1], edge.at[3], 7),
    ):
        halo.append(
            pltpu.make_async_remote_copy(
                src_ref=src,
                dst_ref=dst,
                send_sem=halo_send.at[len(halo)],
                recv_sem=halo_recv.at[len(halo)],
                device_id={"model": (m + d) % 8, "cols": q},
                device_id_type=MESH,
            )
        )
        halo[-1].start()

    def conv1(halves, places, spans, groups):
        width = 10 // groups
        tops = [None] * groups
        taps = [(p, dw, plane(p, d)) for p in parts for dw in range(3) for d in places]
        for first in range(0, len(taps), 2):
            two = taps[first : first + 2]
            right = [[w1g[p, n, v, :, :, :, dw, i].reshape(LANES, LANES) for n in halves for i in range(2)] for p, dw, v in two]
            right = jnp.concatenate([jnp.concatenate(r, axis=1) for r in right], axis=0)
            for group in range(groups):
                left = []
                for rows in spans:
                    some = []
                    for p, dw, v in two:
                        lanes = pl.ds(pl.multiple_of(LANES * v, LANES), LANES)
                        some.append(xs[p][pl.ds(dw + width * group, width), rows, lanes])
                    left.append(jnp.concatenate(some, axis=-1))
                left = jnp.concatenate(left, axis=1).reshape(-1, LANES * len(two))
                term = jnp.dot(left, right, preferred_element_type=F32)
                tops[group] = term if tops[group] is None else tops[group] + term
        return [top.reshape(width, -1, 256 * len(halves)) for top in tops]

    top_rows, inner, low_rows = pl.ds(0, 8), pl.ds(8, 56), pl.ds(64, 8)

    def here(n):
        with jax.named_scope(f"here{n}"):
            for group, top in enumerate(conv1((n,), (0,), (inner,), 2)):
                z_acc[n, pl.ds(5 * group, 5), inner] = top

    def near(n):
        with jax.named_scope(f"wait_lent{n}"):
            lent[n].land()
        with jax.named_scope(f"near{n}"):
            for group, top in enumerate(conv1((n,), (3, 1), (inner,), 2)):
                z_acc[n, pl.ds(5 * group, 5), inner] += top

    def rim():
        with jax.named_scope("rim"):
            (top,) = conv1((0, 1), (0, 3, 1), (top_rows, low_rows), 1)
            for n in range(2):
                part = top[:, :, 256 * n : 256 * n + 256]
                z_acc[n, :, top_rows] = part[:, :8]
                z_acc[n, :, low_rows] = part[:, 8:]

    def far(n):
        with jax.named_scope(f"wait_lent_on{n}"):
            lent_on[n].land()
        lanes = slice(256 * n, 256 * n + 256)
        with jax.named_scope(f"far{n}"):
            for group, top in enumerate(conv1((n,), (2,), (pl.ds(0, 72),), 2)):
                cols = pl.ds(5 * group, 5)
                act = jnp.maximum(z_acc[n, cols] + top + b1v[:, lanes], 0.0)
                for dh in range(3):
                    ys[dh][cols, :, lanes] = act[:, 4 * dh : 4 * dh + 64].astype(BF16)

        def clear(at_edge, refs, cols, rows):
            @pl.when(at_edge)
            def _():
                for ref in refs:
                    ref[cols, rows, lanes] = jnp.zeros((cols.size, rows.size, 256), BF16)

        clear(q == 0, ys, pl.ds(0, 1), pl.ds(0, 64))
        clear(q == 15, ys, pl.ds(9, 1), pl.ds(0, 64))
        clear(m == 0, (y0,), pl.ds(0, 10), pl.ds(0, 4))
        clear(m == 7, (y2,), pl.ds(0, 10), pl.ds(60, 4))

    def conv2(n):
        lanes = slice(256 * n, 256 * n + 256)
        total = None
        for dh in range(3):
            for dw in range(3):
                tap = 3 * dh + dw
                left = ys[dh][dw : dw + 8, :, lanes].reshape(CHANS, 256)
                right = w2v[CHANS * tap + 256 * n : CHANS * tap + 256 * n + 256, :]
                term = jnp.dot(left, right, preferred_element_type=F32)
                total = term if total is None else total + term
        return total

    pass_on(0)
    with jax.named_scope("wait_own"):
        own.land()
    here(0)
    here(1)
    pass_on(1)
    near(0)
    near(1)
    finish(0)
    with jax.named_scope("wait_halo"):
        for copy in halo:
            copy.wait_recv()

    @pl.when(m == 0)
    def _():
        x0[:, 0:8] = jnp.zeros((12, 8, CHANS), BF16)
        x1[:, 0:4] = jnp.zeros((12, 4, CHANS), BF16)

    @pl.when(m > 0)
    def _():
        x1[:, 0:4] = edge[2]

    @pl.when(m == 7)
    def _():
        x2[:, 64:72] = jnp.zeros((12, 8, CHANS), BF16)
        x1[:, 68:72] = jnp.zeros((12, 4, CHANS), BF16)

    @pl.when(m < 7)
    def _():
        x1[:, 68:72] = edge[3]

    rim()
    finish(1)
    with jax.named_scope("wait_w2"):
        for load in loads[2:]:
            load.wait()
    far(0)
    with jax.named_scope("conv2_0"):
        acc2[...] = conv2(0)
    far(1)
    with jax.named_scope("conv2_1"):
        o_ref[...] = acc2[...] + conv2(1) + b2v[...]

    with jax.named_scope("wait_sends"):
        everything.wait_send()
        for step in steps:
            step.all.wait_send()
        for copy in halo:
            copy.wait_send()


def arrange(sum_ref, o_hbm, turned, sems):
    copies = []
    for g in range(4):
        rows = jnp.transpose(sum_ref[:, 16 * g : 16 * g + 16], (1, 0, 2))
        for h in range(4):
            for image in range(4):
                turned[g, image, h] = rows[4 * h + image]
        copies.append(pltpu.make_async_copy(turned.at[g], o_hbm.at[:, pl.ds(4 * g, 4)], sems.at[g]))
        copies[-1].start()
    for copy in copies:
        copy.wait()


def solution(mesh):
    scratch = [
        pltpu.VMEM((4, LANES, 4, LANES), BF16),
        pltpu.VMEM((9, 4, CHANS), BF16),
        pltpu.VMEM((4616, CHANS), BF16),
        pltpu.VMEM((1, CHANS), F32),
        pltpu.VMEM((1, CHANS), F32),
        pltpu.VMEM((CHANS, CHANS), BF16),
        pltpu.VMEM((8, 66, 4, LANES), BF16),
        pltpu.VMEM((LANES, 6, 4, LANES), BF16),
        *[pltpu.VMEM((12, 72, CHANS), BF16) for _ in range(3)],
        pltpu.VMEM((4, 12, 4, CHANS), BF16),
        pltpu.VMEM((3, 2, 4, 2, 4, 4, 3, 2, 4, LANES), BF16),
        pltpu.VMEM((2, 10, 72, 256), F32),
        *[pltpu.VMEM((10, 64, CHANS), BF16) for _ in range(3)],
        pltpu.VMEM((CHANS, CHANS), F32),
        pltpu.SemaphoreType.DMA((5,)),
        pltpu.SemaphoreType.DMA,
        pltpu.SemaphoreType.DMA,
        pltpu.SemaphoreType.DMA((4,)),
        pltpu.SemaphoreType.DMA((4,)),
        pltpu.SemaphoreType.DMA((11,)),
        pltpu.SemaphoreType.DMA((11,)),
    ]
    vmem = pl.BlockSpec(memory_space=pltpu.VMEM)
    anywhere = pl.BlockSpec(memory_space=pl.ANY)

    def run_local(x_in, w_conv1, b_conv1, w_conv2, b_conv2):
        sums = pl.pallas_call(
            kernel,
            out_shape=jax.ShapeDtypeStruct((CHANS, CHANS), F32),
            in_specs=[anywhere] * 5,
            out_specs=vmem,
            scratch_shapes=scratch,
            compiler_params=pltpu.CompilerParams(collective_id=0, has_side_effects=True, vmem_limit_bytes=VMEM_LIMIT),
            name="two_convs",
        )(
            *(
                pltpu.with_memory_space_constraint(a, pltpu.HBM)
                for a in (
                    x_in.transpose(0, 1, 3, 2),
                    w_conv1.reshape(9, 4, CHANS),
                    w_conv2.reshape(4608, CHANS),
                    b_conv1.reshape(1, CHANS),
                    b_conv2.reshape(1, CHANS),
                )
            )
        )
        return pl.pallas_call(
            arrange,
            out_shape=jax.ShapeDtypeStruct((4, 16, 8, CHANS), F32),
            in_specs=[vmem],
            out_specs=anywhere,
            scratch_shapes=[pltpu.VMEM((4, 4, 4, 8, CHANS), F32), pltpu.SemaphoreType.DMA((4,))],
            compiler_params=pltpu.CompilerParams(vmem_limit_bytes=8 * 2**20),
            name="arrange",
        )(sums.reshape(8, 64, CHANS))

    return jax.shard_map(
        run_local,
        mesh=mesh,
        in_specs=(P("data", None, None, GROUP_AXES), P(None, None, GROUP_AXES, None), P(), P(), P()),
        out_specs=P("data", "model", "cols", None),
        check_vma=False,
    )
```

```python
import jax
import jax.numpy as jnp
from jax import lax
from jax.experimental import pallas as pl
from jax.experimental.pallas import tpu as pltpu
from jax.sharding import PartitionSpec as P

GROUP_AXES = ("model", "cols")
MESH = pl.DeviceIdType.MESH
BF16 = jnp.bfloat16
F32 = jnp.float32
CHANS = 512
LANES = 128
CUT = 88
VMEM_LIMIT = 36 * 2**20
ORDERS = (("y", "z", "x"), ("z", "x", "y"), ("x", "y", "z"))


def one_hot(shape, col_of_row):
    rows = lax.broadcasted_iota(jnp.int32, shape, 0)
    cols = lax.broadcasted_iota(jnp.int32, shape, 1)
    return jnp.where(cols == col_of_row(rows), 1.0, 0.0).astype(BF16)


def pack_windows(xv, a_scr, pack):
    to_lanes = one_hot((CHANS, CHANS), lambda r: (r % 4) * LANES + ((r % LANES) // 4) * 4 + r // LANES)
    to_rows = one_hot((CHANS, CHANS), lambda r: (r % 4) * LANES + ((r % 256) // 4) * 2 + r // 256)
    for blk in range(4):
        part = jnp.concatenate([xv[n, 32 * blk : 32 * blk + 32].reshape(LANES, LANES) for n in range(4)], axis=0)
        turned = lax.dot_general(part, to_lanes, (((0,), (0,)), ((), ())), preferred_element_type=F32).astype(BF16)
        for c in range(4):
            a_scr[c * LANES : (c + 1) * LANES, blk * LANES : (blk + 1) * LANES] = turned[:, c * LANES : (c + 1) * LANES]
    mixed = jnp.dot(to_rows, a_scr[...], preferred_element_type=F32)
    for blk in range(4):
        even = mixed[0:256, blk * LANES : (blk + 1) * LANES]
        odd = mixed[256:CHANS, blk * LANES : (blk + 1) * LANES]
        for half in range(2):
            s = slice(64 * half, 64 * half + 64)
            tile = jnp.concatenate([even[:, s], odd[:, s]], axis=1).astype(BF16)
            pack[2 * blk + half, 1:65] = tile.reshape(64, 4, LANES)
    edge = jnp.zeros((8, 1, 4, LANES), BF16)
    pack[:, 0:1] = edge
    pack[:, 65:66] = edge


def kernel(
    x_hbm, w1_hbm, w2_hbm, b1_hbm, b2_hbm, o_ref,
    xv, w1v, w2v, b1v, b2v, a_scr, pack, got, x0, x1, x2, edge, w1g, z_acc, y0, y1, y2, acc2,
    load_sem, xs_send, xs_recv, halo_send, halo_recv, step_send, step_recv,
):
    m = lax.axis_index("model")
    q = lax.axis_index("cols")
    me = {"x": m // 2, "z": q // 4, "y": q % 4}
    core = m % 2
    parts = range(3)
    barrier = pltpu.get_barrier_semaphore()

    at_model = [[(me["x"] + dx) % 4 * 2 + (core + dk) % 2 for dk in range(2)] for dx in range(4)]
    at_cols = [[(me["z"] + dz) % 4 * 4 + (me["y"] + dy) % 4 for dy in range(4)] for dz in range(4)]
    others = [(dx, dz, dy, dk) for dx in range(4) for dz in range(4) for dy in range(4) for dk in range(2)]
    others = sorted(others[1:], key=lambda d: (sum(d[:3]) % 4, d))

    def away(d):
        return {"model": at_model[d[0]][d[3]], "cols": at_cols[d[1]][d[2]]}

    loads = [
        pltpu.make_async_copy(src, dst, load_sem.at[k])
        for k, (src, dst) in enumerate(
            ((x_hbm, xv), (w1_hbm, w1v), (w2_hbm, w2v.at[pl.ds(0, 4608)]), (b1_hbm, b1v), (b2_hbm, b2v))
        )
    ]
    for load in loads:
        load.start()
    with jax.named_scope("announce"):
        for d in sorted(others, key=lambda d: -sum(min(o, 4 - o) for o in d[:3])):
            pl.semaphore_signal(barrier, inc=1, device_id=away(d), device_id_type=MESH)

    def piece(p, t, v, n, c, place=None, half=None):
        done = ORDERS[p][:t]
        rest = [a for a in "xzy" if a != ORDERS[p][2]]
        at = [v if t < 2 and a == ORDERS[p][t] else (pl.ds(0, 4) if a in done else me[a]) for a in rest]
        if half is not None:
            at[0] = pl.ds(2 * half, 2)
        return w1g.at[p, pl.ds(0, 2) if n is None else n, me[ORDERS[p][2]] if t < 2 else v, c, at[0], at[1]]

    with jax.named_scope("place_w1"):
        loads[1].wait()
        for p in parts:
            spot = [me[a] for a in "xzy" if a != ORDERS[p][2]]
            for dw in range(3):
                for lt in range(4):
                    tile = w1v[3 * p + dw, :, lt * LANES : (lt + 1) * LANES]
                    w1g[p, lt // 2, me[ORDERS[p][2]], core, spot[0], spot[1], dw, lt % 2] = tile
    with jax.named_scope("wait_x"):
        loads[0].wait()
    with jax.named_scope("pack"):
        pack_windows(xv, a_scr, pack)
    with jax.named_scope("wait_barrier"):
        pl.semaphore_wait(barrier, 127)

    n_steps = [0]
    steps = []

    class Step:
        def __init__(self, slabs, copies):
            k = n_steps[0]
            n_steps[0] += 1
            sems = dict(send_sem=step_send.at[k], recv_sem=step_recv.at[k], device_id_type=MESH)
            self.copies, self.sems = copies, sems
            span = got.at[pl.ds(0, slabs)]
            self.all = pltpu.make_async_remote_copy(
                src_ref=span, dst_ref=span, device_id={"model": at_model[0][1], "cols": q}, **sems
            )
            steps.append(self)

        def go(self):
            for ref, to in self.copies:
                pltpu.make_async_remote_copy(src_ref=ref, dst_ref=ref, device_id=to, **self.sems).start()
            return self

        def land(self):
            self.all.wait_recv()

    def chip(p, t, d, c=0):
        axis = ORDERS[p][t]
        pos = me | {axis: (me[axis] + d) % 4}
        return {"model": pos["x"] * 2 + (core + c) % 2, "cols": pos["z"] * 4 + pos["y"]}

    def spread(t, slabs):
        return Step(slabs, [(piece(p, t, me[ORDERS[p][t]], None, core), chip(p, t, d)) for p in parts for d in (1, 3, 2)]).go()

    def plane(p, d):
        return (me[ORDERS[p][2]] + d) % 4

    def hand_over(pieces, slabs):
        return Step(slabs, [(ref, {"model": at_model[0][1], "cols": q}) for ref in pieces]).go()

    def send_windows(first, last):
        for d in others[first:last]:
            to = away(d)
            pltpu.make_async_remote_copy(
                src_ref=pack.at[to["model"], pl.ds(4 * to["cols"], 6)],
                dst_ref=got.at[mine],
                send_sem=xs_send,
                recv_sem=xs_recv,
                device_id=to,
                device_id_type=MESH,
            ).start()

    mine = ((core * 4 + me["x"]) * 4 + me["z"]) * 4 + me["y"]
    with jax.named_scope("send_first"):
        first = spread(0, 18)
        for pair in range(6):
            got[mine, pair] = pack[m, 4 * q + pair]
        send_windows(0, CUT)
    with jax.named_scope("wait_first"):
        first.land()
    with jax.named_scope("send_second"):
        second = spread(1, 72)
        send_windows(CUT, 127)
    with jax.named_scope("wait_second"):
        second.land()
    last, passed, lent, lent_on = {}, {}, {}, {}

    def send_plane(n):
        last[n] = Step(96, [(piece(p, 2, plane(p, 0), n, core), chip(p, 2, d)) for p in parts for d in (1, 3)])

    def pass_on(n):
        with jax.named_scope(f"wait_last{n}"):
            last[n].land()
        passed[n] = Step(48, [(piece(p, 2, plane(p, 4 - d), n, core, half=d // 2), chip(p, 2, d)) for p in parts for d in (1, 3)]).go()
        lent[n] = hand_over([piece(p, 2, plane(p, d), n, core) for p in parts for d in (1, 3)], 96)

    def finish(n):
        with jax.named_scope(f"wait_passed{n}"):
            passed[n].land()
        lent_on[n] = hand_over([piece(p, 2, plane(p, 2), n, core) for p in parts], 48)

    with jax.named_scope("send_third"):
        for n in range(2):
            send_plane(n)
        last[0].go()
        own = hand_over([piece(p, 2, plane(p, 0), None, core) for p in parts], 96)
    last[1].go()
    span = got.at[pl.ds(0, 127)]
    everything = pltpu.make_async_remote_copy(
        src_ref=span, dst_ref=span, send_sem=xs_send, recv_sem=xs_recv, device_id=chip(0, 0, 0, 1), device_id_type=MESH
    )
    with jax.named_scope("wait_windows"):
        everything.wait_recv()

    xs, ys = (x0, x1, x2), (y0, y1, y2)
    with jax.named_scope("turn"):
        for pair in range(6):
            for p in parts:
                rows = []
                for v in range(4):
                    for c in range(2):
                        at = 64 * c
                        if p == 0:
                            rows.append(got[at + 16 * v : at + 16 * v + 16, pair])
                        elif p == 1:
                            rows.append(got[at + v : at + 64 : 4, pair])
                        else:
                            rows += [got[at + 16 * a + 4 * v : at + 16 * a + 4 * v + 4, pair] for a in range(4)]
                rows = jnp.concatenate([r.reshape(-1, LANES) for r in rows], axis=0).T
                for odd in range(2):
                    main = rows[64 * odd : 64 * odd + 64]
                    xs[p][2 * pair + odd, 8 - 4 * p : 72 - 4 * p] = main
                    if p == 1:
                        edge[0, 2 * pair + odd] = main[60:64]
                        edge[1, 2 * pair + odd] = main[0:4]
    halo = []
    for src, dst, d in (
        (x0.at[:, pl.ds(64, 8)], x0.at[:, pl.ds(0, 8)], 1),
        (x2.at[:, pl.ds(0, 8)], x2.at[:, pl.ds(64, 8)], 7),
        (edge.at[0], edge.at[2], 1),
        (edge.at[1], edge.at[3], 7),
    ):
        halo.append(
            pltpu.make_async_remote_copy(
                src_ref=src,
                dst_ref=dst,
                send_sem=halo_send.at[len(halo)],
                recv_sem=halo_recv.at[len(halo)],
                device_id={"model": (m + d) % 8, "cols": q},
                device_id_type=MESH,
            )
        )
        halo[-1].start()

    def conv1(halves, places, spans, groups):
        width = 10 // groups
        tops = [None] * groups
        taps = [(p, dw, plane(p, d)) for p in parts for dw in range(3) for d in places]
        for first in range(0, len(taps), 2):
            two = taps[first : first + 2]
            right = [[w1g[p, n, v, :, :, :, dw, i].reshape(LANES, LANES) for n in halves for i in range(2)] for p, dw, v in two]
            right = jnp.concatenate([jnp.concatenate(r, axis=1) for r in right], axis=0)
            for group in range(groups):
                left = []
                for rows in spans:
                    some = []
                    for p, dw, v in two:
                        lanes = pl.ds(pl.multiple_of(LANES * v, LANES), LANES)
                        some.append(xs[p][pl.ds(dw + width * group, width), rows, lanes])
                    left.append(jnp.concatenate(some, axis=-1))
                left = jnp.concatenate(left, axis=1).reshape(-1, LANES * len(two))
                term = jnp.dot(left, right, preferred_element_type=F32)
                tops[group] = term if tops[group] is None else tops[group] + term
        return [top.reshape(width, -1, 256 * len(halves)) for top in tops]

    top_rows, inner, low_rows = pl.ds(0, 8), pl.ds(8, 56), pl.ds(64, 8)

    def here(n):
        with jax.named_scope(f"here{n}"):
            for group, top in enumerate(conv1((n,), (0,), (inner,), 2)):
                z_acc[n, pl.ds(5 * group, 5), inner] = top

    def near(n):
        with jax.named_scope(f"wait_lent{n}"):
            lent[n].land()
        with jax.named_scope(f"near{n}"):
            for group, top in enumerate(conv1((n,), (3, 1), (inner,), 2)):
                z_acc[n, pl.ds(5 * group, 5), inner] += top

    def rim():
        with jax.named_scope("rim"):
            (top,) = conv1((0, 1), (0, 3, 1), (top_rows, low_rows), 1)
            for n in range(2):
                part = top[:, :, 256 * n : 256 * n + 256]
                z_acc[n, :, top_rows] = part[:, :8]
                z_acc[n, :, low_rows] = part[:, 8:]

    def far(n):
        with jax.named_scope(f"wait_lent_on{n}"):
            lent_on[n].land()
        lanes = slice(256 * n, 256 * n + 256)
        with jax.named_scope(f"far{n}"):
            for group, top in enumerate(conv1((n,), (2,), (pl.ds(0, 72),), 2)):
                cols = pl.ds(5 * group, 5)
                act = jnp.maximum(z_acc[n, cols] + top + b1v[:, lanes], 0.0)
                for dh in range(3):
                    ys[dh][cols, :, lanes] = act[:, 4 * dh : 4 * dh + 64].astype(BF16)

        def clear(at_edge, refs, cols, rows):
            @pl.when(at_edge)
            def _():
                for ref in refs:
                    ref[cols, rows, lanes] = jnp.zeros((cols.size, rows.size, 256), BF16)

        clear(q == 0, ys, pl.ds(0, 1), pl.ds(0, 64))
        clear(q == 15, ys, pl.ds(9, 1), pl.ds(0, 64))
        clear(m == 0, (y0,), pl.ds(0, 10), pl.ds(0, 4))
        clear(m == 7, (y2,), pl.ds(0, 10), pl.ds(60, 4))

    def conv2(n):
        lanes = slice(256 * n, 256 * n + 256)
        total = None
        for dh in range(3):
            for dw in range(3):
                tap = 3 * dh + dw
                left = ys[dh][dw : dw + 8, :, lanes].reshape(CHANS, 256)
                right = w2v[CHANS * tap + 256 * n : CHANS * tap + 256 * n + 256, :]
                term = jnp.dot(left, right, preferred_element_type=F32)
                total = term if total is None else total + term
        return total

    pass_on(0)
    with jax.named_scope("wait_own"):
        own.land()
    here(0)
    here(1)
    pass_on(1)
    near(0)
    near(1)
    finish(0)
    with jax.named_scope("wait_halo"):
        for copy in halo:
            copy.wait_recv()

    @pl.when(m == 0)
    def _():
        x0[:, 0:8] = jnp.zeros((12, 8, CHANS), BF16)
        x1[:, 0:4] = jnp.zeros((12, 4, CHANS), BF16)

    @pl.when(m > 0)
    def _():
        x1[:, 0:4] = edge[2]

    @pl.when(m == 7)
    def _():
        x2[:, 64:72] = jnp.zeros((12, 8, CHANS), BF16)
        x1[:, 68:72] = jnp.zeros((12, 4, CHANS), BF16)

    @pl.when(m < 7)
    def _():
        x1[:, 68:72] = edge[3]

    rim()
    finish(1)
    with jax.named_scope("wait_w2"):
        for load in loads[2:]:
            load.wait()
    far(0)
    with jax.named_scope("conv2_0"):
        acc2[...] = conv2(0)
    far(1)
    with jax.named_scope("conv2_1"):
        o_ref[...] = acc2[...] + conv2(1) + b2v[...]

    with jax.named_scope("wait_sends"):
        everything.wait_send()
        for step in steps:
            step.all.wait_send()
        for copy in halo:
            copy.wait_send()


def arrange(sum_ref, o_hbm, turned, sems):
    copies = []
    for g in range(4):
        rows = jnp.transpose(sum_ref[:, 16 * g : 16 * g + 16], (1, 0, 2))
        for h in range(4):
            for image in range(4):
                turned[g, image, h] = rows[4 * h + image]
        copies.append(pltpu.make_async_copy(turned.at[g], o_hbm.at[:, pl.ds(4 * g, 4)], sems.at[g]))
        copies[-1].start()
    for copy in copies:
        copy.wait()


def solution(mesh):
    scratch = [
        pltpu.VMEM((4, LANES, 4, LANES), BF16),
        pltpu.VMEM((9, 4, CHANS), BF16),
        pltpu.VMEM((4616, CHANS), BF16),
        pltpu.VMEM((1, CHANS), F32),
        pltpu.VMEM((1, CHANS), F32),
        pltpu.VMEM((CHANS, CHANS), BF16),
        pltpu.VMEM((8, 66, 4, LANES), BF16),
        pltpu.VMEM((LANES, 6, 4, LANES), BF16),
        *[pltpu.VMEM((12, 72, CHANS), BF16) for _ in range(3)],
        pltpu.VMEM((4, 12, 4, CHANS), BF16),
        pltpu.VMEM((3, 2, 4, 2, 4, 4, 3, 2, 4, LANES), BF16),
        pltpu.VMEM((2, 10, 72, 256), F32),
        *[pltpu.VMEM((10, 64, CHANS), BF16) for _ in range(3)],
        pltpu.VMEM((CHANS, CHANS), F32),
        pltpu.SemaphoreType.DMA((5,)),
        pltpu.SemaphoreType.DMA,
        pltpu.SemaphoreType.DMA,
        pltpu.SemaphoreType.DMA((4,)),
        pltpu.SemaphoreType.DMA((4,)),
        pltpu.SemaphoreType.DMA((11,)),
        pltpu.SemaphoreType.DMA((11,)),
    ]
    vmem = pl.BlockSpec(memory_space=pltpu.VMEM)
    anywhere = pl.BlockSpec(memory_space=pl.ANY)

    def run_local(x_in, w_conv1, b_conv1, w_conv2, b_conv2):
        sums = pl.pallas_call(
            kernel,
            out_shape=jax.ShapeDtypeStruct((CHANS, CHANS), F32),
            in_specs=[anywhere] * 5,
            out_specs=vmem,
            scratch_shapes=scratch,
            compiler_params=pltpu.CompilerParams(collective_id=0, has_side_effects=True, vmem_limit_bytes=VMEM_LIMIT),
            name="two_convs",
        )(
            *(
                pltpu.with_memory_space_constraint(a, pltpu.HBM)
                for a in (
                    x_in.transpose(0, 1, 3, 2),
                    w_conv1.reshape(9, 4, CHANS),
                    w_conv2.reshape(4608, CHANS),
                    b_conv1.reshape(1, CHANS),
                    b_conv2.reshape(1, CHANS),
                )
            )
        )
        return pl.pallas_call(
            arrange,
            out_shape=jax.ShapeDtypeStruct((4, 16, 8, CHANS), F32),
            in_specs=[vmem],
            out_specs=anywhere,
            scratch_shapes=[pltpu.VMEM((4, 4, 4, 8, CHANS), F32), pltpu.SemaphoreType.DMA((4,))],
            compiler_params=pltpu.CompilerParams(vmem_limit_bytes=8 * 2**20),
            name="arrange",
        )(sums.reshape(8, 64, CHANS))

    return jax.shard_map(
        run_local,
        mesh=mesh,
        in_specs=(P("data", None, None, GROUP_AXES), P(None, None, GROUP_AXES, None), P(), P(), P()),
        out_specs=P("data", "model", "cols", None),
        check_vma=False,
    )
```

```python
import jax
import jax.numpy as jnp
from jax import lax
from jax.experimental import pallas as pl
from jax.experimental.pallas import tpu as pltpu
from jax.sharding import PartitionSpec as P

GROUP_AXES = ("model", "cols")
MESH = pl.DeviceIdType.MESH
BF16 = jnp.bfloat16
F32 = jnp.float32
CHANS = 512
LANES = 128
CUT = 96
VMEM_LIMIT = 36 * 2**20
ORDERS = (("z", "y", "x"), ("x", "z", "y"), ("x", "y", "z"))


def one_hot(shape, col_of_row):
    rows = lax.broadcasted_iota(jnp.int32, shape, 0)
    cols = lax.broadcasted_iota(jnp.int32, shape, 1)
    return jnp.where(cols == col_of_row(rows), 1.0, 0.0).astype(BF16)


def pack_windows(xv, a_scr, pack):
    to_lanes = one_hot((CHANS, CHANS), lambda r: (r % 4) * LANES + ((r % LANES) // 4) * 4 + r // LANES)
    to_rows = one_hot((CHANS, CHANS), lambda r: (r % 4) * LANES + ((r % 256) // 4) * 2 + r // 256)
    for blk in range(4):
        part = jnp.concatenate([xv[n, 32 * blk : 32 * blk + 32].reshape(LANES, LANES) for n in range(4)], axis=0)
        turned = lax.dot_general(part, to_lanes, (((0,), (0,)), ((), ())), preferred_element_type=F32).astype(BF16)
        for c in range(4):
            a_scr[c * LANES : (c + 1) * LANES, blk * LANES : (blk + 1) * LANES] = turned[:, c * LANES : (c + 1) * LANES]
    mixed = jnp.dot(to_rows, a_scr[...], preferred_element_type=F32)
    for blk in range(4):
        even = mixed[0:256, blk * LANES : (blk + 1) * LANES]
        odd = mixed[256:CHANS, blk * LANES : (blk + 1) * LANES]
        for half in range(2):
            s = slice(64 * half, 64 * half + 64)
            tile = jnp.concatenate([even[:, s], odd[:, s]], axis=1).astype(BF16)
            pack[2 * blk + half, 1:65] = tile.reshape(64, 4, LANES)
    edge = jnp.zeros((8, 1, 4, LANES), BF16)
    pack[:, 0:1] = edge
    pack[:, 65:66] = edge


def kernel(
    x_hbm, w1_hbm, w2_hbm, b1_hbm, b2_hbm, o_ref,
    xv, w1v, w2v, b1v, b2v, a_scr, pack, got, x0, x1, x2, edge, w1g, z_acc, y0, y1, y2, acc2,
    load_sem, xs_send, xs_recv, halo_send, halo_recv, step_send, step_recv,
):
    m = lax.axis_index("model")
    q = lax.axis_index("cols")
    me = {"x": m // 2, "z": q // 4, "y": q % 4}
    core = m % 2
    parts = range(3)
    barrier = pltpu.get_barrier_semaphore()

    at_model = [[(me["x"] + dx) % 4 * 2 + (core + dk) % 2 for dk in range(2)] for dx in range(4)]
    at_cols = [[(me["z"] + dz) % 4 * 4 + (me["y"] + dy) % 4 for dy in range(4)] for dz in range(4)]
    others = [(dx, dz, dy, dk) for dx in range(4) for dz in range(4) for dy in range(4) for dk in range(2)]
    others = sorted(others[1:], key=lambda d: (sum(d[:3]) % 4, d))

    def away(d):
        return {"model": at_model[d[0]][d[3]], "cols": at_cols[d[1]][d[2]]}

    loads = [
        pltpu.make_async_copy(src, dst, load_sem.at[k])
        for k, (src, dst) in enumerate(
            ((x_hbm, xv), (w1_hbm, w1v), (w2_hbm, w2v.at[pl.ds(0, 4608)]), (b1_hbm, b1v), (b2_hbm, b2v))
        )
    ]
    for load in loads:
        load.start()
    with jax.named_scope("announce"):
        for d in sorted(others, key=lambda d: -sum(min(o, 4 - o) for o in d[:3])):
            pl.semaphore_signal(barrier, inc=1, device_id=away(d), device_id_type=MESH)

    def piece(p, t, v, n, c, place=None, half=None):
        done = ORDERS[p][:t]
        rest = [a for a in "xzy" if a != ORDERS[p][2]]
        at = [v if t < 2 and a == ORDERS[p][t] else (pl.ds(0, 4) if a in done else me[a]) for a in rest]
        if half is not None:
            at[0] = pl.ds(2 * half, 2)
        return w1g.at[p, pl.ds(0, 2) if n is None else n, me[ORDERS[p][2]] if t < 2 else v, c, at[0], at[1]]

    with jax.named_scope("place_w1"):
        loads[1].wait()
        for p in parts:
            spot = [me[a] for a in "xzy" if a != ORDERS[p][2]]
            for dw in range(3):
                for lt in range(4):
                    tile = w1v[3 * p + dw, :, lt * LANES : (lt + 1) * LANES]
                    w1g[p, lt // 2, me[ORDERS[p][2]], core, spot[0], spot[1], dw, lt % 2] = tile
    with jax.named_scope("wait_x"):
        loads[0].wait()
    with jax.named_scope("pack"):
        pack_windows(xv, a_scr, pack)
    with jax.named_scope("wait_barrier"):
        pl.semaphore_wait(barrier, 127)

    n_steps = [0]
    steps = []

    class Step:
        def __init__(self, slabs, copies):
            k = n_steps[0]
            n_steps[0] += 1
            sems = dict(send_sem=step_send.at[k], recv_sem=step_recv.at[k], device_id_type=MESH)
            self.copies, self.sems = copies, sems
            span = got.at[pl.ds(0, slabs)]
            self.all = pltpu.make_async_remote_copy(
                src_ref=span, dst_ref=span, device_id={"model": at_model[0][1], "cols": q}, **sems
            )
            steps.append(self)

        def go(self):
            for ref, to in self.copies:
                pltpu.make_async_remote_copy(src_ref=ref, dst_ref=ref, device_id=to, **self.sems).start()
            return self

        def land(self):
            self.all.wait_recv()

    def chip(p, t, d, c=0):
        axis = ORDERS[p][t]
        pos = me | {axis: (me[axis] + d) % 4}
        return {"model": pos["x"] * 2 + (core + c) % 2, "cols": pos["z"] * 4 + pos["y"]}

    def spread(t, slabs):
        return Step(slabs, [(piece(p, t, me[ORDERS[p][t]], None, core), chip(p, t, d)) for p in parts for d in (1, 3, 2)]).go()

    def plane(p, d):
        return (me[ORDERS[p][2]] + d) % 4

    def hand_over(pieces, slabs):
        return Step(slabs, [(ref, {"model": at_model[0][1], "cols": q}) for ref in pieces]).go()

    def send_windows(first, last):
        for d in others[first:last]:
            to = away(d)
            pltpu.make_async_remote_copy(
                src_ref=pack.at[to["model"], pl.ds(4 * to["cols"], 6)],
                dst_ref=got.at[mine],
                send_sem=xs_send,
                recv_sem=xs_recv,
                device_id=to,
                device_id_type=MESH,
            ).start()

    mine = ((core * 4 + me["x"]) * 4 + me["z"]) * 4 + me["y"]
    with jax.named_scope("send_first"):
        first = spread(0, 18)
        for pair in range(6):
            got[mine, pair] = pack[m, 4 * q + pair]
        send_windows(0, CUT)
    with jax.named_scope("wait_first"):
        first.land()
    with jax.named_scope("send_second"):
        second = spread(1, 72)
        send_windows(CUT, 127)
    with jax.named_scope("wait_second"):
        second.land()
    last, passed, lent, lent_on = {}, {}, {}, {}

    def send_plane(n):
        last[n] = Step(96, [(piece(p, 2, plane(p, 0), n, core), chip(p, 2, d)) for p in parts for d in (1, 3)])

    def pass_on(n):
        with jax.named_scope(f"wait_last{n}"):
            last[n].land()
        passed[n] = Step(48, [(piece(p, 2, plane(p, 4 - d), n, core, half=d // 2), chip(p, 2, d)) for p in parts for d in (1, 3)]).go()
        lent[n] = hand_over([piece(p, 2, plane(p, d), n, core) for p in parts for d in (1, 3)], 96)

    def finish(n):
        with jax.named_scope(f"wait_passed{n}"):
            passed[n].land()
        lent_on[n] = hand_over([piece(p, 2, plane(p, 2), n, core) for p in parts], 48)

    with jax.named_scope("send_third"):
        for n in range(2):
            send_plane(n)
        last[0].go()
        own = hand_over([piece(p, 2, plane(p, 0), None, core) for p in parts], 96)
    last[1].go()
    span = got.at[pl.ds(0, 127)]
    everything = pltpu.make_async_remote_copy(
        src_ref=span, dst_ref=span, send_sem=xs_send, recv_sem=xs_recv, device_id=chip(0, 0, 0, 1), device_id_type=MESH
    )
    with jax.named_scope("wait_windows"):
        everything.wait_recv()

    xs, ys = (x0, x1, x2), (y0, y1, y2)
    with jax.named_scope("turn"):
        for pair in range(6):
            for p in parts:
                rows = []
                for v in range(4):
                    for c in range(2):
                        at = 64 * c
                        if p == 0:
                            rows.append(got[at + 16 * v : at + 16 * v + 16, pair])
                        elif p == 1:
                            rows.append(got[at + v : at + 64 : 4, pair])
                        else:
                            rows += [got[at + 16 * a + 4 * v : at + 16 * a + 4 * v + 4, pair] for a in range(4)]
                rows = jnp.concatenate([r.reshape(-1, LANES) for r in rows], axis=0).T
                for odd in range(2):
                    main = rows[64 * odd : 64 * odd + 64]
                    xs[p][2 * pair + odd, 8 - 4 * p : 72 - 4 * p] = main
                    if p == 1:
                        edge[0, 2 * pair + odd] = main[60:64]
                        edge[1, 2 * pair + odd] = main[0:4]
    halo = []
    for src, dst, d in (
        (x0.at[:, pl.ds(64, 8)], x0.at[:, pl.ds(0, 8)], 1),
        (x2.at[:, pl.ds(0, 8)], x2.at[:, pl.ds(64, 8)], 7),
        (edge.at[0], edge.at[2], 1),
        (edge.at[1], edge.at[3], 7),
    ):
        halo.append(
            pltpu.make_async_remote_copy(
                src_ref=src,
                dst_ref=dst,
                send_sem=halo_send.at[len(halo)],
                recv_sem=halo_recv.at[len(halo)],
                device_id={"model": (m + d) % 8, "cols": q},
                device_id_type=MESH,
            )
        )
        halo[-1].start()

    def conv1(halves, places, spans, groups):
        width = 10 // groups
        tops = [None] * groups
        taps = [(p, dw, plane(p, d)) for p in parts for dw in range(3) for d in places]
        for first in range(0, len(taps), 2):
            two = taps[first : first + 2]
            right = [[w1g[p, n, v, :, :, :, dw, i].reshape(LANES, LANES) for n in halves for i in range(2)] for p, dw, v in two]
            right = jnp.concatenate([jnp.concatenate(r, axis=1) for r in right], axis=0)
            for group in range(groups):
                left = []
                for rows in spans:
                    some = []
                    for p, dw, v in two:
                        lanes = pl.ds(pl.multiple_of(LANES * v, LANES), LANES)
                        some.append(xs[p][pl.ds(dw + width * group, width), rows, lanes])
                    left.append(jnp.concatenate(some, axis=-1))
                left = jnp.concatenate(left, axis=1).reshape(-1, LANES * len(two))
                term = jnp.dot(left, right, preferred_element_type=F32)
                tops[group] = term if tops[group] is None else tops[group] + term
        return [top.reshape(width, -1, 256 * len(halves)) for top in tops]

    top_rows, inner, low_rows = pl.ds(0, 8), pl.ds(8, 56), pl.ds(64, 8)

    def here(n):
        with jax.named_scope(f"here{n}"):
            for group, top in enumerate(conv1((n,), (0,), (inner,), 2)):
                z_acc[n, pl.ds(5 * group, 5), inner] = top

    def near(n):
        with jax.named_scope(f"wait_lent{n}"):
            lent[n].land()
        with jax.named_scope(f"near{n}"):
            for group, top in enumerate(conv1((n,), (3, 1), (inner,), 2)):
                z_acc[n, pl.ds(5 * group, 5), inner] += top

    def rim():
        with jax.named_scope("rim"):
            (top,) = conv1((0, 1), (0, 3, 1), (top_rows, low_rows), 1)
            for n in range(2):
                part = top[:, :, 256 * n : 256 * n + 256]
                z_acc[n, :, top_rows] = part[:, :8]
                z_acc[n, :, low_rows] = part[:, 8:]

    def far(n):
        with jax.named_scope(f"wait_lent_on{n}"):
            lent_on[n].land()
        lanes = slice(256 * n, 256 * n + 256)
        with jax.named_scope(f"far{n}"):
            for group, top in enumerate(conv1((n,), (2,), (pl.ds(0, 72),), 2)):
                cols = pl.ds(5 * group, 5)
                act = jnp.maximum(z_acc[n, cols] + top + b1v[:, lanes], 0.0)
                for dh in range(3):
                    ys[dh][cols, :, lanes] = act[:, 4 * dh : 4 * dh + 64].astype(BF16)

        def clear(at_edge, refs, cols, rows):
            @pl.when(at_edge)
            def _():
                for ref in refs:
                    ref[cols, rows, lanes] = jnp.zeros((cols.size, rows.size, 256), BF16)

        clear(q == 0, ys, pl.ds(0, 1), pl.ds(0, 64))
        clear(q == 15, ys, pl.ds(9, 1), pl.ds(0, 64))
        clear(m == 0, (y0,), pl.ds(0, 10), pl.ds(0, 4))
        clear(m == 7, (y2,), pl.ds(0, 10), pl.ds(60, 4))

    def conv2(n):
        lanes = slice(256 * n, 256 * n + 256)
        total = None
        for dh in range(3):
            for dw in range(3):
                tap = 3 * dh + dw
                left = ys[dh][dw : dw + 8, :, lanes].reshape(CHANS, 256)
                right = w2v[CHANS * tap + 256 * n : CHANS * tap + 256 * n + 256, :]
                term = jnp.dot(left, right, preferred_element_type=F32)
                total = term if total is None else total + term
        return total

    pass_on(0)
    with jax.named_scope("wait_own"):
        own.land()
    here(0)
    here(1)
    pass_on(1)
    near(0)
    near(1)
    finish(0)
    with jax.named_scope("wait_halo"):
        for copy in halo:
            copy.wait_recv()

    @pl.when(m == 0)
    def _():
        x0[:, 0:8] = jnp.zeros((12, 8, CHANS), BF16)
        x1[:, 0:4] = jnp.zeros((12, 4, CHANS), BF16)

    @pl.when(m > 0)
    def _():
        x1[:, 0:4] = edge[2]

    @pl.when(m == 7)
    def _():
        x2[:, 64:72] = jnp.zeros((12, 8, CHANS), BF16)
        x1[:, 68:72] = jnp.zeros((12, 4, CHANS), BF16)

    @pl.when(m < 7)
    def _():
        x1[:, 68:72] = edge[3]

    rim()
    finish(1)
    with jax.named_scope("wait_w2"):
        for load in loads[2:]:
            load.wait()
    far(0)
    with jax.named_scope("conv2_0"):
        acc2[...] = conv2(0)
    far(1)
    with jax.named_scope("conv2_1"):
        o_ref[...] = acc2[...] + conv2(1) + b2v[...]

    with jax.named_scope("wait_sends"):
        everything.wait_send()
        for step in steps:
            step.all.wait_send()
        for copy in halo:
            copy.wait_send()


def arrange(sum_ref, o_hbm, turned, sems):
    copies = []
    for g in range(4):
        rows = jnp.transpose(sum_ref[:, 16 * g : 16 * g + 16], (1, 0, 2))
        for h in range(4):
            for image in range(4):
                turned[g, image, h] = rows[4 * h + image]
        copies.append(pltpu.make_async_copy(turned.at[g], o_hbm.at[:, pl.ds(4 * g, 4)], sems.at[g]))
        copies[-1].start()
    for copy in copies:
        copy.wait()


def solution(mesh):
    scratch = [
        pltpu.VMEM((4, LANES, 4, LANES), BF16),
        pltpu.VMEM((9, 4, CHANS), BF16),
        pltpu.VMEM((4616, CHANS), BF16),
        pltpu.VMEM((1, CHANS), F32),
        pltpu.VMEM((1, CHANS), F32),
        pltpu.VMEM((CHANS, CHANS), BF16),
        pltpu.VMEM((8, 66, 4, LANES), BF16),
        pltpu.VMEM((LANES, 6, 4, LANES), BF16),
        *[pltpu.VMEM((12, 72, CHANS), BF16) for _ in range(3)],
        pltpu.VMEM((4, 12, 4, CHANS), BF16),
        pltpu.VMEM((3, 2, 4, 2, 4, 4, 3, 2, 4, LANES), BF16),
        pltpu.VMEM((2, 10, 72, 256), F32),
        *[pltpu.VMEM((10, 64, CHANS), BF16) for _ in range(3)],
        pltpu.VMEM((CHANS, CHANS), F32),
        pltpu.SemaphoreType.DMA((5,)),
        pltpu.SemaphoreType.DMA,
        pltpu.SemaphoreType.DMA,
        pltpu.SemaphoreType.DMA((4,)),
        pltpu.SemaphoreType.DMA((4,)),
        pltpu.SemaphoreType.DMA((11,)),
        pltpu.SemaphoreType.DMA((11,)),
    ]
    vmem = pl.BlockSpec(memory_space=pltpu.VMEM)
    anywhere = pl.BlockSpec(memory_space=pl.ANY)

    def run_local(x_in, w_conv1, b_conv1, w_conv2, b_conv2):
        sums = pl.pallas_call(
            kernel,
            out_shape=jax.ShapeDtypeStruct((CHANS, CHANS), F32),
            in_specs=[anywhere] * 5,
            out_specs=vmem,
            scratch_shapes=scratch,
            compiler_params=pltpu.CompilerParams(collective_id=0, has_side_effects=True, vmem_limit_bytes=VMEM_LIMIT),
            name="two_convs",
        )(
            *(
                pltpu.with_memory_space_constraint(a, pltpu.HBM)
                for a in (
                    x_in.transpose(0, 1, 3, 2),
                    w_conv1.reshape(9, 4, CHANS),
                    w_conv2.reshape(4608, CHANS),
                    b_conv1.reshape(1, CHANS),
                    b_conv2.reshape(1, CHANS),
                )
            )
        )
        return pl.pallas_call(
            arrange,
            out_shape=jax.ShapeDtypeStruct((4, 16, 8, CHANS), F32),
            in_specs=[vmem],
            out_specs=anywhere,
            scratch_shapes=[pltpu.VMEM((4, 4, 4, 8, CHANS), F32), pltpu.SemaphoreType.DMA((4,))],
            compiler_params=pltpu.CompilerParams(vmem_limit_bytes=8 * 2**20),
            name="arrange",
        )(sums.reshape(8, 64, CHANS))

    return jax.shard_map(
        run_local,
        mesh=mesh,
        in_specs=(P("data", None, None, GROUP_AXES), P(None, None, GROUP_AXES, None), P(), P(), P()),
        out_specs=P("data", "model", "cols", None),
        check_vma=False,
    )
```

```python
import jax
import jax.numpy as jnp
from jax import lax
from jax.experimental import pallas as pl
from jax.experimental.pallas import tpu as pltpu
from jax.sharding import PartitionSpec as P

GROUP_AXES = ("model", "cols")
MESH = pl.DeviceIdType.MESH
BF16 = jnp.bfloat16
F32 = jnp.float32
CHANS = 512
LANES = 128
CUT = 96
VMEM_LIMIT = 36 * 2**20
ORDERS = (("y", "z", "x"), ("z", "x", "y"), ("x", "y", "z"))


def one_hot(shape, col_of_row):
    rows = lax.broadcasted_iota(jnp.int32, shape, 0)
    cols = lax.broadcasted_iota(jnp.int32, shape, 1)
    return jnp.where(cols == col_of_row(rows), 1.0, 0.0).astype(BF16)


def pack_windows(xv, a_scr, pack):
    to_lanes = one_hot((CHANS, CHANS), lambda r: (r % 4) * LANES + ((r % LANES) // 4) * 4 + r // LANES)
    to_rows = one_hot((CHANS, CHANS), lambda r: (r % 4) * LANES + ((r % 256) // 4) * 2 + r // 256)
    for blk in range(4):
        part = jnp.concatenate([xv[n, 32 * blk : 32 * blk + 32].reshape(LANES, LANES) for n in range(4)], axis=0)
        turned = lax.dot_general(part, to_lanes, (((0,), (0,)), ((), ())), preferred_element_type=F32).astype(BF16)
        for c in range(4):
            a_scr[c * LANES : (c + 1) * LANES, blk * LANES : (blk + 1) * LANES] = turned[:, c * LANES : (c + 1) * LANES]
    mixed = jnp.dot(to_rows, a_scr[...], preferred_element_type=F32)
    for blk in range(4):
        even = mixed[0:256, blk * LANES : (blk + 1) * LANES]
        odd = mixed[256:CHANS, blk * LANES : (blk + 1) * LANES]
        for half in range(2):
            s = slice(64 * half, 64 * half + 64)
            tile = jnp.concatenate([even[:, s], odd[:, s]], axis=1).astype(BF16)
            pack[2 * blk + half, 1:65] = tile.reshape(64, 4, LANES)
    edge = jnp.zeros((8, 1, 4, LANES), BF16)
    pack[:, 0:1] = edge
    pack[:, 65:66] = edge


def kernel(
    x_hbm, w1_hbm, w2_hbm, b1_hbm, b2_hbm, o_ref,
    xv, w1v, w2v, b1v, b2v, a_scr, pack, got, x0, x1, x2, edge, w1g, z_acc, y0, y1, y2, acc2,
    load_sem, xs_send, xs_recv, halo_send, halo_recv, step_send, step_recv,
):
    m = lax.axis_index("model")
    q = lax.axis_index("cols")
    me = {"x": m // 2, "z": q // 4, "y": q % 4}
    core = m % 2
    parts = range(3)
    barrier = pltpu.get_barrier_semaphore()

    at_model = [[(me["x"] + dx) % 4 * 2 + (core + dk) % 2 for dk in range(2)] for dx in range(4)]
    at_cols = [[(me["z"] + dz) % 4 * 4 + (me["y"] + dy) % 4 for dy in range(4)] for dz in range(4)]
    others = [(dx, dz, dy, dk) for dx in range(4) for dz in range(4) for dy in range(4) for dk in range(2)]
    others = sorted(others[1:], key=lambda d: (sum(d[:3]) % 4, d))

    def away(d):
        return {"model": at_model[d[0]][d[3]], "cols": at_cols[d[1]][d[2]]}

    loads = [
        pltpu.make_async_copy(src, dst, load_sem.at[k])
        for k, (src, dst) in enumerate(
            ((x_hbm, xv), (w1_hbm, w1v), (w2_hbm, w2v.at[pl.ds(0, 4608)]), (b1_hbm, b1v), (b2_hbm, b2v))
        )
    ]
    for load in loads:
        load.start()
    with jax.named_scope("announce"):
        for d in sorted(others, key=lambda d: -sum(min(o, 4 - o) for o in d[:3])):
            pl.semaphore_signal(barrier, inc=1, device_id=away(d), device_id_type=MESH)

    def piece(p, t, v, n, c, place=None, half=None):
        done = ORDERS[p][:t]
        rest = [a for a in "xzy" if a != ORDERS[p][2]]
        at = [v if t < 2 and a == ORDERS[p][t] else (pl.ds(0, 4) if a in done else me[a]) for a in rest]
        if half is not None:
            at[0] = pl.ds(2 * half, 2)
        return w1g.at[p, pl.ds(0, 2) if n is None else n, me[ORDERS[p][2]] if t < 2 else v, c, at[0], at[1]]

    with jax.named_scope("place_w1"):
        loads[1].wait()
        for p in parts:
            spot = [me[a] for a in "xzy" if a != ORDERS[p][2]]
            for dw in range(3):
                for lt in range(4):
                    tile = w1v[3 * p + dw, :, lt * LANES : (lt + 1) * LANES]
                    w1g[p, lt // 2, me[ORDERS[p][2]], core, spot[0], spot[1], dw, lt % 2] = tile
    with jax.named_scope("wait_x"):
        loads[0].wait()
    with jax.named_scope("pack"):
        pack_windows(xv, a_scr, pack)
    with jax.named_scope("wait_barrier"):
        pl.semaphore_wait(barrier, 127)

    n_steps = [0]
    steps = []

    class Step:
        def __init__(self, slabs, copies):
            k = n_steps[0]
            n_steps[0] += 1
            sems = dict(send_sem=step_send.at[k], recv_sem=step_recv.at[k], device_id_type=MESH)
            self.copies, self.sems = copies, sems
            span = got.at[pl.ds(0, slabs)]
            self.all = pltpu.make_async_remote_copy(
                src_ref=span, dst_ref=span, device_id={"model": at_model[0][1], "cols": q}, **sems
            )
            steps.append(self)

        def go(self):
            for ref, to in self.copies:
                pltpu.make_async_remote_copy(src_ref=ref, dst_ref=ref, device_id=to, **self.sems).start()
            return self

        def land(self):
            self.all.wait_recv()

    def chip(p, t, d, c=0):
        axis = ORDERS[p][t]
        pos = me | {axis: (me[axis] + d) % 4}
        return {"model": pos["x"] * 2 + (core + c) % 2, "cols": pos["z"] * 4 + pos["y"]}

    def spread(t, slabs):
        return Step(slabs, [(piece(p, t, me[ORDERS[p][t]], None, core), chip(p, t, d)) for p in parts for d in (1, 3, 2)]).go()

    def plane(p, d):
        return (me[ORDERS[p][2]] + d) % 4

    def hand_over(pieces, slabs):
        return Step(slabs, [(ref, {"model": at_model[0][1], "cols": q}) for ref in pieces]).go()

    def send_windows(first, last):
        for d in others[first:last]:
            to = away(d)
            pltpu.make_async_remote_copy(
                src_ref=pack.at[to["model"], pl.ds(4 * to["cols"], 6)],
                dst_ref=got.at[mine],
                send_sem=xs_send,
                recv_sem=xs_recv,
                device_id=to,
                device_id_type=MESH,
            ).start()

    mine = ((core * 4 + me["x"]) * 4 + me["z"]) * 4 + me["y"]
    with jax.named_scope("send_first"):
        first = spread(0, 18)
        for pair in range(6):
            got[mine, pair] = pack[m, 4 * q + pair]
        send_windows(0, CUT)
    with jax.named_scope("wait_first"):
        first.land()
    with jax.named_scope("send_second"):
        second = spread(1, 72)
        send_windows(CUT, 127)
    with jax.named_scope("wait_second"):
        second.land()
    last, passed, lent, lent_on = {}, {}, {}, {}

    def send_plane(n):
        last[n] = [Step(32, [(piece(p, 2, plane(p, 0), n, core), chip(p, 2, d)) for d in (1, 3)]) for p in parts]

    def pass_on(n):
        passed[n], lent[n] = {}, {}
        for p in (1, 2, 0):
            with jax.named_scope(f"wait_last{n}{p}"):
                last[n][p].land()
            on = [(piece(p, 2, plane(p, 4 - d), n, core, half=d // 2), chip(p, 2, d)) for d in (1, 3)]
            passed[n][p] = Step(16, on).go()
            lent[n][p] = hand_over([piece(p, 2, plane(p, d), n, core) for d in (1, 3)], 32)

    def finish(n):
        lent_on[n] = {}
        for p in (1, 2, 0):
            with jax.named_scope(f"wait_passed{n}{p}"):
                passed[n][p].land()
            lent_on[n][p] = hand_over([piece(p, 2, plane(p, 2), n, core)], 16)

    with jax.named_scope("send_third"):
        for n in range(2):
            send_plane(n)
        for step in last[0]:
            step.go()
        own = hand_over([piece(p, 2, plane(p, 0), None, core) for p in parts], 96)
    for step in last[1]:
        step.go()
    span = got.at[pl.ds(0, 127)]
    everything = pltpu.make_async_remote_copy(
        src_ref=span, dst_ref=span, send_sem=xs_send, recv_sem=xs_recv, device_id=chip(0, 0, 0, 1), device_id_type=MESH
    )
    with jax.named_scope("wait_windows"):
        everything.wait_recv()

    xs, ys = (x0, x1, x2), (y0, y1, y2)
    with jax.named_scope("turn"):
        for pair in range(6):
            for p in parts:
                rows = []
                for v in range(4):
                    for c in range(2):
                        at = 64 * c
                        if p == 0:
                            rows.append(got[at + 16 * v : at + 16 * v + 16, pair])
                        elif p == 1:
                            rows.append(got[at + v : at + 64 : 4, pair])
                        else:
                            rows += [got[at + 16 * a + 4 * v : at + 16 * a + 4 * v + 4, pair] for a in range(4)]
                rows = jnp.concatenate([r.reshape(-1, LANES) for r in rows], axis=0).T
                for odd in range(2):
                    main = rows[64 * odd : 64 * odd + 64]
                    xs[p][2 * pair + odd, 8 - 4 * p : 72 - 4 * p] = main
                    if p == 1:
                        edge[0, 2 * pair + odd] = main[60:64]
                        edge[1, 2 * pair + odd] = main[0:4]
    halo = []
    for src, dst, d in (
        (x0.at[:, pl.ds(64, 8)], x0.at[:, pl.ds(0, 8)], 1),
        (x2.at[:, pl.ds(0, 8)], x2.at[:, pl.ds(64, 8)], 7),
        (edge.at[0], edge.at[2], 1),
        (edge.at[1], edge.at[3], 7),
    ):
        halo.append(
            pltpu.make_async_remote_copy(
                src_ref=src,
                dst_ref=dst,
                send_sem=halo_send.at[len(halo)],
                recv_sem=halo_recv.at[len(halo)],
                device_id={"model": (m + d) % 8, "cols": q},
                device_id_type=MESH,
            )
        )
        halo[-1].start()

    def conv1(halves, places, spans, groups):
        width = 10 // groups
        tops = [None] * groups
        taps = [(p, dw, plane(p, d)) for p in parts for dw in range(3) for d in places]
        for first in range(0, len(taps), 2):
            two = taps[first : first + 2]
            right = [[w1g[p, n, v, :, :, :, dw, i].reshape(LANES, LANES) for n in halves for i in range(2)] for p, dw, v in two]
            right = jnp.concatenate([jnp.concatenate(r, axis=1) for r in right], axis=0)
            for group in range(groups):
                left = []
                for rows in spans:
                    some = []
                    for p, dw, v in two:
                        lanes = pl.ds(pl.multiple_of(LANES * v, LANES), LANES)
                        some.append(xs[p][pl.ds(dw + width * group, width), rows, lanes])
                    left.append(jnp.concatenate(some, axis=-1))
                left = jnp.concatenate(left, axis=1).reshape(-1, LANES * len(two))
                term = jnp.dot(left, right, preferred_element_type=F32)
                tops[group] = term if tops[group] is None else tops[group] + term
        return [top.reshape(width, -1, 256 * len(halves)) for top in tops]

    top_rows, inner, low_rows = pl.ds(0, 8), pl.ds(8, 56), pl.ds(64, 8)

    def here(n):
        with jax.named_scope(f"here{n}"):
            for group, top in enumerate(conv1((n,), (0,), (inner,), 2)):
                z_acc[n, pl.ds(5 * group, 5), inner] = top

    def near(n):
        with jax.named_scope(f"wait_lent{n}"):
            for step in lent[n].values():
                step.land()
        with jax.named_scope(f"near{n}"):
            for group, top in enumerate(conv1((n,), (3, 1), (inner,), 2)):
                z_acc[n, pl.ds(5 * group, 5), inner] += top

    def rim():
        with jax.named_scope("rim"):
            (top,) = conv1((0, 1), (0, 3, 1), (top_rows, low_rows), 1)
            for n in range(2):
                part = top[:, :, 256 * n : 256 * n + 256]
                z_acc[n, :, top_rows] = part[:, :8]
                z_acc[n, :, low_rows] = part[:, 8:]

    def far(n):
        with jax.named_scope(f"wait_lent_on{n}"):
            for step in lent_on[n].values():
                step.land()
        lanes = slice(256 * n, 256 * n + 256)
        with jax.named_scope(f"far{n}"):
            for group, top in enumerate(conv1((n,), (2,), (pl.ds(0, 72),), 2)):
                cols = pl.ds(5 * group, 5)
                act = jnp.maximum(z_acc[n, cols] + top + b1v[:, lanes], 0.0)
                for dh in range(3):
                    ys[dh][cols, :, lanes] = act[:, 4 * dh : 4 * dh + 64].astype(BF16)

        def clear(at_edge, refs, cols, rows):
            @pl.when(at_edge)
            def _():
                for ref in refs:
                    ref[cols, rows, lanes] = jnp.zeros((cols.size, rows.size, 256), BF16)

        clear(q == 0, ys, pl.ds(0, 1), pl.ds(0, 64))
        clear(q == 15, ys, pl.ds(9, 1), pl.ds(0, 64))
        clear(m == 0, (y0,), pl.ds(0, 10), pl.ds(0, 4))
        clear(m == 7, (y2,), pl.ds(0, 10), pl.ds(60, 4))

    def conv2(n):
        lanes = slice(256 * n, 256 * n + 256)
        total = None
        for dh in range(3):
            for dw in range(3):
                tap = 3 * dh + dw
                left = ys[dh][dw : dw + 8, :, lanes].reshape(CHANS, 256)
                right = w2v[CHANS * tap + 256 * n : CHANS * tap + 256 * n + 256, :]
                term = jnp.dot(left, right, preferred_element_type=F32)
                total = term if total is None else total + term
        return total

    pass_on(0)
    with jax.named_scope("wait_own"):
        own.land()
    here(0)
    here(1)
    pass_on(1)
    near(0)
    near(1)
    finish(0)
    with jax.named_scope("wait_halo"):
        for copy in halo:
            copy.wait_recv()

    @pl.when(m == 0)
    def _():
        x0[:, 0:8] = jnp.zeros((12, 8, CHANS), BF16)
        x1[:, 0:4] = jnp.zeros((12, 4, CHANS), BF16)

    @pl.when(m > 0)
    def _():
        x1[:, 0:4] = edge[2]

    @pl.when(m == 7)
    def _():
        x2[:, 64:72] = jnp.zeros((12, 8, CHANS), BF16)
        x1[:, 68:72] = jnp.zeros((12, 4, CHANS), BF16)

    @pl.when(m < 7)
    def _():
        x1[:, 68:72] = edge[3]

    rim()
    finish(1)
    with jax.named_scope("wait_w2"):
        for load in loads[2:]:
            load.wait()
    far(0)
    with jax.named_scope("conv2_0"):
        acc2[...] = conv2(0)
    far(1)
    with jax.named_scope("conv2_1"):
        o_ref[...] = acc2[...] + conv2(1) + b2v[...]

    with jax.named_scope("wait_sends"):
        everything.wait_send()
        for step in steps:
            step.all.wait_send()
        for copy in halo:
            copy.wait_send()


def arrange(sum_ref, o_hbm, turned, sems):
    copies = []
    for g in range(4):
        rows = jnp.transpose(sum_ref[:, 16 * g : 16 * g + 16], (1, 0, 2))
        for h in range(4):
            for image in range(4):
                turned[g, image, h] = rows[4 * h + image]
        copies.append(pltpu.make_async_copy(turned.at[g], o_hbm.at[:, pl.ds(4 * g, 4)], sems.at[g]))
        copies[-1].start()
    for copy in copies:
        copy.wait()


def solution(mesh):
    scratch = [
        pltpu.VMEM((4, LANES, 4, LANES), BF16),
        pltpu.VMEM((9, 4, CHANS), BF16),
        pltpu.VMEM((4616, CHANS), BF16),
        pltpu.VMEM((1, CHANS), F32),
        pltpu.VMEM((1, CHANS), F32),
        pltpu.VMEM((CHANS, CHANS), BF16),
        pltpu.VMEM((8, 66, 4, LANES), BF16),
        pltpu.VMEM((LANES, 6, 4, LANES), BF16),
        *[pltpu.VMEM((12, 72, CHANS), BF16) for _ in range(3)],
        pltpu.VMEM((4, 12, 4, CHANS), BF16),
        pltpu.VMEM((3, 2, 4, 2, 4, 4, 3, 2, 4, LANES), BF16),
        pltpu.VMEM((2, 10, 72, 256), F32),
        *[pltpu.VMEM((10, 64, CHANS), BF16) for _ in range(3)],
        pltpu.VMEM((CHANS, CHANS), F32),
        pltpu.SemaphoreType.DMA((5,)),
        pltpu.SemaphoreType.DMA,
        pltpu.SemaphoreType.DMA,
        pltpu.SemaphoreType.DMA((4,)),
        pltpu.SemaphoreType.DMA((4,)),
        pltpu.SemaphoreType.DMA((27,)),
        pltpu.SemaphoreType.DMA((27,)),
    ]
    vmem = pl.BlockSpec(memory_space=pltpu.VMEM)
    anywhere = pl.BlockSpec(memory_space=pl.ANY)

    def run_local(x_in, w_conv1, b_conv1, w_conv2, b_conv2):
        sums = pl.pallas_call(
            kernel,
            out_shape=jax.ShapeDtypeStruct((CHANS, CHANS), F32),
            in_specs=[anywhere] * 5,
            out_specs=vmem,
            scratch_shapes=scratch,
            compiler_params=pltpu.CompilerParams(collective_id=0, has_side_effects=True, vmem_limit_bytes=VMEM_LIMIT),
            name="two_convs",
        )(
            *(
                pltpu.with_memory_space_constraint(a, pltpu.HBM)
                for a in (
                    x_in.transpose(0, 1, 3, 2),
                    w_conv1.reshape(9, 4, CHANS),
                    w_conv2.reshape(4608, CHANS),
                    b_conv1.reshape(1, CHANS),
                    b_conv2.reshape(1, CHANS),
                )
            )
        )
        return pl.pallas_call(
            arrange,
            out_shape=jax.ShapeDtypeStruct((4, 16, 8, CHANS), F32),
            in_specs=[vmem],
            out_specs=anywhere,
            scratch_shapes=[pltpu.VMEM((4, 4, 4, 8, CHANS), F32), pltpu.SemaphoreType.DMA((4,))],
            compiler_params=pltpu.CompilerParams(vmem_limit_bytes=8 * 2**20),
            name="arrange",
        )(sums.reshape(8, 64, CHANS))

    return jax.shard_map(
        run_local,
        mesh=mesh,
        in_specs=(P("data", None, None, GROUP_AXES), P(None, None, GROUP_AXES, None), P(), P(), P()),
        out_specs=P("data", "model", "cols", None),
        check_vma=False,
    )
```

```python
import jax
import jax.numpy as jnp
from jax import lax
from jax.experimental import pallas as pl
from jax.experimental.pallas import tpu as pltpu
from jax.sharding import PartitionSpec as P

GROUP_AXES = ("model", "cols")
MESH = pl.DeviceIdType.MESH
BF16 = jnp.bfloat16
F32 = jnp.float32
CHANS = 512
LANES = 128
CUT = 96
VMEM_LIMIT = 36 * 2**20
ORDERS = (("y", "z", "x"), ("z", "x", "y"), ("x", "y", "z"))


def one_hot(shape, col_of_row):
    rows = lax.broadcasted_iota(jnp.int32, shape, 0)
    cols = lax.broadcasted_iota(jnp.int32, shape, 1)
    return jnp.where(cols == col_of_row(rows), 1.0, 0.0).astype(BF16)


def pack_windows(xv, a_scr, pack):
    to_lanes = one_hot((CHANS, CHANS), lambda r: (r % 4) * LANES + ((r % LANES) // 4) * 4 + r // LANES)
    to_rows = one_hot((CHANS, CHANS), lambda r: (r % 4) * LANES + ((r % 256) // 4) * 2 + r // 256)
    for blk in range(4):
        part = jnp.concatenate([xv[n, 32 * blk : 32 * blk + 32].reshape(LANES, LANES) for n in range(4)], axis=0)
        turned = lax.dot_general(part, to_lanes, (((0,), (0,)), ((), ())), preferred_element_type=F32).astype(BF16)
        for c in range(4):
            a_scr[c * LANES : (c + 1) * LANES, blk * LANES : (blk + 1) * LANES] = turned[:, c * LANES : (c + 1) * LANES]
    mixed = jnp.dot(to_rows, a_scr[...], preferred_element_type=F32)
    for blk in range(4):
        even = mixed[0:256, blk * LANES : (blk + 1) * LANES]
        odd = mixed[256:CHANS, blk * LANES : (blk + 1) * LANES]
        for half in range(2):
            s = slice(64 * half, 64 * half + 64)
            tile = jnp.concatenate([even[:, s], odd[:, s]], axis=1).astype(BF16)
            pack[2 * blk + half, 1:65] = tile.reshape(64, 4, LANES)
    edge = jnp.zeros((8, 1, 4, LANES), BF16)
    pack[:, 0:1] = edge
    pack[:, 65:66] = edge


def kernel(
    x_hbm, w1_hbm, w2_hbm, b1_hbm, b2_hbm, o_ref,
    xv, w1v, w2v, b1v, b2v, a_scr, pack, got, x0, x1, x2, edge, w1g, z_acc, y0, y1, y2, acc2,
    load_sem, xs_send, xs_recv, halo_send, halo_recv, step_send, step_recv,
):
    m = lax.axis_index("model")
    q = lax.axis_index("cols")
    me = {"x": m // 2, "z": q // 4, "y": q % 4}
    core = m % 2
    parts = range(3)
    barrier = pltpu.get_barrier_semaphore()

    at_model = [[(me["x"] + dx) % 4 * 2 + (core + dk) % 2 for dk in range(2)] for dx in range(4)]
    at_cols = [[(me["z"] + dz) % 4 * 4 + (me["y"] + dy) % 4 for dy in range(4)] for dz in range(4)]
    others = [(dx, dz, dy, dk) for dx in range(4) for dz in range(4) for dy in range(4) for dk in range(2)]
    others = sorted(others[1:], key=lambda d: (sum(d[:3]) % 4, d))

    def away(d):
        return {"model": at_model[d[0]][d[3]], "cols": at_cols[d[1]][d[2]]}

    loads = [
        pltpu.make_async_copy(src, dst, load_sem.at[k])
        for k, (src, dst) in enumerate(
            ((x_hbm, xv), (w1_hbm, w1v), (w2_hbm, w2v.at[pl.ds(0, 4608)]), (b1_hbm, b1v), (b2_hbm, b2v))
        )
    ]
    for load in loads:
        load.start()
    with jax.named_scope("announce"):
        for d in sorted(others, key=lambda d: -sum(min(o, 4 - o) for o in d[:3])):
            pl.semaphore_signal(barrier, inc=1, device_id=away(d), device_id_type=MESH)

    def piece(p, t, v, n, c, place=None, half=None):
        done = ORDERS[p][:t]
        rest = [a for a in "xzy" if a != ORDERS[p][2]]
        at = [v if t < 2 and a == ORDERS[p][t] else (pl.ds(0, 4) if a in done else me[a]) for a in rest]
        if half is not None:
            at[0] = pl.ds(2 * half, 2)
        return w1g.at[p, pl.ds(0, 2) if n is None else n, me[ORDERS[p][2]] if t < 2 else v, c, at[0], at[1]]

    with jax.named_scope("place_w1"):
        loads[1].wait()
        for p in parts:
            spot = [me[a] for a in "xzy" if a != ORDERS[p][2]]
            for dw in range(3):
                for lt in range(4):
                    tile = w1v[3 * p + dw, :, lt * LANES : (lt + 1) * LANES]
                    w1g[p, lt // 2, me[ORDERS[p][2]], core, spot[0], spot[1], dw, lt % 2] = tile
    with jax.named_scope("wait_x"):
        loads[0].wait()
    with jax.named_scope("pack"):
        pack_windows(xv, a_scr, pack)
    with jax.named_scope("wait_barrier"):
        pl.semaphore_wait(barrier, 127)

    n_steps = [0]
    groups = {}

    class Step:
        def __init__(self, group, slabs, copies):
            sent = groups.setdefault(group, [len(groups), 0])
            sent[1] += slabs
            self.copies = copies
            self.sems = dict(
                send_sem=step_send.at[sent[0]], recv_sem=step_recv.at[n_steps[0]], device_id_type=MESH
            )
            n_steps[0] += 1
            self.slabs = slabs

        def go(self):
            for ref, to in self.copies:
                pltpu.make_async_remote_copy(src_ref=ref, dst_ref=ref, device_id=to, **self.sems).start()
            return self

        def land(self):
            span = got.at[pl.ds(0, self.slabs)]
            partner = {"model": at_model[0][1], "cols": q}
            pltpu.make_async_remote_copy(src_ref=span, dst_ref=span, device_id=partner, **self.sems).wait_recv()

    def chip(p, t, d, c=0):
        axis = ORDERS[p][t]
        pos = me | {axis: (me[axis] + d) % 4}
        return {"model": pos["x"] * 2 + (core + c) % 2, "cols": pos["z"] * 4 + pos["y"]}

    def spread(t, slabs):
        return Step(f"spread{t}", slabs, [(piece(p, t, me[ORDERS[p][t]], None, core), chip(p, t, d)) for p in parts for d in (1, 3, 2)]).go()

    def plane(p, d):
        return (me[ORDERS[p][2]] + d) % 4

    def hand_over(group, pieces, slabs):
        return Step(group, slabs, [(ref, {"model": at_model[0][1], "cols": q}) for ref in pieces]).go()

    def send_windows(first, last):
        for d in others[first:last]:
            to = away(d)
            pltpu.make_async_remote_copy(
                src_ref=pack.at[to["model"], pl.ds(4 * to["cols"], 6)],
                dst_ref=got.at[mine],
                send_sem=xs_send,
                recv_sem=xs_recv,
                device_id=to,
                device_id_type=MESH,
            ).start()

    mine = ((core * 4 + me["x"]) * 4 + me["z"]) * 4 + me["y"]
    with jax.named_scope("send_first"):
        first = spread(0, 18)
        for pair in range(6):
            got[mine, pair] = pack[m, 4 * q + pair]
        send_windows(0, CUT)
    with jax.named_scope("wait_first"):
        first.land()
    with jax.named_scope("send_second"):
        second = spread(1, 72)
        send_windows(CUT, 127)
    with jax.named_scope("wait_second"):
        second.land()
    last, passed, lent, lent_on = {}, {}, {}, {}

    def send_plane(n):
        last[n] = [Step(f"last{n}", 32, [(piece(p, 2, plane(p, 0), n, core), chip(p, 2, d)) for d in (1, 3)]) for p in parts]

    def pass_on(n):
        passed[n], lent[n] = {}, {}
        for p in (0, 2, 1):
            with jax.named_scope(f"wait_last{n}{p}"):
                last[n][p].land()
            on = [(piece(p, 2, plane(p, 4 - d), n, core, half=d // 2), chip(p, 2, d)) for d in (1, 3)]
            passed[n][p] = Step(f"passed{n}", 16, on).go()
            lent[n][p] = hand_over(f"lent{n}", [piece(p, 2, plane(p, d), n, core) for d in (1, 3)], 32)

    def finish(n):
        lent_on[n] = {}
        for p in (1, 2, 0):
            with jax.named_scope(f"wait_passed{n}{p}"):
                passed[n][p].land()
            lent_on[n][p] = hand_over(f"lent_on{n}", [piece(p, 2, plane(p, 2), n, core)], 16)

    with jax.named_scope("send_third"):
        for n in range(2):
            send_plane(n)
        for step in last[0]:
            step.go()
        own = hand_over("own", [piece(p, 2, plane(p, 0), None, core) for p in parts], 96)
    for step in last[1]:
        step.go()
    span = got.at[pl.ds(0, 127)]
    everything = pltpu.make_async_remote_copy(
        src_ref=span, dst_ref=span, send_sem=xs_send, recv_sem=xs_recv, device_id=chip(0, 0, 0, 1), device_id_type=MESH
    )
    with jax.named_scope("wait_windows"):
        everything.wait_recv()

    xs, ys = (x0, x1, x2), (y0, y1, y2)
    with jax.named_scope("turn"):
        for pair in range(6):
            for p in parts:
                rows = []
                for v in range(4):
                    for c in range(2):
                        at = 64 * c
                        if p == 0:
                            rows.append(got[at + 16 * v : at + 16 * v + 16, pair])
                        elif p == 1:
                            rows.append(got[at + v : at + 64 : 4, pair])
                        else:
                            rows += [got[at + 16 * a + 4 * v : at + 16 * a + 4 * v + 4, pair] for a in range(4)]
                rows = jnp.concatenate([r.reshape(-1, LANES) for r in rows], axis=0).T
                for odd in range(2):
                    main = rows[64 * odd : 64 * odd + 64]
                    xs[p][2 * pair + odd, 8 - 4 * p : 72 - 4 * p] = main
                    if p == 1:
                        edge[0, 2 * pair + odd] = main[60:64]
                        edge[1, 2 * pair + odd] = main[0:4]
    halo = []
    for src, dst, d in (
        (x0.at[:, pl.ds(64, 8)], x0.at[:, pl.ds(0, 8)], 1),
        (x2.at[:, pl.ds(0, 8)], x2.at[:, pl.ds(64, 8)], 7),
        (edge.at[0], edge.at[2], 1),
        (edge.at[1], edge.at[3], 7),
    ):
        halo.append(
            pltpu.make_async_remote_copy(
                src_ref=src,
                dst_ref=dst,
                send_sem=halo_send.at[len(halo)],
                recv_sem=halo_recv.at[len(halo)],
                device_id={"model": (m + d) % 8, "cols": q},
                device_id_type=MESH,
            )
        )
        halo[-1].start()

    def conv1(halves, places, spans, groups):
        width = 10 // groups
        tops = [None] * groups
        taps = [(p, dw, plane(p, d)) for p in parts for dw in range(3) for d in places]
        for first in range(0, len(taps), 2):
            two = taps[first : first + 2]
            right = [[w1g[p, n, v, :, :, :, dw, i].reshape(LANES, LANES) for n in halves for i in range(2)] for p, dw, v in two]
            right = jnp.concatenate([jnp.concatenate(r, axis=1) for r in right], axis=0)
            for group in range(groups):
                left = []
                for rows in spans:
                    some = []
                    for p, dw, v in two:
                        lanes = pl.ds(pl.multiple_of(LANES * v, LANES), LANES)
                        some.append(xs[p][pl.ds(dw + width * group, width), rows, lanes])
                    left.append(jnp.concatenate(some, axis=-1))
                left = jnp.concatenate(left, axis=1).reshape(-1, LANES * len(two))
                term = jnp.dot(left, right, preferred_element_type=F32)
                tops[group] = term if tops[group] is None else tops[group] + term
        return [top.reshape(width, -1, 256 * len(halves)) for top in tops]

    top_rows, inner, low_rows = pl.ds(0, 8), pl.ds(8, 56), pl.ds(64, 8)

    def here(n):
        with jax.named_scope(f"here{n}"):
            for group, top in enumerate(conv1((n,), (0,), (inner,), 2)):
                z_acc[n, pl.ds(5 * group, 5), inner] = top

    def near(n):
        with jax.named_scope(f"wait_lent{n}"):
            for step in lent[n].values():
                step.land()
        with jax.named_scope(f"near{n}"):
            for group, top in enumerate(conv1((n,), (3, 1), (inner,), 2)):
                z_acc[n, pl.ds(5 * group, 5), inner] += top

    def rim():
        with jax.named_scope("rim"):
            (top,) = conv1((0, 1), (0, 3, 1), (top_rows, low_rows), 1)
            for n in range(2):
                part = top[:, :, 256 * n : 256 * n + 256]
                z_acc[n, :, top_rows] = part[:, :8]
                z_acc[n, :, low_rows] = part[:, 8:]

    def far(n):
        with jax.named_scope(f"wait_lent_on{n}"):
            for step in lent_on[n].values():
                step.land()
        lanes = slice(256 * n, 256 * n + 256)
        with jax.named_scope(f"far{n}"):
            for group, top in enumerate(conv1((n,), (2,), (pl.ds(0, 72),), 2)):
                cols = pl.ds(5 * group, 5)
                act = jnp.maximum(z_acc[n, cols] + top + b1v[:, lanes], 0.0)
                for dh in range(3):
                    ys[dh][cols, :, lanes] = act[:, 4 * dh : 4 * dh + 64].astype(BF16)

        def clear(at_edge, refs, cols, rows):
            @pl.when(at_edge)
            def _():
                for ref in refs:
                    ref[cols, rows, lanes] = jnp.zeros((cols.size, rows.size, 256), BF16)

        clear(q == 0, ys, pl.ds(0, 1), pl.ds(0, 64))
        clear(q == 15, ys, pl.ds(9, 1), pl.ds(0, 64))
        clear(m == 0, (y0,), pl.ds(0, 10), pl.ds(0, 4))
        clear(m == 7, (y2,), pl.ds(0, 10), pl.ds(60, 4))

    def conv2(n):
        lanes = slice(256 * n, 256 * n + 256)
        total = None
        for dh in range(3):
            for dw in range(3):
                tap = 3 * dh + dw
                left = ys[dh][dw : dw + 8, :, lanes].reshape(CHANS, 256)
                right = w2v[CHANS * tap + 256 * n : CHANS * tap + 256 * n + 256, :]
                term = jnp.dot(left, right, preferred_element_type=F32)
                total = term if total is None else total + term
        return total

    pass_on(0)
    with jax.named_scope("wait_own"):
        own.land()
    here(0)
    here(1)
    pass_on(1)
    near(0)
    near(1)
    finish(0)
    with jax.named_scope("wait_halo"):
        for copy in halo:
            copy.wait_recv()

    @pl.when(m == 0)
    def _():
        x0[:, 0:8] = jnp.zeros((12, 8, CHANS), BF16)
        x1[:, 0:4] = jnp.zeros((12, 4, CHANS), BF16)

    @pl.when(m > 0)
    def _():
        x1[:, 0:4] = edge[2]

    @pl.when(m == 7)
    def _():
        x2[:, 64:72] = jnp.zeros((12, 8, CHANS), BF16)
        x1[:, 68:72] = jnp.zeros((12, 4, CHANS), BF16)

    @pl.when(m < 7)
    def _():
        x1[:, 68:72] = edge[3]

    rim()
    finish(1)
    with jax.named_scope("wait_w2"):
        for load in loads[2:]:
            load.wait()
    far(0)
    with jax.named_scope("conv2_0"):
        acc2[...] = conv2(0)
    far(1)
    with jax.named_scope("conv2_1"):
        o_ref[...] = acc2[...] + conv2(1) + b2v[...]

    with jax.named_scope("wait_sends"):
        everything.wait_send()
        for k, slabs in groups.values():
            span = got.at[pl.ds(0, slabs)]
            partner = {"model": at_model[0][1], "cols": q}
            pltpu.make_async_remote_copy(
                src_ref=span,
                dst_ref=span,
                send_sem=step_send.at[k],
                recv_sem=step_recv.at[k],
                device_id=partner,
                device_id_type=MESH,
            ).wait_send()
        for copy in halo:
            copy.wait_send()


def arrange(sum_ref, o_hbm, turned, sems):
    copies = []
    for g in range(4):
        rows = jnp.transpose(sum_ref[:, 16 * g : 16 * g + 16], (1, 0, 2))
        for h in range(4):
            for image in range(4):
                turned[g, image, h] = rows[4 * h + image]
        copies.append(pltpu.make_async_copy(turned.at[g], o_hbm.at[:, pl.ds(4 * g, 4)], sems.at[g]))
        copies[-1].start()
    for copy in copies:
        copy.wait()


def solution(mesh):
    scratch = [
        pltpu.VMEM((4, LANES, 4, LANES), BF16),
        pltpu.VMEM((9, 4, CHANS), BF16),
        pltpu.VMEM((4616, CHANS), BF16),
        pltpu.VMEM((1, CHANS), F32),
        pltpu.VMEM((1, CHANS), F32),
        pltpu.VMEM((CHANS, CHANS), BF16),
        pltpu.VMEM((8, 66, 4, LANES), BF16),
        pltpu.VMEM((LANES, 6, 4, LANES), BF16),
        *[pltpu.VMEM((12, 72, CHANS), BF16) for _ in range(3)],
        pltpu.VMEM((4, 12, 4, CHANS), BF16),
        pltpu.VMEM((3, 2, 4, 2, 4, 4, 3, 2, 4, LANES), BF16),
        pltpu.VMEM((2, 10, 72, 256), F32),
        *[pltpu.VMEM((10, 64, CHANS), BF16) for _ in range(3)],
        pltpu.VMEM((CHANS, CHANS), F32),
        pltpu.SemaphoreType.DMA((5,)),
        pltpu.SemaphoreType.DMA,
        pltpu.SemaphoreType.DMA,
        pltpu.SemaphoreType.DMA((4,)),
        pltpu.SemaphoreType.DMA((4,)),
        pltpu.SemaphoreType.DMA((11,)),
        pltpu.SemaphoreType.DMA((27,)),
    ]
    vmem = pl.BlockSpec(memory_space=pltpu.VMEM)
    anywhere = pl.BlockSpec(memory_space=pl.ANY)

    def run_local(x_in, w_conv1, b_conv1, w_conv2, b_conv2):
        sums = pl.pallas_call(
            kernel,
            out_shape=jax.ShapeDtypeStruct((CHANS, CHANS), F32),
            in_specs=[anywhere] * 5,
            out_specs=vmem,
            scratch_shapes=scratch,
            compiler_params=pltpu.CompilerParams(collective_id=0, has_side_effects=True, vmem_limit_bytes=VMEM_LIMIT),
            name="two_convs",
        )(
            *(
                pltpu.with_memory_space_constraint(a, pltpu.HBM)
                for a in (
                    x_in.transpose(0, 1, 3, 2),
                    w_conv1.reshape(9, 4, CHANS),
                    w_conv2.reshape(4608, CHANS),
                    b_conv1.reshape(1, CHANS),
                    b_conv2.reshape(1, CHANS),
                )
            )
        )
        return pl.pallas_call(
            arrange,
            out_shape=jax.ShapeDtypeStruct((4, 16, 8, CHANS), F32),
            in_specs=[vmem],
            out_specs=anywhere,
            scratch_shapes=[pltpu.VMEM((4, 4, 4, 8, CHANS), F32), pltpu.SemaphoreType.DMA((4,))],
            compiler_params=pltpu.CompilerParams(vmem_limit_bytes=8 * 2**20),
            name="arrange",
        )(sums.reshape(8, 64, CHANS))

    return jax.shard_map(
        run_local,
        mesh=mesh,
        in_specs=(P("data", None, None, GROUP_AXES), P(None, None, GROUP_AXES, None), P(), P(), P()),
        out_specs=P("data", "model", "cols", None),
        check_vma=False,
    )
```
